16 devices in a mesh: dp: 4 (over z, y), cp: 4 (over x, core).
Axes of the slice: x: 2, y: 2, z: 2, core: 2. Of those that a mesh axis runs over, the one named last changes fastest.
Arguments:
- x_in: bfloat16 [4, 4096, 1152], P('dp', 'cp'), parts along dimension 0
- positions: int32 [4, 4096], P('dp', 'cp'), parts along dimension 0
- dy_out: bfloat16 [4, 4096, 1152], P('dp', 'cp'), parts along dimension 0
- w_query: bfloat16 [1152, 4, 256], replicated
- w_key: bfloat16 [1152, 1, 256], replicated
- w_value: bfloat16 [1152, 1, 256], replicated
- w_out: bfloat16 [4, 256, 1152], replicated
- w_pre: float32 [1152], replicated
- w_post: float32 [1152], replicated
Outputs:
- output 1: bfloat16 [4, 4096, 1152], P('dp', 'cp'), parts along dimension 0
- output 2: bfloat16 [4, 4096, 1152], P('dp', 'cp'), parts along dimension 0
- output 3: float32 [4608, 4, 256], P('dp'), parts along dimension 0
- output 4: float32 [4608, 1, 256], P('dp'), parts along dimension 0
- output 5: float32 [4608, 1, 256], P('dp'), parts along dimension 0
- output 6: float32 [16, 256, 1152], P('dp'), parts along dimension 0
- output 7: float32 [4608], P('dp'), parts along dimension 0
- output 8: float32 [4608], P('dp'), parts along dimension 0
There are 4 independent parts. The reference program is written for one: setup_inputs(seed, part) draws one part's arguments, and reference() takes and returns one part's arrays. A program takes and returns all parts, laid end to end along the dimension named above; an argument that names none is the same for every part.
All inputs are finite; a program needn't handle non-finite values.
Results may differ from the reference program's by a relative error of at most 0.02.
Values are sent between devices in bfloat16 or wider.
A program may use at most 1 GiB of HBM per device.

```python
import jax
import jax.numpy as jnp
from jax import lax

BATCH = 1
SEQ_LEN = 4096
QUERY_BLOCK = 1024
MODEL_DIM = 1152
HEADS = 4
KV_HEADS = 1
HEAD_DIM = 256

NORM_EPS = 1e-6
SOFT_CAP = 50.0
QUERY_SCALE = 144.0
ROPE_BASE = 10000.0


def rms_scale(values, gain):
    return values * lax.rsqrt(jnp.mean(values * values, axis=-1, keepdims=True) + NORM_EPS) * (1.0 + gain)


def rope_tables(positions):
    half = HEAD_DIM // 2
    inv_freq = ROPE_BASE ** (jnp.arange(half, dtype=jnp.float32) * (-2.0 / HEAD_DIM))
    angles = positions.astype(jnp.float32)[:, :, None, None] * inv_freq
    return jnp.cos(angles), jnp.sin(angles)


def rotate(values, cosine, sine):
    half = values.shape[-1] // 2
    first = values[..., :half]
    second = values[..., half:]
    return jnp.concatenate([first * cosine - second * sine, second * cosine + first * sine], axis=-1)


def rotate_back(values, cosine, sine):
    half = values.shape[-1] // 2
    first = values[..., :half]
    second = values[..., half:]
    return jnp.concatenate([first * cosine + second * sine, second * cosine - first * sine], axis=-1)


def setup_inputs(seed: int = 0, part: int = 0) -> dict:
    base = jax.random.key(seed)
    shared = jax.random.split(base, 6)
    local = jax.random.split(jax.random.fold_in(base, part), 4)
    in_scale = MODEL_DIM ** -0.5
    x_in = jax.random.normal(local[0], (BATCH, SEQ_LEN, MODEL_DIM), jnp.float32).astype(jnp.bfloat16)
    start = jax.random.randint(local[1], (BATCH, 1), 0, SEQ_LEN, dtype=jnp.int32)
    steps = jax.random.randint(local[2], (BATCH, SEQ_LEN), 1, 4, dtype=jnp.int32)
    positions = start + jnp.cumsum(steps, axis=1) - steps[:, :1]
    dy_out = jax.random.normal(local[3], (BATCH, SEQ_LEN, MODEL_DIM), jnp.float32).astype(jnp.bfloat16)
    w_query = (jax.random.normal(shared[0], (MODEL_DIM, HEADS, HEAD_DIM), jnp.float32) * (1.5 * in_scale)).astype(jnp.bfloat16)
    w_key = (jax.random.normal(shared[1], (MODEL_DIM, KV_HEADS, HEAD_DIM), jnp.float32) * (1.5 * in_scale)).astype(jnp.bfloat16)
    w_value = (jax.random.normal(shared[2], (MODEL_DIM, KV_HEADS, HEAD_DIM), jnp.float32) * in_scale).astype(jnp.bfloat16)
    w_out = (jax.random.normal(shared[3], (HEADS, HEAD_DIM, MODEL_DIM), jnp.float32) * (HEADS * HEAD_DIM) ** -0.5).astype(jnp.bfloat16)
    w_pre = 0.3 * jax.random.normal(shared[4], (MODEL_DIM,), jnp.float32)
    w_post = 0.3 * jax.random.normal(shared[5], (MODEL_DIM,), jnp.float32)
    return {"x_in": x_in, "positions": positions, "dy_out": dy_out, "w_query": w_query, "w_key": w_key, "w_value": w_value, "w_out": w_out, "w_pre": w_pre, "w_post": w_post}


def reference(x_in, positions, dy_out, w_query, w_key, w_value, w_out, w_pre, w_post):
    group = HEADS // KV_HEADS
    tokens = BATCH * SEQ_LEN
    blocks = SEQ_LEN // QUERY_BLOCK
    width_q = HEADS * HEAD_DIM
    width_kv = KV_HEADS * HEAD_DIM
    wq_flat = w_query.reshape(MODEL_DIM, width_q)
    wk_flat = w_key.reshape(MODEL_DIM, width_kv)
    wv_flat = w_value.reshape(MODEL_DIM, width_kv)
    wo_flat = w_out.reshape(width_q, MODEL_DIM)
    x_float = x_in.astype(jnp.float32).reshape(tokens, MODEL_DIM)
    normed, pre_vjp = jax.vjp(rms_scale, x_float, w_pre)
    act_flat = normed.astype(jnp.bfloat16)
    query_proj = jnp.dot(act_flat, wq_flat, preferred_element_type=jnp.float32).astype(jnp.bfloat16)
    key_proj = jnp.dot(act_flat, wk_flat, preferred_element_type=jnp.float32).astype(jnp.bfloat16)
    value_proj = jnp.dot(act_flat, wv_flat, preferred_element_type=jnp.float32).astype(jnp.bfloat16)
    cosine, sine = rope_tables(positions)
    query_rot = (rotate(query_proj.astype(jnp.float32).reshape(BATCH, SEQ_LEN, HEADS, HEAD_DIM), cosine, sine) * QUERY_SCALE ** -0.5).astype(jnp.bfloat16)
    key_rot = rotate(key_proj.astype(jnp.float32).reshape(BATCH, SEQ_LEN, KV_HEADS, HEAD_DIM), cosine, sine).astype(jnp.bfloat16)
    key_float = key_rot.astype(jnp.float32)
    value_float = value_proj.reshape(BATCH, SEQ_LEN, KV_HEADS, HEAD_DIM).astype(jnp.float32)

    def to_blocks(arr):
        moved = arr.reshape((BATCH, blocks, QUERY_BLOCK) + arr.shape[2:])
        return jnp.moveaxis(moved, 1, 0)

    def from_blocks(arr):
        return jnp.moveaxis(arr, 0, 1).reshape((BATCH, SEQ_LEN) + arr.shape[3:])

    query_blocks = to_blocks(query_rot.reshape(BATCH, SEQ_LEN, KV_HEADS, group, HEAD_DIM))
    pos_blocks = to_blocks(positions)

    def block_probs(query_blk, pos_blk):
        scores = jnp.einsum("bqngd,bknd->bnqgk", query_blk.astype(jnp.float32), key_float)
        capped = SOFT_CAP * jnp.tanh(scores / SOFT_CAP)
        allowed = positions[:, None, None, None, :] <= pos_blk[:, None, :, None, None]
        soft_probs = jax.nn.softmax(jnp.where(allowed, capped, -1e30), axis=-1)
        return soft_probs, capped

    def forward_block(pair):
        soft_probs, capped = block_probs(pair[0], pair[1])
        return jnp.einsum("bnqgk,bknd->bqngd", soft_probs.astype(jnp.bfloat16).astype(jnp.float32), value_float)

    attn_float = from_blocks(lax.map(forward_block, (query_blocks, pos_blocks)))
    attn_flat = attn_float.astype(jnp.bfloat16).reshape(tokens, width_q)
    z_out = jnp.dot(attn_flat, wo_flat, preferred_element_type=jnp.float32).astype(jnp.bfloat16)
    post_normed, post_vjp = jax.vjp(rms_scale, z_out.astype(jnp.float32), w_post)
    y_out = (x_float + post_normed.astype(jnp.bfloat16).astype(jnp.float32)).astype(jnp.bfloat16)

    dy_float = dy_out.astype(jnp.float32).reshape(tokens, MODEL_DIM)
    dz_float, dw_post = post_vjp(dy_float)
    dz_out = dz_float.astype(jnp.bfloat16)
    dw_out = jnp.dot(attn_flat.T, dz_out, preferred_element_type=jnp.float32)
    d_attn = jnp.dot(dz_out, wo_flat.T, preferred_element_type=jnp.float32).astype(jnp.bfloat16).reshape(BATCH, SEQ_LEN, KV_HEADS, group, HEAD_DIM)
    row_dot = jnp.sum(d_attn.astype(jnp.float32) * attn_float, axis=-1)

    def backward_block(carry, items):
        dkey_sum, dvalue_sum = carry
        query_blk, pos_blk, dattn_blk, delta_blk = items
        soft_probs, capped = block_probs(query_blk, pos_blk)
        dattn_float = dattn_blk.astype(jnp.float32)
        d_probs = jnp.einsum("bqngd,bknd->bnqgk", dattn_float, value_float)
        dvalue_sum = dvalue_sum + jnp.einsum("bnqgk,bqngd->bknd", soft_probs.astype(jnp.bfloat16).astype(jnp.float32), dattn_float)
        delta_t = jnp.moveaxis(delta_blk, 1, 2)
        d_scores = (soft_probs * (d_probs - delta_t[..., None]) * (1.0 - (capped / SOFT_CAP) ** 2)).astype(jnp.bfloat16).astype(jnp.float32)
        dquery_blk = jnp.einsum("bnqgk,bknd->bqngd", d_scores, key_float)
        dkey_sum = dkey_sum + jnp.einsum("bnqgk,bqngd->bknd", d_scores, query_blk.astype(jnp.float32))
        return (dkey_sum, dvalue_sum), dquery_blk

    kv_zeros = jnp.zeros((BATCH, SEQ_LEN, KV_HEADS, HEAD_DIM), jnp.float32)
    sums_kv, dquery_blocks = lax.scan(backward_block, (kv_zeros, kv_zeros), (query_blocks, pos_blocks, to_blocks(d_attn), to_blocks(row_dot)))
    dquery_rot = from_blocks(dquery_blocks).reshape(BATCH, SEQ_LEN, HEADS, HEAD_DIM)
    dquery = (rotate_back(dquery_rot, cosine, sine) * QUERY_SCALE ** -0.5).astype(jnp.bfloat16).reshape(tokens, width_q)
    dkey = rotate_back(sums_kv[0], cosine, sine).astype(jnp.bfloat16).reshape(tokens, width_kv)
    dvalue = sums_kv[1].astype(jnp.bfloat16).reshape(tokens, width_kv)
    dw_query = jnp.dot(act_flat.T, dquery, preferred_element_type=jnp.float32).reshape(MODEL_DIM, HEADS, HEAD_DIM)
    dw_key = jnp.dot(act_flat.T, dkey, preferred_element_type=jnp.float32).reshape(MODEL_DIM, KV_HEADS, HEAD_DIM)
    dw_value = jnp.dot(act_flat.T, dvalue, preferred_element_type=jnp.float32).reshape(MODEL_DIM, KV_HEADS, HEAD_DIM)
    d_act = (jnp.dot(dquery, wq_flat.T, preferred_element_type=jnp.float32) + jnp.dot(dkey, wk_flat.T, preferred_element_type=jnp.float32) + jnp.dot(dvalue, wv_flat.T, preferred_element_type=jnp.float32))
    dx_float, dw_pre = pre_vjp(d_act)
    dx_in = (dy_float + dx_float).astype(jnp.bfloat16).reshape(BATCH, SEQ_LEN, MODEL_DIM)
    return (y_out.reshape(BATCH, SEQ_LEN, MODEL_DIM), dx_in, dw_query, dw_key, dw_value, dw_out.reshape(HEADS, HEAD_DIM, MODEL_DIM), dw_pre, dw_post)
```

```python
import functools
import math

import jax
import jax.numpy as jnp
from jax import lax
from jax.experimental import pallas as pl
from jax.experimental.pallas import tpu as pltpu
from jax.sharding import PartitionSpec as P

NORM_EPS = 1e-6
SOFT_CAP = 50.0
QUERY_SCALE = 144.0
ROPE_BASE = 10000.0
LOG2E = math.log2(math.e)
CAP2 = SOFT_CAP * LOG2E
INV_CAP = 1.0 / SOFT_CAP

F32 = jnp.float32
BF16 = jnp.bfloat16
VMEM_LIMIT = 60 * 1024 * 1024

NT = (((1,), (1,)), ((), ()))
NN = (((1,), (0,)), ((), ()))


def dot(a, b, dims=NN):
    return lax.dot_general(a, b, dims, preferred_element_type=F32)


def params():
    return pltpu.CompilerParams(vmem_limit_bytes=VMEM_LIMIT)


def whole(shape):
    zeros = (0,) * len(shape)
    return pl.BlockSpec(shape, lambda *_: zeros)


def cost(flops, nbytes, trans=0):
    return pl.CostEstimate(flops=int(flops), bytes_accessed=int(nbytes), transcendentals=int(trans))


def kv_kernel(x_ref, gain_ref, wk_ref, wv_ref, cos_ref, sin_ref, a_ref, at_ref, kv_ref):
    half = cos_ref.shape[1]
    x = x_ref[...].astype(F32)
    rstd = lax.rsqrt(jnp.mean(x * x, axis=-1, keepdims=True) + NORM_EPS)
    a = (x * rstd * (1.0 + gain_ref[...])).astype(BF16)
    a_ref[...] = a
    at_ref[...] = a.T
    k = dot(a, wk_ref[...]).astype(BF16).astype(F32)
    first, second = k[:, :half], k[:, half:]
    cosine, sine = cos_ref[...], sin_ref[...]
    kv_ref[0, :, :half] = (first * cosine - second * sine).astype(BF16)
    kv_ref[0, :, half:] = (second * cosine + first * sine).astype(BF16)
    kv_ref[1] = dot(a, wv_ref[...]).astype(BF16)


def project_kv(x, gain, wk, wv, cosine, sine):
    tokens, dim = x.shape
    hd = wk.shape[1]
    half = hd // 2
    bt = 256
    return pl.pallas_call(
        kv_kernel,
        grid=(tokens // bt,),
        in_specs=[
            pl.BlockSpec((bt, dim), lambda i: (i, 0)),
            whole((1, dim)),
            whole((dim, hd)),
            whole((dim, hd)),
            pl.BlockSpec((bt, half), lambda i: (i, 0)),
            pl.BlockSpec((bt, half), lambda i: (i, 0)),
        ],
        out_specs=[
            pl.BlockSpec((bt, dim), lambda i: (i, 0)),
            pl.BlockSpec((dim, bt), lambda i: (0, i)),
            pl.BlockSpec((2, bt, hd), lambda i: (0, i, 0)),
        ],
        out_shape=[
            jax.ShapeDtypeStruct((tokens, dim), BF16),
            jax.ShapeDtypeStruct((dim, tokens), BF16),
            jax.ShapeDtypeStruct((2, tokens, hd), BF16),
        ],
        compiler_params=params(),
        cost_estimate=cost(4 * tokens * dim * hd, 6 * tokens * dim),
        name="project_kv",
    )(x, gain, wk, wv, cosine, sine)


def q_kernel(a_ref, wq_ref, cos_ref, sin_ref, q_ref):
    heads, _, hd = q_ref.shape
    half = hd // 2
    cosine, sine = cos_ref[...], sin_ref[...]
    a = a_ref[...]
    scale = QUERY_SCALE ** -0.5
    for h in range(heads):
        q = dot(a, wq_ref[:, h * hd:(h + 1) * hd]).astype(BF16).astype(F32)
        first, second = q[:, :half], q[:, half:]
        q_ref[h, :, :half] = ((first * cosine - second * sine) * scale).astype(BF16)
        q_ref[h, :, half:] = ((second * cosine + first * sine) * scale).astype(BF16)


def project_q(a, wq, cosine, sine, heads):
    tokens, dim = a.shape
    hd = wq.shape[1] // heads
    half = hd // 2
    bt = 256
    return pl.pallas_call(
        q_kernel,
        grid=(tokens // bt,),
        in_specs=[
            pl.BlockSpec((bt, dim), lambda i: (i, 0)),
            whole(wq.shape),
            pl.BlockSpec((bt, half), lambda i: (i, 0)),
            pl.BlockSpec((bt, half), lambda i: (i, 0)),
        ],
        out_specs=pl.BlockSpec((heads, bt, hd), lambda i: (0, i, 0)),
        out_shape=jax.ShapeDtypeStruct((heads, tokens, hd), BF16),
        compiler_params=params(),
        cost_estimate=cost(2 * tokens * dim * heads * hd, 6 * tokens * dim),
        name="project_q",
    )(a, wq, cosine, sine)


def forward_tile(q_ref, acc_ref, sum_ref, k, v, masked):
    heads, bq, _ = q_ref.shape
    bk = k.shape[0]
    if masked:
        keep = lax.broadcasted_iota(jnp.int32, (bq, bk), 1) <= lax.broadcasted_iota(jnp.int32, (bq, bk), 0)
    for h in range(heads):
        s = dot(q_ref[h], k, NT)
        p = jnp.exp2(jnp.tanh(s * INV_CAP) * CAP2)
        if masked:
            p = jnp.where(keep, p, 0.0)
        part = p[:, 0:128]
        for c in range(128, bk, 128):
            part = part + p[:, c:c + 128]
        sum_ref[h] += part
        acc_ref[h] += dot(p.astype(BF16), v)


def forward_local_kernel(idx_ref, q_ref, own_ref, near_ref, acc_ref, sum_ref):
    bq = q_ref.shape[1]
    tokens = own_ref.shape[1]
    i = pl.program_id(0)
    acc_ref[...] = jnp.zeros_like(acc_ref)
    sum_ref[...] = jnp.zeros_like(sum_ref)

    def keys(ref, start, size):
        rows = pl.ds(pl.multiple_of(start, 128), size)
        return ref[0, rows, :], ref[1, rows, :]

    forward_tile(q_ref, acc_ref, sum_ref, *keys(own_ref, i * bq, bq), True)

    def own_step(j, _):
        forward_tile(q_ref, acc_ref, sum_ref, *keys(own_ref, j * bq, bq), False)
        return 0

    lax.fori_loop(0, i, own_step, 0)

    @pl.when(idx_ref[0] % 2 == 1)
    def _():
        def near_step(j, _):
            forward_tile(q_ref, acc_ref, sum_ref, *keys(near_ref, j * 512, 512), False)
            return 0

        lax.fori_loop(0, tokens // 512, near_step, 0)


def forward_local(idx, q, own, near):
    heads, tokens, hd = q.shape
    bq = 256
    return pl.pallas_call(
        forward_local_kernel,
        grid=(tokens // bq,),
        in_specs=[
            pl.BlockSpec(memory_space=pltpu.SMEM),
            pl.BlockSpec((heads, bq, hd), lambda i: (0, i, 0)),
            whole(own.shape),
            whole(near.shape),
        ],
        out_specs=[
            pl.BlockSpec((heads, bq, hd), lambda i: (0, i, 0)),
            pl.BlockSpec((heads, bq, 128), lambda i: (0, i, 0)),
        ],
        out_shape=[
            jax.ShapeDtypeStruct((heads, tokens, hd), F32),
            jax.ShapeDtypeStruct((heads, tokens, 128), F32),
        ],
        compiler_params=params(),
        cost_estimate=cost(6 * heads * tokens * tokens * hd, 8 * heads * tokens * hd),
        name="forward_local",
    )(idx, q, own, near)


def forward_post_kernel(idx_ref, q_ref, far_ref, mid_ref, acc_in_ref, sum_in_ref, x_ref, dy_ref, wo_ref, gain_ref,
                        y_ref, do_ref, stat_ref, dwo_ref, dgain_ref, acc_ref, sum_ref, o_ref, dz_ref):
    heads, bq, hd = q_ref.shape
    tokens = far_ref.shape[1]
    i = pl.program_id(0)
    steps = pl.num_programs(0)
    acc_ref[...] = acc_in_ref[...]
    sum_ref[...] = sum_in_ref[...]

    @pl.when(idx_ref[0] >= 2)
    def _():
        def step(j, _):
            rows = pl.ds(pl.multiple_of(j * 512, 512), 512)
            forward_tile(q_ref, acc_ref, sum_ref, far_ref[0, rows, :], far_ref[1, rows, :], False)
            forward_tile(q_ref, acc_ref, sum_ref, mid_ref[0, rows, :], mid_ref[1, rows, :], False)
            return 0

        lax.fori_loop(0, tokens // 512, step, 0)

    lane = lax.broadcasted_iota(jnp.int32, (bq, 128), 1)
    stat = jnp.zeros((bq, 128), F32)
    for h in range(heads):
        total = jnp.sum(sum_ref[h], axis=-1, keepdims=True)
        stat = jnp.where(lane == h, jnp.log2(total), stat)
        out = acc_ref[h] / total
        acc_ref[h] = out
        o_ref[pl.ds(pl.multiple_of(i * bq, bq), bq), h * hd:(h + 1) * hd] = out.astype(BF16)
    rows = pl.ds(pl.multiple_of(i * bq, bq), bq)
    z = dot(o_ref[rows, :], wo_ref[...]).astype(BF16).astype(F32)
    gain = 1.0 + gain_ref[...]
    rstd = lax.rsqrt(jnp.mean(z * z, axis=-1, keepdims=True) + NORM_EPS)
    z_unit = z * rstd
    y_ref[...] = (x_ref[...].astype(F32) + (z_unit * gain).astype(BF16).astype(F32)).astype(BF16)
    dy = dy_ref[...].astype(F32)

    @pl.when(i == 0)
    def _():
        dgain_ref[...] = jnp.zeros_like(dgain_ref)

    dgain_ref[...] += jnp.sum(dy * z_unit, axis=0, keepdims=True)
    g = dy * gain
    dz = (rstd * (g - z_unit * jnp.mean(g * z_unit, axis=-1, keepdims=True))).astype(BF16)
    dz_ref[rows, :] = dz
    for h in range(heads):
        d_out = dot(dz, wo_ref[h * hd:(h + 1) * hd, :], NT).astype(BF16)
        do_ref[h] = d_out
        delta = jnp.sum(d_out.astype(F32) * acc_ref[h], axis=-1, keepdims=True)
        stat = jnp.where(lane == heads + h, delta, stat)
    stat_ref[...] = stat.T[0:8, :]

    @pl.when(i == steps - 1)
    def _():
        core = idx_ref[0] % 2
        per = heads // 2
        for which in range(2):
            for hh in range(per):
                cols = pl.ds(pl.multiple_of((((core + which) % 2) * per + hh) * hd, hd), hd)
                dwo_ref[which, hh * hd:(hh + 1) * hd, :] = dot(o_ref[:, cols].T, dz_ref[...])


def forward_post(idx, q, far, mid, acc, row_sum, x, dy, wo, gain):
    heads, tokens, hd = q.shape
    dim = x.shape[1]
    bq = 256
    rows3 = lambda last: pl.BlockSpec((heads, bq, last), lambda i: (0, i, 0))
    rows2 = pl.BlockSpec((bq, dim), lambda i: (i, 0))
    return pl.pallas_call(
        forward_post_kernel,
        grid=(tokens // bq,),
        in_specs=[
            pl.BlockSpec(memory_space=pltpu.SMEM),
            rows3(hd),
            whole(far.shape),
            whole(mid.shape),
            rows3(hd),
            rows3(128),
            rows2,
            rows2,
            whole(wo.shape),
            whole((1, dim)),
        ],
        out_specs=[
            rows2,
            rows3(hd),
            pl.BlockSpec((8, bq), lambda i: (0, i)),
            whole((2, heads * hd // 2, dim)),
            whole((1, dim)),
        ],
        out_shape=[
            jax.ShapeDtypeStruct((tokens, dim), BF16),
            jax.ShapeDtypeStruct((heads, tokens, hd), BF16),
            jax.ShapeDtypeStruct((8, tokens), F32),
            jax.ShapeDtypeStruct((2, heads * hd // 2, dim), F32),
            jax.ShapeDtypeStruct((1, dim), F32),
        ],
        scratch_shapes=[
            pltpu.VMEM((heads, bq, hd), F32),
            pltpu.VMEM((heads, bq, 128), F32),
            pltpu.VMEM((tokens, heads * hd), BF16),
            pltpu.VMEM((tokens, dim), BF16),
        ],
        compiler_params=params(),
        cost_estimate=cost(8 * heads * tokens * tokens * hd + 6 * tokens * heads * hd * dim, 12 * heads * tokens * hd),
        name="forward_post",
    )(idx, q, far, mid, acc, row_sum, x, dy, wo, gain)


def backward_tile(q_ref, do_ref, stat_ref, dqt_ref, dkv_ref, k, v, kt, start, bq, masked):
    heads = q_ref.shape[0]
    bk = k.shape[0]
    rows = pl.ds(pl.multiple_of(start, 128), bq)
    if masked:
        keep = lax.broadcasted_iota(jnp.int32, (bk, bq), 0) <= lax.broadcasted_iota(jnp.int32, (bk, bq), 1)
    for h in range(heads):
        q = q_ref[h, rows, :]
        d_out = do_ref[h, rows, :]
        t = jnp.tanh(dot(k, q, NT) * INV_CAP)
        p = jnp.exp2(t * CAP2 - stat_ref[h:h + 1, rows])
        if masked:
            p = jnp.where(keep, p, 0.0)
        dp = dot(v, d_out, NT)
        ds = (p * (dp - stat_ref[heads + h:heads + h + 1, rows]) * (1.0 - t * t)).astype(BF16)
        dkv_ref[1] += dot(p.astype(BF16), d_out)
        dkv_ref[0] += dot(ds, q)
        dqt_ref[h, :, rows] += dot(kt, ds)


def backward_far_kernel(idx_ref, q_ref, do_ref, stat_ref, kv_ref, dqt_in_ref, dkv_ref, dqt_ref, *, first):
    tokens = q_ref.shape[1]
    bq = 512

    @pl.when(pl.program_id(0) == 0)
    def _():
        dqt_ref[...] = jnp.zeros_like(dqt_ref) if first else dqt_in_ref[...]

    dkv_ref[...] = jnp.zeros_like(dkv_ref)

    @pl.when(idx_ref[0] >= 2)
    def _():
        k, v = kv_ref[0], kv_ref[1]
        kt = k.T

        def step(j, _):
            backward_tile(q_ref, do_ref, stat_ref, dqt_ref, dkv_ref, k, v, kt, j * bq, bq, False)
            return 0

        lax.fori_loop(0, tokens // bq, step, 0)


def backward_far(idx, q, d_out, stat, kv, dqt):
    heads, tokens, hd = q.shape
    bk = 256
    first = dqt is None
    if first:
        dqt = jnp.zeros((8, 128), F32)
    return pl.pallas_call(
        functools.partial(backward_far_kernel, first=first),
        grid=(tokens // bk,),
        in_specs=[
            pl.BlockSpec(memory_space=pltpu.SMEM),
            whole(q.shape),
            whole(d_out.shape),
            whole(stat.shape),
            pl.BlockSpec((2, bk, hd), lambda i: (0, i, 0)),
            whole(dqt.shape),
        ],
        out_specs=[
            pl.BlockSpec((2, bk, hd), lambda i: (0, i, 0)),
            whole((heads, hd, tokens)),
        ],
        out_shape=[
            jax.ShapeDtypeStruct((2, tokens, hd), F32),
            jax.ShapeDtypeStruct((heads, hd, tokens), F32),
        ],
        compiler_params=params(),
        cost_estimate=cost(10 * heads * tokens * tokens * hd, 12 * heads * tokens * hd),
        name="backward_far",
    )(idx, q, d_out, stat, kv, dqt)


def backward_local_kernel(idx_ref, q_ref, do_ref, stat_ref, own_ref, near_ref, dqt_in_ref, cos_ref, sin_ref,
                          dnear_ref, down_ref, dq_ref, dqt_ref):
    heads, tokens, hd = q_ref.shape
    half = hd // 2
    bk = own_ref.shape[1]
    i = pl.program_id(0)
    steps = pl.num_programs(0)

    @pl.when(i == 0)
    def _():
        dqt_ref[...] = dqt_in_ref[...]

    dnear_ref[...] = jnp.zeros_like(dnear_ref)
    down_ref[...] = jnp.zeros_like(down_ref)

    @pl.when(idx_ref[0] % 2 == 1)
    def _():
        k, v = near_ref[0], near_ref[1]
        kt = k.T

        def step(j, _):
            backward_tile(q_ref, do_ref, stat_ref, dqt_ref, dnear_ref, k, v, kt, j * 512, 512, False)
            return 0

        lax.fori_loop(0, tokens // 512, step, 0)

    k, v = own_ref[0], own_ref[1]
    kt = k.T
    backward_tile(q_ref, do_ref, stat_ref, dqt_ref, down_ref, k, v, kt, i * bk, bk, True)

    def own_step(j, _):
        backward_tile(q_ref, do_ref, stat_ref, dqt_ref, down_ref, k, v, kt, j * bk, bk, False)
        return 0

    lax.fori_loop(i + 1, steps, own_step, 0)

    @pl.when(i == steps - 1)
    def _():
        scale = QUERY_SCALE ** -0.5
        for h in range(heads):
            dq = dqt_ref[h].T
            first, second = dq[:, :half], dq[:, half:]
            cosine, sine = cos_ref[...], sin_ref[...]
            dq_ref[:, h * hd:h * hd + half] = ((first * cosine + second * sine) * scale).astype(BF16)
            dq_ref[:, h * hd + half:(h + 1) * hd] = ((second * cosine - first * sine) * scale).astype(BF16)


def backward_local(idx, q, d_out, stat, own, near, dqt, cosine, sine):
    heads, tokens, hd = q.shape
    bk = 256
    kv_spec = pl.BlockSpec((2, bk, hd), lambda i: (0, i, 0))
    return pl.pallas_call(
        backward_local_kernel,
        grid=(tokens // bk,),
        in_specs=[
            pl.BlockSpec(memory_space=pltpu.SMEM),
            whole(q.shape),
            whole(d_out.shape),
            whole(stat.shape),
            kv_spec,
            kv_spec,
            whole(dqt.shape),
            whole(cosine.shape),
            whole(sine.shape),
        ],
        out_specs=[kv_spec, kv_spec, whole((tokens, heads * hd))],
        out_shape=[
            jax.ShapeDtypeStruct((2, tokens, hd), F32),
            jax.ShapeDtypeStruct((2, tokens, hd), F32),
            jax.ShapeDtypeStruct((tokens, heads * hd), BF16),
        ],
        scratch_shapes=[pltpu.VMEM((heads, hd, tokens), F32)],
        compiler_params=params(),
        cost_estimate=cost(15 * heads * tokens * tokens * hd, 12 * heads * tokens * hd),
        name="backward_local",
    )(idx, q, d_out, stat, own, near, dqt, cosine, sine)


def dwq_kernel(idx_ref, at_ref, dq_ref, out_ref):
    out_ref[0] = dot(at_ref[...], dq_ref[...])


def grad_wq(idx, at, dq):
    dim, tokens = at.shape
    width = dq.shape[1]
    cols = 256
    per = width // 2 // cols
    grid_spec = pltpu.PrefetchScalarGridSpec(
        num_scalar_prefetch=1,
        grid=(2, per),
        in_specs=[
            pl.BlockSpec((dim, tokens), lambda w, j, idx: (0, 0)),
            pl.BlockSpec((tokens, cols), lambda w, j, idx: (0, ((w + 1 + idx[0]) % 2) * per + j)),
        ],
        out_specs=pl.BlockSpec((1, dim, cols), lambda w, j, idx: (1 - w, 0, j)),
    )
    return pl.pallas_call(
        dwq_kernel,
        grid_spec=grid_spec,
        out_shape=jax.ShapeDtypeStruct((2, dim, width // 2), F32),
        compiler_params=params(),
        cost_estimate=cost(2 * dim * tokens * width, 4 * dim * width),
        name="grad_wq",
    )(idx, at, dq)


def tail_kernel(idx_ref, down_ref, dnear_ref, dfar_ref, cos_ref, sin_ref, at_ref, dq_ref, wq_ref, wk_ref, wv_ref,
                x_ref, dy_ref, gain_ref, dx_ref, dwkv_ref, dgain_ref):
    bt, half = cos_ref.shape
    i = pl.program_id(0)
    dk = down_ref[0] + dnear_ref[0] + dfar_ref[0]
    cosine, sine = cos_ref[...], sin_ref[...]
    first, second = dk[:, :half], dk[:, half:]
    dk = jnp.concatenate([first * cosine + second * sine, second * cosine - first * sine], axis=1).astype(BF16)
    dv = (down_ref[1] + dnear_ref[1] + dfar_ref[1]).astype(BF16)

    @pl.when(i == 0)
    def _():
        dwkv_ref[...] = jnp.zeros_like(dwkv_ref)
        dgain_ref[...] = jnp.zeros_like(dgain_ref)

    core = idx_ref[0] % 2
    at = at_ref[...]
    is_core0 = core == 0
    mine = jnp.where(is_core0, dk, dv)
    theirs = jnp.where(is_core0, dv, dk)
    dwkv_ref[0] += dot(at, mine)
    dwkv_ref[1] += dot(at, theirs)
    da = dot(dq_ref[...], wq_ref[...], NT) + dot(dk, wk_ref[...], NT) + dot(dv, wv_ref[...], NT)
    x = x_ref[...].astype(F32)
    rstd = lax.rsqrt(jnp.mean(x * x, axis=-1, keepdims=True) + NORM_EPS)
    unit = x * rstd
    dgain_ref[...] += jnp.sum(da * unit, axis=0, keepdims=True)
    g = da * (1.0 + gain_ref[...])
    dx = rstd * (g - unit * jnp.mean(g * unit, axis=-1, keepdims=True))
    dx_ref[...] = (dy_ref[...].astype(F32) + dx).astype(BF16)


def tail(idx, down, dnear, dfar, cosine, sine, at, dq, wq, wk, wv, x, dy, gain):
    tokens, dim = x.shape
    hd = wk.shape[1]
    width = wq.shape[1]
    bt = 256
    kv_spec = pl.BlockSpec((2, bt, hd), lambda i: (0, i, 0))
    rope_spec = pl.BlockSpec((bt, hd // 2), lambda i: (i, 0))
    rows2 = pl.BlockSpec((bt, dim), lambda i: (i, 0))
    return pl.pallas_call(
        tail_kernel,
        grid=(tokens // bt,),
        in_specs=[
            pl.BlockSpec(memory_space=pltpu.SMEM),
            kv_spec,
            kv_spec,
            kv_spec,
            rope_spec,
            rope_spec,
            pl.BlockSpec((dim, bt), lambda i: (0, i)),
            pl.BlockSpec((bt, width), lambda i: (i, 0)),
            whole(wq.shape),
            whole(wk.shape),
            whole(wv.shape),
            rows2,
            rows2,
            whole((1, dim)),
        ],
        out_specs=[rows2, whole((2, dim, hd)), whole((1, dim))],
        out_shape=[
            jax.ShapeDtypeStruct((tokens, dim), BF16),
            jax.ShapeDtypeStruct((2, dim, hd), F32),
            jax.ShapeDtypeStruct((1, dim), F32),
        ],
        compiler_params=params(),
        cost_estimate=cost(2 * tokens * dim * (width + 4 * hd), 8 * tokens * dim),
        name="tail",
    )(idx, down, dnear, dfar, cosine, sine, at, dq, wq, wk, wv, x, dy, gain)


def solution(mesh):
    across = [(0, 2), (2, 0), (1, 3), (3, 1)]
    beside = [(0, 1), (1, 0), (2, 3), (3, 2)]

    def permute(value, pairs):
        return lax.ppermute(value, "cp", pairs)

    def sum_halves(parts):
        mine = parts[0] + permute(parts[1], beside)
        return mine + permute(mine, across)

    def local_step(x_in, positions, dy_out, w_query, w_key, w_value, w_out, w_pre, w_post):
        batch, tokens, dim = x_in.shape
        heads, hd = w_query.shape[1], w_query.shape[2]
        half = hd // 2
        rank = lax.axis_index("cp").astype(jnp.int32)
        idx = rank.reshape(1)
        core = rank % 2
        wq = w_query.reshape(dim, heads * hd)
        wk = w_key.reshape(dim, hd)
        wv = w_value.reshape(dim, hd)
        wo = w_out.reshape(heads * hd, dim)
        x = x_in.reshape(tokens, dim)
        dy = dy_out.reshape(tokens, dim)
        gain_pre = w_pre.reshape(1, dim)
        gain_post = w_post.reshape(1, dim)
        inv_freq = ROPE_BASE ** (jnp.arange(half, dtype=F32) * (-2.0 / hd))
        angles = positions.reshape(tokens, 1).astype(F32) * inv_freq
        cosine, sine = jnp.cos(angles), jnp.sin(angles)

        act, act_t, own = project_kv(x, gain_pre, wk, wv, cosine, sine)
        far = permute(own, [(0, 2), (1, 3)])
        near = permute(own, [(0, 1), (2, 3)])
        q = project_q(act, wq, cosine, sine, heads)
        acc, row_sum = forward_local(idx, q, own, near)
        mid = permute(far, [(2, 3), (3, 2)])
        y, d_out, stat, dwo, dgain_post = forward_post(idx, q, far, mid, acc, row_sum, x, dy, wo, gain_post)
        dwo_mine = sum_halves(dwo)

        dmid, dqt = backward_far(idx, q, d_out, stat, mid, None)
        dmid_in = permute(dmid, [(2, 3), (3, 2)])
        dfar, dqt = backward_far(idx, q, d_out, stat, far, dqt)
        dfar_in = permute(dfar + dmid_in, [(2, 0), (3, 1)])
        dnear, down, dq = backward_local(idx, q, d_out, stat, own, near, dqt, cosine, sine)
        dnear_in = permute(dnear, [(1, 0), (3, 2)])
        dwq = grad_wq(idx, act_t, dq)
        dwq_mine = sum_halves(dwq)
        dx, dwkv, dgain_pre = tail(idx, down, dnear_in, dfar_in, cosine, sine, act_t, dq, wq, wk, wv, x, dy, gain_pre)
        dwkv_mine = sum_halves(dwkv)
        gains = jnp.concatenate([dgain_pre, dgain_post], axis=0)
        gains = gains + permute(gains, beside)
        gains = gains + permute(gains, across)

        def join(mine, axis):
            other = permute(mine, beside)
            low = jnp.where(core == 0, mine, other)
            high = jnp.where(core == 0, other, mine)
            return low, high

        dwo_full = jnp.concatenate(join(dwo_mine, 0), axis=0)
        dwq_full = jnp.concatenate(join(dwq_mine, 1), axis=1)
        dwk_full, dwv_full = join(dwkv_mine, 0)
        return (
            y.reshape(batch, tokens, dim),
            dx.reshape(batch, tokens, dim),
            dwq_full.reshape(dim, heads, hd),
            dwk_full.reshape(dim, 1, hd),
            dwv_full.reshape(dim, 1, hd),
            dwo_full.reshape(heads, hd, dim),
            gains[0],
            gains[1],
        )

    seq_spec = P("dp", "cp", None)
    in_specs = (seq_spec, P("dp", "cp"), seq_spec, P(), P(), P(), P(), P(), P())
    out_specs = (seq_spec, seq_spec, P("dp", None, None), P("dp", None, None), P("dp", None, None), P("dp", None, None), P("dp"), P("dp"))
    return jax.shard_map(local_step, mesh=mesh, in_specs=in_specs, out_specs=out_specs, check_vma=False)
```

```python
import functools
import math

import jax
import jax.numpy as jnp
from jax import lax
from jax.experimental import pallas as pl
from jax.experimental.pallas import tpu as pltpu
from jax.sharding import PartitionSpec as P


NORM_EPS = 1e-6
SOFT_CAP = 50.0
QUERY_SCALE = 144.0
ROPE_BASE = 10000.0
LOG2E = math.log2(math.e)
CAP2 = SOFT_CAP * LOG2E
INV_CAP = 1.0 / SOFT_CAP

F32 = jnp.float32
BF16 = jnp.bfloat16
VMEM_LIMIT = 60 * 1024 * 1024

NT = (((1,), (1,)), ((), ()))
NN = (((1,), (0,)), ((), ()))


def dot(a, b, dims=NN):
    return lax.dot_general(a, b, dims, preferred_element_type=F32)


def params():
    return pltpu.CompilerParams(vmem_limit_bytes=VMEM_LIMIT)


def whole(shape):
    zeros = (0,) * len(shape)
    return pl.BlockSpec(shape, lambda *_: zeros)


def cost(flops, nbytes, trans=0):
    return pl.CostEstimate(flops=int(flops), bytes_accessed=int(nbytes), transcendentals=int(trans))


def kv_kernel(x_ref, gain_ref, wk_ref, wv_ref, cos_ref, sin_ref, a_ref, at_ref, kv_ref):
    half = cos_ref.shape[1]
    x = x_ref[...].astype(F32)
    rstd = lax.rsqrt(jnp.mean(x * x, axis=-1, keepdims=True) + NORM_EPS)
    a = (x * rstd * (1.0 + gain_ref[...])).astype(BF16)
    a_ref[...] = a
    at_ref[...] = a.T
    k = dot(a, wk_ref[...]).astype(BF16).astype(F32)
    first, second = k[:, :half], k[:, half:]
    cosine, sine = cos_ref[...], sin_ref[...]
    kv_ref[0, :, :half] = (first * cosine - second * sine).astype(BF16)
    kv_ref[0, :, half:] = (second * cosine + first * sine).astype(BF16)
    kv_ref[1] = dot(a, wv_ref[...]).astype(BF16)


def project_kv(x, gain, wk, wv, cosine, sine):
    tokens, dim = x.shape
    hd = wk.shape[1]
    half = hd // 2
    bt = 256
    return pl.pallas_call(
        kv_kernel,
        grid=(tokens // bt,),
        in_specs=[
            pl.BlockSpec((bt, dim), lambda i: (i, 0)),
            whole((1, dim)),
            whole((dim, hd)),
            whole((dim, hd)),
            pl.BlockSpec((bt, half), lambda i: (i, 0)),
            pl.BlockSpec((bt, half), lambda i: (i, 0)),
        ],
        out_specs=[
            pl.BlockSpec((bt, dim), lambda i: (i, 0)),
            pl.BlockSpec((dim, bt), lambda i: (0, i)),
            pl.BlockSpec((2, bt, hd), lambda i: (0, i, 0)),
        ],
        out_shape=[
            jax.ShapeDtypeStruct((tokens, dim), BF16),
            jax.ShapeDtypeStruct((dim, tokens), BF16),
            jax.ShapeDtypeStruct((2, tokens, hd), BF16),
        ],
        compiler_params=params(),
        cost_estimate=cost(4 * tokens * dim * hd, 6 * tokens * dim),
        name="project_kv",
    )(x, gain, wk, wv, cosine, sine)


def q_kernel(a_ref, wq_ref, cos_ref, sin_ref, q_ref):
    heads, _, hd = q_ref.shape
    half = hd // 2
    cosine, sine = cos_ref[...], sin_ref[...]
    a = a_ref[...]
    scale = QUERY_SCALE ** -0.5
    for h in range(heads):
        q = dot(a, wq_ref[:, h * hd:(h + 1) * hd]).astype(BF16).astype(F32)
        first, second = q[:, :half], q[:, half:]
        q_ref[h, :, :half] = ((first * cosine - second * sine) * scale).astype(BF16)
        q_ref[h, :, half:] = ((second * cosine + first * sine) * scale).astype(BF16)


def project_q(a, wq, cosine, sine, heads):
    tokens, dim = a.shape
    hd = wq.shape[1] // heads
    half = hd // 2
    bt = 256
    return pl.pallas_call(
        q_kernel,
        grid=(tokens // bt,),
        in_specs=[
            pl.BlockSpec((bt, dim), lambda i: (i, 0)),
            whole(wq.shape),
            pl.BlockSpec((bt, half), lambda i: (i, 0)),
            pl.BlockSpec((bt, half), lambda i: (i, 0)),
        ],
        out_specs=pl.BlockSpec((heads, bt, hd), lambda i: (0, i, 0)),
        out_shape=jax.ShapeDtypeStruct((heads, tokens, hd), BF16),
        compiler_params=params(),
        cost_estimate=cost(2 * tokens * dim * heads * hd, 6 * tokens * dim),
        name="project_q",
    )(a, wq, cosine, sine)


def forward_tile(q_ref, acc_ref, sum_ref, k, v, masked):
    heads, bq, _ = q_ref.shape
    bk = k.shape[0]
    if masked:
        keep = lax.broadcasted_iota(jnp.int32, (bq, bk), 1) <= lax.broadcasted_iota(jnp.int32, (bq, bk), 0)
    for h in range(heads):
        s = dot(q_ref[h], k, NT)
        p = jnp.exp2(jnp.tanh(s * INV_CAP) * CAP2)
        if masked:
            p = jnp.where(keep, p, 0.0)
        part = p[:, 0:128]
        for c in range(128, bk, 128):
            part = part + p[:, c:c + 128]
        sum_ref[h] += part
        acc_ref[h] += dot(p.astype(BF16), v)


def forward_local_kernel(idx_ref, q_ref, own_ref, near_ref, acc_ref, sum_ref):
    bq = q_ref.shape[1]
    tokens = own_ref.shape[1]
    i = pl.program_id(0)
    acc_ref[...] = jnp.zeros_like(acc_ref)
    sum_ref[...] = jnp.zeros_like(sum_ref)

    def keys(ref, start, size):
        rows = pl.ds(pl.multiple_of(start, 128), size)
        return ref[0, rows, :], ref[1, rows, :]

    forward_tile(q_ref, acc_ref, sum_ref, *keys(own_ref, i * bq, bq), True)

    def own_step(j, _):
        forward_tile(q_ref, acc_ref, sum_ref, *keys(own_ref, j * bq, bq), False)
        return 0

    lax.fori_loop(0, i, own_step, 0)

    @pl.when(idx_ref[0] % 2 == 1)
    def _():
        def near_step(j, _):
            forward_tile(q_ref, acc_ref, sum_ref, *keys(near_ref, j * 512, 512), False)
            return 0

        lax.fori_loop(0, tokens // 512, near_step, 0)


def forward_local(idx, q, own, near):
    heads, tokens, hd = q.shape
    bq = 256
    return pl.pallas_call(
        forward_local_kernel,
        grid=(tokens // bq,),
        in_specs=[
            pl.BlockSpec(memory_space=pltpu.SMEM),
            pl.BlockSpec((heads, bq, hd), lambda i: (0, i, 0)),
            whole(own.shape),
            whole(near.shape),
        ],
        out_specs=[
            pl.BlockSpec((heads, bq, hd), lambda i: (0, i, 0)),
            pl.BlockSpec((heads, bq, 128), lambda i: (0, i, 0)),
        ],
        out_shape=[
            jax.ShapeDtypeStruct((heads, tokens, hd), F32),
            jax.ShapeDtypeStruct((heads, tokens, 128), F32),
        ],
        compiler_params=params(),
        cost_estimate=cost(6 * heads * tokens * tokens * hd, 8 * heads * tokens * hd),
        name="forward_local",
    )(idx, q, own, near)


def forward_post_kernel(idx_ref, q_ref, far_ref, mid_ref, acc_in_ref, sum_in_ref, x_ref, dy_ref, wo_ref, gain_ref,
                        y_ref, do_ref, stat_ref, dwo_ref, dgain_ref, acc_ref, sum_ref, o_ref, dz_ref):
    heads, bq, hd = q_ref.shape
    tokens = far_ref.shape[1]
    i = pl.program_id(0)
    steps = pl.num_programs(0)
    acc_ref[...] = acc_in_ref[...]
    sum_ref[...] = sum_in_ref[...]

    @pl.when(idx_ref[0] >= 2)
    def _():
        def step(j, _):
            rows = pl.ds(pl.multiple_of(j * 512, 512), 512)
            forward_tile(q_ref, acc_ref, sum_ref, far_ref[0, rows, :], far_ref[1, rows, :], False)
            forward_tile(q_ref, acc_ref, sum_ref, mid_ref[0, rows, :], mid_ref[1, rows, :], False)
            return 0

        lax.fori_loop(0, tokens // 512, step, 0)

    lane = lax.broadcasted_iota(jnp.int32, (bq, 128), 1)
    stat = jnp.zeros((bq, 128), F32)
    for h in range(heads):
        total = jnp.sum(sum_ref[h], axis=-1, keepdims=True)
        stat = jnp.where(lane == h, jnp.log2(total), stat)
        out = acc_ref[h] / total
        acc_ref[h] = out
        o_ref[pl.ds(pl.multiple_of(i * bq, bq), bq), h * hd:(h + 1) * hd] = out.astype(BF16)
    rows = pl.ds(pl.multiple_of(i * bq, bq), bq)
    z = dot(o_ref[rows, :], wo_ref[...]).astype(BF16).astype(F32)
    gain = 1.0 + gain_ref[...]
    rstd = lax.rsqrt(jnp.mean(z * z, axis=-1, keepdims=True) + NORM_EPS)
    z_unit = z * rstd
    y_ref[...] = (x_ref[...].astype(F32) + (z_unit * gain).astype(BF16).astype(F32)).astype(BF16)
    dy = dy_ref[...].astype(F32)

    @pl.when(i == 0)
    def _():
        dgain_ref[...] = jnp.zeros_like(dgain_ref)

    dgain_ref[...] += jnp.sum(dy * z_unit, axis=0, keepdims=True)
    g = dy * gain
    dz = (rstd * (g - z_unit * jnp.mean(g * z_unit, axis=-1, keepdims=True))).astype(BF16)
    dz_ref[rows, :] = dz
    for h in range(heads):
        d_out = dot(dz, wo_ref[h * hd:(h + 1) * hd, :], NT).astype(BF16)
        do_ref[h] = d_out
        delta = jnp.sum(d_out.astype(F32) * acc_ref[h], axis=-1, keepdims=True)
        stat = jnp.where(lane == heads + h, delta, stat)
    stat_ref[...] = stat.T[0:8, :]

    @pl.when(i == steps - 1)
    def _():
        core = idx_ref[0] % 2
        per = heads // 2
        for which in range(2):
            for hh in range(per):
                cols = pl.ds(pl.multiple_of((((core + which) % 2) * per + hh) * hd, hd), hd)
                dwo_ref[which, hh * hd:(hh + 1) * hd, :] = dot(o_ref[:, cols].T, dz_ref[...])


def forward_post(idx, q, far, mid, acc, row_sum, x, dy, wo, gain):
    heads, tokens, hd = q.shape
    dim = x.shape[1]
    bq = 256
    rows3 = lambda last: pl.BlockSpec((heads, bq, last), lambda i: (0, i, 0))
    rows2 = pl.BlockSpec((bq, dim), lambda i: (i, 0))
    return pl.pallas_call(
        forward_post_kernel,
        grid=(tokens // bq,),
        in_specs=[
            pl.BlockSpec(memory_space=pltpu.SMEM),
            rows3(hd),
            whole(far.shape),
            whole(mid.shape),
            rows3(hd),
            rows3(128),
            rows2,
            rows2,
            whole(wo.shape),
            whole((1, dim)),
        ],
        out_specs=[
            rows2,
            rows3(hd),
            pl.BlockSpec((8, bq), lambda i: (0, i)),
            whole((2, heads * hd // 2, dim)),
            whole((1, dim)),
        ],
        out_shape=[
            jax.ShapeDtypeStruct((tokens, dim), BF16),
            jax.ShapeDtypeStruct((heads, tokens, hd), BF16),
            jax.ShapeDtypeStruct((8, tokens), F32),
            jax.ShapeDtypeStruct((2, heads * hd // 2, dim), F32),
            jax.ShapeDtypeStruct((1, dim), F32),
        ],
        scratch_shapes=[
            pltpu.VMEM((heads, bq, hd), F32),
            pltpu.VMEM((heads, bq, 128), F32),
            pltpu.VMEM((tokens, heads * hd), BF16),
            pltpu.VMEM((tokens, dim), BF16),
        ],
        compiler_params=params(),
        cost_estimate=cost(8 * heads * tokens * tokens * hd + 6 * tokens * heads * hd * dim, 12 * heads * tokens * hd),
        name="forward_post",
    )(idx, q, far, mid, acc, row_sum, x, dy, wo, gain)


def backward_tile(q_ref, do_ref, stat_ref, dqt_ref, dkv_ref, k, v, kt, start, bq, masked):
    heads = q_ref.shape[0]
    bk = k.shape[0]
    rows = pl.ds(pl.multiple_of(start, 128), bq)
    if masked:
        keep = lax.broadcasted_iota(jnp.int32, (bk, bq), 0) <= lax.broadcasted_iota(jnp.int32, (bk, bq), 1)
    for h in range(heads):
        q = q_ref[h, rows, :]
        d_out = do_ref[h, rows, :]
        t = jnp.tanh(dot(k, q, NT) * INV_CAP)
        p = jnp.exp2(t * CAP2 - stat_ref[h:h + 1, rows])
        if masked:
            p = jnp.where(keep, p, 0.0)
        dp = dot(v, d_out, NT)
        ds = (p * (dp - stat_ref[heads + h:heads + h + 1, rows]) * (1.0 - t * t)).astype(BF16)
        dkv_ref[1] += dot(p.astype(BF16), d_out)
        dkv_ref[0] += dot(ds, q)
        dqt_ref[h, :, rows] += dot(kt, ds)


def backward_far_kernel(idx_ref, q_ref, do_ref, stat_ref, kv_ref, dqt_in_ref, dkv_ref, dqt_ref, *, first):
    tokens = q_ref.shape[1]
    bq = 512

    @pl.when(pl.program_id(0) == 0)
    def _():
        dqt_ref[...] = jnp.zeros_like(dqt_ref) if first else dqt_in_ref[...]

    dkv_ref[...] = jnp.zeros_like(dkv_ref)

    @pl.when(idx_ref[0] >= 2)
    def _():
        k, v = kv_ref[0], kv_ref[1]
        kt = k.T

        def step(j, _):
            backward_tile(q_ref, do_ref, stat_ref, dqt_ref, dkv_ref, k, v, kt, j * bq, bq, False)
            return 0

        lax.fori_loop(0, tokens // bq, step, 0)


def backward_far(idx, q, d_out, stat, kv, dqt):
    heads, tokens, hd = q.shape
    bk = 256
    first = dqt is None
    if first:
        dqt = jnp.zeros((8, 128), F32)
    return pl.pallas_call(
        functools.partial(backward_far_kernel, first=first),
        grid=(tokens // bk,),
        in_specs=[
            pl.BlockSpec(memory_space=pltpu.SMEM),
            whole(q.shape),
            whole(d_out.shape),
            whole(stat.shape),
            pl.BlockSpec((2, bk, hd), lambda i: (0, i, 0)),
            whole(dqt.shape),
        ],
        out_specs=[
            pl.BlockSpec((2, bk, hd), lambda i: (0, i, 0)),
            whole((heads, hd, tokens)),
        ],
        out_shape=[
            jax.ShapeDtypeStruct((2, tokens, hd), F32),
            jax.ShapeDtypeStruct((heads, hd, tokens), F32),
        ],
        compiler_params=params(),
        cost_estimate=cost(10 * heads * tokens * tokens * hd, 12 * heads * tokens * hd),
        name="backward_far",
    )(idx, q, d_out, stat, kv, dqt)


def backward_local_kernel(idx_ref, q_ref, do_ref, stat_ref, own_ref, near_ref, dqt_in_ref, cos_ref, sin_ref,
                          dnear_ref, down_ref, dq_ref, dqt_ref):
    heads, tokens, hd = q_ref.shape
    half = hd // 2
    bk = own_ref.shape[1]
    i = pl.program_id(0)
    steps = pl.num_programs(0)

    @pl.when(i == 0)
    def _():
        dqt_ref[...] = dqt_in_ref[...]

    dnear_ref[...] = jnp.zeros_like(dnear_ref)
    down_ref[...] = jnp.zeros_like(down_ref)

    @pl.when(idx_ref[0] % 2 == 1)
    def _():
        k, v = near_ref[0], near_ref[1]
        kt = k.T

        def step(j, _):
            backward_tile(q_ref, do_ref, stat_ref, dqt_ref, dnear_ref, k, v, kt, j * 512, 512, False)
            return 0

        lax.fori_loop(0, tokens // 512, step, 0)

    k, v = own_ref[0], own_ref[1]
    kt = k.T
    backward_tile(q_ref, do_ref, stat_ref, dqt_ref, down_ref, k, v, kt, i * bk, bk, True)

    def own_step(j, _):
        backward_tile(q_ref, do_ref, stat_ref, dqt_ref, down_ref, k, v, kt, j * bk, bk, False)
        return 0

    lax.fori_loop(i + 1, steps, own_step, 0)

    @pl.when(i == steps - 1)
    def _():
        scale = QUERY_SCALE ** -0.5
        for h in range(heads):
            dq = dqt_ref[h].T
            first, second = dq[:, :half], dq[:, half:]
            cosine, sine = cos_ref[...], sin_ref[...]
            dq_ref[:, h * hd:h * hd + half] = ((first * cosine + second * sine) * scale).astype(BF16)
            dq_ref[:, h * hd + half:(h + 1) * hd] = ((second * cosine - first * sine) * scale).astype(BF16)


def backward_local(idx, q, d_out, stat, own, near, dqt, cosine, sine):
    heads, tokens, hd = q.shape
    bk = 256
    kv_spec = pl.BlockSpec((2, bk, hd), lambda i: (0, i, 0))
    return pl.pallas_call(
        backward_local_kernel,
        grid=(tokens // bk,),
        in_specs=[
            pl.BlockSpec(memory_space=pltpu.SMEM),
            whole(q.shape),
            whole(d_out.shape),
            whole(stat.shape),
            kv_spec,
            kv_spec,
            whole(dqt.shape),
            whole(cosine.shape),
            whole(sine.shape),
        ],
        out_specs=[kv_spec, kv_spec, whole((tokens, heads * hd))],
        out_shape=[
            jax.ShapeDtypeStruct((2, tokens, hd), F32),
            jax.ShapeDtypeStruct((2, tokens, hd), F32),
            jax.ShapeDtypeStruct((tokens, heads * hd), BF16),
        ],
        scratch_shapes=[pltpu.VMEM((heads, hd, tokens), F32)],
        compiler_params=params(),
        cost_estimate=cost(15 * heads * tokens * tokens * hd, 12 * heads * tokens * hd),
        name="backward_local",
    )(idx, q, d_out, stat, own, near, dqt, cosine, sine)


def dwq_kernel(idx_ref, at_ref, dq_ref, out_ref):
    out_ref[0] = dot(at_ref[...], dq_ref[...])


def grad_wq(idx, at, dq):
    dim, tokens = at.shape
    width = dq.shape[1]
    cols = 256
    per = width // 2 // cols
    grid_spec = pltpu.PrefetchScalarGridSpec(
        num_scalar_prefetch=1,
        grid=(2, per),
        in_specs=[
            pl.BlockSpec((dim, tokens), lambda w, j, idx: (0, 0)),
            pl.BlockSpec((tokens, cols), lambda w, j, idx: (0, ((w + 1 + idx[0]) % 2) * per + j)),
        ],
        out_specs=pl.BlockSpec((1, dim, cols), lambda w, j, idx: (1 - w, 0, j)),
    )
    return pl.pallas_call(
        dwq_kernel,
        grid_spec=grid_spec,
        out_shape=jax.ShapeDtypeStruct((2, dim, width // 2), F32),
        compiler_params=params(),
        cost_estimate=cost(2 * dim * tokens * width, 4 * dim * width),
        name="grad_wq",
    )(idx, at, dq)


def tail_kernel(idx_ref, down_ref, dnear_ref, dfar_ref, cos_ref, sin_ref, at_ref, dq_ref, wq_ref, wk_ref, wv_ref,
                x_ref, dy_ref, gain_ref, dx_ref, dwkv_ref, dgain_ref):
    _, half = cos_ref.shape
    i = pl.program_id(0)
    dk = down_ref[0] + dnear_ref[0] + dfar_ref[0]
    cosine, sine = cos_ref[...], sin_ref[...]
    first, second = dk[:, :half], dk[:, half:]
    dk = jnp.concatenate([first * cosine + second * sine, second * cosine - first * sine], axis=1).astype(BF16)
    dv = (down_ref[1] + dnear_ref[1] + dfar_ref[1]).astype(BF16)

    @pl.when(i == 0)
    def _():
        dwkv_ref[...] = jnp.zeros_like(dwkv_ref)
        dgain_ref[...] = jnp.zeros_like(dgain_ref)

    core = idx_ref[0] % 2
    at = at_ref[...]
    is_core0 = core == 0
    mine = jnp.where(is_core0, dk, dv)
    theirs = jnp.where(is_core0, dv, dk)
    dwkv_ref[0] += dot(at, mine)
    dwkv_ref[1] += dot(at, theirs)
    da = dot(dq_ref[...], wq_ref[...], NT) + dot(dk, wk_ref[...], NT) + dot(dv, wv_ref[...], NT)
    x = x_ref[...].astype(F32)
    rstd = lax.rsqrt(jnp.mean(x * x, axis=-1, keepdims=True) + NORM_EPS)
    unit = x * rstd
    dgain_ref[...] += jnp.sum(da * unit, axis=0, keepdims=True)
    g = da * (1.0 + gain_ref[...])
    dx = rstd * (g - unit * jnp.mean(g * unit, axis=-1, keepdims=True))
    dx_ref[...] = (dy_ref[...].astype(F32) + dx).astype(BF16)


def tail(idx, down, dnear, dfar, cosine, sine, at, dq, wq, wk, wv, x, dy, gain):
    tokens, dim = x.shape
    hd = wk.shape[1]
    width = wq.shape[1]
    bt = 256
    kv_spec = pl.BlockSpec((2, bt, hd), lambda i: (0, i, 0))
    rope_spec = pl.BlockSpec((bt, hd // 2), lambda i: (i, 0))
    rows2 = pl.BlockSpec((bt, dim), lambda i: (i, 0))
    return pl.pallas_call(
        tail_kernel,
        grid=(tokens // bt,),
        in_specs=[
            pl.BlockSpec(memory_space=pltpu.SMEM),
            kv_spec,
            kv_spec,
            kv_spec,
            rope_spec,
            rope_spec,
            pl.BlockSpec((dim, bt), lambda i: (0, i)),
            pl.BlockSpec((bt, width), lambda i: (i, 0)),
            whole(wq.shape),
            whole(wk.shape),
            whole(wv.shape),
            rows2,
            rows2,
            whole((1, dim)),
        ],
        out_specs=[rows2, whole((2, dim, hd)), whole((1, dim))],
        out_shape=[
            jax.ShapeDtypeStruct((tokens, dim), BF16),
            jax.ShapeDtypeStruct((2, dim, hd), F32),
            jax.ShapeDtypeStruct((1, dim), F32),
        ],
        compiler_params=params(),
        cost_estimate=cost(2 * tokens * dim * (width + 4 * hd), 8 * tokens * dim),
        name="tail",
    )(idx, down, dnear, dfar, cosine, sine, at, dq, wq, wk, wv, x, dy, gain)


def join_wide_kernel(idx_ref, mine_ref, other_ref, out_ref):
    first = idx_ref[0] % 2 == 0
    rows, _ = mine_ref.shape
    mine, other = mine_ref[...], other_ref[...]
    low, high = jnp.where(first, mine, other), jnp.where(first, other, mine)
    heads = 4
    for h in range(heads):
        src = low if h < heads // 2 else high
        base = (h % (heads // 2)) * 256
        for c in range(2):
            out_ref[pl.ds(c * heads + h, rows, stride=2 * heads), :] = src[:, base + c * 128:base + (c + 1) * 128]


def join_wide(idx, mine, other, heads):
    dim, width = mine.shape
    bd = 128
    spec = pl.BlockSpec((bd, width), lambda i: (i, 0))
    out = pl.pallas_call(
        join_wide_kernel,
        grid=(dim // bd,),
        in_specs=[pl.BlockSpec(memory_space=pltpu.SMEM), spec, spec],
        out_specs=pl.BlockSpec((bd * 8, 128), lambda i: (i, 0)),
        out_shape=jax.ShapeDtypeStruct((dim * 8, 128), F32),
        compiler_params=params(),
        cost_estimate=cost(1000, 16 * dim * width),
        name="join_wide",
    )(idx, mine, other)
    return out.reshape(dim, 2, heads, 128).transpose(0, 2, 1, 3).reshape(dim, heads, 256)


def join_pair_kernel(idx_ref, mine_ref, other_ref, first_ref, second_ref):
    core0 = idx_ref[0] % 2 == 0
    rows = mine_ref.shape[0]
    mine, other = mine_ref[...], other_ref[...]
    first, second = jnp.where(core0, mine, other), jnp.where(core0, other, mine)
    for c in range(2):
        first_ref[pl.ds(c, rows, stride=2), :] = first[:, c * 128:(c + 1) * 128]
        second_ref[pl.ds(c, rows, stride=2), :] = second[:, c * 128:(c + 1) * 128]


def join_pair(idx, mine, other):
    dim, width = mine.shape
    bd = dim // 3
    spec = pl.BlockSpec((bd, width), lambda i: (i, 0))
    out_spec = pl.BlockSpec((bd * 2, 128), lambda i: (i, 0))
    outs = pl.pallas_call(
        join_pair_kernel,
        grid=(dim // bd,),
        in_specs=[pl.BlockSpec(memory_space=pltpu.SMEM), spec, spec],
        out_specs=[out_spec, out_spec],
        out_shape=[jax.ShapeDtypeStruct((dim * 2, 128), F32)] * 2,
        compiler_params=params(),
        cost_estimate=cost(1000, 16 * dim * width),
        name="join_pair",
    )(idx, mine, other)
    return [o.reshape(dim, 1, width) for o in outs]


def join_rows_kernel(idx_ref, mine_ref, other_ref, out_ref):
    first = idx_ref[0] % 2 == 0
    out_ref[...] = jnp.where(first == (pl.program_id(0) == 0), mine_ref[...], other_ref[...])


def join_rows(idx, mine, other):
    rows, dim = mine.shape
    br = 256
    steps = rows // br
    spec = pl.BlockSpec((br, dim), lambda w, i: (i, 0))
    return pl.pallas_call(
        join_rows_kernel,
        grid=(2, steps),
        in_specs=[pl.BlockSpec(memory_space=pltpu.SMEM), spec, spec],
        out_specs=pl.BlockSpec((br, dim), lambda w, i: (w * steps + i, 0)),
        out_shape=jax.ShapeDtypeStruct((rows * 2, dim), F32),
        compiler_params=params(),
        cost_estimate=cost(1000, 16 * dim * rows),
        name="join_rows",
    )(idx, mine, other)


def solution(mesh):
    across = [(0, 2), (2, 0), (1, 3), (3, 1)]
    beside = [(0, 1), (1, 0), (2, 3), (3, 2)]

    def permute(value, pairs):
        return lax.ppermute(value, "cp", pairs)

    def sum_halves(parts):
        mine = parts[0] + permute(parts[1], beside)
        mine = mine + permute(mine, across)
        return mine, permute(mine, beside)

    def local_step(x_in, positions, dy_out, w_query, w_key, w_value, w_out, w_pre, w_post):
        batch, tokens, dim = x_in.shape
        heads, hd = w_query.shape[1], w_query.shape[2]
        half = hd // 2
        idx = lax.axis_index("cp").astype(jnp.int32).reshape(1)
        wq = w_query.reshape(dim, heads * hd)
        wk = w_key.reshape(dim, hd)
        wv = w_value.reshape(dim, hd)
        wo = w_out.reshape(heads * hd, dim)
        x = x_in.reshape(tokens, dim)
        dy = dy_out.reshape(tokens, dim)
        gain_pre = w_pre.reshape(1, dim)
        gain_post = w_post.reshape(1, dim)
        inv_freq = ROPE_BASE ** (jnp.arange(half, dtype=F32) * (-2.0 / hd))
        angles = positions.reshape(tokens, 1).astype(F32) * inv_freq
        cosine, sine = jnp.cos(angles), jnp.sin(angles)

        act, act_t, own = project_kv(x, gain_pre, wk, wv, cosine, sine)
        far = permute(own, [(0, 2), (1, 3)])
        near = permute(own, [(0, 1), (2, 3)])
        q = project_q(act, wq, cosine, sine, heads)
        acc, row_sum = forward_local(idx, q, own, near)
        mid = permute(far, [(2, 3), (3, 2)])
        y, d_out, stat, dwo, dgain_post = forward_post(idx, q, far, mid, acc, row_sum, x, dy, wo, gain_post)
        dwo_mine, dwo_other = sum_halves(dwo)

        dmid, dqt = backward_far(idx, q, d_out, stat, mid, None)
        dmid_in = permute(dmid, [(2, 3), (3, 2)])
        dfar, dqt = backward_far(idx, q, d_out, stat, far, dqt)
        dfar_in = permute(dfar + dmid_in, [(2, 0), (3, 1)])
        dnear, down, dq = backward_local(idx, q, d_out, stat, own, near, dqt, cosine, sine)
        dnear_in = permute(dnear, [(1, 0), (3, 2)])
        dwq = grad_wq(idx, act_t, dq)
        dwq_mine, dwq_other = sum_halves(dwq)
        dx, dwkv, dgain_pre = tail(idx, down, dnear_in, dfar_in, cosine, sine, act_t, dq, wq, wk, wv, x, dy, gain_pre)
        dwkv_mine, dwkv_other = sum_halves(dwkv)
        gains = jnp.concatenate([dgain_pre, dgain_post], axis=0)
        gains = gains + permute(gains, beside)
        gains = gains + permute(gains, across)

        dwo_full = join_rows(idx, dwo_mine, dwo_other)
        dwq_full = join_wide(idx, dwq_mine, dwq_other, heads)
        dwk_full, dwv_full = join_pair(idx, dwkv_mine, dwkv_other)
        return (
            y.reshape(batch, tokens, dim),
            dx.reshape(batch, tokens, dim),
            dwq_full,
            dwk_full,
            dwv_full,
            dwo_full.reshape(heads, hd, dim),
            gains[0],
            gains[1],
        )

    seq_spec = P("dp", "cp", None)
    in_specs = (seq_spec, P("dp", "cp"), seq_spec, P(), P(), P(), P(), P(), P())
    out_specs = (seq_spec, seq_spec, P("dp", None, None), P("dp", None, None), P("dp", None, None), P("dp", None, None), P("dp"), P("dp"))
    return jax.shard_map(local_step, mesh=mesh, in_specs=in_specs, out_specs=out_specs, check_vma=False)
```

```python
import math

import jax
import jax.numpy as jnp
from jax import lax
from jax.experimental import pallas as pl
from jax.experimental.pallas import tpu as pltpu
from jax.sharding import PartitionSpec as P


NORM_EPS = 1e-6
SOFT_CAP = 50.0
QUERY_SCALE = 144.0
ROPE_BASE = 10000.0
LOG2E = math.log2(math.e)
CAP2 = SOFT_CAP * LOG2E
INV_CAP = 1.0 / SOFT_CAP


F32 = jnp.float32
BF16 = jnp.bfloat16
VMEM_LIMIT = 60 * 1024 * 1024

NT = (((1,), (1,)), ((), ()))
NN = (((1,), (0,)), ((), ()))


def dot(a, b, dims=NN):
    return lax.dot_general(a, b, dims, preferred_element_type=F32)


def params():
    return pltpu.CompilerParams(vmem_limit_bytes=VMEM_LIMIT)


def whole(shape):
    zeros = (0,) * len(shape)
    return pl.BlockSpec(shape, lambda *_: zeros)


def cost(flops, nbytes, trans=0):
    return pl.CostEstimate(flops=int(flops), bytes_accessed=int(nbytes), transcendentals=int(trans))


def kv_kernel(x_ref, gain_ref, wk_ref, wv_ref, cos_ref, sin_ref, a_ref, at_ref, kv_ref):
    half = cos_ref.shape[1]
    x = x_ref[...].astype(F32)
    rstd = lax.rsqrt(jnp.mean(x * x, axis=-1, keepdims=True) + NORM_EPS)
    a = (x * rstd * (1.0 + gain_ref[...])).astype(BF16)
    a_ref[...] = a
    at_ref[...] = a.T
    k = dot(a, wk_ref[...]).astype(BF16).astype(F32)
    first, second = k[:, :half], k[:, half:]
    cosine, sine = cos_ref[...], sin_ref[...]
    kv_ref[0, :, :half] = (first * cosine - second * sine).astype(BF16)
    kv_ref[0, :, half:] = (second * cosine + first * sine).astype(BF16)
    kv_ref[1] = dot(a, wv_ref[...]).astype(BF16)


def project_kv(x, gain, wk, wv, cosine, sine):
    tokens, dim = x.shape
    hd = wk.shape[1]
    half = hd // 2
    bt = 256
    return pl.pallas_call(
        kv_kernel,
        grid=(tokens // bt,),
        in_specs=[
            pl.BlockSpec((bt, dim), lambda i: (i, 0)),
            whole((1, dim)),
            whole((dim, hd)),
            whole((dim, hd)),
            pl.BlockSpec((bt, half), lambda i: (i, 0)),
            pl.BlockSpec((bt, half), lambda i: (i, 0)),
        ],
        out_specs=[
            pl.BlockSpec((bt, dim), lambda i: (i, 0)),
            pl.BlockSpec((dim, bt), lambda i: (0, i)),
            pl.BlockSpec((2, bt, hd), lambda i: (0, i, 0)),
        ],
        out_shape=[
            jax.ShapeDtypeStruct((tokens, dim), BF16),
            jax.ShapeDtypeStruct((dim, tokens), BF16),
            jax.ShapeDtypeStruct((2, tokens, hd), BF16),
        ],
        compiler_params=params(),
        cost_estimate=cost(4 * tokens * dim * hd, 6 * tokens * dim),
        name="project_kv",
    )(x, gain, wk, wv, cosine, sine)


def q_kernel(a_ref, wq_ref, cos_ref, sin_ref, q_ref):
    heads, _, hd = q_ref.shape
    half = hd // 2
    cosine, sine = cos_ref[...], sin_ref[...]
    a = a_ref[...]
    scale = QUERY_SCALE ** -0.5
    for h in range(heads):
        q = dot(a, wq_ref[:, h * hd:(h + 1) * hd]).astype(BF16).astype(F32)
        first, second = q[:, :half], q[:, half:]
        q_ref[h, :, :half] = ((first * cosine - second * sine) * scale).astype(BF16)
        q_ref[h, :, half:] = ((second * cosine + first * sine) * scale).astype(BF16)


def project_q(a, wq, cosine, sine, heads):
    tokens, dim = a.shape
    hd = wq.shape[1] // heads
    half = hd // 2
    bt = 256
    return pl.pallas_call(
        q_kernel,
        grid=(tokens // bt,),
        in_specs=[
            pl.BlockSpec((bt, dim), lambda i: (i, 0)),
            whole(wq.shape),
            pl.BlockSpec((bt, half), lambda i: (i, 0)),
            pl.BlockSpec((bt, half), lambda i: (i, 0)),
        ],
        out_specs=pl.BlockSpec((heads, bt, hd), lambda i: (0, i, 0)),
        out_shape=jax.ShapeDtypeStruct((heads, tokens, hd), BF16),
        compiler_params=params(),
        cost_estimate=cost(2 * tokens * dim * heads * hd, 6 * tokens * dim),
        name="project_q",
    )(a, wq, cosine, sine)


def forward_tile(q_ref, acc_ref, sum_ref, k, v, masked):
    heads, bq, _ = q_ref.shape
    bk = k.shape[0]
    if masked:
        keep = lax.broadcasted_iota(jnp.int32, (bq, bk), 1) <= lax.broadcasted_iota(jnp.int32, (bq, bk), 0)
    for h in range(heads):
        s = dot(q_ref[h], k, NT)
        p = jnp.exp2(jnp.tanh(s * INV_CAP) * CAP2)
        if masked:
            p = jnp.where(keep, p, 0.0)
        part = p[:, 0:128]
        for c in range(128, bk, 128):
            part = part + p[:, c:c + 128]
        sum_ref[h] += part
        acc_ref[h] += dot(p.astype(BF16), v)


def forward_local_kernel(idx_ref, q_ref, own_ref, near_ref, acc_ref, sum_ref):
    bq = q_ref.shape[1]
    tokens = own_ref.shape[1]
    i = pl.program_id(0)
    acc_ref[...] = jnp.zeros_like(acc_ref)
    sum_ref[...] = jnp.zeros_like(sum_ref)

    def keys(ref, start, size):
        rows = pl.ds(pl.multiple_of(start, 128), size)
        return ref[0, rows, :], ref[1, rows, :]

    forward_tile(q_ref, acc_ref, sum_ref, *keys(own_ref, i * bq, bq), True)

    def own_step(j, _):
        forward_tile(q_ref, acc_ref, sum_ref, *keys(own_ref, j * bq, bq), False)
        return 0

    lax.fori_loop(0, i, own_step, 0)

    @pl.when(idx_ref[0] % 2 == 1)
    def _():
        def near_step(j, _):
            forward_tile(q_ref, acc_ref, sum_ref, *keys(near_ref, j * 512, 512), False)
            return 0

        lax.fori_loop(0, tokens // 512, near_step, 0)


def forward_local(idx, q, own, near):
    heads, tokens, hd = q.shape
    bq = 256
    return pl.pallas_call(
        forward_local_kernel,
        grid=(tokens // bq,),
        in_specs=[
            pl.BlockSpec(memory_space=pltpu.SMEM),
            pl.BlockSpec((heads, bq, hd), lambda i: (0, i, 0)),
            whole(own.shape),
            whole(near.shape),
        ],
        out_specs=[
            pl.BlockSpec((heads, bq, hd), lambda i: (0, i, 0)),
            pl.BlockSpec((heads, bq, 128), lambda i: (0, i, 0)),
        ],
        out_shape=[
            jax.ShapeDtypeStruct((heads, tokens, hd), F32),
            jax.ShapeDtypeStruct((heads, tokens, 128), F32),
        ],
        compiler_params=params(),
        cost_estimate=cost(6 * heads * tokens * tokens * hd, 8 * heads * tokens * hd),
        name="forward_local",
    )(idx, q, own, near)


def forward_far_kernel(idx_ref, q_ref, far_ref, mid_ref, acc_in_ref, sum_in_ref, o_ref, out_ref, lse_ref, acc_ref, sum_ref):
    heads, bq, hd = q_ref.shape
    tokens = far_ref.shape[1]
    acc_ref[...] = acc_in_ref[...]
    sum_ref[...] = sum_in_ref[...]

    @pl.when(idx_ref[0] >= 2)
    def _():
        def step(ref):
            def run(j, _):
                rows = pl.ds(pl.multiple_of(j * 512, 512), 512)
                forward_tile(q_ref, acc_ref, sum_ref, ref[0, rows, :], ref[1, rows, :], False)
                return 0

            return run

        lax.fori_loop(0, tokens // 512, step(far_ref), 0)
        lax.fori_loop(0, tokens // 512, step(mid_ref), 0)

    lane = lax.broadcasted_iota(jnp.int32, (bq, 128), 1)
    lse = jnp.zeros((bq, 128), F32)
    for h in range(heads):
        total = jnp.sum(sum_ref[h], axis=-1, keepdims=True)
        lse = jnp.where(lane == h, jnp.log2(total), lse)
        out = acc_ref[h] / total
        out_ref[h] = out
        o_ref[:, h * hd:(h + 1) * hd] = out.astype(BF16)
    lse_ref[...] = lse


def forward_far(idx, q, far, mid, acc, row_sum):
    heads, tokens, hd = q.shape
    bq = 256
    rows3 = lambda last: pl.BlockSpec((heads, bq, last), lambda i: (0, i, 0))
    return pl.pallas_call(
        forward_far_kernel,
        grid=(tokens // bq,),
        in_specs=[
            pl.BlockSpec(memory_space=pltpu.SMEM),
            rows3(hd),
            whole(far.shape),
            whole(mid.shape),
            rows3(hd),
            rows3(128),
        ],
        out_specs=[
            pl.BlockSpec((bq, heads * hd), lambda i: (i, 0)),
            rows3(hd),
            pl.BlockSpec((bq, 128), lambda i: (i, 0)),
        ],
        out_shape=[
            jax.ShapeDtypeStruct((tokens, heads * hd), BF16),
            jax.ShapeDtypeStruct((heads, tokens, hd), F32),
            jax.ShapeDtypeStruct((tokens, 128), F32),
        ],
        scratch_shapes=[
            pltpu.VMEM((heads, bq, hd), F32),
            pltpu.VMEM((heads, bq, 128), F32),
        ],
        compiler_params=params(),
        cost_estimate=cost(8 * heads * tokens * tokens * hd, 12 * heads * tokens * hd),
        name="forward_far",
    )(idx, q, far, mid, acc, row_sum)


def post_norm(o, wo, gain, dy):
    z = dot(o, wo).astype(BF16).astype(F32)
    rstd = lax.rsqrt(jnp.mean(z * z, axis=-1, keepdims=True) + NORM_EPS)
    unit = z * rstd
    g = dy * gain
    dz = (rstd * (g - unit * jnp.mean(g * unit, axis=-1, keepdims=True))).astype(BF16)
    return unit, dz


def post_kernel(o_ref, out_ref, lse_ref, x_ref, dy_ref, wo_ref, gain_ref, y_ref, do_ref, dz_ref, stat_ref, dgain_ref):
    heads, bq, hd = out_ref.shape
    gain = 1.0 + gain_ref[...]
    dy = dy_ref[...].astype(F32)
    unit, dz = post_norm(o_ref[...], wo_ref[...], gain, dy)
    y_ref[...] = (x_ref[...].astype(F32) + (unit * gain).astype(BF16).astype(F32)).astype(BF16)
    dz_ref[...] = dz

    @pl.when(pl.program_id(0) == 0)
    def _():
        dgain_ref[...] = jnp.zeros_like(dgain_ref)

    dgain_ref[...] += jnp.sum(dy * unit, axis=0, keepdims=True)
    lane = lax.broadcasted_iota(jnp.int32, (bq, 128), 1)
    stat = lse_ref[...]
    for h in range(heads):
        d_out = dot(dz, wo_ref[h * hd:(h + 1) * hd, :], NT).astype(BF16)
        do_ref[h] = d_out
        delta = jnp.sum(d_out.astype(F32) * out_ref[h], axis=-1, keepdims=True)
        stat = jnp.where(lane == heads + h, delta, stat)
    stat_ref[...] = stat.T[0:8, :]


def post(o, out, lse, x, dy, wo, gain):
    heads, tokens, hd = out.shape
    dim = x.shape[1]
    bq = 256
    rows3 = pl.BlockSpec((heads, bq, hd), lambda i: (0, i, 0))
    rows2 = lambda width: pl.BlockSpec((bq, width), lambda i: (i, 0))
    return pl.pallas_call(
        post_kernel,
        grid=(tokens // bq,),
        in_specs=[rows2(heads * hd), rows3, rows2(128), rows2(dim), rows2(dim), whole(wo.shape), whole((1, dim))],
        out_specs=[rows2(dim), rows3, rows2(dim), pl.BlockSpec((8, bq), lambda i: (0, i)), whole((1, dim))],
        out_shape=[
            jax.ShapeDtypeStruct((tokens, dim), BF16),
            jax.ShapeDtypeStruct((heads, tokens, hd), BF16),
            jax.ShapeDtypeStruct((tokens, dim), BF16),
            jax.ShapeDtypeStruct((8, tokens), F32),
            jax.ShapeDtypeStruct((1, dim), F32),
        ],
        compiler_params=params(),
        cost_estimate=cost(4 * tokens * heads * hd * dim, 12 * heads * tokens * hd),
        name="post",
    )(o, out, lse, x, dy, wo, gain)


def grad_wo_kernel(idx_ref, o_ref, dz_ref, po_ref, pdy_low_ref, pdy_high_ref, wo_ref, gain_ref, dwo_ref, pdz_ref):
    _, width = o_ref.shape
    bt = pdy_low_ref.shape[0]
    hd = 256
    i = pl.program_id(0)
    rows = pl.ds(pl.multiple_of(i * bt, bt), bt)
    dy = jnp.where(idx_ref[0] >= 2, pdy_high_ref[...], pdy_low_ref[...]).astype(F32)
    pdz_ref[rows, :] = post_norm(po_ref[rows, :], wo_ref[...], 1.0 + gain_ref[...], dy)[1]

    @pl.when(i == pl.num_programs(0) - 1)
    def _():
        core = idx_ref[0] % 2
        per = width // hd // 2
        for which in range(2):
            for hh in range(per):
                cols = pl.ds(pl.multiple_of((((core + which) % 2) * per + hh) * hd, hd), hd)
                dwo_ref[which, hh * hd:(hh + 1) * hd, :] = dot(o_ref[:, cols].T, dz_ref[...]) + dot(po_ref[:, cols].T, pdz_ref[...])


def grad_wo(idx, o, dz, po, pdy_low, pdy_high, wo, gain):
    tokens, width = o.shape
    dim = dz.shape[1]
    bt = 256
    rows2 = pl.BlockSpec((bt, dim), lambda i: (i, 0))
    return pl.pallas_call(
        grad_wo_kernel,
        grid=(tokens // bt,),
        in_specs=[
            pl.BlockSpec(memory_space=pltpu.SMEM),
            whole(o.shape),
            whole(dz.shape),
            whole(o.shape),
            rows2,
            rows2,
            whole(wo.shape),
            whole((1, dim)),
        ],
        out_specs=whole((2, width // 2, dim)),
        out_shape=jax.ShapeDtypeStruct((2, width // 2, dim), F32),
        scratch_shapes=[pltpu.VMEM((tokens, dim), BF16)],
        compiler_params=params(),
        cost_estimate=cost(6 * tokens * width * dim, 12 * tokens * dim),
        name="grad_wo",
    )(idx, o, dz, po, pdy_low, pdy_high, wo, gain)


def backward_tile(q_ref, do_ref, stat_ref, dqt_ref, dkv_ref, k, v, kt, start, bq, masked):
    heads = q_ref.shape[0]
    bk = k.shape[0]
    rows = pl.ds(pl.multiple_of(start, 128), bq)
    if masked:
        keep = lax.broadcasted_iota(jnp.int32, (bk, bq), 0) <= lax.broadcasted_iota(jnp.int32, (bk, bq), 1)
    for h in range(heads):
        q = q_ref[h, rows, :]
        d_out = do_ref[h, rows, :]
        t = jnp.tanh(dot(k, q, NT) * INV_CAP)
        p = jnp.exp2(t * CAP2 - stat_ref[h:h + 1, rows])
        if masked:
            p = jnp.where(keep, p, 0.0)
        dp = dot(v, d_out, NT)
        ds = (p * (dp - stat_ref[heads + h:heads + h + 1, rows]) * (1.0 - t * t)).astype(BF16)
        dkv_ref[1] += dot(p.astype(BF16), d_out)
        dkv_ref[0] += dot(ds, q)
        dqt_ref[h, :, rows] += dot(kt, ds)


def backward_far_kernel(idx_ref, q_ref, do_ref, stat_ref, mid_ref, far_ref, dmid_ref, dfar_ref, dqt_ref):
    tokens = q_ref.shape[1]
    bq = 512
    i = pl.program_id(0)
    per = pl.num_programs(0) // 2

    @pl.when(i == 0)
    def _():
        dqt_ref[...] = jnp.zeros_like(dqt_ref)

    def block(kv_ref, dkv_ref):
        dkv_ref[...] = jnp.zeros_like(dkv_ref)

        @pl.when(idx_ref[0] >= 2)
        def _():
            k, v = kv_ref[0], kv_ref[1]
            kt = k.T

            def step(j, _):
                backward_tile(q_ref, do_ref, stat_ref, dqt_ref, dkv_ref, k, v, kt, j * bq, bq, False)
                return 0

            lax.fori_loop(0, tokens // bq, step, 0)

    pl.when(i < per)(lambda: block(mid_ref, dmid_ref))
    pl.when(i >= per)(lambda: block(far_ref, dfar_ref))


def backward_far(idx, q, d_out, stat, mid, far):
    heads, tokens, hd = q.shape
    bk = 256
    per = tokens // bk
    early = pl.BlockSpec((2, bk, hd), lambda i: (0, jnp.minimum(i, per - 1), 0))
    late = pl.BlockSpec((2, bk, hd), lambda i: (0, jnp.maximum(i - per, 0), 0))
    return pl.pallas_call(
        backward_far_kernel,
        grid=(2 * per,),
        in_specs=[
            pl.BlockSpec(memory_space=pltpu.SMEM),
            whole(q.shape),
            whole(d_out.shape),
            whole(stat.shape),
            early,
            late,
        ],
        out_specs=[early, late, whole((heads, hd, tokens))],
        out_shape=[
            jax.ShapeDtypeStruct((2, tokens, hd), F32),
            jax.ShapeDtypeStruct((2, tokens, hd), F32),
            jax.ShapeDtypeStruct((heads, hd, tokens), F32),
        ],
        compiler_params=params(),
        cost_estimate=cost(20 * heads * tokens * tokens * hd, 12 * heads * tokens * hd),
        name="backward_far",
    )(idx, q, d_out, stat, mid, far)


def backward_local_kernel(idx_ref, q_ref, do_ref, stat_ref, own_ref, near_ref, dqt_in_ref, cos_ref, sin_ref,
                          dnear_ref, down_ref, dq_ref, dqt_ref):
    heads, tokens, hd = q_ref.shape
    half = hd // 2
    bk = own_ref.shape[1]
    i = pl.program_id(0)
    steps = pl.num_programs(0)

    @pl.when(i == 0)
    def _():
        dqt_ref[...] = dqt_in_ref[...]

    dnear_ref[...] = jnp.zeros_like(dnear_ref)
    down_ref[...] = jnp.zeros_like(down_ref)

    @pl.when(idx_ref[0] % 2 == 1)
    def _():
        k, v = near_ref[0], near_ref[1]
        kt = k.T

        def step(j, _):
            backward_tile(q_ref, do_ref, stat_ref, dqt_ref, dnear_ref, k, v, kt, j * 512, 512, False)
            return 0

        lax.fori_loop(0, tokens // 512, step, 0)

    k, v = own_ref[0], own_ref[1]
    kt = k.T
    backward_tile(q_ref, do_ref, stat_ref, dqt_ref, down_ref, k, v, kt, i * bk, bk, True)

    def own_step(j, _):
        backward_tile(q_ref, do_ref, stat_ref, dqt_ref, down_ref, k, v, kt, j * bk, bk, False)
        return 0

    lax.fori_loop(i + 1, steps, own_step, 0)

    @pl.when(i == steps - 1)
    def _():
        scale = QUERY_SCALE ** -0.5
        for h in range(heads):
            dq = dqt_ref[h].T
            first, second = dq[:, :half], dq[:, half:]
            cosine, sine = cos_ref[...], sin_ref[...]
            dq_ref[:, h * hd:h * hd + half] = ((first * cosine + second * sine) * scale).astype(BF16)
            dq_ref[:, h * hd + half:(h + 1) * hd] = ((second * cosine - first * sine) * scale).astype(BF16)


def backward_local(idx, q, d_out, stat, own, near, dqt, cosine, sine):
    heads, tokens, hd = q.shape
    bk = 256
    kv_spec = pl.BlockSpec((2, bk, hd), lambda i: (0, i, 0))
    return pl.pallas_call(
        backward_local_kernel,
        grid=(tokens // bk,),
        in_specs=[
            pl.BlockSpec(memory_space=pltpu.SMEM),
            whole(q.shape),
            whole(d_out.shape),
            whole(stat.shape),
            kv_spec,
            kv_spec,
            whole(dqt.shape),
            whole(cosine.shape),
            whole(sine.shape),
        ],
        out_specs=[kv_spec, kv_spec, whole((tokens, heads * hd))],
        out_shape=[
            jax.ShapeDtypeStruct((2, tokens, hd), F32),
            jax.ShapeDtypeStruct((2, tokens, hd), F32),
            jax.ShapeDtypeStruct((tokens, heads * hd), BF16),
        ],
        scratch_shapes=[pltpu.VMEM((heads, hd, tokens), F32)],
        compiler_params=params(),
        cost_estimate=cost(15 * heads * tokens * tokens * hd, 12 * heads * tokens * hd),
        name="backward_local",
    )(idx, q, d_out, stat, own, near, dqt, cosine, sine)


def dwq_kernel(idx_ref, at_ref, dq_ref, out_ref):
    out_ref[0] = dot(at_ref[...], dq_ref[...])


def grad_wq(idx, at, dq):
    dim, tokens = at.shape
    width = dq.shape[1]
    cols = 256
    per = width // 2 // cols
    grid_spec = pltpu.PrefetchScalarGridSpec(
        num_scalar_prefetch=1,
        grid=(2, per),
        in_specs=[
            pl.BlockSpec((dim, tokens), lambda w, j, idx: (0, 0)),
            pl.BlockSpec((tokens, cols), lambda w, j, idx: (0, ((w + 1 + idx[0]) % 2) * per + j)),
        ],
        out_specs=pl.BlockSpec((1, dim, cols), lambda w, j, idx: (1 - w, 0, j)),
    )
    return pl.pallas_call(
        dwq_kernel,
        grid_spec=grid_spec,
        out_shape=jax.ShapeDtypeStruct((2, dim, width // 2), F32),
        compiler_params=params(),
        cost_estimate=cost(2 * dim * tokens * width, 4 * dim * width),
        name="grad_wq",
    )(idx, at, dq)


def tail_kernel(idx_ref, down_ref, dnear_ref, dfar_ref, cos_ref, sin_ref, at_ref, dq_ref, wq_ref, wk_ref, wv_ref,
                x_ref, dy_ref, gain_ref, dpost_ref, dx_ref, dwkv_ref, dgain_ref):
    _, half = cos_ref.shape
    dim = x_ref.shape[1]
    i = pl.program_id(0)
    dk = down_ref[0] + dnear_ref[0] + dfar_ref[0]
    cosine, sine = cos_ref[...], sin_ref[...]
    first, second = dk[:, :half], dk[:, half:]
    dk = jnp.concatenate([first * cosine + second * sine, second * cosine - first * sine], axis=1).astype(BF16)
    dv = (down_ref[1] + dnear_ref[1] + dfar_ref[1]).astype(BF16)

    @pl.when(i == 0)
    def _():
        dwkv_ref[...] = jnp.zeros_like(dwkv_ref)
        dgain_ref[...] = jnp.zeros_like(dgain_ref)

    core = idx_ref[0] % 2
    at = at_ref[...]
    is_core0 = core == 0
    mine = jnp.where(is_core0, dk, dv)
    theirs = jnp.where(is_core0, dv, dk)
    dwkv_ref[0, 0:dim, :] += dot(at, mine)
    dwkv_ref[1, 0:dim, :] += dot(at, theirs)
    da = dot(dq_ref[...], wq_ref[...], NT) + dot(dk, wk_ref[...], NT) + dot(dv, wv_ref[...], NT)
    x = x_ref[...].astype(F32)
    rstd = lax.rsqrt(jnp.mean(x * x, axis=-1, keepdims=True) + NORM_EPS)
    unit = x * rstd
    dgain_ref[...] += jnp.sum(da * unit, axis=0, keepdims=True)
    g = da * (1.0 + gain_ref[...])
    dx = rstd * (g - unit * jnp.mean(g * unit, axis=-1, keepdims=True))
    dx_ref[...] = (dy_ref[...].astype(F32) + dx).astype(BF16)

    @pl.when(i == pl.num_programs(0) - 1)
    def _():
        dpre, dpost = dgain_ref[...], dpost_ref[...]
        for which, row in enumerate((jnp.where(is_core0, dpre, dpost), jnp.where(is_core0, dpost, dpre))):
            for c in range(dim // 128):
                dwkv_ref[which, dim + c // 2:dim + c // 2 + 1, c % 2 * 128:(c % 2 + 1) * 128] = row[:, c * 128:(c + 1) * 128]


def tail(idx, down, dnear, dfar, cosine, sine, at, dq, wq, wk, wv, x, dy, gain, dpost):
    tokens, dim = x.shape
    hd = wk.shape[1]
    width = wq.shape[1]
    bt = 256
    kv_spec = pl.BlockSpec((2, bt, hd), lambda i: (0, i, 0))
    rope_spec = pl.BlockSpec((bt, hd // 2), lambda i: (i, 0))
    rows2 = pl.BlockSpec((bt, dim), lambda i: (i, 0))
    return pl.pallas_call(
        tail_kernel,
        grid=(tokens // bt,),
        in_specs=[
            pl.BlockSpec(memory_space=pltpu.SMEM),
            kv_spec,
            kv_spec,
            kv_spec,
            rope_spec,
            rope_spec,
            pl.BlockSpec((dim, bt), lambda i: (0, i)),
            pl.BlockSpec((bt, width), lambda i: (i, 0)),
            whole(wq.shape),
            whole(wk.shape),
            whole(wv.shape),
            rows2,
            rows2,
            whole((1, dim)),
            whole((1, dim)),
        ],
        out_specs=[rows2, whole((2, dim + 8, hd))],
        out_shape=[
            jax.ShapeDtypeStruct((tokens, dim), BF16),
            jax.ShapeDtypeStruct((2, dim + 8, hd), F32),
        ],
        scratch_shapes=[pltpu.VMEM((1, dim), F32)],
        compiler_params=params(),
        cost_estimate=cost(2 * tokens * dim * (width + 4 * hd), 8 * tokens * dim),
        name="tail",
    )(idx, down, dnear, dfar, cosine, sine, at, dq, wq, wk, wv, x, dy, gain, dpost)


def join_wide_kernel(idx_ref, mine_ref, other_ref, out_ref):
    first = idx_ref[0] % 2 == 0
    rows, _ = mine_ref.shape
    mine, other = mine_ref[...], other_ref[...]
    low, high = jnp.where(first, mine, other), jnp.where(first, other, mine)
    heads = 4
    for h in range(heads):
        src = low if h < heads // 2 else high
        base = (h % (heads // 2)) * 256
        for c in range(2):
            out_ref[pl.ds(c * heads + h, rows, stride=2 * heads), :] = src[:, base + c * 128:base + (c + 1) * 128]


def join_wide(idx, mine, other, heads):
    dim, width = mine.shape
    bd = 128
    spec = pl.BlockSpec((bd, width), lambda i: (i, 0))
    out = pl.pallas_call(
        join_wide_kernel,
        grid=(dim // bd,),
        in_specs=[pl.BlockSpec(memory_space=pltpu.SMEM), spec, spec],
        out_specs=pl.BlockSpec((bd * 8, 128), lambda i: (i, 0)),
        out_shape=jax.ShapeDtypeStruct((dim * 8, 128), F32),
        compiler_params=params(),
        cost_estimate=cost(1000, 16 * dim * width),
        name="join_wide",
    )(idx, mine, other)
    return out.reshape(dim, 2, heads, 128).transpose(0, 2, 1, 3).reshape(dim, heads, 256)


def join_pair_kernel(idx_ref, mine_ref, other_ref, first_ref, second_ref, dpre_ref, dpost_ref):
    core0 = idx_ref[0] % 2 == 0
    dim = dpre_ref.shape[1]
    mine, other = mine_ref[...], other_ref[...]
    first, second = jnp.where(core0, mine, other), jnp.where(core0, other, mine)
    for src, out_ref, gain_ref in ((first, first_ref, dpre_ref), (second, second_ref, dpost_ref)):
        for c in range(2):
            out_ref[pl.ds(c, dim, stride=2), :] = src[0:dim, c * 128:(c + 1) * 128]
        for c in range(dim // 128):
            gain_ref[:, c * 128:(c + 1) * 128] = src[dim + c // 2:dim + c // 2 + 1, c % 2 * 128:(c % 2 + 1) * 128]


def join_pair(idx, mine, other):
    dim, width = mine.shape[0] - 8, mine.shape[1]
    outs = pl.pallas_call(
        join_pair_kernel,
        in_specs=[pl.BlockSpec(memory_space=pltpu.SMEM), whole(mine.shape), whole(mine.shape)],
        out_specs=[whole((dim * 2, 128))] * 2 + [whole((1, dim))] * 2,
        out_shape=[jax.ShapeDtypeStruct((dim * 2, 128), F32)] * 2 + [jax.ShapeDtypeStruct((1, dim), F32)] * 2,
        compiler_params=params(),
        cost_estimate=cost(1000, 16 * dim * width),
        name="join_pair",
    )(idx, mine, other)
    return [o.reshape(dim, 1, width) for o in outs[:2]] + [o.reshape(dim) for o in outs[2:]]


def join_rows_kernel(idx_ref, mine_ref, other_ref, out_ref):
    first = idx_ref[0] % 2 == 0
    out_ref[...] = jnp.where(first == (pl.program_id(0) == 0), mine_ref[...], other_ref[...])


def join_rows(idx, mine, other):
    rows, dim = mine.shape
    br = 256
    steps = rows // br
    spec = pl.BlockSpec((br, dim), lambda w, i: (i, 0))
    return pl.pallas_call(
        join_rows_kernel,
        grid=(2, steps),
        in_specs=[pl.BlockSpec(memory_space=pltpu.SMEM), spec, spec],
        out_specs=pl.BlockSpec((br, dim), lambda w, i: (w * steps + i, 0)),
        out_shape=jax.ShapeDtypeStruct((rows * 2, dim), F32),
        compiler_params=params(),
        cost_estimate=cost(1000, 16 * dim * rows),
        name="join_rows",
    )(idx, mine, other)


def solution(mesh):
    across = [(0, 2), (2, 0), (1, 3), (3, 1)]
    beside = [(0, 1), (1, 0), (2, 3), (3, 2)]

    def permute(value, pairs):
        return lax.ppermute(value, "cp", pairs)

    def sum_halves(parts):
        theirs = permute(parts[1], beside)
        mine = parts[0] + theirs
        mine = mine + permute(mine, across)
        return mine, permute(mine, beside)

    def local_step(x_in, positions, dy_out, w_query, w_key, w_value, w_out, w_pre, w_post):
        batch, tokens, dim = x_in.shape
        heads, hd = w_query.shape[1], w_query.shape[2]
        half = hd // 2
        idx = lax.axis_index("cp").astype(jnp.int32).reshape(1)
        wq = w_query.reshape(dim, heads * hd)
        wk = w_key.reshape(dim, hd)
        wv = w_value.reshape(dim, hd)
        wo = w_out.reshape(heads * hd, dim)
        x = x_in.reshape(tokens, dim)
        dy = dy_out.reshape(tokens, dim)
        gain_pre = w_pre.reshape(1, dim)
        gain_post = w_post.reshape(1, dim)
        inv_freq = ROPE_BASE ** (jnp.arange(half, dtype=F32) * (-2.0 / hd))
        angles = positions.reshape(tokens, 1).astype(F32) * inv_freq
        cosine, sine = jnp.cos(angles), jnp.sin(angles)

        act, act_t, own = project_kv(x, gain_pre, wk, wv, cosine, sine)
        far = permute(own, [(0, 2), (1, 3)])
        near = permute(own, [(0, 1), (2, 3)])
        q = project_q(act, wq, cosine, sine, heads)
        acc, row_sum = forward_local(idx, q, own, near)
        mid = permute(far, [(2, 3), (3, 2)])
        dy_high = permute(dy, [(2, 0), (3, 1)])
        o, out, lse = forward_far(idx, q, far, mid, acc, row_sum)
        dy_low = permute(dy, [(0, 2), (1, 3)])
        partner_o = permute(o, across)
        y, d_out, dz, stat, dgain_post = post(o, out, lse, x, dy, wo, gain_post)

        dmid, dfar, dqt = backward_far(idx, q, d_out, stat, mid, far)
        dmid_in = permute(dmid, [(2, 3), (3, 2)])
        dfar_in = permute(dfar + dmid_in, [(2, 0), (3, 1)])
        dnear, down, dq = backward_local(idx, q, d_out, stat, own, near, dqt, cosine, sine)
        dnear_in = permute(dnear, [(1, 0), (3, 2)])
        dwq = grad_wq(idx, act_t, dq)
        dwq_mine, dwq_other = sum_halves(dwq)
        dwo = grad_wo(idx, o, dz, partner_o, dy_high, dy_low, wo, gain_post)
        dwo_mine = dwo[0] + permute(dwo[1], beside)
        dwo_other = permute(dwo_mine, beside)
        dx, dwkv = tail(idx, down, dnear_in, dfar_in, cosine, sine, act_t, dq, wq, wk, wv, x, dy, gain_pre, dgain_post)
        dwkv_mine, dwkv_other = sum_halves(dwkv)

        dwo_full = join_rows(idx, dwo_mine, dwo_other)
        dwq_full = join_wide(idx, dwq_mine, dwq_other, heads)
        dwk_full, dwv_full, dpre_full, dpost_full = join_pair(idx, dwkv_mine, dwkv_other)
        return (
            y.reshape(batch, tokens, dim),
            dx.reshape(batch, tokens, dim),
            dwq_full,
            dwk_full,
            dwv_full,
            dwo_full.reshape(heads, hd, dim),
            dpre_full,
            dpost_full,
        )

    seq_spec = P("dp", "cp", None)
    in_specs = (seq_spec, P("dp", "cp"), seq_spec, P(), P(), P(), P(), P(), P())
    out_specs = (seq_spec, seq_spec, P("dp", None, None), P("dp", None, None), P("dp", None, None), P("dp", None, None), P("dp"), P("dp"))
    return jax.shard_map(local_step, mesh=mesh, in_specs=in_specs, out_specs=out_specs, check_vma=False)
```

```python
import math

import jax
import jax.numpy as jnp
from jax import lax
from jax.experimental import pallas as pl
from jax.experimental.pallas import tpu as pltpu
from jax.sharding import PartitionSpec as P


NORM_EPS = 1e-6
SOFT_CAP = 50.0
QUERY_SCALE = 144.0
ROPE_BASE = 10000.0
LOG2E = math.log2(math.e)
CAP2 = SOFT_CAP * LOG2E
INV_CAP = 1.0 / SOFT_CAP


F32 = jnp.float32
BF16 = jnp.bfloat16
VMEM_LIMIT = 60 * 1024 * 1024

NT = (((1,), (1,)), ((), ()))
NN = (((1,), (0,)), ((), ()))


def dot(a, b, dims=NN):
    return lax.dot_general(a, b, dims, preferred_element_type=F32)


def params():
    return pltpu.CompilerParams(vmem_limit_bytes=VMEM_LIMIT)


def whole(shape):
    zeros = (0,) * len(shape)
    return pl.BlockSpec(shape, lambda *_: zeros)


def rows_spec(rows, width):
    return pl.BlockSpec((rows, width), lambda i: (i, 0))


def stack_spec(depth, rows, width):
    return pl.BlockSpec((depth, rows, width), lambda i: (0, i, 0))


COST = pl.CostEstimate(flops=10**10, bytes_accessed=10**7, transcendentals=0)


def meet_sibling(rank):
    sibling = {"cp": rank + 1 - 2 * (rank % 2)}
    barrier = pltpu.get_barrier_semaphore()
    pl.semaphore_signal(barrier, inc=1, device_id=sibling, device_id_type=pl.DeviceIdType.MESH)
    pl.semaphore_wait(barrier, 1)


def to_sibling(rank, src, dst, send, recv):
    return pltpu.make_async_remote_copy(
        src_ref=src, dst_ref=dst, send_sem=send, recv_sem=recv,
        device_id={"cp": rank + 1 - 2 * (rank % 2)}, device_id_type=pl.DeviceIdType.MESH,
    )


def kv_kernel(x_ref, gain_ref, wk_ref, wv_ref, cos_ref, sin_ref, a_ref, at_ref, kv_ref):
    half = cos_ref.shape[1]
    x = x_ref[...].astype(F32)
    rstd = lax.rsqrt(jnp.mean(x * x, axis=-1, keepdims=True) + NORM_EPS)
    a = (x * rstd * (1.0 + gain_ref[...])).astype(BF16)
    a_ref[...] = a
    at_ref[...] = a.T
    k = dot(a, wk_ref[...]).astype(BF16).astype(F32)
    first, second = k[:, :half], k[:, half:]
    cosine, sine = cos_ref[...], sin_ref[...]
    kv_ref[0, :, :half] = (first * cosine - second * sine).astype(BF16)
    kv_ref[0, :, half:] = (second * cosine + first * sine).astype(BF16)
    kv_ref[1] = dot(a, wv_ref[...]).astype(BF16)


def project_kv(x, gain, wk, wv, cosine, sine):
    tokens, dim = x.shape
    hd = wk.shape[1]
    half = hd // 2
    bt = 256
    return pl.pallas_call(
        kv_kernel,
        grid=(tokens // bt,),
        in_specs=[
            rows_spec(bt, dim),
            whole((1, dim)),
            whole((dim, hd)),
            whole((dim, hd)),
            rows_spec(bt, half),
            rows_spec(bt, half),
        ],
        out_specs=[
            rows_spec(bt, dim),
            pl.BlockSpec((dim, bt), lambda i: (0, i)),
            stack_spec(2, bt, hd),
        ],
        out_shape=[
            jax.ShapeDtypeStruct((tokens, dim), BF16),
            jax.ShapeDtypeStruct((dim, tokens), BF16),
            jax.ShapeDtypeStruct((2, tokens, hd), BF16),
        ],
        compiler_params=params(),
        cost_estimate=COST,
        name="project_kv",
    )(x, gain, wk, wv, cosine, sine)


def q_kernel(a_ref, wq_ref, cos_ref, sin_ref, q_ref):
    heads, _, hd = q_ref.shape
    half = hd // 2
    cosine, sine = cos_ref[...], sin_ref[...]
    a = a_ref[...]
    scale = QUERY_SCALE ** -0.5
    for h in range(heads):
        q = dot(a, wq_ref[:, h * hd:(h + 1) * hd]).astype(BF16).astype(F32)
        first, second = q[:, :half], q[:, half:]
        q_ref[h, :, :half] = ((first * cosine - second * sine) * scale).astype(BF16)
        q_ref[h, :, half:] = ((second * cosine + first * sine) * scale).astype(BF16)


def project_q(a, wq, cosine, sine, heads):
    tokens, dim = a.shape
    hd = wq.shape[1] // heads
    half = hd // 2
    bt = 256
    return pl.pallas_call(
        q_kernel,
        grid=(tokens // bt,),
        in_specs=[
            rows_spec(bt, dim),
            whole(wq.shape),
            rows_spec(bt, half),
            rows_spec(bt, half),
        ],
        out_specs=stack_spec(heads, bt, hd),
        out_shape=jax.ShapeDtypeStruct((heads, tokens, hd), BF16),
        compiler_params=params(),
        cost_estimate=COST,
        name="project_q",
    )(a, wq, cosine, sine)


def forward_tile(q_ref, acc_ref, sum_ref, k, v, masked):
    heads, bq, _ = q_ref.shape
    bk = k.shape[0]
    if masked:
        keep = lax.broadcasted_iota(jnp.int32, (bq, bk), 1) <= lax.broadcasted_iota(jnp.int32, (bq, bk), 0)
    for h in range(heads):
        s = dot(q_ref[h], k, NT)
        p = jnp.exp2(jnp.tanh(s * INV_CAP) * CAP2)
        if masked:
            p = jnp.where(keep, p, 0.0)
        part = p[:, 0:128]
        for c in range(128, bk, 128):
            part = part + p[:, c:c + 128]
        sum_ref[h] += part
        acc_ref[h] += dot(p.astype(BF16), v)


def forward_local_kernel(idx_ref, q_ref, own_ref, near_ref, acc_ref, sum_ref):
    bq = q_ref.shape[1]
    tokens = own_ref.shape[1]
    i = pl.program_id(0)
    acc_ref[...] = jnp.zeros_like(acc_ref)
    sum_ref[...] = jnp.zeros_like(sum_ref)

    def keys(ref, start, size):
        rows = pl.ds(pl.multiple_of(start, 128), size)
        return ref[0, rows, :], ref[1, rows, :]

    forward_tile(q_ref, acc_ref, sum_ref, *keys(own_ref, i * bq, bq), True)

    def own_step(j, _):
        forward_tile(q_ref, acc_ref, sum_ref, *keys(own_ref, j * bq, bq), False)
        return 0

    lax.fori_loop(0, i, own_step, 0)

    @pl.when(idx_ref[0] % 2 == 1)
    def _():
        def near_step(j, _):
            forward_tile(q_ref, acc_ref, sum_ref, *keys(near_ref, j * 512, 512), False)
            return 0

        lax.fori_loop(0, tokens // 512, near_step, 0)


def forward_local(idx, q, own, near):
    heads, tokens, hd = q.shape
    bq = 256
    return pl.pallas_call(
        forward_local_kernel,
        grid=(tokens // bq,),
        in_specs=[
            pl.BlockSpec(memory_space=pltpu.SMEM),
            stack_spec(heads, bq, hd),
            whole(own.shape),
            whole(near.shape),
        ],
        out_specs=[
            stack_spec(heads, bq, hd),
            stack_spec(heads, bq, 128),
        ],
        out_shape=[
            jax.ShapeDtypeStruct((heads, tokens, hd), F32),
            jax.ShapeDtypeStruct((heads, tokens, 128), F32),
        ],
        compiler_params=params(),
        cost_estimate=COST,
        name="forward_local",
    )(idx, q, own, near)


def forward_far_kernel(idx_ref, q_ref, far_ref, mid_ref, acc_in_ref, sum_in_ref, o_ref, out_ref, lse_ref, acc_ref, sum_ref):
    heads, bq, hd = q_ref.shape
    tokens = far_ref.shape[1]
    acc_ref[...] = acc_in_ref[...]
    sum_ref[...] = sum_in_ref[...]

    @pl.when(idx_ref[0] >= 2)
    def _():
        def step(ref):
            def run(j, _):
                rows = pl.ds(pl.multiple_of(j * 512, 512), 512)
                forward_tile(q_ref, acc_ref, sum_ref, ref[0, rows, :], ref[1, rows, :], False)
                return 0

            return run

        lax.fori_loop(0, tokens // 512, step(far_ref), 0)
        lax.fori_loop(0, tokens // 512, step(mid_ref), 0)

    lane = lax.broadcasted_iota(jnp.int32, (bq, 128), 1)
    lse = jnp.zeros((bq, 128), F32)
    for h in range(heads):
        total = jnp.sum(sum_ref[h], axis=-1, keepdims=True)
        lse = jnp.where(lane == h, jnp.log2(total), lse)
        out = acc_ref[h] / total
        out_ref[h] = out
        o_ref[:, h * hd:(h + 1) * hd] = out.astype(BF16)
    lse_ref[...] = lse


def forward_far(idx, q, far, mid, acc, row_sum):
    heads, tokens, hd = q.shape
    bq = 256
    rows3 = lambda last: stack_spec(heads, bq, last)
    return pl.pallas_call(
        forward_far_kernel,
        grid=(tokens // bq,),
        in_specs=[
            pl.BlockSpec(memory_space=pltpu.SMEM),
            rows3(hd),
            whole(far.shape),
            whole(mid.shape),
            rows3(hd),
            rows3(128),
        ],
        out_specs=[
            rows_spec(bq, heads * hd),
            rows3(hd),
            rows_spec(bq, 128),
        ],
        out_shape=[
            jax.ShapeDtypeStruct((tokens, heads * hd), BF16),
            jax.ShapeDtypeStruct((heads, tokens, hd), F32),
            jax.ShapeDtypeStruct((tokens, 128), F32),
        ],
        scratch_shapes=[
            pltpu.VMEM((heads, bq, hd), F32),
            pltpu.VMEM((heads, bq, 128), F32),
        ],
        compiler_params=params(),
        cost_estimate=COST,
        name="forward_far",
    )(idx, q, far, mid, acc, row_sum)


def post_norm(o, wo, gain, dy):
    z = dot(o, wo).astype(BF16).astype(F32)
    rstd = lax.rsqrt(jnp.mean(z * z, axis=-1, keepdims=True) + NORM_EPS)
    unit = z * rstd
    g = dy * gain
    dz = (rstd * (g - unit * jnp.mean(g * unit, axis=-1, keepdims=True))).astype(BF16)
    return unit, dz


def post_kernel(o_ref, out_ref, lse_ref, x_ref, dy_ref, wo_ref, gain_ref, y_ref, do_ref, dz_ref, stat_ref, dgain_ref):
    heads, bq, hd = out_ref.shape
    gain = 1.0 + gain_ref[...]
    dy = dy_ref[...].astype(F32)
    unit, dz = post_norm(o_ref[...], wo_ref[...], gain, dy)
    y_ref[...] = (x_ref[...].astype(F32) + (unit * gain).astype(BF16).astype(F32)).astype(BF16)
    dz_ref[...] = dz

    @pl.when(pl.program_id(0) == 0)
    def _():
        dgain_ref[...] = jnp.zeros_like(dgain_ref)

    dgain_ref[...] += jnp.sum(dy * unit, axis=0, keepdims=True)
    lane = lax.broadcasted_iota(jnp.int32, (bq, 128), 1)
    stat = lse_ref[...]
    for h in range(heads):
        d_out = dot(dz, wo_ref[h * hd:(h + 1) * hd, :], NT).astype(BF16)
        do_ref[h] = d_out
        delta = jnp.sum(d_out.astype(F32) * out_ref[h], axis=-1, keepdims=True)
        stat = jnp.where(lane == heads + h, delta, stat)
    stat_ref[...] = stat.T[0:8, :]


def post(o, out, lse, x, dy, wo, gain):
    heads, tokens, hd = out.shape
    dim = x.shape[1]
    bq = 256
    rows3 = stack_spec(heads, bq, hd)
    rows2 = lambda width: rows_spec(bq, width)
    return pl.pallas_call(
        post_kernel,
        grid=(tokens // bq,),
        in_specs=[rows2(heads * hd), rows3, rows2(128), rows2(dim), rows2(dim), whole(wo.shape), whole((1, dim))],
        out_specs=[rows2(dim), rows3, rows2(dim), pl.BlockSpec((8, bq), lambda i: (0, i)), whole((1, dim))],
        out_shape=[
            jax.ShapeDtypeStruct((tokens, dim), BF16),
            jax.ShapeDtypeStruct((heads, tokens, hd), BF16),
            jax.ShapeDtypeStruct((tokens, dim), BF16),
            jax.ShapeDtypeStruct((8, tokens), F32),
            jax.ShapeDtypeStruct((1, dim), F32),
        ],
        compiler_params=params(),
        cost_estimate=COST,
        name="post",
    )(o, out, lse, x, dy, wo, gain)


def grad_wo_kernel(idx_ref, o_ref, dz_ref, po_ref, pdy_low_ref, pdy_high_ref, wo_ref, gain_ref, mine_ref, theirs_ref, pdz_ref):
    _, width = o_ref.shape
    bt = pdy_low_ref.shape[0]
    hd = 256
    i = pl.program_id(0)
    rows = pl.ds(pl.multiple_of(i * bt, bt), bt)
    dy = jnp.where(idx_ref[0] >= 2, pdy_high_ref[...], pdy_low_ref[...]).astype(F32)
    pdz_ref[rows, :] = post_norm(po_ref[rows, :], wo_ref[...], 1.0 + gain_ref[...], dy)[1]

    @pl.when(i == pl.num_programs(0) - 1)
    def _():
        core = idx_ref[0] % 2
        per = width // hd // 2
        for which, ref in enumerate((mine_ref, theirs_ref)):
            for hh in range(per):
                cols = pl.ds(pl.multiple_of((((core + which) % 2) * per + hh) * hd, hd), hd)
                ref[hh * hd:(hh + 1) * hd, :] = dot(o_ref[:, cols].T, dz_ref[...]) + dot(po_ref[:, cols].T, pdz_ref[...])


def grad_wo(idx, o, dz, po, pdy_low, pdy_high, wo, gain):
    tokens, width = o.shape
    dim = dz.shape[1]
    bt = 256
    rows2 = rows_spec(bt, dim)
    return pl.pallas_call(
        grad_wo_kernel,
        grid=(tokens // bt,),
        in_specs=[
            pl.BlockSpec(memory_space=pltpu.SMEM),
            whole(o.shape),
            whole(dz.shape),
            whole(o.shape),
            rows2,
            rows2,
            whole(wo.shape),
            whole((1, dim)),
        ],
        out_specs=[whole((width // 2, dim))] * 2,
        out_shape=[jax.ShapeDtypeStruct((width // 2, dim), F32)] * 2,
        scratch_shapes=[pltpu.VMEM((tokens, dim), BF16)],
        compiler_params=params(),
        cost_estimate=COST,
        name="grad_wo",
    )(idx, o, dz, po, pdy_low, pdy_high, wo, gain)


def backward_tile(q_ref, do_ref, stat_ref, dqt_ref, dkv_ref, k, v, kt, start, bq, masked):
    heads = q_ref.shape[0]
    bk = k.shape[0]
    rows = pl.ds(pl.multiple_of(start, 128), bq)
    if masked:
        keep = lax.broadcasted_iota(jnp.int32, (bk, bq), 0) <= lax.broadcasted_iota(jnp.int32, (bk, bq), 1)
    for h in range(heads):
        q = q_ref[h, rows, :]
        d_out = do_ref[h, rows, :]
        t = jnp.tanh(dot(k, q, NT) * INV_CAP)
        p = jnp.exp2(t * CAP2 - stat_ref[h:h + 1, rows])
        if masked:
            p = jnp.where(keep, p, 0.0)
        dp = dot(v, d_out, NT)
        ds = (p * (dp - stat_ref[heads + h:heads + h + 1, rows]) * (1.0 - t * t)).astype(BF16)
        dkv_ref[1] += dot(p.astype(BF16), d_out)
        dkv_ref[0] += dot(ds, q)
        dqt_ref[h, :, rows] += dot(kt, ds)


def backward_far_kernel(q_ref, do_ref, stat_ref, mid_ref, far_ref, dfar_ref, dqt_ref, send_ref, recv_ref, send_sem, recv_sem):
    tokens = q_ref.shape[1]
    bq = 512
    rank = lax.axis_index("cp")
    i = pl.program_id(0)
    per = send_ref.shape[0]

    @pl.when(i == 0)
    def _():
        dqt_ref[...] = jnp.zeros_like(dqt_ref)
        meet_sibling(rank)

    def copy(slot):
        return to_sibling(rank, send_ref.at[slot], recv_ref.at[slot], send_sem.at[slot], recv_sem.at[slot])

    def block(kv_ref, dkv_ref):
        k, v = kv_ref[0], kv_ref[1]
        kt = k.T

        def step(j, _):
            backward_tile(q_ref, do_ref, stat_ref, dqt_ref, dkv_ref, k, v, kt, j * bq, bq, False)
            return 0

        lax.fori_loop(0, tokens // bq, step, 0)

    @pl.when(jnp.logical_and(rank >= 2, i < per))
    def _():
        mine = send_ref.at[i]
        mine[...] = jnp.zeros_like(mine)
        block(mid_ref, mine)
        copy(i).start()

    @pl.when(jnp.logical_and(rank >= 2, i >= per))
    def _():
        copy(i - per).wait()
        dfar_ref[...] = recv_ref[i - per]
        block(far_ref, dfar_ref)


def backward_far(q, d_out, stat, mid, far):
    heads, tokens, hd = q.shape
    bk = 256
    per = tokens // bk
    early = pl.BlockSpec((2, bk, hd), lambda i: (0, jnp.minimum(i, per - 1), 0))
    late = pl.BlockSpec((2, bk, hd), lambda i: (0, jnp.maximum(i - per, 0), 0))
    return pl.pallas_call(
        backward_far_kernel,
        grid=(2 * per,),
        in_specs=[whole(q.shape), whole(d_out.shape), whole(stat.shape), early, late],
        out_specs=[late, whole((heads, hd, tokens))],
        out_shape=[
            jax.ShapeDtypeStruct((2, tokens, hd), F32),
            jax.ShapeDtypeStruct((heads, hd, tokens), F32),
        ],
        scratch_shapes=[
            pltpu.VMEM((per, 2, bk, hd), F32),
            pltpu.VMEM((per, 2, bk, hd), F32),
            pltpu.SemaphoreType.DMA((per,)),
            pltpu.SemaphoreType.DMA((per,)),
        ],
        compiler_params=pltpu.CompilerParams(vmem_limit_bytes=VMEM_LIMIT, collective_id=0, has_side_effects=True),
        cost_estimate=COST,
        name="backward_far",
    )(q, d_out, stat, mid, far)


def backward_local_kernel(q_ref, do_ref, stat_ref, own_ref, near_ref, dqt_in_ref, cos_ref, sin_ref, at_ref,
                          down_ref, dq_ref, dwq_ref, dqt_ref, near_send, near_recv, dwq_send, dwq_recv,
                          near_send_sem, near_recv_sem, dwq_send_sem, dwq_recv_sem):
    heads, tokens, hd = q_ref.shape
    half = hd // 2
    bk = own_ref.shape[1]
    rank = lax.axis_index("cp")
    core = rank % 2
    i = pl.program_id(0)
    steps = pl.num_programs(0)

    @pl.when(i == 0)
    def _():
        dqt_ref[...] = dqt_in_ref[...]
        meet_sibling(rank)

    def near_copy(slot):
        return to_sibling(rank, near_send.at[slot], near_recv.at[slot], near_send_sem.at[slot], near_recv_sem.at[slot])

    @pl.when(core == 1)
    def _():
        k, v = near_ref[0], near_ref[1]
        kt = k.T
        mine = near_send.at[i]
        mine[...] = jnp.zeros_like(mine)

        def step(j, _):
            backward_tile(q_ref, do_ref, stat_ref, dqt_ref, mine, k, v, kt, j * 512, 512, False)
            return 0

        lax.fori_loop(0, tokens // 512, step, 0)
        near_copy(i).start()

    own_rows = pl.ds(pl.multiple_of(i * bk, bk), bk)
    down = down_ref.at[:, own_rows, :]
    down[...] = jnp.zeros_like(down)
    k, v = own_ref[0], own_ref[1]
    kt = k.T
    backward_tile(q_ref, do_ref, stat_ref, dqt_ref, down, k, v, kt, i * bk, bk, True)

    def own_step(j, _):
        backward_tile(q_ref, do_ref, stat_ref, dqt_ref, down, k, v, kt, j * bk, bk, False)
        return 0

    lax.fori_loop(i + 1, steps, own_step, 0)

    @pl.when(i == steps - 1)
    def _():
        scale = QUERY_SCALE ** -0.5
        for h in range(heads):
            dq = dqt_ref[h].T
            first, second = dq[:, :half], dq[:, half:]
            cosine, sine = cos_ref[...], sin_ref[...]
            dq_ref[:, h * hd:h * hd + half] = ((first * cosine + second * sine) * scale).astype(BF16)
            dq_ref[:, h * hd + half:(h + 1) * hd] = ((second * cosine - first * sine) * scale).astype(BF16)
        dim, width = dwq_ref.shape
        bd = dim // 3

        def product(out_ref, which):
            dq = dq_ref[:, pl.ds(pl.multiple_of((core + which) % 2 * width, width), width)]

            def rows_step(r, _):
                rows = pl.ds(pl.multiple_of(r * bd, bd), bd)
                out_ref[rows, :] = dot(at_ref[rows, :], dq)
                return 0

            lax.fori_loop(0, dim // bd, rows_step, 0)

        product(dwq_send, 1)
        copy = to_sibling(rank, dwq_send, dwq_recv, dwq_send_sem, dwq_recv_sem)
        copy.start()
        product(dwq_ref, 0)

        @pl.when(core == 1)
        def _():
            for slot in range(near_send.shape[0]):
                near_copy(slot).wait_send()

        @pl.when(core == 0)
        def _():
            for slot in range(near_recv.shape[0]):
                near_copy(slot).wait_recv()
                down_ref[:, slot * bk:(slot + 1) * bk, :] += near_recv[slot]

        copy.wait()
        dwq_ref[...] += dwq_recv[...]


def backward_local(q, d_out, stat, own, near, dqt, cosine, sine, at):
    heads, tokens, hd = q.shape
    dim = at.shape[0]
    bk = 256
    per = tokens // bk
    width = heads * hd // 2
    kv_spec = stack_spec(2, bk, hd)
    dma = pltpu.SemaphoreType.DMA
    return pl.pallas_call(
        backward_local_kernel,
        grid=(per,),
        in_specs=[
            whole(q.shape),
            whole(d_out.shape),
            whole(stat.shape),
            kv_spec,
            kv_spec,
            whole(dqt.shape),
            whole(cosine.shape),
            whole(sine.shape),
            whole(at.shape),
        ],
        out_specs=[whole((2, tokens, hd)), whole((tokens, heads * hd)), whole((dim, width))],
        out_shape=[
            jax.ShapeDtypeStruct((2, tokens, hd), F32),
            jax.ShapeDtypeStruct((tokens, heads * hd), BF16),
            jax.ShapeDtypeStruct((dim, width), F32),
        ],
        scratch_shapes=[
            pltpu.VMEM((heads, hd, tokens), F32),
            pltpu.VMEM((per, 2, bk, hd), F32),
            pltpu.VMEM((per, 2, bk, hd), F32),
            pltpu.VMEM((dim, width), F32),
            pltpu.VMEM((dim, width), F32),
            dma((per,)),
            dma((per,)),
            dma,
            dma,
        ],
        compiler_params=pltpu.CompilerParams(vmem_limit_bytes=VMEM_LIMIT, collective_id=1, has_side_effects=True),
        cost_estimate=COST,
        name="backward_local",
    )(q, d_out, stat, own, near, dqt, cosine, sine, at)


def tail_kernel(idx_ref, down_ref, dfar_ref, cos_ref, sin_ref, at_ref, dq_ref, wq_ref, wk_ref, wv_ref,
                x_ref, dy_ref, gain_ref, dpost_ref, dx_ref, mine_ref, theirs_ref, dgain_ref):
    _, half = cos_ref.shape
    dim = x_ref.shape[1]
    i = pl.program_id(0)
    dk = down_ref[0] + dfar_ref[0]
    cosine, sine = cos_ref[...], sin_ref[...]
    first, second = dk[:, :half], dk[:, half:]
    dk = jnp.concatenate([first * cosine + second * sine, second * cosine - first * sine], axis=1).astype(BF16)
    dv = (down_ref[1] + dfar_ref[1]).astype(BF16)

    @pl.when(i == 0)
    def _():
        mine_ref[...] = jnp.zeros_like(mine_ref)
        theirs_ref[...] = jnp.zeros_like(theirs_ref)
        dgain_ref[...] = jnp.zeros_like(dgain_ref)

    core = idx_ref[0] % 2
    at = at_ref[...]
    is_core0 = core == 0
    mine = jnp.where(is_core0, dk, dv)
    theirs = jnp.where(is_core0, dv, dk)
    mine_ref[0:dim, :] += dot(at, mine)
    theirs_ref[0:dim, :] += dot(at, theirs)
    da = dot(dq_ref[...], wq_ref[...], NT) + dot(dk, wk_ref[...], NT) + dot(dv, wv_ref[...], NT)
    x = x_ref[...].astype(F32)
    rstd = lax.rsqrt(jnp.mean(x * x, axis=-1, keepdims=True) + NORM_EPS)
    unit = x * rstd
    dgain_ref[...] += jnp.sum(da * unit, axis=0, keepdims=True)
    g = da * (1.0 + gain_ref[...])
    dx = rstd * (g - unit * jnp.mean(g * unit, axis=-1, keepdims=True))
    dx_ref[...] = (dy_ref[...].astype(F32) + dx).astype(BF16)

    @pl.when(i == pl.num_programs(0) - 1)
    def _():
        dpre, dpost = dgain_ref[...], dpost_ref[...]
        for ref, row in ((mine_ref, jnp.where(is_core0, dpre, dpost)), (theirs_ref, jnp.where(is_core0, dpost, dpre))):
            for c in range(dim // 128):
                ref[dim + c // 2:dim + c // 2 + 1, c % 2 * 128:(c % 2 + 1) * 128] = row[:, c * 128:(c + 1) * 128]


def tail(idx, down, dfar, cosine, sine, at, dq, wq, wk, wv, x, dy, gain, dpost):
    tokens, dim = x.shape
    hd = wk.shape[1]
    width = wq.shape[1]
    bt = 256
    kv_spec = stack_spec(2, bt, hd)
    rope_spec = rows_spec(bt, hd // 2)
    rows2 = rows_spec(bt, dim)
    return pl.pallas_call(
        tail_kernel,
        grid=(tokens // bt,),
        in_specs=[
            pl.BlockSpec(memory_space=pltpu.SMEM),
            kv_spec,
            kv_spec,
            rope_spec,
            rope_spec,
            pl.BlockSpec((dim, bt), lambda i: (0, i)),
            rows_spec(bt, width),
            whole(wq.shape),
            whole(wk.shape),
            whole(wv.shape),
            rows2,
            rows2,
            whole((1, dim)),
            whole((1, dim)),
        ],
        out_specs=[rows2, whole((dim + 8, hd)), whole((dim + 8, hd))],
        out_shape=[
            jax.ShapeDtypeStruct((tokens, dim), BF16),
            jax.ShapeDtypeStruct((dim + 8, hd), F32),
            jax.ShapeDtypeStruct((dim + 8, hd), F32),
        ],
        scratch_shapes=[pltpu.VMEM((1, dim), F32)],
        compiler_params=params(),
        cost_estimate=COST,
        name="tail",
    )(idx, down, dfar, cosine, sine, at, dq, wq, wk, wv, x, dy, gain, dpost)


def join_wide_kernel(idx_ref, mine_ref, other_ref, out_ref):
    first = idx_ref[0] % 2 == 0
    rows, _ = mine_ref.shape
    mine, other = mine_ref[...], other_ref[...]
    low, high = jnp.where(first, mine, other), jnp.where(first, other, mine)
    heads = 4
    for h in range(heads):
        src = low if h < heads // 2 else high
        base = (h % (heads // 2)) * 256
        for c in range(2):
            out_ref[pl.ds(c * heads + h, rows, stride=2 * heads), :] = src[:, base + c * 128:base + (c + 1) * 128]


def join_wide(idx, mine, other, heads):
    dim, width = mine.shape
    bd = 128
    spec = rows_spec(bd, width)
    out = pl.pallas_call(
        join_wide_kernel,
        grid=(dim // bd,),
        in_specs=[pl.BlockSpec(memory_space=pltpu.SMEM), spec, spec],
        out_specs=rows_spec(bd * 8, 128),
        out_shape=jax.ShapeDtypeStruct((dim * 8, 128), F32),
        compiler_params=params(),
        cost_estimate=COST,
        name="join_wide",
    )(idx, mine, other)
    return out.reshape(dim, 2, heads, 128).transpose(0, 2, 1, 3).reshape(dim, heads, 256)


def join_pair_kernel(idx_ref, mine_ref, other_ref, first_ref, second_ref, dpre_ref, dpost_ref):
    core0 = idx_ref[0] % 2 == 0
    dim = dpre_ref.shape[1]
    mine, other = mine_ref[...], other_ref[...]
    first, second = jnp.where(core0, mine, other), jnp.where(core0, other, mine)
    for src, out_ref, gain_ref in ((first, first_ref, dpre_ref), (second, second_ref, dpost_ref)):
        for c in range(2):
            out_ref[pl.ds(c, dim, stride=2), :] = src[0:dim, c * 128:(c + 1) * 128]
        for c in range(dim // 128):
            gain_ref[:, c * 128:(c + 1) * 128] = src[dim + c // 2:dim + c // 2 + 1, c % 2 * 128:(c % 2 + 1) * 128]


def join_pair(idx, mine, other):
    dim, width = mine.shape[0] - 8, mine.shape[1]
    outs = pl.pallas_call(
        join_pair_kernel,
        in_specs=[pl.BlockSpec(memory_space=pltpu.SMEM), whole(mine.shape), whole(mine.shape)],
        out_specs=[whole((dim * 2, 128))] * 2 + [whole((1, dim))] * 2,
        out_shape=[jax.ShapeDtypeStruct((dim * 2, 128), F32)] * 2 + [jax.ShapeDtypeStruct((1, dim), F32)] * 2,
        compiler_params=params(),
        cost_estimate=COST,
        name="join_pair",
    )(idx, mine, other)
    return [o.reshape(dim, 1, width) for o in outs[:2]] + [o.reshape(dim) for o in outs[2:]]


def join_rows_kernel(idx_ref, mine_ref, other_ref, out_ref):
    first = idx_ref[0] % 2 == 0
    out_ref[...] = jnp.where(first == (pl.program_id(0) == 0), mine_ref[...], other_ref[...])


def join_rows(idx, mine, other):
    rows, dim = mine.shape
    br = 256
    steps = rows // br
    spec = pl.BlockSpec((br, dim), lambda w, i: (i, 0))
    return pl.pallas_call(
        join_rows_kernel,
        grid=(2, steps),
        in_specs=[pl.BlockSpec(memory_space=pltpu.SMEM), spec, spec],
        out_specs=pl.BlockSpec((br, dim), lambda w, i: (w * steps + i, 0)),
        out_shape=jax.ShapeDtypeStruct((rows * 2, dim), F32),
        compiler_params=params(),
        cost_estimate=COST,
        name="join_rows",
    )(idx, mine, other)


def solution(mesh):
    across = [(0, 2), (2, 0), (1, 3), (3, 1)]
    beside = [(0, 1), (1, 0), (2, 3), (3, 2)]

    def permute(value, pairs):
        return lax.ppermute(value, "cp", pairs)

    def sum_halves(parts):
        theirs = permute(parts[1], beside)
        mine = parts[0] + theirs
        mine = mine + permute(mine, across)
        return mine, permute(mine, beside)

    def local_step(x_in, positions, dy_out, w_query, w_key, w_value, w_out, w_pre, w_post):
        batch, tokens, dim = x_in.shape
        heads, hd = w_query.shape[1], w_query.shape[2]
        half = hd // 2
        idx = lax.axis_index("cp").astype(jnp.int32).reshape(1)
        wq = w_query.reshape(dim, heads * hd)
        wk = w_key.reshape(dim, hd)
        wv = w_value.reshape(dim, hd)
        wo = w_out.reshape(heads * hd, dim)
        x = x_in.reshape(tokens, dim)
        dy = dy_out.reshape(tokens, dim)
        gain_pre = w_pre.reshape(1, dim)
        gain_post = w_post.reshape(1, dim)
        inv_freq = ROPE_BASE ** (jnp.arange(half, dtype=F32) * (-2.0 / hd))
        angles = positions.reshape(tokens, 1).astype(F32) * inv_freq
        cosine, sine = jnp.cos(angles), jnp.sin(angles)

        act, act_t, own = project_kv(x, gain_pre, wk, wv, cosine, sine)
        far = permute(own, [(0, 2), (1, 3)])
        near = permute(own, [(0, 1), (2, 3)])
        q = project_q(act, wq, cosine, sine, heads)
        acc, row_sum = forward_local(idx, q, own, near)
        mid = permute(far, [(2, 3), (3, 2)])
        dy_high = permute(dy, [(2, 0), (3, 1)])
        o, out, lse = forward_far(idx, q, far, mid, acc, row_sum)
        dy_low = permute(dy, [(0, 2), (1, 3)])
        partner_o = permute(o, across)
        y, d_out, dz, stat, dgain_post = post(o, out, lse, x, dy, wo, gain_post)

        dfar, dqt = backward_far(q, d_out, stat, mid, far)
        dfar_in = permute(dfar, [(2, 0), (3, 1)])
        down, dq, dwq_part = backward_local(q, d_out, stat, own, near, dqt, cosine, sine, act_t)
        dwq_mine = dwq_part + permute(dwq_part, across)
        dwq_other = permute(dwq_mine, beside)
        dwo = grad_wo(idx, o, dz, partner_o, dy_high, dy_low, wo, gain_post)
        dwo_mine = dwo[0] + permute(dwo[1], beside)
        dwo_other = permute(dwo_mine, beside)
        dx, *dwkv = tail(idx, down, dfar_in, cosine, sine, act_t, dq, wq, wk, wv, x, dy, gain_pre, dgain_post)
        dwkv_mine, dwkv_other = sum_halves(dwkv)

        dwo_full = join_rows(idx, dwo_mine, dwo_other)
        dwq_full = join_wide(idx, dwq_mine, dwq_other, heads)
        dwk_full, dwv_full, dpre_full, dpost_full = join_pair(idx, dwkv_mine, dwkv_other)
        return (
            y.reshape(batch, tokens, dim),
            dx.reshape(batch, tokens, dim),
            dwq_full,
            dwk_full,
            dwv_full,
            dwo_full.reshape(heads, hd, dim),
            dpre_full,
            dpost_full,
        )

    seq_spec = P("dp", "cp", None)
    in_specs = (seq_spec, P("dp", "cp"), seq_spec, P(), P(), P(), P(), P(), P())
    out_specs = (seq_spec, seq_spec, P("dp", None, None), P("dp", None, None), P("dp", None, None), P("dp", None, None), P("dp"), P("dp"))
    return jax.shard_map(local_step, mesh=mesh, in_specs=in_specs, out_specs=out_specs, check_vma=False)
```

```python
import math

import jax
import jax.numpy as jnp
from jax import lax
from jax.experimental import pallas as pl
from jax.experimental.pallas import tpu as pltpu
from jax.sharding import PartitionSpec as P


NORM_EPS = 1e-6
SOFT_CAP = 50.0
QUERY_SCALE = 144.0
ROPE_BASE = 10000.0
LOG2E = math.log2(math.e)
CAP2 = SOFT_CAP * LOG2E
INV_CAP = 1.0 / SOFT_CAP


F32 = jnp.float32
BF16 = jnp.bfloat16
VMEM_LIMIT = 60 * 1024 * 1024

NT = (((1,), (1,)), ((), ()))
NN = (((1,), (0,)), ((), ()))


def dot(a, b, dims=NN):
    return lax.dot_general(a, b, dims, preferred_element_type=F32)


def params():
    return pltpu.CompilerParams(vmem_limit_bytes=VMEM_LIMIT)


def whole(shape):
    zeros = (0,) * len(shape)
    return pl.BlockSpec(shape, lambda *_: zeros)


def rows_spec(rows, width):
    return pl.BlockSpec((rows, width), lambda i: (i, 0))


def stack_spec(depth, rows, width):
    return pl.BlockSpec((depth, rows, width), lambda i: (0, i, 0))


COST = pl.CostEstimate(flops=10**10, bytes_accessed=10**7, transcendentals=0)


def meet_sibling(rank):
    sibling = {"cp": rank + 1 - 2 * (rank % 2)}
    barrier = pltpu.get_barrier_semaphore()
    pl.semaphore_signal(barrier, inc=1, device_id=sibling, device_id_type=pl.DeviceIdType.MESH)
    pl.semaphore_wait(barrier, 1)


def to_sibling(rank, src, dst, send, recv):
    return pltpu.make_async_remote_copy(
        src_ref=src, dst_ref=dst, send_sem=send, recv_sem=recv,
        device_id={"cp": rank + 1 - 2 * (rank % 2)}, device_id_type=pl.DeviceIdType.MESH,
    )


def rope(values, cosine, sine):
    half = cosine.shape[-1]
    first, second = values[:, :half], values[:, half:]
    return jnp.concatenate([first * cosine - second * sine, second * cosine + first * sine], axis=-1)


def forward_tile(q_ref, acc_ref, sum_ref, k, v, masked):
    heads, bq, _ = q_ref.shape
    bk = k.shape[0]
    if masked:
        keep = lax.broadcasted_iota(jnp.int32, (bq, bk), 1) <= lax.broadcasted_iota(jnp.int32, (bq, bk), 0)
    for h in range(heads):
        s = dot(q_ref[h], k, NT)
        p = jnp.exp2(jnp.tanh(s * INV_CAP) * CAP2)
        if masked:
            p = jnp.where(keep, p, 0.0)
        part = p[:, 0:128]
        for c in range(128, bk, 128):
            part = part + p[:, c:c + 128]
        sum_ref[h] += part
        acc_ref[h] += dot(p.astype(BF16), v)


def forward_kernel(x_ref, gain_ref, wk_ref, wv_ref, wq_ref, cos_ref, sin_ref,
                   at_ref, q_ref, own_ref, near_ref, far_ref, mid_ref, o_ref, out_ref, lse_ref,
                   a_s, own_s, near_s, far_s, mid_s, acc_s, sum_s,
                   far_send, far_recv, near_send, near_recv, mid_send, mid_recv):
    heads, tokens, hd = q_ref.shape
    bt = x_ref.shape[0]
    tiles = tokens // bt
    big = 2 * bt
    rank = lax.axis_index("cp")
    core = rank % 2
    i = pl.program_id(0)
    across = {"cp": (rank + 2) % 4}
    mesh_id = pl.DeviceIdType.MESH

    def rows_of(t, size=bt):
        return pl.ds(pl.multiple_of(t * size, size), size)

    def far_copy(t):
        rows = rows_of(t)
        return pltpu.make_async_remote_copy(
            src_ref=own_s.at[:, rows, :], dst_ref=far_s.at[:, rows, :], send_sem=far_send.at[t], recv_sem=far_recv.at[t],
            device_id=across, device_id_type=mesh_id,
        )

    def near_copy(t):
        rows = rows_of(t)
        return to_sibling(rank, own_s.at[:, rows, :], near_s.at[:, rows, :], near_send.at[t], near_recv.at[t])

    def mid_copy(c):
        rows = rows_of(c, big)
        return to_sibling(rank, far_s.at[:, rows, :], mid_s.at[:, rows, :], mid_send.at[c], mid_recv.at[c])

    @pl.when(i == 0)
    def _():
        barrier = pltpu.get_barrier_semaphore()
        for other in (across, {"cp": rank + 1 - 2 * core}):
            pl.semaphore_signal(barrier, inc=1, device_id=other, device_id_type=mesh_id)
        pl.semaphore_wait(barrier, 2)

    @pl.when(i < tiles)
    def _():
        rows = rows_of(i)
        x = x_ref[...].astype(F32)
        rstd = lax.rsqrt(jnp.mean(x * x, axis=-1, keepdims=True) + NORM_EPS)
        a = (x * rstd * (1.0 + gain_ref[...])).astype(BF16)
        a_s[rows, :] = a
        own_s[0, rows, :] = rope(dot(a, wk_ref[...]).astype(BF16).astype(F32), cos_ref[rows, :], sin_ref[rows, :]).astype(BF16)
        own_s[1, rows, :] = dot(a, wv_ref[...]).astype(BF16)
        pl.when(rank < 2)(lambda: far_copy(i).start())
        pl.when(core == 0)(lambda: near_copy(i).start())
        at_ref[...] = a.T

    def attend(t, kv_ref, start, size, masked):
        rows, keys = rows_of(t), pl.ds(pl.multiple_of(start, bt), size)
        forward_tile(q_ref.at[:, rows, :], acc_s.at[:, rows, :], sum_s.at[:, rows, :],
                     kv_ref[0, keys, :], kv_ref[1, keys, :], masked)

    @pl.when(jnp.logical_and(i >= tiles, i < 2 * tiles))
    def _():
        t = i - tiles
        rows = rows_of(t)
        a = a_s[rows, :]
        scale = QUERY_SCALE ** -0.5
        for h in range(heads):
            q = dot(a, wq_ref[:, h * hd:(h + 1) * hd]).astype(BF16).astype(F32)
            q_ref[h, rows, :] = (rope(q, cos_ref[rows, :], sin_ref[rows, :]) * scale).astype(BF16)
        acc_s[:, rows, :] = jnp.zeros((heads, bt, hd), F32)
        sum_s[:, rows, :] = jnp.zeros((heads, bt, 128), F32)
        attend(t, own_s, t * bt, bt, True)

        def own_step(j, _):
            attend(t, own_s, j * bt, bt, False)
            return 0

        lax.fori_loop(0, t, own_step, 0)

        @pl.when(core == 1)
        def _():
            pl.when(t == 0)(lambda: [near_copy(n).wait_recv() for n in range(tiles)] and None)

            def near_step(j, _):
                attend(t, near_s, j * big, big, False)
                return 0

            lax.fori_loop(0, tokens // big, near_step, 0)

    chunks = tokens // big
    c = i - 2 * tiles

    def far_chunk(kv_ref, start):
        def step(t, _):
            attend(t, kv_ref, start, big, False)
            return 0

        lax.fori_loop(0, tiles, step, 0)

    @pl.when(jnp.logical_and(rank >= 2, jnp.logical_and(c >= 0, c < chunks)))
    def _():
        far_copy(2 * c).wait_recv()
        far_copy(2 * c + 1).wait_recv()
        mid_copy(c).start()
        far_chunk(far_s, c * big)

    @pl.when(jnp.logical_and(rank >= 2, jnp.logical_and(c >= chunks, c < 2 * chunks)))
    def _():
        mid_copy(c - chunks).wait_recv()
        far_chunk(mid_s, (c - chunks) * big)

    last = i - 2 * tiles - 2 * chunks

    @pl.when(last >= 0)
    def _():
        rows = rows_of(last)
        lane = lax.broadcasted_iota(jnp.int32, (bt, 128), 1)
        lse = jnp.zeros((bt, 128), F32)
        for h in range(heads):
            total = jnp.sum(sum_s[h, rows, :], axis=-1, keepdims=True)
            lse = jnp.where(lane == h, jnp.log2(total), lse)
            out = acc_s[h, rows, :] / total
            out_ref[h] = out
            o_ref[:, h * hd:(h + 1) * hd] = out.astype(BF16)
        lse_ref[...] = lse
        for dst, src in ((own_ref, own_s), (near_ref, near_s), (far_ref, far_s), (mid_ref, mid_s)):
            dst[...] = src[:, rows, :]

    @pl.when(last == tiles - 1)
    def _():
        pl.when(rank < 2)(lambda: [far_copy(n).wait_send() for n in range(tiles)] and None)
        pl.when(core == 0)(lambda: [near_copy(n).wait_send() for n in range(tiles)] and None)
        pl.when(rank >= 2)(lambda: [mid_copy(n).wait_send() for n in range(chunks)] and None)


def forward(x, gain, wk, wv, wq, cosine, sine, heads):
    tokens, dim = x.shape
    hd = wk.shape[1]
    bt = 256
    tiles = tokens // bt
    chunks = tiles // 2
    done = 2 * tiles + 2 * chunks
    dma = pltpu.SemaphoreType.DMA
    early = lambda i: jnp.minimum(i, tiles - 1)
    late = lambda i: jnp.maximum(i - done, 0)
    kv_shape = jax.ShapeDtypeStruct((2, tokens, hd), BF16)
    kv_out = pl.BlockSpec((2, bt, hd), lambda i: (0, late(i), 0))
    return pl.pallas_call(
        forward_kernel,
        grid=(done + tiles,),
        in_specs=[
            pl.BlockSpec((bt, dim), lambda i: (early(i), 0)),
            whole(gain.shape),
            whole(wk.shape),
            whole(wv.shape),
            whole(wq.shape),
            whole(cosine.shape),
            whole(sine.shape),
        ],
        out_specs=[
            pl.BlockSpec((dim, bt), lambda i: (0, early(i))),
            whole((heads, tokens, hd)),
            kv_out,
            kv_out,
            kv_out,
            kv_out,
            pl.BlockSpec((bt, heads * hd), lambda i: (late(i), 0)),
            pl.BlockSpec((heads, bt, hd), lambda i: (0, late(i), 0)),
            pl.BlockSpec((bt, 128), lambda i: (late(i), 0)),
        ],
        out_shape=[
            jax.ShapeDtypeStruct((dim, tokens), BF16),
            jax.ShapeDtypeStruct((heads, tokens, hd), BF16),
            kv_shape,
            kv_shape,
            kv_shape,
            kv_shape,
            jax.ShapeDtypeStruct((tokens, heads * hd), BF16),
            jax.ShapeDtypeStruct((heads, tokens, hd), F32),
            jax.ShapeDtypeStruct((tokens, 128), F32),
        ],
        scratch_shapes=[pltpu.VMEM((tokens, dim), BF16)] + [pltpu.VMEM((2, tokens, hd), BF16)] * 4 + [
            pltpu.VMEM((heads, tokens, hd), F32),
            pltpu.VMEM((heads, tokens, 128), F32),
            dma((tiles,)),
            dma((tiles,)),
            dma((tiles,)),
            dma((tiles,)),
            dma((chunks,)),
            dma((chunks,)),
        ],
        compiler_params=pltpu.CompilerParams(vmem_limit_bytes=VMEM_LIMIT, collective_id=2, has_side_effects=True),
        cost_estimate=COST,
        name="forward",
    )(x, gain, wk, wv, wq, cosine, sine)


def post_norm(o, wo, gain, dy):
    z = dot(o, wo).astype(BF16).astype(F32)
    rstd = lax.rsqrt(jnp.mean(z * z, axis=-1, keepdims=True) + NORM_EPS)
    unit = z * rstd
    g = dy * gain
    dz = (rstd * (g - unit * jnp.mean(g * unit, axis=-1, keepdims=True))).astype(BF16)
    return unit, dz


def post_kernel(o_ref, out_ref, lse_ref, x_ref, dy_ref, wo_ref, gain_ref, y_ref, do_ref, dz_ref, stat_ref, dgain_ref):
    heads, bq, hd = out_ref.shape
    gain = 1.0 + gain_ref[...]
    dy = dy_ref[...].astype(F32)
    unit, dz = post_norm(o_ref[...], wo_ref[...], gain, dy)
    y_ref[...] = (x_ref[...].astype(F32) + (unit * gain).astype(BF16).astype(F32)).astype(BF16)
    dz_ref[...] = dz

    @pl.when(pl.program_id(0) == 0)
    def _():
        dgain_ref[...] = jnp.zeros_like(dgain_ref)

    dgain_ref[...] += jnp.sum(dy * unit, axis=0, keepdims=True)
    lane = lax.broadcasted_iota(jnp.int32, (bq, 128), 1)
    stat = lse_ref[...]
    for h in range(heads):
        d_out = dot(dz, wo_ref[h * hd:(h + 1) * hd, :], NT).astype(BF16)
        do_ref[h] = d_out
        delta = jnp.sum(d_out.astype(F32) * out_ref[h], axis=-1, keepdims=True)
        stat = jnp.where(lane == heads + h, delta, stat)
    stat_ref[...] = stat.T[0:8, :]


def post(o, out, lse, x, dy, wo, gain):
    heads, tokens, hd = out.shape
    dim = x.shape[1]
    bq = 256
    rows3 = stack_spec(heads, bq, hd)
    rows2 = lambda width: rows_spec(bq, width)
    return pl.pallas_call(
        post_kernel,
        grid=(tokens // bq,),
        in_specs=[rows2(heads * hd), rows3, rows2(128), rows2(dim), rows2(dim), whole(wo.shape), whole((1, dim))],
        out_specs=[rows2(dim), rows3, rows2(dim), pl.BlockSpec((8, bq), lambda i: (0, i)), whole((1, dim))],
        out_shape=[
            jax.ShapeDtypeStruct((tokens, dim), BF16),
            jax.ShapeDtypeStruct((heads, tokens, hd), BF16),
            jax.ShapeDtypeStruct((tokens, dim), BF16),
            jax.ShapeDtypeStruct((8, tokens), F32),
            jax.ShapeDtypeStruct((1, dim), F32),
        ],
        compiler_params=params(),
        cost_estimate=COST,
        name="post",
    )(o, out, lse, x, dy, wo, gain)


def grad_wo_kernel(idx_ref, o_ref, dz_ref, po_ref, pdy_low_ref, pdy_high_ref, wo_ref, gain_ref, mine_ref, theirs_ref, pdz_ref):
    _, width = o_ref.shape
    bt = pdy_low_ref.shape[0]
    hd = 256
    i = pl.program_id(0)
    rows = pl.ds(pl.multiple_of(i * bt, bt), bt)
    dy = jnp.where(idx_ref[0] >= 2, pdy_high_ref[...], pdy_low_ref[...]).astype(F32)
    pdz_ref[rows, :] = post_norm(po_ref[rows, :], wo_ref[...], 1.0 + gain_ref[...], dy)[1]

    @pl.when(i == pl.num_programs(0) - 1)
    def _():
        core = idx_ref[0] % 2
        per = width // hd // 2
        for which, ref in enumerate((mine_ref, theirs_ref)):
            for hh in range(per):
                cols = pl.ds(pl.multiple_of((((core + which) % 2) * per + hh) * hd, hd), hd)
                ref[hh * hd:(hh + 1) * hd, :] = dot(o_ref[:, cols].T, dz_ref[...]) + dot(po_ref[:, cols].T, pdz_ref[...])


def grad_wo(idx, o, dz, po, pdy_low, pdy_high, wo, gain):
    tokens, width = o.shape
    dim = dz.shape[1]
    bt = 256
    rows2 = rows_spec(bt, dim)
    return pl.pallas_call(
        grad_wo_kernel,
        grid=(tokens // bt,),
        in_specs=[
            pl.BlockSpec(memory_space=pltpu.SMEM),
            whole(o.shape),
            whole(dz.shape),
            whole(o.shape),
            rows2,
            rows2,
            whole(wo.shape),
            whole((1, dim)),
        ],
        out_specs=[whole((width // 2, dim))] * 2,
        out_shape=[jax.ShapeDtypeStruct((width // 2, dim), F32)] * 2,
        scratch_shapes=[pltpu.VMEM((tokens, dim), BF16)],
        compiler_params=params(),
        cost_estimate=COST,
        name="grad_wo",
    )(idx, o, dz, po, pdy_low, pdy_high, wo, gain)


def backward_tile(q_ref, do_ref, stat_ref, dqt_ref, dkv_ref, k, v, kt, start, bq, masked):
    heads = q_ref.shape[0]
    bk = k.shape[0]
    rows = pl.ds(pl.multiple_of(start, 128), bq)
    if masked:
        keep = lax.broadcasted_iota(jnp.int32, (bk, bq), 0) <= lax.broadcasted_iota(jnp.int32, (bk, bq), 1)
    for h in range(heads):
        q = q_ref[h, rows, :]
        d_out = do_ref[h, rows, :]
        t = jnp.tanh(dot(k, q, NT) * INV_CAP)
        p = jnp.exp2(t * CAP2 - stat_ref[h:h + 1, rows])
        if masked:
            p = jnp.where(keep, p, 0.0)
        dp = dot(v, d_out, NT)
        ds = (p * (dp - stat_ref[heads + h:heads + h + 1, rows]) * (1.0 - t * t)).astype(BF16)
        dkv_ref[1] += dot(p.astype(BF16), d_out)
        dkv_ref[0] += dot(ds, q)
        dqt_ref[h, :, rows] += dot(kt, ds)


def backward_far_kernel(q_ref, do_ref, stat_ref, mid_ref, far_ref, dfar_ref, dqt_ref, send_ref, recv_ref, send_sem, recv_sem):
    tokens = q_ref.shape[1]
    bq = 512
    rank = lax.axis_index("cp")
    i = pl.program_id(0)
    per = send_ref.shape[0]

    @pl.when(i == 0)
    def _():
        dqt_ref[...] = jnp.zeros_like(dqt_ref)
        meet_sibling(rank)

    def copy(slot):
        return to_sibling(rank, send_ref.at[slot], recv_ref.at[slot], send_sem.at[slot], recv_sem.at[slot])

    def block(kv_ref, dkv_ref):
        k, v = kv_ref[0], kv_ref[1]
        kt = k.T

        def step(j, _):
            backward_tile(q_ref, do_ref, stat_ref, dqt_ref, dkv_ref, k, v, kt, j * bq, bq, False)
            return 0

        lax.fori_loop(0, tokens // bq, step, 0)

    @pl.when(jnp.logical_and(rank >= 2, i < per))
    def _():
        mine = send_ref.at[i]
        mine[...] = jnp.zeros_like(mine)
        block(mid_ref, mine)
        copy(i).start()

    @pl.when(jnp.logical_and(rank >= 2, i >= per))
    def _():
        copy(i - per).wait()
        dfar_ref[...] = recv_ref[i - per]
        block(far_ref, dfar_ref)


def backward_far(q, d_out, stat, mid, far):
    heads, tokens, hd = q.shape
    bk = 256
    per = tokens // bk
    early = pl.BlockSpec((2, bk, hd), lambda i: (0, jnp.minimum(i, per - 1), 0))
    late = pl.BlockSpec((2, bk, hd), lambda i: (0, jnp.maximum(i - per, 0), 0))
    return pl.pallas_call(
        backward_far_kernel,
        grid=(2 * per,),
        in_specs=[whole(q.shape), whole(d_out.shape), whole(stat.shape), early, late],
        out_specs=[late, whole((heads, hd, tokens))],
        out_shape=[
            jax.ShapeDtypeStruct((2, tokens, hd), F32),
            jax.ShapeDtypeStruct((heads, hd, tokens), F32),
        ],
        scratch_shapes=[
            pltpu.VMEM((per, 2, bk, hd), F32),
            pltpu.VMEM((per, 2, bk, hd), F32),
            pltpu.SemaphoreType.DMA((per,)),
            pltpu.SemaphoreType.DMA((per,)),
        ],
        compiler_params=pltpu.CompilerParams(vmem_limit_bytes=VMEM_LIMIT, collective_id=0, has_side_effects=True),
        cost_estimate=COST,
        name="backward_far",
    )(q, d_out, stat, mid, far)


def backward_local_kernel(q_ref, do_ref, stat_ref, own_ref, near_ref, dqt_in_ref, cos_ref, sin_ref, at_ref,
                          down_ref, dq_ref, dwq_ref, dqt_ref, near_send, near_recv, dwq_send, dwq_recv,
                          near_send_sem, near_recv_sem, dwq_send_sem, dwq_recv_sem):
    heads, tokens, hd = q_ref.shape
    half = hd // 2
    bk = own_ref.shape[1]
    rank = lax.axis_index("cp")
    core = rank % 2
    i = pl.program_id(0)
    steps = pl.num_programs(0)

    @pl.when(i == 0)
    def _():
        dqt_ref[...] = dqt_in_ref[...]
        meet_sibling(rank)

    def near_copy(slot):
        return to_sibling(rank, near_send.at[slot], near_recv.at[slot], near_send_sem.at[slot], near_recv_sem.at[slot])

    @pl.when(core == 1)
    def _():
        k, v = near_ref[0], near_ref[1]
        kt = k.T
        mine = near_send.at[i]
        mine[...] = jnp.zeros_like(mine)

        def step(j, _):
            backward_tile(q_ref, do_ref, stat_ref, dqt_ref, mine, k, v, kt, j * 512, 512, False)
            return 0

        lax.fori_loop(0, tokens // 512, step, 0)
        near_copy(i).start()

    own_rows = pl.ds(pl.multiple_of(i * bk, bk), bk)
    down = down_ref.at[:, own_rows, :]
    down[...] = jnp.zeros_like(down)
    k, v = own_ref[0], own_ref[1]
    kt = k.T
    backward_tile(q_ref, do_ref, stat_ref, dqt_ref, down, k, v, kt, i * bk, bk, True)

    def own_step(j, _):
        backward_tile(q_ref, do_ref, stat_ref, dqt_ref, down, k, v, kt, j * bk, bk, False)
        return 0

    lax.fori_loop(i + 1, steps, own_step, 0)

    @pl.when(i == steps - 1)
    def _():
        scale = QUERY_SCALE ** -0.5
        for h in range(heads):
            dq = dqt_ref[h].T
            first, second = dq[:, :half], dq[:, half:]
            cosine, sine = cos_ref[...], sin_ref[...]
            dq_ref[:, h * hd:h * hd + half] = ((first * cosine + second * sine) * scale).astype(BF16)
            dq_ref[:, h * hd + half:(h + 1) * hd] = ((second * cosine - first * sine) * scale).astype(BF16)
        dim, width = dwq_ref.shape
        bd = dim // 3

        def product(out_ref, which):
            dq = dq_ref[:, pl.ds(pl.multiple_of((core + which) % 2 * width, width), width)]

            def rows_step(r, _):
                rows = pl.ds(pl.multiple_of(r * bd, bd), bd)
                out_ref[rows, :] = dot(at_ref[rows, :], dq)
                return 0

            lax.fori_loop(0, dim // bd, rows_step, 0)

        product(dwq_send, 1)
        copy = to_sibling(rank, dwq_send, dwq_recv, dwq_send_sem, dwq_recv_sem)
        copy.start()
        product(dwq_ref, 0)

        @pl.when(core == 1)
        def _():
            for slot in range(near_send.shape[0]):
                near_copy(slot).wait_send()

        @pl.when(core == 0)
        def _():
            for slot in range(near_recv.shape[0]):
                near_copy(slot).wait_recv()
                down_ref[:, slot * bk:(slot + 1) * bk, :] += near_recv[slot]

        copy.wait()
        dwq_ref[...] += dwq_recv[...]


def backward_local(q, d_out, stat, own, near, dqt, cosine, sine, at):
    heads, tokens, hd = q.shape
    dim = at.shape[0]
    bk = 256
    per = tokens // bk
    width = heads * hd // 2
    kv_spec = stack_spec(2, bk, hd)
    dma = pltpu.SemaphoreType.DMA
    return pl.pallas_call(
        backward_local_kernel,
        grid=(per,),
        in_specs=[
            whole(q.shape),
            whole(d_out.shape),
            whole(stat.shape),
            kv_spec,
            kv_spec,
            whole(dqt.shape),
            whole(cosine.shape),
            whole(sine.shape),
            whole(at.shape),
        ],
        out_specs=[whole((2, tokens, hd)), whole((tokens, heads * hd)), whole((dim, width))],
        out_shape=[
            jax.ShapeDtypeStruct((2, tokens, hd), F32),
            jax.ShapeDtypeStruct((tokens, heads * hd), BF16),
            jax.ShapeDtypeStruct((dim, width), F32),
        ],
        scratch_shapes=[
            pltpu.VMEM((heads, hd, tokens), F32),
            pltpu.VMEM((per, 2, bk, hd), F32),
            pltpu.VMEM((per, 2, bk, hd), F32),
            pltpu.VMEM((dim, width), F32),
            pltpu.VMEM((dim, width), F32),
            dma((per,)),
            dma((per,)),
            dma,
            dma,
        ],
        compiler_params=pltpu.CompilerParams(vmem_limit_bytes=VMEM_LIMIT, collective_id=1, has_side_effects=True),
        cost_estimate=COST,
        name="backward_local",
    )(q, d_out, stat, own, near, dqt, cosine, sine, at)


def tail_kernel(idx_ref, down_ref, dfar_ref, cos_ref, sin_ref, at_ref, dq_ref, wq_ref, wk_ref, wv_ref,
                x_ref, dy_ref, gain_ref, dpost_ref, dx_ref, mine_ref, theirs_ref, dgain_ref):
    _, half = cos_ref.shape
    dim = x_ref.shape[1]
    i = pl.program_id(0)
    dk = down_ref[0] + dfar_ref[0]
    cosine, sine = cos_ref[...], sin_ref[...]
    first, second = dk[:, :half], dk[:, half:]
    dk = jnp.concatenate([first * cosine + second * sine, second * cosine - first * sine], axis=1).astype(BF16)
    dv = (down_ref[1] + dfar_ref[1]).astype(BF16)

    @pl.when(i == 0)
    def _():
        mine_ref[...] = jnp.zeros_like(mine_ref)
        theirs_ref[...] = jnp.zeros_like(theirs_ref)
        dgain_ref[...] = jnp.zeros_like(dgain_ref)

    core = idx_ref[0] % 2
    at = at_ref[...]
    is_core0 = core == 0
    mine = jnp.where(is_core0, dk, dv)
    theirs = jnp.where(is_core0, dv, dk)
    mine_ref[0:dim, :] += dot(at, mine)
    theirs_ref[0:dim, :] += dot(at, theirs)
    da = dot(dq_ref[...], wq_ref[...], NT) + dot(dk, wk_ref[...], NT) + dot(dv, wv_ref[...], NT)
    x = x_ref[...].astype(F32)
    rstd = lax.rsqrt(jnp.mean(x * x, axis=-1, keepdims=True) + NORM_EPS)
    unit = x * rstd
    dgain_ref[...] += jnp.sum(da * unit, axis=0, keepdims=True)
    g = da * (1.0 + gain_ref[...])
    dx = rstd * (g - unit * jnp.mean(g * unit, axis=-1, keepdims=True))
    dx_ref[...] = (dy_ref[...].astype(F32) + dx).astype(BF16)

    @pl.when(i == pl.num_programs(0) - 1)
    def _():
        dpre, dpost = dgain_ref[...], dpost_ref[...]
        for ref, row in ((mine_ref, jnp.where(is_core0, dpre, dpost)), (theirs_ref, jnp.where(is_core0, dpost, dpre))):
            for c in range(dim // 128):
                ref[dim + c // 2:dim + c // 2 + 1, c % 2 * 128:(c % 2 + 1) * 128] = row[:, c * 128:(c + 1) * 128]


def tail(idx, down, dfar, cosine, sine, at, dq, wq, wk, wv, x, dy, gain, dpost):
    tokens, dim = x.shape
    hd = wk.shape[1]
    width = wq.shape[1]
    bt = 256
    kv_spec = stack_spec(2, bt, hd)
    rope_spec = rows_spec(bt, hd // 2)
    rows2 = rows_spec(bt, dim)
    return pl.pallas_call(
        tail_kernel,
        grid=(tokens // bt,),
        in_specs=[
            pl.BlockSpec(memory_space=pltpu.SMEM),
            kv_spec,
            kv_spec,
            rope_spec,
            rope_spec,
            pl.BlockSpec((dim, bt), lambda i: (0, i)),
            rows_spec(bt, width),
            whole(wq.shape),
            whole(wk.shape),
            whole(wv.shape),
            rows2,
            rows2,
            whole((1, dim)),
            whole((1, dim)),
        ],
        out_specs=[rows2, whole((dim + 8, hd)), whole((dim + 8, hd))],
        out_shape=[
            jax.ShapeDtypeStruct((tokens, dim), BF16),
            jax.ShapeDtypeStruct((dim + 8, hd), F32),
            jax.ShapeDtypeStruct((dim + 8, hd), F32),
        ],
        scratch_shapes=[pltpu.VMEM((1, dim), F32)],
        compiler_params=params(),
        cost_estimate=COST,
        name="tail",
    )(idx, down, dfar, cosine, sine, at, dq, wq, wk, wv, x, dy, gain, dpost)


def join_wide_kernel(idx_ref, mine_ref, other_ref, out_ref):
    first = idx_ref[0] % 2 == 0
    rows, _ = mine_ref.shape
    mine, other = mine_ref[...], other_ref[...]
    low, high = jnp.where(first, mine, other), jnp.where(first, other, mine)
    heads = 4
    for h in range(heads):
        src = low if h < heads // 2 else high
        base = (h % (heads // 2)) * 256
        for c in range(2):
            out_ref[pl.ds(c * heads + h, rows, stride=2 * heads), :] = src[:, base + c * 128:base + (c + 1) * 128]


def join_wide(idx, mine, other, heads):
    dim, width = mine.shape
    bd = 128
    spec = rows_spec(bd, width)
    out = pl.pallas_call(
        join_wide_kernel,
        grid=(dim // bd,),
        in_specs=[pl.BlockSpec(memory_space=pltpu.SMEM), spec, spec],
        out_specs=rows_spec(bd * 8, 128),
        out_shape=jax.ShapeDtypeStruct((dim * 8, 128), F32),
        compiler_params=params(),
        cost_estimate=COST,
        name="join_wide",
    )(idx, mine, other)
    return out.reshape(dim, 2, heads, 128).transpose(0, 2, 1, 3).reshape(dim, heads, 256)


def join_pair_kernel(idx_ref, mine_ref, other_ref, first_ref, second_ref, dpre_ref, dpost_ref):
    core0 = idx_ref[0] % 2 == 0
    dim = dpre_ref.shape[1]
    mine, other = mine_ref[...], other_ref[...]
    first, second = jnp.where(core0, mine, other), jnp.where(core0, other, mine)
    for src, out_ref, gain_ref in ((first, first_ref, dpre_ref), (second, second_ref, dpost_ref)):
        for c in range(2):
            out_ref[pl.ds(c, dim, stride=2), :] = src[0:dim, c * 128:(c + 1) * 128]
        for c in range(dim // 128):
            gain_ref[:, c * 128:(c + 1) * 128] = src[dim + c // 2:dim + c // 2 + 1, c % 2 * 128:(c % 2 + 1) * 128]


def join_pair(idx, mine, other):
    dim, width = mine.shape[0] - 8, mine.shape[1]
    outs = pl.pallas_call(
        join_pair_kernel,
        in_specs=[pl.BlockSpec(memory_space=pltpu.SMEM), whole(mine.shape), whole(mine.shape)],
        out_specs=[whole((dim * 2, 128))] * 2 + [whole((1, dim))] * 2,
        out_shape=[jax.ShapeDtypeStruct((dim * 2, 128), F32)] * 2 + [jax.ShapeDtypeStruct((1, dim), F32)] * 2,
        compiler_params=params(),
        cost_estimate=COST,
        name="join_pair",
    )(idx, mine, other)
    return [o.reshape(dim, 1, width) for o in outs[:2]] + [o.reshape(dim) for o in outs[2:]]


def join_rows_kernel(idx_ref, mine_ref, other_ref, out_ref):
    first = idx_ref[0] % 2 == 0
    out_ref[...] = jnp.where(first == (pl.program_id(0) == 0), mine_ref[...], other_ref[...])


def join_rows(idx, mine, other):
    rows, dim = mine.shape
    br = 256
    steps = rows // br
    spec = pl.BlockSpec((br, dim), lambda w, i: (i, 0))
    return pl.pallas_call(
        join_rows_kernel,
        grid=(2, steps),
        in_specs=[pl.BlockSpec(memory_space=pltpu.SMEM), spec, spec],
        out_specs=pl.BlockSpec((br, dim), lambda w, i: (w * steps + i, 0)),
        out_shape=jax.ShapeDtypeStruct((rows * 2, dim), F32),
        compiler_params=params(),
        cost_estimate=COST,
        name="join_rows",
    )(idx, mine, other)


def solution(mesh):
    across = [(0, 2), (2, 0), (1, 3), (3, 1)]
    beside = [(0, 1), (1, 0), (2, 3), (3, 2)]

    def permute(value, pairs):
        return lax.ppermute(value, "cp", pairs)

    def sum_halves(parts):
        theirs = permute(parts[1], beside)
        mine = parts[0] + theirs
        mine = mine + permute(mine, across)
        return mine, permute(mine, beside)

    def local_step(x_in, positions, dy_out, w_query, w_key, w_value, w_out, w_pre, w_post):
        batch, tokens, dim = x_in.shape
        heads, hd = w_query.shape[1], w_query.shape[2]
        half = hd // 2
        idx = lax.axis_index("cp").astype(jnp.int32).reshape(1)
        wq = w_query.reshape(dim, heads * hd)
        wk = w_key.reshape(dim, hd)
        wv = w_value.reshape(dim, hd)
        wo = w_out.reshape(heads * hd, dim)
        x = x_in.reshape(tokens, dim)
        dy = dy_out.reshape(tokens, dim)
        gain_pre = w_pre.reshape(1, dim)
        gain_post = w_post.reshape(1, dim)
        inv_freq = ROPE_BASE ** (jnp.arange(half, dtype=F32) * (-2.0 / hd))
        angles = positions.reshape(tokens, 1).astype(F32) * inv_freq
        cosine, sine = jnp.cos(angles), jnp.sin(angles)

        dy_high = permute(dy, [(2, 0), (3, 1)])
        act_t, q, own, near, far, mid, o, out, lse = forward(x, gain_pre, wk, wv, wq, cosine, sine, heads)
        dy_low = permute(dy, [(0, 2), (1, 3)])
        partner_o = permute(o, across)
        y, d_out, dz, stat, dgain_post = post(o, out, lse, x, dy, wo, gain_post)

        dfar, dqt = backward_far(q, d_out, stat, mid, far)
        dfar_in = permute(dfar, [(2, 0), (3, 1)])
        down, dq, dwq_part = backward_local(q, d_out, stat, own, near, dqt, cosine, sine, act_t)
        dwq_mine = dwq_part + permute(dwq_part, across)
        dwq_other = permute(dwq_mine, beside)
        dwo = grad_wo(idx, o, dz, partner_o, dy_high, dy_low, wo, gain_post)
        dwo_mine = dwo[0] + permute(dwo[1], beside)
        dwo_other = permute(dwo_mine, beside)
        dx, *dwkv = tail(idx, down, dfar_in, cosine, sine, act_t, dq, wq, wk, wv, x, dy, gain_pre, dgain_post)
        dwkv_mine, dwkv_other = sum_halves(dwkv)

        dwo_full = join_rows(idx, dwo_mine, dwo_other)
        dwq_full = join_wide(idx, dwq_mine, dwq_other, heads)
        dwk_full, dwv_full, dpre_full, dpost_full = join_pair(idx, dwkv_mine, dwkv_other)
        return (
            y.reshape(batch, tokens, dim),
            dx.reshape(batch, tokens, dim),
            dwq_full,
            dwk_full,
            dwv_full,
            dwo_full.reshape(heads, hd, dim),
            dpre_full,
            dpost_full,
        )

    seq_spec = P("dp", "cp", None)
    in_specs = (seq_spec, P("dp", "cp"), seq_spec, P(), P(), P(), P(), P(), P())
    out_specs = (seq_spec, seq_spec, P("dp", None, None), P("dp", None, None), P("dp", None, None), P("dp", None, None), P("dp"), P("dp"))
    return jax.shard_map(local_step, mesh=mesh, in_specs=in_specs, out_specs=out_specs, check_vma=False)
```

```python
import math

import jax
import jax.numpy as jnp
from jax import lax
from jax.experimental import pallas as pl
from jax.experimental.pallas import tpu as pltpu
from jax.sharding import PartitionSpec as P


NORM_EPS = 1e-6
SOFT_CAP = 50.0
QUERY_SCALE = 144.0
ROPE_BASE = 10000.0
LOG2E = math.log2(math.e)
CAP2 = SOFT_CAP * LOG2E
INV_CAP = 1.0 / SOFT_CAP


F32 = jnp.float32
BF16 = jnp.bfloat16
VMEM_LIMIT = 60 * 1024 * 1024

NT = (((1,), (1,)), ((), ()))
NN = (((1,), (0,)), ((), ()))


def dot(a, b, dims=NN):
    return lax.dot_general(a, b, dims, preferred_element_type=F32)


def params():
    return pltpu.CompilerParams(vmem_limit_bytes=VMEM_LIMIT)


def whole(shape):
    zeros = (0,) * len(shape)
    return pl.BlockSpec(shape, lambda *_: zeros)


def rows_spec(rows, width):
    return pl.BlockSpec((rows, width), lambda i: (i, 0))


def stack_spec(depth, rows, width):
    return pl.BlockSpec((depth, rows, width), lambda i: (0, i, 0))


COST = pl.CostEstimate(flops=10**10, bytes_accessed=10**7, transcendentals=0)


def to_sibling(rank, src, dst, send, recv):
    return pltpu.make_async_remote_copy(
        src_ref=src, dst_ref=dst, send_sem=send, recv_sem=recv,
        device_id={"cp": rank + 1 - 2 * (rank % 2)}, device_id_type=pl.DeviceIdType.MESH,
    )


def rope(values, cosine, sine):
    half = cosine.shape[-1]
    first, second = values[:, :half], values[:, half:]
    return jnp.concatenate([first * cosine - second * sine, second * cosine + first * sine], axis=-1)


def forward_tile(q_ref, acc_ref, sum_ref, k, v, masked):
    heads, bq, _ = q_ref.shape
    bk = k.shape[0]
    if masked:
        keep = lax.broadcasted_iota(jnp.int32, (bq, bk), 1) <= lax.broadcasted_iota(jnp.int32, (bq, bk), 0)
    for h in range(heads):
        s = dot(q_ref[h], k, NT)
        p = jnp.exp2(jnp.tanh(s * INV_CAP) * CAP2)
        if masked:
            p = jnp.where(keep, p, 0.0)
        part = p[:, 0:128]
        for c in range(128, bk, 128):
            part = part + p[:, c:c + 128]
        sum_ref[h] += part
        acc_ref[h] += dot(p.astype(BF16), v)


def forward_kernel(x_ref, gain_ref, wk_ref, wv_ref, wq_ref, cos_ref, sin_ref,
                   at_ref, q_ref, own_ref, near_ref, far_ref, mid_ref, o_ref, out_ref, lse_ref,
                   a_s, own_s, near_s, far_s, mid_s, acc_s, sum_s,
                   far_send, far_recv, near_send, near_recv, mid_send, mid_recv):
    heads, tokens, hd = q_ref.shape
    bt = x_ref.shape[0]
    tiles = tokens // bt
    big = 2 * bt
    rank = lax.axis_index("cp")
    core = rank % 2
    i = pl.program_id(0)
    across = {"cp": (rank + 2) % 4}
    mesh_id = pl.DeviceIdType.MESH

    def rows_of(t, size=bt):
        return pl.ds(pl.multiple_of(t * size, size), size)

    def far_copy(t):
        rows = rows_of(t)
        return pltpu.make_async_remote_copy(
            src_ref=own_s.at[:, rows, :], dst_ref=far_s.at[:, rows, :], send_sem=far_send.at[t], recv_sem=far_recv.at[t],
            device_id=across, device_id_type=mesh_id,
        )

    def near_copy(t):
        rows = rows_of(t)
        return to_sibling(rank, own_s.at[:, rows, :], near_s.at[:, rows, :], near_send.at[t], near_recv.at[t])

    def mid_copy(c):
        rows = rows_of(c, big)
        return to_sibling(rank, far_s.at[:, rows, :], mid_s.at[:, rows, :], mid_send.at[c], mid_recv.at[c])

    @pl.when(i == 0)
    def _():
        barrier = pltpu.get_barrier_semaphore()
        for other in (across, {"cp": rank + 1 - 2 * core}):
            pl.semaphore_signal(barrier, inc=1, device_id=other, device_id_type=mesh_id)
        pl.semaphore_wait(barrier, 2)

    @pl.when(i < tiles)
    def _():
        rows = rows_of(i)
        x = x_ref[...].astype(F32)
        rstd = lax.rsqrt(jnp.mean(x * x, axis=-1, keepdims=True) + NORM_EPS)
        a = (x * rstd * (1.0 + gain_ref[...][None, :])).astype(BF16)
        a_s[rows, :] = a
        own_s[0, rows, :] = rope(dot(a, wk_ref[...]).astype(BF16).astype(F32), cos_ref[rows, :], sin_ref[rows, :]).astype(BF16)
        own_s[1, rows, :] = dot(a, wv_ref[...]).astype(BF16)
        pl.when(rank < 2)(lambda: far_copy(i).start())
        pl.when(core == 0)(lambda: near_copy(i).start())
        at_ref[...] = a.T

    def attend(t, kv_ref, start, size, masked):
        rows, keys = rows_of(t), pl.ds(pl.multiple_of(start, bt), size)
        forward_tile(q_ref.at[:, rows, :], acc_s.at[:, rows, :], sum_s.at[:, rows, :],
                     kv_ref[0, keys, :], kv_ref[1, keys, :], masked)

    @pl.when(jnp.logical_and(i >= tiles, i < 2 * tiles))
    def _():
        t = i - tiles
        rows = rows_of(t)
        a = a_s[rows, :]
        scale = QUERY_SCALE ** -0.5
        for h in range(heads):
            q = dot(a, wq_ref[:, h * hd:(h + 1) * hd]).astype(BF16).astype(F32)
            q_ref[h, rows, :] = (rope(q, cos_ref[rows, :], sin_ref[rows, :]) * scale).astype(BF16)
        acc_s[:, rows, :] = jnp.zeros((heads, bt, hd), F32)
        sum_s[:, rows, :] = jnp.zeros((heads, bt, 128), F32)
        attend(t, own_s, t * bt, bt, True)

        def own_step(j, _):
            attend(t, own_s, j * bt, bt, False)
            return 0

        lax.fori_loop(0, t, own_step, 0)

        @pl.when(core == 1)
        def _():
            pl.when(t == 0)(lambda: [near_copy(n).wait_recv() for n in range(tiles)] and None)

            def near_step(j, _):
                attend(t, near_s, j * big, big, False)
                return 0

            lax.fori_loop(0, tokens // big, near_step, 0)

    chunks = tokens // big
    c = i - 2 * tiles

    def far_chunk(kv_ref, start):
        def step(t, _):
            attend(t, kv_ref, start, big, False)
            return 0

        lax.fori_loop(0, tiles, step, 0)

    @pl.when(jnp.logical_and(rank >= 2, jnp.logical_and(c >= 0, c < chunks)))
    def _():
        far_copy(2 * c).wait_recv()
        far_copy(2 * c + 1).wait_recv()
        mid_copy(c).start()
        far_chunk(far_s, c * big)

    @pl.when(jnp.logical_and(rank >= 2, jnp.logical_and(c >= chunks, c < 2 * chunks)))
    def _():
        mid_copy(c - chunks).wait_recv()
        far_chunk(mid_s, (c - chunks) * big)

    last = i - 2 * tiles - 2 * chunks

    @pl.when(last >= 0)
    def _():
        rows = rows_of(last)
        lane = lax.broadcasted_iota(jnp.int32, (bt, 128), 1)
        lse = jnp.zeros((bt, 128), F32)
        for h in range(heads):
            total = jnp.sum(sum_s[h, rows, :], axis=-1, keepdims=True)
            lse = jnp.where(lane == h, jnp.log2(total), lse)
            out = acc_s[h, rows, :] / total
            out_ref[h] = out
            o_ref[:, h * hd:(h + 1) * hd] = out.astype(BF16)
        lse_ref[...] = lse
        for dst, src in ((own_ref, own_s), (near_ref, near_s), (far_ref, far_s), (mid_ref, mid_s)):
            dst[...] = src[:, rows, :]

    @pl.when(last == tiles - 1)
    def _():
        pl.when(rank < 2)(lambda: [far_copy(n).wait_send() for n in range(tiles)] and None)
        pl.when(core == 0)(lambda: [near_copy(n).wait_send() for n in range(tiles)] and None)
        pl.when(rank >= 2)(lambda: [mid_copy(n).wait_send() for n in range(chunks)] and None)


def forward(x, gain, wk, wv, wq, cosine, sine, heads):
    tokens, dim = x.shape
    hd = wk.shape[1]
    bt = 256
    tiles = tokens // bt
    chunks = tiles // 2
    done = 2 * tiles + 2 * chunks
    dma = pltpu.SemaphoreType.DMA
    early = lambda i: jnp.minimum(i, tiles - 1)
    late = lambda i: jnp.maximum(i - done, 0)
    kv_shape = jax.ShapeDtypeStruct((2, tokens, hd), BF16)
    kv_out = pl.BlockSpec((2, bt, hd), lambda i: (0, late(i), 0))
    return pl.pallas_call(
        forward_kernel,
        grid=(done + tiles,),
        in_specs=[
            pl.BlockSpec((bt, dim), lambda i: (early(i), 0)),
            whole(gain.shape),
            whole(wk.shape),
            whole(wv.shape),
            whole(wq.shape),
            whole(cosine.shape),
            whole(sine.shape),
        ],
        out_specs=[
            pl.BlockSpec((dim, bt), lambda i: (0, early(i))),
            whole((heads, tokens, hd)),
            kv_out,
            kv_out,
            kv_out,
            kv_out,
            pl.BlockSpec((bt, heads * hd), lambda i: (late(i), 0)),
            pl.BlockSpec((heads, bt, hd), lambda i: (0, late(i), 0)),
            pl.BlockSpec((bt, 128), lambda i: (late(i), 0)),
        ],
        out_shape=[
            jax.ShapeDtypeStruct((dim, tokens), BF16),
            jax.ShapeDtypeStruct((heads, tokens, hd), BF16),
            kv_shape,
            kv_shape,
            kv_shape,
            kv_shape,
            jax.ShapeDtypeStruct((tokens, heads * hd), BF16),
            jax.ShapeDtypeStruct((heads, tokens, hd), F32),
            jax.ShapeDtypeStruct((tokens, 128), F32),
        ],
        scratch_shapes=[pltpu.VMEM((tokens, dim), BF16)] + [pltpu.VMEM((2, tokens, hd), BF16)] * 4 + [
            pltpu.VMEM((heads, tokens, hd), F32),
            pltpu.VMEM((heads, tokens, 128), F32),
            dma((tiles,)),
            dma((tiles,)),
            dma((tiles,)),
            dma((tiles,)),
            dma((chunks,)),
            dma((chunks,)),
        ],
        compiler_params=pltpu.CompilerParams(vmem_limit_bytes=VMEM_LIMIT, collective_id=2, has_side_effects=True),
        cost_estimate=COST,
        name="forward",
    )(x, gain, wk, wv, wq, cosine, sine)


def post_norm(o, wo, gain, dy):
    z = dot(o, wo).astype(BF16).astype(F32)
    rstd = lax.rsqrt(jnp.mean(z * z, axis=-1, keepdims=True) + NORM_EPS)
    unit = z * rstd
    g = dy * gain
    dz = (rstd * (g - unit * jnp.mean(g * unit, axis=-1, keepdims=True))).astype(BF16)
    return unit, dz


def post_kernel(o_ref, out_ref, lse_ref, x_ref, dy_ref, wo_ref, gain_ref, y_ref, do_ref, dz_ref, stat_ref, dgain_ref):
    heads, bq, hd = out_ref.shape
    gain = 1.0 + gain_ref[...][None, :]
    dy = dy_ref[...].astype(F32)
    unit, dz = post_norm(o_ref[...], wo_ref[...], gain, dy)
    y_ref[...] = (x_ref[...].astype(F32) + (unit * gain).astype(BF16).astype(F32)).astype(BF16)
    dz_ref[...] = dz

    @pl.when(pl.program_id(0) == 0)
    def _():
        dgain_ref[...] = jnp.zeros_like(dgain_ref)

    dgain_ref[...] += jnp.sum(dy * unit, axis=0, keepdims=True)
    lane = lax.broadcasted_iota(jnp.int32, (bq, 128), 1)
    stat = lse_ref[...]
    for h in range(heads):
        d_out = dot(dz, wo_ref[h * hd:(h + 1) * hd, :], NT).astype(BF16)
        do_ref[h] = d_out
        delta = jnp.sum(d_out.astype(F32) * out_ref[h], axis=-1, keepdims=True)
        stat = jnp.where(lane == heads + h, delta, stat)
    stat_ref[...] = stat.T[0:8, :]


def post(o, out, lse, x, dy, wo, gain):
    heads, tokens, hd = out.shape
    dim = x.shape[1]
    bq = 256
    rows3 = stack_spec(heads, bq, hd)
    rows2 = lambda width: rows_spec(bq, width)
    return pl.pallas_call(
        post_kernel,
        grid=(tokens // bq,),
        in_specs=[rows2(heads * hd), rows3, rows2(128), rows2(dim), rows2(dim), whole(wo.shape), whole((dim,))],
        out_specs=[rows2(dim), rows3, rows2(dim), pl.BlockSpec((8, bq), lambda i: (0, i)), whole((1, dim))],
        out_shape=[
            jax.ShapeDtypeStruct((tokens, dim), BF16),
            jax.ShapeDtypeStruct((heads, tokens, hd), BF16),
            jax.ShapeDtypeStruct((tokens, dim), BF16),
            jax.ShapeDtypeStruct((8, tokens), F32),
            jax.ShapeDtypeStruct((1, dim), F32),
        ],
        compiler_params=params(),
        cost_estimate=COST,
        name="post",
    )(o, out, lse, x, dy, wo, gain)


def grad_wo_kernel(idx_ref, o_ref, dz_ref, po_ref, pdy_low_ref, pdy_high_ref, wo_ref, gain_ref, mine_ref, theirs_ref, pdz_ref):
    _, width = o_ref.shape
    bt = pdy_low_ref.shape[0]
    hd = 256
    i = pl.program_id(0)
    rows = pl.ds(pl.multiple_of(i * bt, bt), bt)
    dy = jnp.where(idx_ref[0] >= 2, pdy_high_ref[...], pdy_low_ref[...]).astype(F32)
    pdz_ref[rows, :] = post_norm(po_ref[rows, :], wo_ref[...], 1.0 + gain_ref[...][None, :], dy)[1]

    @pl.when(i == pl.num_programs(0) - 1)
    def _():
        core = idx_ref[0] % 2
        per = width // hd // 2
        for which, ref in enumerate((mine_ref, theirs_ref)):
            for hh in range(per):
                cols = pl.ds(pl.multiple_of((((core + which) % 2) * per + hh) * hd, hd), hd)
                ref[hh * hd:(hh + 1) * hd, :] = dot(o_ref[:, cols].T, dz_ref[...]) + dot(po_ref[:, cols].T, pdz_ref[...])


def grad_wo(idx, o, dz, po, pdy_low, pdy_high, wo, gain):
    tokens, width = o.shape
    dim = dz.shape[1]
    bt = 256
    rows2 = rows_spec(bt, dim)
    return pl.pallas_call(
        grad_wo_kernel,
        grid=(tokens // bt,),
        in_specs=[
            pl.BlockSpec(memory_space=pltpu.SMEM),
            whole(o.shape),
            whole(dz.shape),
            whole(o.shape),
            rows2,
            rows2,
            whole(wo.shape),
            whole((dim,)),
        ],
        out_specs=[whole((width // 2, dim))] * 2,
        out_shape=[jax.ShapeDtypeStruct((width // 2, dim), F32)] * 2,
        scratch_shapes=[pltpu.VMEM((tokens, dim), BF16)],
        compiler_params=params(),
        cost_estimate=COST,
        name="grad_wo",
    )(idx, o, dz, po, pdy_low, pdy_high, wo, gain)


def backward_tile(q_ref, do_ref, stat_ref, dqt_ref, dkv_ref, k, v, kt, start, bq, masked):
    heads = q_ref.shape[0]
    bk = k.shape[0]
    rows = pl.ds(pl.multiple_of(start, 128), bq)
    if masked:
        keep = lax.broadcasted_iota(jnp.int32, (bk, bq), 0) <= lax.broadcasted_iota(jnp.int32, (bk, bq), 1)
    for h in range(heads):
        q = q_ref[h, rows, :]
        d_out = do_ref[h, rows, :]
        t = jnp.tanh(dot(k, q, NT) * INV_CAP)
        p = jnp.exp2(t * CAP2 - stat_ref[h:h + 1, rows])
        if masked:
            p = jnp.where(keep, p, 0.0)
        dp = dot(v, d_out, NT)
        ds = (p * (dp - stat_ref[heads + h:heads + h + 1, rows]) * (1.0 - t * t)).astype(BF16)
        dkv_ref[1] += dot(p.astype(BF16), d_out)
        dkv_ref[0] += dot(ds, q)
        dqt_ref[h, :, rows] += dot(kt, ds)


def backward_kernel(q_ref, do_ref, stat_ref, own_ref, near_ref, far_ref, mid_ref, cos_ref, sin_ref, at_ref,
                    down_ref, dq_ref, dwq_ref,
                    dqt_s, near_out, near_in, mid_out, mid_in, far_out, far_in, dwq_out, dwq_in,
                    near_send, near_recv, mid_send, mid_recv, far_send, far_recv, dwq_send, dwq_recv):
    heads, tokens, hd = q_ref.shape
    half = hd // 2
    bk = own_ref.shape[1]
    big = 2 * bk
    tiles = tokens // bk
    rank = lax.axis_index("cp")
    core = rank % 2
    i = pl.program_id(0)
    across = {"cp": (rank + 2) % 4}
    mesh_id = pl.DeviceIdType.MESH

    def near_copy(n):
        return to_sibling(rank, near_out.at[n], near_in.at[n], near_send.at[n], near_recv.at[n])

    def mid_copy(n):
        return to_sibling(rank, mid_out.at[n], mid_in.at[n], mid_send.at[n], mid_recv.at[n])

    def far_copy(n):
        return pltpu.make_async_remote_copy(
            src_ref=far_out.at[n], dst_ref=far_in.at[n], send_sem=far_send.at[n], recv_sem=far_recv.at[n],
            device_id=across, device_id_type=mesh_id,
        )

    @pl.when(i == 0)
    def _():
        dqt_s[...] = jnp.zeros_like(dqt_s)
        barrier = pltpu.get_barrier_semaphore()
        for other in (across, {"cp": rank + 1 - 2 * core}):
            pl.semaphore_signal(barrier, inc=1, device_id=other, device_id_type=mesh_id)
        pl.semaphore_wait(barrier, 2)

    def all_rows(kv_ref, dkv_ref):
        k, v = kv_ref[0], kv_ref[1]
        kt = k.T

        def step(j, _):
            backward_tile(q_ref, do_ref, stat_ref, dqt_s, dkv_ref, k, v, kt, j * big, big, False)
            return 0

        lax.fori_loop(0, tokens // big, step, 0)

    @pl.when(jnp.logical_and(rank >= 2, i < tiles))
    def _():
        mine = mid_out.at[i]
        mine[...] = jnp.zeros_like(mine)
        all_rows(mid_ref, mine)
        mid_copy(i).start()

    @pl.when(jnp.logical_and(rank >= 2, jnp.logical_and(i >= tiles, i < 2 * tiles)))
    def _():
        n = i - tiles
        mid_copy(n).wait()
        mine = far_out.at[n]
        mine[...] = mid_in[n]
        all_rows(far_ref, mine)
        far_copy(n).start()

    n = i - 2 * tiles

    @pl.when(jnp.logical_and(core == 1, n >= 0))
    def _():
        mine = near_out.at[n]
        mine[...] = jnp.zeros_like(mine)
        all_rows(near_ref, mine)
        near_copy(n).start()

    @pl.when(n >= 0)
    def _():
        down = down_ref.at[:, pl.ds(pl.multiple_of(n * bk, bk), bk), :]
        down[...] = jnp.zeros_like(down)
        k, v = own_ref[0], own_ref[1]
        kt = k.T
        backward_tile(q_ref, do_ref, stat_ref, dqt_s, down, k, v, kt, n * bk, bk, True)

        def own_step(j, _):
            backward_tile(q_ref, do_ref, stat_ref, dqt_s, down, k, v, kt, j * bk, bk, False)
            return 0

        lax.fori_loop(n + 1, tiles, own_step, 0)

    @pl.when(n == tiles - 1)
    def _():
        scale = QUERY_SCALE ** -0.5
        for h in range(heads):
            dq = dqt_s[h].T
            first, second = dq[:, :half], dq[:, half:]
            cosine, sine = cos_ref[...], sin_ref[...]
            dq_ref[:, h * hd:h * hd + half] = ((first * cosine + second * sine) * scale).astype(BF16)
            dq_ref[:, h * hd + half:(h + 1) * hd] = ((second * cosine - first * sine) * scale).astype(BF16)
        dim, width = dwq_ref.shape
        bd = dim // 3

        def product(out_ref, which):
            dq = dq_ref[:, pl.ds(pl.multiple_of((core + which) % 2 * width, width), width)]

            def rows_step(r, _):
                rows = pl.ds(pl.multiple_of(r * bd, bd), bd)
                out_ref[rows, :] = dot(at_ref[rows, :], dq)
                return 0

            lax.fori_loop(0, dim // bd, rows_step, 0)

        product(dwq_out, 1)
        copy = to_sibling(rank, dwq_out, dwq_in, dwq_send, dwq_recv)
        copy.start()
        product(dwq_ref, 0)

        def gather(copy_of, arrived):
            for t in range(tiles):
                copy_of(t).wait_recv()
                down_ref[:, t * bk:(t + 1) * bk, :] += arrived[t]

        def left(copy_of):
            for t in range(tiles):
                copy_of(t).wait_send()

        pl.when(core == 1)(lambda: left(near_copy))
        pl.when(core == 0)(lambda: gather(near_copy, near_in))
        copy.wait()
        dwq_ref[...] += dwq_in[...]
        pl.when(rank < 2)(lambda: gather(far_copy, far_in))
        pl.when(rank >= 2)(lambda: left(far_copy))


def backward(q, d_out, stat, own, near, far, mid, cosine, sine, at):
    heads, tokens, hd = q.shape
    dim = at.shape[0]
    bk = 256
    tiles = tokens // bk
    width = heads * hd // 2

    def phase(first):
        return pl.BlockSpec((2, bk, hd), lambda i: (0, jnp.clip(i - first, 0, tiles - 1), 0))

    def held(array):
        zeros = (0,) * array.ndim
        return pl.BlockSpec(array.shape, lambda i: zeros, pipeline_mode=pl.Buffered(1))

    dma = pltpu.SemaphoreType.DMA
    return pl.pallas_call(
        backward_kernel,
        grid=(3 * tiles,),
        in_specs=[
            held(q),
            held(d_out),
            held(stat),
            phase(2 * tiles),
            phase(2 * tiles),
            phase(tiles),
            phase(0),
            held(cosine),
            held(sine),
            held(at),
        ],
        out_specs=[whole((2, tokens, hd)), whole((tokens, heads * hd)), whole((dim, width))],
        out_shape=[
            jax.ShapeDtypeStruct((2, tokens, hd), F32),
            jax.ShapeDtypeStruct((tokens, heads * hd), BF16),
            jax.ShapeDtypeStruct((dim, width), F32),
        ],
        scratch_shapes=[pltpu.VMEM((heads, hd, tokens), F32)] + [pltpu.VMEM((tiles, 2, bk, hd), F32)] * 6
        + [pltpu.VMEM((dim, width), F32)] * 2 + [dma((tiles,))] * 6 + [dma] * 2,
        compiler_params=pltpu.CompilerParams(vmem_limit_bytes=VMEM_LIMIT, collective_id=0, has_side_effects=True),
        cost_estimate=COST,
        name="backward",
    )(q, d_out, stat, own, near, far, mid, cosine, sine, at)


def tail_kernel(idx_ref, down_ref, cos_ref, sin_ref, at_ref, dq_ref, wq_ref, wk_ref, wv_ref,
                x_ref, dy_ref, gain_ref, dpost_ref, dx_ref, mine_ref, theirs_ref, dgain_ref):
    _, half = cos_ref.shape
    dim = x_ref.shape[1]
    i = pl.program_id(0)
    dk = down_ref[0]
    cosine, sine = cos_ref[...], sin_ref[...]
    first, second = dk[:, :half], dk[:, half:]
    dk = jnp.concatenate([first * cosine + second * sine, second * cosine - first * sine], axis=1).astype(BF16)
    dv = down_ref[1].astype(BF16)

    @pl.when(i == 0)
    def _():
        mine_ref[...] = jnp.zeros_like(mine_ref)
        theirs_ref[...] = jnp.zeros_like(theirs_ref)
        dgain_ref[...] = jnp.zeros_like(dgain_ref)

    core = idx_ref[0] % 2
    at = at_ref[...]
    is_core0 = core == 0
    mine = jnp.where(is_core0, dk, dv)
    theirs = jnp.where(is_core0, dv, dk)
    mine_ref[0:dim, :] += dot(at, mine)
    theirs_ref[0:dim, :] += dot(at, theirs)
    da = dot(dq_ref[...], wq_ref[...], NT) + dot(dk, wk_ref[...], NT) + dot(dv, wv_ref[...], NT)
    x = x_ref[...].astype(F32)
    rstd = lax.rsqrt(jnp.mean(x * x, axis=-1, keepdims=True) + NORM_EPS)
    unit = x * rstd
    dgain_ref[...] += jnp.sum(da * unit, axis=0, keepdims=True)
    g = da * (1.0 + gain_ref[...][None, :])
    dx = rstd * (g - unit * jnp.mean(g * unit, axis=-1, keepdims=True))
    dx_ref[...] = (dy_ref[...].astype(F32) + dx).astype(BF16)

    @pl.when(i == pl.num_programs(0) - 1)
    def _():
        dpre, dpost = dgain_ref[...], dpost_ref[...]
        for ref, row in ((mine_ref, jnp.where(is_core0, dpre, dpost)), (theirs_ref, jnp.where(is_core0, dpost, dpre))):
            for c in range(dim // 128):
                ref[dim + c // 2:dim + c // 2 + 1, c % 2 * 128:(c % 2 + 1) * 128] = row[:, c * 128:(c + 1) * 128]


def tail(idx, down, cosine, sine, at, dq, wq, wk, wv, x, dy, gain, dpost):
    tokens, dim = x.shape
    hd = wk.shape[1]
    width = wq.shape[1]
    bt = 256
    kv_spec = stack_spec(2, bt, hd)
    rope_spec = rows_spec(bt, hd // 2)
    rows2 = rows_spec(bt, dim)
    return pl.pallas_call(
        tail_kernel,
        grid=(tokens // bt,),
        in_specs=[
            pl.BlockSpec(memory_space=pltpu.SMEM),
            kv_spec,
            rope_spec,
            rope_spec,
            pl.BlockSpec((dim, bt), lambda i: (0, i)),
            rows_spec(bt, width),
            whole(wq.shape),
            whole(wk.shape),
            whole(wv.shape),
            rows2,
            rows2,
            whole((dim,)),
            whole((1, dim)),
        ],
        out_specs=[rows2, whole((dim + 8, hd)), whole((dim + 8, hd))],
        out_shape=[
            jax.ShapeDtypeStruct((tokens, dim), BF16),
            jax.ShapeDtypeStruct((dim + 8, hd), F32),
            jax.ShapeDtypeStruct((dim + 8, hd), F32),
        ],
        scratch_shapes=[pltpu.VMEM((1, dim), F32)],
        compiler_params=params(),
        cost_estimate=COST,
        name="tail",
    )(idx, down, cosine, sine, at, dq, wq, wk, wv, x, dy, gain, dpost)


def join_wide_kernel(idx_ref, mine_ref, other_ref, out_ref):
    first = idx_ref[0] % 2 == 0
    rows, _ = mine_ref.shape
    mine, other = mine_ref[...], other_ref[...]
    low, high = jnp.where(first, mine, other), jnp.where(first, other, mine)
    heads = 4
    for h in range(heads):
        src = low if h < heads // 2 else high
        base = (h % (heads // 2)) * 256
        for c in range(2):
            out_ref[pl.ds(c * heads + h, rows, stride=2 * heads), :] = src[:, base + c * 128:base + (c + 1) * 128]


def join_wide(idx, mine, other, heads):
    dim, width = mine.shape
    bd = 128
    spec = rows_spec(bd, width)
    out = pl.pallas_call(
        join_wide_kernel,
        grid=(dim // bd,),
        in_specs=[pl.BlockSpec(memory_space=pltpu.SMEM), spec, spec],
        out_specs=rows_spec(bd * 8, 128),
        out_shape=jax.ShapeDtypeStruct((dim * 8, 128), F32),
        compiler_params=params(),
        cost_estimate=COST,
        name="join_wide",
    )(idx, mine, other)
    return out.reshape(dim, 2, heads, 128).transpose(0, 2, 1, 3).reshape(dim, heads, 256)


def join_pair_kernel(idx_ref, mine_ref, other_ref, first_ref, second_ref, dpre_ref, dpost_ref):
    core0 = idx_ref[0] % 2 == 0
    dim = dpre_ref.shape[0]
    mine, other = mine_ref[...], other_ref[...]
    first, second = jnp.where(core0, mine, other), jnp.where(core0, other, mine)
    for src, out_ref, gain_ref in ((first, first_ref, dpre_ref), (second, second_ref, dpost_ref)):
        for c in range(2):
            out_ref[pl.ds(c, dim, stride=2), :] = src[0:dim, c * 128:(c + 1) * 128]
        for c in range(dim // 128):
            gain_ref[c * 128:(c + 1) * 128] = src[dim + c // 2, c % 2 * 128:(c % 2 + 1) * 128]


def join_pair(idx, mine, other):
    dim, width = mine.shape[0] - 8, mine.shape[1]
    outs = pl.pallas_call(
        join_pair_kernel,
        in_specs=[pl.BlockSpec(memory_space=pltpu.SMEM), whole(mine.shape), whole(mine.shape)],
        out_specs=[whole((dim * 2, 128))] * 2 + [whole((dim,))] * 2,
        out_shape=[jax.ShapeDtypeStruct((dim * 2, 128), F32)] * 2 + [jax.ShapeDtypeStruct((dim,), F32)] * 2,
        compiler_params=params(),
        cost_estimate=COST,
        name="join_pair",
    )(idx, mine, other)
    return [o.reshape(dim, 1, width) for o in outs[:2]] + list(outs[2:])


def join_rows_kernel(idx_ref, mine_ref, other_ref, out_ref):
    first = idx_ref[0] % 2 == 0
    out_ref[...] = jnp.where(first == (pl.program_id(0) == 0), mine_ref[...], other_ref[...])


def join_rows(idx, mine, other):
    rows, dim = mine.shape
    br = 256
    steps = rows // br
    spec = pl.BlockSpec((br, dim), lambda w, i: (i, 0))
    return pl.pallas_call(
        join_rows_kernel,
        grid=(2, steps),
        in_specs=[pl.BlockSpec(memory_space=pltpu.SMEM), spec, spec],
        out_specs=pl.BlockSpec((br, dim), lambda w, i: (w * steps + i, 0)),
        out_shape=jax.ShapeDtypeStruct((rows * 2, dim), F32),
        compiler_params=params(),
        cost_estimate=COST,
        name="join_rows",
    )(idx, mine, other)


def solution(mesh):
    across = [(0, 2), (2, 0), (1, 3), (3, 1)]
    beside = [(0, 1), (1, 0), (2, 3), (3, 2)]

    def permute(value, pairs):
        return lax.ppermute(value, "cp", pairs)

    def sum_halves(parts):
        theirs = permute(parts[1], beside)
        mine = parts[0] + theirs
        mine = mine + permute(mine, across)
        return mine, permute(mine, beside)

    def local_step(x_in, positions, dy_out, w_query, w_key, w_value, w_out, w_pre, w_post):
        batch, tokens, dim = x_in.shape
        heads, hd = w_query.shape[1], w_query.shape[2]
        half = hd // 2
        idx = lax.axis_index("cp").astype(jnp.int32).reshape(1)
        wq = w_query.reshape(dim, heads * hd)
        wk = w_key.reshape(dim, hd)
        wv = w_value.reshape(dim, hd)
        wo = w_out.reshape(heads * hd, dim)
        x = x_in.reshape(tokens, dim)
        dy = dy_out.reshape(tokens, dim)
        gain_pre = w_pre
        gain_post = w_post
        inv_freq = ROPE_BASE ** (jnp.arange(half, dtype=F32) * (-2.0 / hd))
        angles = positions.reshape(tokens, 1).astype(F32) * inv_freq
        cosine, sine = jnp.cos(angles), jnp.sin(angles)

        dy_high = permute(dy, [(2, 0), (3, 1)])
        act_t, q, own, near, far, mid, o, out, lse = forward(x, gain_pre, wk, wv, wq, cosine, sine, heads)
        dy_low = permute(dy, [(0, 2), (1, 3)])
        partner_o = permute(o, across)
        y, d_out, dz, stat, dgain_post = post(o, out, lse, x, dy, wo, gain_post)

        down, dq, dwq_part = backward(q, d_out, stat, own, near, far, mid, cosine, sine, act_t)
        dwq_mine = dwq_part + permute(dwq_part, across)
        dwq_other = permute(dwq_mine, beside)
        dwo = grad_wo(idx, o, dz, partner_o, dy_high, dy_low, wo, gain_post)
        dwo_mine = dwo[0] + permute(dwo[1], beside)
        dwo_other = permute(dwo_mine, beside)
        dx, *dwkv = tail(idx, down, cosine, sine, act_t, dq, wq, wk, wv, x, dy, gain_pre, dgain_post)
        dwkv_mine, dwkv_other = sum_halves(dwkv)

        dwo_full = join_rows(idx, dwo_mine, dwo_other)
        dwq_full = join_wide(idx, dwq_mine, dwq_other, heads)
        dwk_full, dwv_full, dpre_full, dpost_full = join_pair(idx, dwkv_mine, dwkv_other)
        return (
            y.reshape(batch, tokens, dim),
            dx.reshape(batch, tokens, dim),
            dwq_full,
            dwk_full,
            dwv_full,
            dwo_full.reshape(heads, hd, dim),
            dpre_full,
            dpost_full,
        )

    seq_spec = P("dp", "cp", None)
    in_specs = (seq_spec, P("dp", "cp"), seq_spec, P(), P(), P(), P(), P(), P())
    out_specs = (seq_spec, seq_spec, P("dp", None, None), P("dp", None, None), P("dp", None, None), P("dp", None, None), P("dp"), P("dp"))
    return jax.shard_map(local_step, mesh=mesh, in_specs=in_specs, out_specs=out_specs, check_vma=False)
```

```python
import math

import jax
import jax.numpy as jnp
from jax import lax
from jax.experimental import pallas as pl
from jax.experimental.pallas import tpu as pltpu
from jax.sharding import PartitionSpec as P


NORM_EPS = 1e-6
SOFT_CAP = 50.0
QUERY_SCALE = 144.0
ROPE_BASE = 10000.0
LOG2E = math.log2(math.e)
CAP2 = SOFT_CAP * LOG2E
INV_CAP = 1.0 / SOFT_CAP


F32 = jnp.float32
BF16 = jnp.bfloat16
VMEM_LIMIT = 60 * 1024 * 1024

NT = (((1,), (1,)), ((), ()))
NN = (((1,), (0,)), ((), ()))


def dot(a, b, dims=NN):
    return lax.dot_general(a, b, dims, preferred_element_type=F32)


def params():
    return pltpu.CompilerParams(vmem_limit_bytes=VMEM_LIMIT)


def whole(shape):
    zeros = (0,) * len(shape)
    return pl.BlockSpec(shape, lambda *_: zeros)


def rows_spec(rows, width):
    return pl.BlockSpec((rows, width), lambda i: (i, 0))


def stack_spec(depth, rows, width):
    return pl.BlockSpec((depth, rows, width), lambda i: (0, i, 0))


COST = pl.CostEstimate(flops=10**10, bytes_accessed=10**7, transcendentals=0)


def to_sibling(rank, src, dst, send, recv):
    return pltpu.make_async_remote_copy(
        src_ref=src, dst_ref=dst, send_sem=send, recv_sem=recv,
        device_id={"cp": rank + 1 - 2 * (rank % 2)}, device_id_type=pl.DeviceIdType.MESH,
    )


def rope(values, cosine, sine):
    half = cosine.shape[-1]
    first, second = values[:, :half], values[:, half:]
    return jnp.concatenate([first * cosine - second * sine, second * cosine + first * sine], axis=-1)


def forward_tile(q_ref, acc_ref, sum_ref, k, v, masked):
    heads, bq, _ = q_ref.shape
    bk = k.shape[0]
    if masked:
        keep = lax.broadcasted_iota(jnp.int32, (bq, bk), 1) <= lax.broadcasted_iota(jnp.int32, (bq, bk), 0)
    for h in range(heads):
        s = dot(q_ref[h], k, NT)
        p = jnp.exp2(jnp.tanh(s * INV_CAP) * CAP2)
        if masked:
            p = jnp.where(keep, p, 0.0)
        part = p[:, 0:128]
        for c in range(128, bk, 128):
            part = part + p[:, c:c + 128]
        sum_ref[h] += part
        acc_ref[h] += dot(p.astype(BF16), v)


def forward_kernel(x_ref, gain_ref, wk_ref, wv_ref, wq_ref, cos_ref, sin_ref,
                   at_ref, q_ref, own_ref, near_ref, far_ref, mid_ref, o_ref, out_ref, lse_ref,
                   a_s, own_s, near_s, far_s, mid_s, acc_s, sum_s,
                   far_send, far_recv, near_send, near_recv, mid_send, mid_recv):
    heads, tokens, hd = q_ref.shape
    bt = x_ref.shape[0]
    tiles = tokens // bt
    big = 2 * bt
    rank = lax.axis_index("cp")
    core = rank % 2
    i = pl.program_id(0)
    across = {"cp": (rank + 2) % 4}
    mesh_id = pl.DeviceIdType.MESH

    def rows_of(t, size=bt):
        return pl.ds(pl.multiple_of(t * size, size), size)

    def far_copy(t):
        rows = rows_of(t)
        return pltpu.make_async_remote_copy(
            src_ref=own_s.at[:, rows, :], dst_ref=far_s.at[:, rows, :], send_sem=far_send.at[t], recv_sem=far_recv.at[t],
            device_id=across, device_id_type=mesh_id,
        )

    def near_copy(t):
        rows = rows_of(t)
        return to_sibling(rank, own_s.at[:, rows, :], near_s.at[:, rows, :], near_send.at[t], near_recv.at[t])

    def mid_copy(c):
        rows = rows_of(c, big)
        return to_sibling(rank, far_s.at[:, rows, :], mid_s.at[:, rows, :], mid_send.at[c], mid_recv.at[c])

    @pl.when(i == 0)
    def _():
        barrier = pltpu.get_barrier_semaphore()
        for other in (across, {"cp": rank + 1 - 2 * core}):
            pl.semaphore_signal(barrier, inc=1, device_id=other, device_id_type=mesh_id)
        pl.semaphore_wait(barrier, 2)

    @pl.when(i < tiles)
    def _():
        rows = rows_of(i)
        x = x_ref[...].astype(F32)
        rstd = lax.rsqrt(jnp.mean(x * x, axis=-1, keepdims=True) + NORM_EPS)
        a = (x * rstd * (1.0 + gain_ref[...][None, :])).astype(BF16)
        a_s[rows, :] = a
        own_s[0, rows, :] = rope(dot(a, wk_ref[...]).astype(BF16).astype(F32), cos_ref[rows, :], sin_ref[rows, :]).astype(BF16)
        own_s[1, rows, :] = dot(a, wv_ref[...]).astype(BF16)
        pl.when(rank < 2)(lambda: far_copy(i).start())
        pl.when(core == 0)(lambda: near_copy(i).start())
        at_ref[...] = a.T

    def attend(t, kv_ref, start, size, masked):
        rows, keys = rows_of(t), pl.ds(pl.multiple_of(start, bt), size)
        forward_tile(q_ref.at[:, rows, :], acc_s.at[:, rows, :], sum_s.at[:, rows, :],
                     kv_ref[0, keys, :], kv_ref[1, keys, :], masked)

    @pl.when(jnp.logical_and(i >= tiles, i < 2 * tiles))
    def _():
        t = i - tiles
        rows = rows_of(t)
        a = a_s[rows, :]
        scale = QUERY_SCALE ** -0.5
        for h in range(heads):
            q = dot(a, wq_ref[:, h * hd:(h + 1) * hd]).astype(BF16).astype(F32)
            q_ref[h, rows, :] = (rope(q, cos_ref[rows, :], sin_ref[rows, :]) * scale).astype(BF16)
        acc_s[:, rows, :] = jnp.zeros((heads, bt, hd), F32)
        sum_s[:, rows, :] = jnp.zeros((heads, bt, 128), F32)
        attend(t, own_s, t * bt, bt, True)

        def own_step(j, _):
            attend(t, own_s, j * bt, bt, False)
            return 0

        lax.fori_loop(0, t, own_step, 0)

        @pl.when(core == 1)
        def _():
            pl.when(t == 0)(lambda: [near_copy(n).wait_recv() for n in range(tiles)] and None)

            def near_step(j, _):
                attend(t, near_s, j * big, big, False)
                return 0

            lax.fori_loop(0, tokens // big, near_step, 0)

    chunks = tokens // big
    c = i - 2 * tiles

    def far_chunk(kv_ref, start):
        def step(t, _):
            attend(t, kv_ref, start, big, False)
            return 0

        lax.fori_loop(0, tiles, step, 0)

    @pl.when(jnp.logical_and(rank >= 2, jnp.logical_and(c >= 0, c < chunks)))
    def _():
        far_copy(2 * c).wait_recv()
        far_copy(2 * c + 1).wait_recv()
        mid_copy(c).start()
        far_chunk(far_s, c * big)

    @pl.when(jnp.logical_and(rank >= 2, jnp.logical_and(c >= chunks, c < 2 * chunks)))
    def _():
        mid_copy(c - chunks).wait_recv()
        far_chunk(mid_s, (c - chunks) * big)

    last = i - 2 * tiles - 2 * chunks

    @pl.when(last >= 0)
    def _():
        rows = rows_of(last)
        lane = lax.broadcasted_iota(jnp.int32, (bt, 128), 1)
        lse = jnp.zeros((bt, 128), F32)
        for h in range(heads):
            total = jnp.sum(sum_s[h, rows, :], axis=-1, keepdims=True)
            lse = jnp.where(lane == h, jnp.log2(total), lse)
            out = acc_s[h, rows, :] / total
            out_ref[h] = out
            o_ref[:, h * hd:(h + 1) * hd] = out.astype(BF16)
        lse_ref[...] = lse
        for dst, src in ((own_ref, own_s), (near_ref, near_s), (far_ref, far_s), (mid_ref, mid_s)):
            dst[...] = src[:, rows, :]

    @pl.when(last == tiles - 1)
    def _():
        pl.when(rank < 2)(lambda: [far_copy(n).wait_send() for n in range(tiles)] and None)
        pl.when(core == 0)(lambda: [near_copy(n).wait_send() for n in range(tiles)] and None)
        pl.when(rank >= 2)(lambda: [mid_copy(n).wait_send() for n in range(chunks)] and None)


def forward(x, gain, wk, wv, wq, cosine, sine, heads):
    tokens, dim = x.shape
    hd = wk.shape[1]
    bt = 256
    tiles = tokens // bt
    chunks = tiles // 2
    done = 2 * tiles + 2 * chunks
    dma = pltpu.SemaphoreType.DMA
    early = lambda i: jnp.minimum(i, tiles - 1)
    late = lambda i: jnp.maximum(i - done, 0)
    kv_shape = jax.ShapeDtypeStruct((2, tokens, hd), BF16)
    kv_out = pl.BlockSpec((2, bt, hd), lambda i: (0, late(i), 0))
    return pl.pallas_call(
        forward_kernel,
        grid=(done + tiles,),
        in_specs=[
            pl.BlockSpec((bt, dim), lambda i: (early(i), 0)),
            whole(gain.shape),
            whole(wk.shape),
            whole(wv.shape),
            whole(wq.shape),
            whole(cosine.shape),
            whole(sine.shape),
        ],
        out_specs=[
            pl.BlockSpec((dim, bt), lambda i: (0, early(i))),
            whole((heads, tokens, hd)),
            kv_out,
            kv_out,
            kv_out,
            kv_out,
            pl.BlockSpec((bt, heads * hd), lambda i: (late(i), 0)),
            pl.BlockSpec((heads, bt, hd), lambda i: (0, late(i), 0)),
            pl.BlockSpec((bt, 128), lambda i: (late(i), 0)),
        ],
        out_shape=[
            jax.ShapeDtypeStruct((dim, tokens), BF16),
            jax.ShapeDtypeStruct((heads, tokens, hd), BF16),
            kv_shape,
            kv_shape,
            kv_shape,
            kv_shape,
            jax.ShapeDtypeStruct((tokens, heads * hd), BF16),
            jax.ShapeDtypeStruct((heads, tokens, hd), F32),
            jax.ShapeDtypeStruct((tokens, 128), F32),
        ],
        scratch_shapes=[pltpu.VMEM((tokens, dim), BF16)] + [pltpu.VMEM((2, tokens, hd), BF16)] * 4 + [
            pltpu.VMEM((heads, tokens, hd), F32),
            pltpu.VMEM((heads, tokens, 128), F32),
            dma((tiles,)),
            dma((tiles,)),
            dma((tiles,)),
            dma((tiles,)),
            dma((chunks,)),
            dma((chunks,)),
        ],
        compiler_params=pltpu.CompilerParams(vmem_limit_bytes=VMEM_LIMIT, collective_id=2, has_side_effects=True),
        cost_estimate=COST,
        name="forward",
    )(x, gain, wk, wv, wq, cosine, sine)


def post_norm(o, wo, gain, dy):
    z = dot(o, wo).astype(BF16).astype(F32)
    rstd = lax.rsqrt(jnp.mean(z * z, axis=-1, keepdims=True) + NORM_EPS)
    unit = z * rstd
    g = dy * gain
    dz = (rstd * (g - unit * jnp.mean(g * unit, axis=-1, keepdims=True))).astype(BF16)
    return unit, dz


def post_kernel(o_ref, out_ref, lse_ref, x_ref, dy_ref, wo_ref, gain_ref, y_ref, do_ref, dz_ref, stat_ref, dgain_ref):
    heads, bq, hd = out_ref.shape
    gain = 1.0 + gain_ref[...][None, :]
    dy = dy_ref[...].astype(F32)
    unit, dz = post_norm(o_ref[...], wo_ref[...], gain, dy)
    y_ref[...] = (x_ref[...].astype(F32) + (unit * gain).astype(BF16).astype(F32)).astype(BF16)
    dz_ref[...] = dz

    @pl.when(pl.program_id(0) == 0)
    def _():
        dgain_ref[...] = jnp.zeros_like(dgain_ref)

    dgain_ref[...] += jnp.sum(dy * unit, axis=0, keepdims=True)
    lane = lax.broadcasted_iota(jnp.int32, (bq, 128), 1)
    stat = lse_ref[...]
    for h in range(heads):
        d_out = dot(dz, wo_ref[h * hd:(h + 1) * hd, :], NT).astype(BF16)
        do_ref[h] = d_out
        delta = jnp.sum(d_out.astype(F32) * out_ref[h], axis=-1, keepdims=True)
        stat = jnp.where(lane == heads + h, delta, stat)
    stat_ref[...] = stat.T[0:8, :]


def post(o, out, lse, x, dy, wo, gain):
    heads, tokens, hd = out.shape
    dim = x.shape[1]
    bq = 256
    rows3 = stack_spec(heads, bq, hd)
    rows2 = lambda width: rows_spec(bq, width)
    return pl.pallas_call(
        post_kernel,
        grid=(tokens // bq,),
        in_specs=[rows2(heads * hd), rows3, rows2(128), rows2(dim), rows2(dim), whole(wo.shape), whole((dim,))],
        out_specs=[rows2(dim), rows3, rows2(dim), pl.BlockSpec((8, bq), lambda i: (0, i)), whole((1, dim))],
        out_shape=[
            jax.ShapeDtypeStruct((tokens, dim), BF16),
            jax.ShapeDtypeStruct((heads, tokens, hd), BF16),
            jax.ShapeDtypeStruct((tokens, dim), BF16),
            jax.ShapeDtypeStruct((8, tokens), F32),
            jax.ShapeDtypeStruct((1, dim), F32),
        ],
        compiler_params=params(),
        cost_estimate=COST,
        name="post",
    )(o, out, lse, x, dy, wo, gain)


def grad_wo_kernel(idx_ref, o_ref, dz_ref, po_ref, pdy_low_ref, pdy_high_ref, wo_ref, gain_ref, mine_ref, theirs_ref, pdz_ref):
    _, width = o_ref.shape
    bt = pdy_low_ref.shape[0]
    hd = 256
    i = pl.program_id(0)
    rows = pl.ds(pl.multiple_of(i * bt, bt), bt)
    dy = jnp.where(idx_ref[0] >= 2, pdy_high_ref[...], pdy_low_ref[...]).astype(F32)
    pdz_ref[rows, :] = post_norm(po_ref[rows, :], wo_ref[...], 1.0 + gain_ref[...][None, :], dy)[1]

    @pl.when(i == pl.num_programs(0) - 1)
    def _():
        core = idx_ref[0] % 2
        per = width // hd // 2
        for which, ref in enumerate((mine_ref, theirs_ref)):
            for hh in range(per):
                cols = pl.ds(pl.multiple_of((((core + which) % 2) * per + hh) * hd, hd), hd)
                ref[hh * hd:(hh + 1) * hd, :] = dot(o_ref[:, cols].T, dz_ref[...]) + dot(po_ref[:, cols].T, pdz_ref[...])


def grad_wo(idx, o, dz, po, pdy_low, pdy_high, wo, gain):
    tokens, width = o.shape
    dim = dz.shape[1]
    bt = 256
    rows2 = rows_spec(bt, dim)
    return pl.pallas_call(
        grad_wo_kernel,
        grid=(tokens // bt,),
        in_specs=[
            pl.BlockSpec(memory_space=pltpu.SMEM),
            whole(o.shape),
            whole(dz.shape),
            whole(o.shape),
            rows2,
            rows2,
            whole(wo.shape),
            whole((dim,)),
        ],
        out_specs=[whole((width // 2, dim))] * 2,
        out_shape=[jax.ShapeDtypeStruct((width // 2, dim), F32)] * 2,
        scratch_shapes=[pltpu.VMEM((tokens, dim), BF16)],
        compiler_params=params(),
        cost_estimate=COST,
        name="grad_wo",
    )(idx, o, dz, po, pdy_low, pdy_high, wo, gain)


def backward_tile(q_ref, do_ref, stat_ref, dqt_ref, dkv_ref, k, v, kt, start, bq, masked):
    heads = q_ref.shape[0]
    bk = k.shape[0]
    rows = pl.ds(pl.multiple_of(start, 128), bq)
    if masked:
        keep = lax.broadcasted_iota(jnp.int32, (bk, bq), 0) <= lax.broadcasted_iota(jnp.int32, (bk, bq), 1)
    for h in range(heads):
        q = q_ref[h, rows, :]
        d_out = do_ref[h, rows, :]
        t = jnp.tanh(dot(k, q, NT) * INV_CAP)
        p = jnp.exp2(t * CAP2 - stat_ref[h:h + 1, rows])
        if masked:
            p = jnp.where(keep, p, 0.0)
        dp = dot(v, d_out, NT)
        ds = (p * (dp - stat_ref[heads + h:heads + h + 1, rows]) * (1.0 - t * t)).astype(BF16)
        dkv_ref[1] += dot(p.astype(BF16), d_out)
        dkv_ref[0] += dot(ds, q)
        dqt_ref[h, :, rows] += dot(kt, ds)


def backward_kernel(q_ref, do_ref, stat_ref, own_ref, near_ref, far_ref, mid_ref, cos_ref, sin_ref, at_ref,
                    down_ref, dq_ref, dwq_ref,
                    dqt_s, near_out, near_in, mid_out, mid_in, far_out, far_in, dwq_out, dwq_in,
                    near_send, near_recv, mid_send, mid_recv, far_send, far_recv, dwq_send, dwq_recv):
    heads, tokens, hd = q_ref.shape
    half = hd // 2
    bk = own_ref.shape[1]
    big = 2 * bk
    tiles = tokens // bk
    rank = lax.axis_index("cp")
    core = rank % 2
    i = pl.program_id(0)
    across = {"cp": (rank + 2) % 4}
    mesh_id = pl.DeviceIdType.MESH

    def near_copy(n):
        return to_sibling(rank, near_out.at[n], near_in.at[n], near_send.at[n], near_recv.at[n])

    def mid_copy(n):
        return to_sibling(rank, mid_out.at[n], mid_in.at[n], mid_send.at[n], mid_recv.at[n])

    def far_copy(n):
        return pltpu.make_async_remote_copy(
            src_ref=far_out.at[n], dst_ref=far_in.at[n], send_sem=far_send.at[n], recv_sem=far_recv.at[n],
            device_id=across, device_id_type=mesh_id,
        )

    @pl.when(i == 0)
    def _():
        dqt_s[...] = jnp.zeros_like(dqt_s)
        barrier = pltpu.get_barrier_semaphore()
        for other in (across, {"cp": rank + 1 - 2 * core}):
            pl.semaphore_signal(barrier, inc=1, device_id=other, device_id_type=mesh_id)
        pl.semaphore_wait(barrier, 2)

    def all_rows(kv_ref, dkv_ref):
        k, v = kv_ref[0], kv_ref[1]
        kt = k.T

        def step(j, _):
            backward_tile(q_ref, do_ref, stat_ref, dqt_s, dkv_ref, k, v, kt, j * big, big, False)
            return 0

        lax.fori_loop(0, tokens // big, step, 0)

    @pl.when(jnp.logical_and(rank >= 2, i < tiles))
    def _():
        mine = mid_out.at[i]
        mine[...] = jnp.zeros_like(mine)
        all_rows(mid_ref, mine)
        mid_copy(i).start()

    @pl.when(jnp.logical_and(rank >= 2, jnp.logical_and(i >= tiles, i < 2 * tiles)))
    def _():
        n = i - tiles
        mid_copy(n).wait()
        mine = far_out.at[n]
        mine[...] = mid_in[n]
        all_rows(far_ref, mine)
        far_copy(n).start()

    n = i - 2 * tiles

    @pl.when(jnp.logical_and(core == 1, n >= 0))
    def _():
        mine = near_out.at[n]
        mine[...] = jnp.zeros_like(mine)
        all_rows(near_ref, mine)
        near_copy(n).start()

    @pl.when(n >= 0)
    def _():
        down = down_ref.at[:, pl.ds(pl.multiple_of(n * bk, bk), bk), :]
        down[...] = jnp.zeros_like(down)
        k, v = own_ref[0], own_ref[1]
        kt = k.T
        backward_tile(q_ref, do_ref, stat_ref, dqt_s, down, k, v, kt, n * bk, bk, True)

        def own_step(j, _):
            backward_tile(q_ref, do_ref, stat_ref, dqt_s, down, k, v, kt, j * bk, bk, False)
            return 0

        lax.fori_loop(n + 1, tiles, own_step, 0)

    @pl.when(n == tiles - 1)
    def _():
        scale = QUERY_SCALE ** -0.5
        for h in range(heads):
            dq = dqt_s[h].T
            first, second = dq[:, :half], dq[:, half:]
            cosine, sine = cos_ref[...], sin_ref[...]
            dq_ref[:, h * hd:h * hd + half] = ((first * cosine + second * sine) * scale).astype(BF16)
            dq_ref[:, h * hd + half:(h + 1) * hd] = ((second * cosine - first * sine) * scale).astype(BF16)
        dim, width = dwq_ref.shape
        bd = dim // 3

        def product(out_ref, which):
            dq = dq_ref[:, pl.ds(pl.multiple_of((core + which) % 2 * width, width), width)]

            def rows_step(r, _):
                rows = pl.ds(pl.multiple_of(r * bd, bd), bd)
                out_ref[rows, :] = dot(at_ref[rows, :], dq)
                return 0

            lax.fori_loop(0, dim // bd, rows_step, 0)

        product(dwq_out, 1)
        copy = to_sibling(rank, dwq_out, dwq_in, dwq_send, dwq_recv)
        copy.start()
        product(dwq_ref, 0)

        def gather(copy_of, arrived):
            for t in range(tiles):
                copy_of(t).wait_recv()
                down_ref[:, t * bk:(t + 1) * bk, :] += arrived[t]

        def left(copy_of):
            for t in range(tiles):
                copy_of(t).wait_send()

        pl.when(core == 1)(lambda: left(near_copy))
        pl.when(core == 0)(lambda: gather(near_copy, near_in))
        copy.wait()
        dwq_ref[...] += dwq_in[...]
        pl.when(rank < 2)(lambda: gather(far_copy, far_in))
        pl.when(rank >= 2)(lambda: left(far_copy))


def backward(q, d_out, stat, own, near, far, mid, cosine, sine, at):
    heads, tokens, hd = q.shape
    dim = at.shape[0]
    bk = 256
    tiles = tokens // bk
    width = heads * hd // 2

    def phase(first):
        return pl.BlockSpec((2, bk, hd), lambda i: (0, jnp.clip(i - first, 0, tiles - 1), 0))

    def held(array):
        zeros = (0,) * array.ndim
        return pl.BlockSpec(array.shape, lambda i: zeros, pipeline_mode=pl.Buffered(1))

    dma = pltpu.SemaphoreType.DMA
    return pl.pallas_call(
        backward_kernel,
        grid=(3 * tiles,),
        in_specs=[
            held(q),
            held(d_out),
            held(stat),
            phase(2 * tiles),
            phase(2 * tiles),
            phase(tiles),
            phase(0),
            held(cosine),
            held(sine),
            held(at),
        ],
        out_specs=[whole((2, tokens, hd)), whole((tokens, heads * hd)), whole((dim, width))],
        out_shape=[
            jax.ShapeDtypeStruct((2, tokens, hd), F32),
            jax.ShapeDtypeStruct((tokens, heads * hd), BF16),
            jax.ShapeDtypeStruct((dim, width), F32),
        ],
        scratch_shapes=[pltpu.VMEM((heads, hd, tokens), F32)] + [pltpu.VMEM((tiles, 2, bk, hd), F32)] * 6
        + [pltpu.VMEM((dim, width), F32)] * 2 + [dma((tiles,))] * 6 + [dma] * 2,
        compiler_params=pltpu.CompilerParams(vmem_limit_bytes=VMEM_LIMIT, collective_id=0, has_side_effects=True),
        cost_estimate=COST,
        name="backward",
    )(q, d_out, stat, own, near, far, mid, cosine, sine, at)


def tail_kernel(idx_ref, down_ref, cos_ref, sin_ref, at_ref, dq_ref, wq_ref, wk_ref, wv_ref,
                x_ref, dy_ref, gain_ref, dpost_ref, dx_ref, mine_ref, theirs_ref, dgain_ref):
    _, half = cos_ref.shape
    dim = x_ref.shape[1]
    i = pl.program_id(0)
    dk = down_ref[0]
    cosine, sine = cos_ref[...], sin_ref[...]
    first, second = dk[:, :half], dk[:, half:]
    dk = jnp.concatenate([first * cosine + second * sine, second * cosine - first * sine], axis=1).astype(BF16)
    dv = down_ref[1].astype(BF16)

    @pl.when(i == 0)
    def _():
        mine_ref[...] = jnp.zeros_like(mine_ref)
        theirs_ref[...] = jnp.zeros_like(theirs_ref)
        dgain_ref[...] = jnp.zeros_like(dgain_ref)

    core = idx_ref[0] % 2
    at = at_ref[...]
    is_core0 = core == 0
    mine = jnp.where(is_core0, dk, dv)
    theirs = jnp.where(is_core0, dv, dk)
    mine_ref[0:dim, :] += dot(at, mine)
    theirs_ref[0:dim, :] += dot(at, theirs)
    da = dot(dq_ref[...], wq_ref[...], NT) + dot(dk, wk_ref[...], NT) + dot(dv, wv_ref[...], NT)
    x = x_ref[...].astype(F32)
    rstd = lax.rsqrt(jnp.mean(x * x, axis=-1, keepdims=True) + NORM_EPS)
    unit = x * rstd
    dgain_ref[...] += jnp.sum(da * unit, axis=0, keepdims=True)
    g = da * (1.0 + gain_ref[...][None, :])
    dx = rstd * (g - unit * jnp.mean(g * unit, axis=-1, keepdims=True))
    dx_ref[...] = (dy_ref[...].astype(F32) + dx).astype(BF16)

    @pl.when(i == pl.num_programs(0) - 1)
    def _():
        dpre, dpost = dgain_ref[...], dpost_ref[...]
        for ref, row in ((mine_ref, jnp.where(is_core0, dpre, dpost)), (theirs_ref, jnp.where(is_core0, dpost, dpre))):
            for c in range(dim // 128):
                ref[dim + c // 2:dim + c // 2 + 1, c % 2 * 128:(c % 2 + 1) * 128] = row[:, c * 128:(c + 1) * 128]


def tail(idx, down, cosine, sine, at, dq, wq, wk, wv, x, dy, gain, dpost):
    tokens, dim = x.shape
    hd = wk.shape[1]
    width = wq.shape[1]
    bt = 256
    kv_spec = stack_spec(2, bt, hd)
    rope_spec = rows_spec(bt, hd // 2)
    rows2 = rows_spec(bt, dim)
    return pl.pallas_call(
        tail_kernel,
        grid=(tokens // bt,),
        in_specs=[
            pl.BlockSpec(memory_space=pltpu.SMEM),
            kv_spec,
            rope_spec,
            rope_spec,
            pl.BlockSpec((dim, bt), lambda i: (0, i)),
            rows_spec(bt, width),
            whole(wq.shape),
            whole(wk.shape),
            whole(wv.shape),
            rows2,
            rows2,
            whole((dim,)),
            whole((1, dim)),
        ],
        out_specs=[rows2, whole((dim + 8, hd)), whole((dim + 8, hd))],
        out_shape=[
            jax.ShapeDtypeStruct((tokens, dim), BF16),
            jax.ShapeDtypeStruct((dim + 8, hd), F32),
            jax.ShapeDtypeStruct((dim + 8, hd), F32),
        ],
        scratch_shapes=[pltpu.VMEM((1, dim), F32)],
        compiler_params=params(),
        cost_estimate=COST,
        name="tail",
    )(idx, down, cosine, sine, at, dq, wq, wk, wv, x, dy, gain, dpost)


def join_wide_kernel(idx_ref, mine_ref, other_ref, out_ref):
    first = idx_ref[0] % 2 == 0
    rows, _ = mine_ref.shape
    mine, other = mine_ref[...], other_ref[...]
    low, high = jnp.where(first, mine, other), jnp.where(first, other, mine)
    heads = 4
    for h in range(heads):
        src = low if h < heads // 2 else high
        base = (h % (heads // 2)) * 256
        for c in range(2):
            out_ref[pl.ds(c * heads + h, rows, stride=2 * heads), :] = src[:, base + c * 128:base + (c + 1) * 128]


def join_wide(idx, mine, other, heads):
    dim, width = mine.shape
    bd = 128
    spec = rows_spec(bd, width)
    out = pl.pallas_call(
        join_wide_kernel,
        grid=(dim // bd,),
        in_specs=[pl.BlockSpec(memory_space=pltpu.SMEM), spec, spec],
        out_specs=rows_spec(bd * 8, 128),
        out_shape=jax.ShapeDtypeStruct((dim * 8, 128), F32),
        compiler_params=params(),
        cost_estimate=COST,
        name="join_wide",
    )(idx, mine, other)
    return out.reshape(dim, 2, heads, 128).transpose(0, 2, 1, 3).reshape(dim, heads, 256)


def join_pair_kernel(idx_ref, a_ref, b_ref, c_ref, d_ref, ga_ref, gb_ref, gc_ref, gd_ref, first_ref, second_ref, dpre_ref, dpost_ref):
    core0 = idx_ref[0] % 2 == 0
    dim = dpre_ref.shape[0]
    rows = a_ref.shape[0]

    def ordered(mine, other):
        return jnp.where(core0, mine, other), jnp.where(core0, other, mine)

    for src, out_ref in zip(ordered(a_ref[...] + b_ref[...], c_ref[...] + d_ref[...]), (first_ref, second_ref)):
        for c in range(2):
            out_ref[pl.ds(c, rows, stride=2), :] = src[:, c * 128:(c + 1) * 128]

    @pl.when(pl.program_id(0) == 0)
    def _():
        for src, gain_ref in zip(ordered(ga_ref[...] + gb_ref[...], gc_ref[...] + gd_ref[...]), (dpre_ref, dpost_ref)):
            for c in range(dim // 128):
                gain_ref[c * 128:(c + 1) * 128] = src[c // 2, c % 2 * 128:(c % 2 + 1) * 128]


def join_pair(idx, *parts):
    dim, width = parts[0].shape[0] - 8, parts[0].shape[1]
    bd = dim // 3
    gain_rows = dim // 8
    outs = pl.pallas_call(
        join_pair_kernel,
        grid=(dim // bd,),
        in_specs=[pl.BlockSpec(memory_space=pltpu.SMEM)] + [rows_spec(bd, width)] * 4
        + [pl.BlockSpec((8, width), lambda i: (gain_rows, 0))] * 4,
        out_specs=[rows_spec(bd * 2, 128)] * 2 + [whole((dim,))] * 2,
        out_shape=[jax.ShapeDtypeStruct((dim * 2, 128), F32)] * 2 + [jax.ShapeDtypeStruct((dim,), F32)] * 2,
        compiler_params=params(),
        cost_estimate=COST,
        name="join_pair",
    )(idx, *parts, *parts)
    return [o.reshape(dim, 1, width) for o in outs[:2]] + list(outs[2:])


def join_rows_kernel(idx_ref, mine_ref, other_ref, out_ref):
    first = idx_ref[0] % 2 == 0
    out_ref[...] = jnp.where(first == (pl.program_id(0) == 0), mine_ref[...], other_ref[...])


def join_rows(idx, mine, other):
    rows, dim = mine.shape
    br = 256
    steps = rows // br
    spec = pl.BlockSpec((br, dim), lambda w, i: (i, 0))
    return pl.pallas_call(
        join_rows_kernel,
        grid=(2, steps),
        in_specs=[pl.BlockSpec(memory_space=pltpu.SMEM), spec, spec],
        out_specs=pl.BlockSpec((br, dim), lambda w, i: (w * steps + i, 0)),
        out_shape=jax.ShapeDtypeStruct((rows * 2, dim), F32),
        compiler_params=params(),
        cost_estimate=COST,
        name="join_rows",
    )(idx, mine, other)


def solution(mesh):
    across = [(0, 2), (2, 0), (1, 3), (3, 1)]
    beside = [(0, 1), (1, 0), (2, 3), (3, 2)]

    def permute(value, pairs):
        return lax.ppermute(value, "cp", pairs)

    def local_step(x_in, positions, dy_out, w_query, w_key, w_value, w_out, w_pre, w_post):
        batch, tokens, dim = x_in.shape
        heads, hd = w_query.shape[1], w_query.shape[2]
        half = hd // 2
        idx = lax.axis_index("cp").astype(jnp.int32).reshape(1)
        wq = w_query.reshape(dim, heads * hd)
        wk = w_key.reshape(dim, hd)
        wv = w_value.reshape(dim, hd)
        wo = w_out.reshape(heads * hd, dim)
        x = x_in.reshape(tokens, dim)
        dy = dy_out.reshape(tokens, dim)
        gain_pre = w_pre
        gain_post = w_post
        inv_freq = ROPE_BASE ** (jnp.arange(half, dtype=F32) * (-2.0 / hd))
        angles = positions.reshape(tokens, 1).astype(F32) * inv_freq
        cosine, sine = jnp.cos(angles), jnp.sin(angles)

        dy_high = permute(dy, [(2, 0), (3, 1)])
        act_t, q, own, near, far, mid, o, out, lse = forward(x, gain_pre, wk, wv, wq, cosine, sine, heads)
        dy_low = permute(dy, [(0, 2), (1, 3)])
        partner_o = permute(o, across)
        y, d_out, dz, stat, dgain_post = post(o, out, lse, x, dy, wo, gain_post)

        down, dq, dwq_part = backward(q, d_out, stat, own, near, far, mid, cosine, sine, act_t)
        dwq_mine = dwq_part + permute(dwq_part, across)
        dwq_other = permute(dwq_mine, beside)
        dwo = grad_wo(idx, o, dz, partner_o, dy_high, dy_low, wo, gain_post)
        dwo_mine = dwo[0] + permute(dwo[1], beside)
        dwo_other = permute(dwo_mine, beside)
        dx, *dwkv = tail(idx, down, cosine, sine, act_t, dq, wq, wk, wv, x, dy, gain_pre, dgain_post)
        theirs_in, mine_in = permute(dwkv[1], beside), permute(dwkv[0], beside)
        chip_mine = dwkv[0] + theirs_in
        chip_other = dwkv[1] + mine_in
        far_mine = permute(chip_mine, across)
        far_other = permute(far_mine, beside)

        dwo_full = join_rows(idx, dwo_mine, dwo_other)
        dwq_full = join_wide(idx, dwq_mine, dwq_other, heads)
        dwk_full, dwv_full, dpre_full, dpost_full = join_pair(idx, chip_mine, far_mine, chip_other, far_other)
        return (
            y.reshape(batch, tokens, dim),
            dx.reshape(batch, tokens, dim),
            dwq_full,
            dwk_full,
            dwv_full,
            dwo_full.reshape(heads, hd, dim),
            dpre_full,
            dpost_full,
        )

    seq_spec = P("dp", "cp", None)
    in_specs = (seq_spec, P("dp", "cp"), seq_spec, P(), P(), P(), P(), P(), P())
    out_specs = (seq_spec, seq_spec, P("dp", None, None), P("dp", None, None), P("dp", None, None), P("dp", None, None), P("dp"), P("dp"))
    return jax.shard_map(local_step, mesh=mesh, in_specs=in_specs, out_specs=out_specs, check_vma=False)
```

```python
import functools
import math

import jax
import jax.numpy as jnp
from jax import lax
from jax.experimental import pallas as pl
from jax.experimental.pallas import tpu as pltpu
from jax.sharding import PartitionSpec as P


NORM_EPS = 1e-6
SOFT_CAP = 50.0
QUERY_SCALE = 144.0
ROPE_BASE = 10000.0
LOG2E = math.log2(math.e)
CAP2 = SOFT_CAP * LOG2E
INV_CAP = 1.0 / SOFT_CAP


F32 = jnp.float32
BF16 = jnp.bfloat16
VMEM_LIMIT = 60 * 1024 * 1024

NT = (((1,), (1,)), ((), ()))
NN = (((1,), (0,)), ((), ()))


def dot(a, b, dims=NN):
    return lax.dot_general(a, b, dims, preferred_element_type=F32)


def params():
    return pltpu.CompilerParams(vmem_limit_bytes=VMEM_LIMIT)


def whole(shape):
    zeros = (0,) * len(shape)
    return pl.BlockSpec(shape, lambda *_: zeros)


def rows_spec(rows, width):
    return pl.BlockSpec((rows, width), lambda i: (i, 0))


def stack_spec(depth, rows, width):
    return pl.BlockSpec((depth, rows, width), lambda i: (0, i, 0))


COST = pl.CostEstimate(flops=10**10, bytes_accessed=10**7, transcendentals=0)


def to_sibling(rank, src, dst, send, recv):
    return pltpu.make_async_remote_copy(
        src_ref=src, dst_ref=dst, send_sem=send, recv_sem=recv,
        device_id={"cp": rank + 1 - 2 * (rank % 2)}, device_id_type=pl.DeviceIdType.MESH,
    )


def rope(values, cosine, sine):
    half = cosine.shape[-1]
    first, second = values[:, :half], values[:, half:]
    return jnp.concatenate([first * cosine - second * sine, second * cosine + first * sine], axis=-1)


def forward_tile(q_ref, acc_ref, sum_ref, k, v, masked):
    heads, bq, _ = q_ref.shape
    bk = k.shape[0]
    if masked:
        keep = lax.broadcasted_iota(jnp.int32, (bq, bk), 1) <= lax.broadcasted_iota(jnp.int32, (bq, bk), 0)
    for h in range(heads):
        s = dot(q_ref[h], k, NT)
        p = jnp.exp2(jnp.tanh(s * INV_CAP) * CAP2)
        if masked:
            p = jnp.where(keep, p, 0.0)
        part = p[:, 0:128]
        for c in range(128, bk, 128):
            part = part + p[:, c:c + 128]
        sum_ref[h] += part
        acc_ref[h] += dot(p.astype(BF16), v)


def forward_kernel(x_ref, gain_ref, wk_ref, wv_ref, wq_ref, cos_ref, sin_ref,
                   at_ref, q_ref, own_ref, near_ref, far_ref, mid_ref, o_ref, out_ref, lse_ref,
                   a_s, own_s, near_s, far_s, mid_s, acc_s, sum_s,
                   far_send, far_recv, near_send, near_recv, mid_send, mid_recv):
    heads, tokens, hd = q_ref.shape
    bt = x_ref.shape[0]
    tiles = tokens // bt
    big = 2 * bt
    rank = lax.axis_index("cp")
    core = rank % 2
    i = pl.program_id(0)
    across = {"cp": (rank + 2) % 4}
    mesh_id = pl.DeviceIdType.MESH

    def rows_of(t, size=bt):
        return pl.ds(pl.multiple_of(t * size, size), size)

    def far_copy(t):
        rows = rows_of(t)
        return pltpu.make_async_remote_copy(
            src_ref=own_s.at[:, rows, :], dst_ref=far_s.at[:, rows, :], send_sem=far_send.at[t], recv_sem=far_recv.at[t],
            device_id=across, device_id_type=mesh_id,
        )

    def near_copy(t):
        rows = rows_of(t)
        return to_sibling(rank, own_s.at[:, rows, :], near_s.at[:, rows, :], near_send.at[t], near_recv.at[t])

    def mid_copy(c):
        rows = rows_of(c, big)
        return to_sibling(rank, far_s.at[:, rows, :], mid_s.at[:, rows, :], mid_send.at[c], mid_recv.at[c])

    @pl.when(i == 0)
    def _():
        barrier = pltpu.get_barrier_semaphore()
        for other in (across, {"cp": rank + 1 - 2 * core}):
            pl.semaphore_signal(barrier, inc=1, device_id=other, device_id_type=mesh_id)
        pl.semaphore_wait(barrier, 2)

    @pl.when(i < tiles)
    def _():
        rows = rows_of(i)
        x = x_ref[...].astype(F32)
        rstd = lax.rsqrt(jnp.mean(x * x, axis=-1, keepdims=True) + NORM_EPS)
        a = (x * rstd * (1.0 + gain_ref[...][None, :])).astype(BF16)
        a_s[rows, :] = a
        own_s[0, rows, :] = rope(dot(a, wk_ref[...]).astype(BF16).astype(F32), cos_ref[rows, :], sin_ref[rows, :]).astype(BF16)
        own_s[1, rows, :] = dot(a, wv_ref[...]).astype(BF16)
        pl.when(rank < 2)(lambda: far_copy(i).start())
        pl.when(core == 0)(lambda: near_copy(i).start())
        at_ref[...] = a.T

    def attend(t, kv_ref, start, size, masked):
        rows, keys = rows_of(t), pl.ds(pl.multiple_of(start, bt), size)
        forward_tile(q_ref.at[:, rows, :], acc_s.at[:, rows, :], sum_s.at[:, rows, :],
                     kv_ref[0, keys, :], kv_ref[1, keys, :], masked)

    @pl.when(jnp.logical_and(i >= tiles, i < 2 * tiles))
    def _():
        t = i - tiles
        rows = rows_of(t)
        a = a_s[rows, :]
        scale = QUERY_SCALE ** -0.5
        for h in range(heads):
            q = dot(a, wq_ref[:, h * hd:(h + 1) * hd]).astype(BF16).astype(F32)
            q_ref[h, rows, :] = (rope(q, cos_ref[rows, :], sin_ref[rows, :]) * scale).astype(BF16)
        acc_s[:, rows, :] = jnp.zeros((heads, bt, hd), F32)
        sum_s[:, rows, :] = jnp.zeros((heads, bt, 128), F32)
        attend(t, own_s, t * bt, bt, True)

        def own_step(j, _):
            attend(t, own_s, j * bt, bt, False)
            return 0

        lax.fori_loop(0, t, own_step, 0)

        @pl.when(core == 1)
        def _():
            pl.when(t == 0)(lambda: [near_copy(n).wait_recv() for n in range(tiles)] and None)

            def near_step(j, _):
                attend(t, near_s, j * big, big, False)
                return 0

            lax.fori_loop(0, tokens // big, near_step, 0)

    chunks = tokens // big
    c = i - 2 * tiles

    def far_chunk(kv_ref, start):
        def step(t, _):
            attend(t, kv_ref, start, big, False)
            return 0

        lax.fori_loop(0, tiles, step, 0)

    @pl.when(jnp.logical_and(rank >= 2, jnp.logical_and(c >= 0, c < chunks)))
    def _():
        far_copy(2 * c).wait_recv()
        far_copy(2 * c + 1).wait_recv()
        mid_copy(c).start()
        far_chunk(far_s, c * big)

    @pl.when(jnp.logical_and(rank >= 2, jnp.logical_and(c >= chunks, c < 2 * chunks)))
    def _():
        mid_copy(c - chunks).wait_recv()
        far_chunk(mid_s, (c - chunks) * big)

    last = i - 2 * tiles - 2 * chunks

    @pl.when(last >= 0)
    def _():
        rows = rows_of(last)
        lane = lax.broadcasted_iota(jnp.int32, (bt, 128), 1)
        lse = jnp.zeros((bt, 128), F32)
        for h in range(heads):
            total = jnp.sum(sum_s[h, rows, :], axis=-1, keepdims=True)
            lse = jnp.where(lane == h, jnp.log2(total), lse)
            out = acc_s[h, rows, :] / total
            out_ref[h] = out
            o_ref[:, h * hd:(h + 1) * hd] = out.astype(BF16)
        lse_ref[...] = lse
        for dst, src in ((own_ref, own_s), (near_ref, near_s), (far_ref, far_s), (mid_ref, mid_s)):
            dst[...] = src[:, rows, :]

    @pl.when(last == tiles - 1)
    def _():
        pl.when(rank < 2)(lambda: [far_copy(n).wait_send() for n in range(tiles)] and None)
        pl.when(core == 0)(lambda: [near_copy(n).wait_send() for n in range(tiles)] and None)
        pl.when(rank >= 2)(lambda: [mid_copy(n).wait_send() for n in range(chunks)] and None)


def forward(x, gain, wk, wv, wq, cosine, sine, heads):
    tokens, dim = x.shape
    hd = wk.shape[1]
    bt = 256
    tiles = tokens // bt
    chunks = tiles // 2
    done = 2 * tiles + 2 * chunks
    dma = pltpu.SemaphoreType.DMA
    early = lambda i: jnp.minimum(i, tiles - 1)
    late = lambda i: jnp.maximum(i - done, 0)
    kv_shape = jax.ShapeDtypeStruct((2, tokens, hd), BF16)
    kv_out = pl.BlockSpec((2, bt, hd), lambda i: (0, late(i), 0))
    return pl.pallas_call(
        forward_kernel,
        grid=(done + tiles,),
        in_specs=[
            pl.BlockSpec((bt, dim), lambda i: (early(i), 0)),
            whole(gain.shape),
            whole(wk.shape),
            whole(wv.shape),
            whole(wq.shape),
            whole(cosine.shape),
            whole(sine.shape),
        ],
        out_specs=[
            pl.BlockSpec((dim, bt), lambda i: (0, early(i))),
            whole((heads, tokens, hd)),
            kv_out,
            kv_out,
            kv_out,
            kv_out,
            pl.BlockSpec((bt, heads * hd), lambda i: (late(i), 0)),
            pl.BlockSpec((heads, bt, hd), lambda i: (0, late(i), 0)),
            pl.BlockSpec((bt, 128), lambda i: (late(i), 0)),
        ],
        out_shape=[
            jax.ShapeDtypeStruct((dim, tokens), BF16),
            jax.ShapeDtypeStruct((heads, tokens, hd), BF16),
            kv_shape,
            kv_shape,
            kv_shape,
            kv_shape,
            jax.ShapeDtypeStruct((tokens, heads * hd), BF16),
            jax.ShapeDtypeStruct((heads, tokens, hd), F32),
            jax.ShapeDtypeStruct((tokens, 128), F32),
        ],
        scratch_shapes=[pltpu.VMEM((tokens, dim), BF16)] + [pltpu.VMEM((2, tokens, hd), BF16)] * 4 + [
            pltpu.VMEM((heads, tokens, hd), F32),
            pltpu.VMEM((heads, tokens, 128), F32),
            dma((tiles,)),
            dma((tiles,)),
            dma((tiles,)),
            dma((tiles,)),
            dma((chunks,)),
            dma((chunks,)),
        ],
        compiler_params=pltpu.CompilerParams(vmem_limit_bytes=VMEM_LIMIT, collective_id=2, has_side_effects=True),
        cost_estimate=COST,
        name="forward",
    )(x, gain, wk, wv, wq, cosine, sine)


def post_norm(o, wo, gain, dy):
    z = dot(o, wo).astype(BF16).astype(F32)
    rstd = lax.rsqrt(jnp.mean(z * z, axis=-1, keepdims=True) + NORM_EPS)
    unit = z * rstd
    g = dy * gain
    dz = (rstd * (g - unit * jnp.mean(g * unit, axis=-1, keepdims=True))).astype(BF16)
    return unit, dz


def post_kernel(o_ref, out_ref, lse_ref, x_ref, dy_ref, wo_ref, gain_ref, y_ref, do_ref, dz_ref, stat_ref, dgain_ref):
    heads, bq, hd = out_ref.shape
    gain = 1.0 + gain_ref[...][None, :]
    dy = dy_ref[...].astype(F32)
    unit, dz = post_norm(o_ref[...], wo_ref[...], gain, dy)
    y_ref[...] = (x_ref[...].astype(F32) + (unit * gain).astype(BF16).astype(F32)).astype(BF16)
    dz_ref[...] = dz

    @pl.when(pl.program_id(0) == 0)
    def _():
        dgain_ref[...] = jnp.zeros_like(dgain_ref)

    dgain_ref[...] += jnp.sum(dy * unit, axis=0, keepdims=True)
    lane = lax.broadcasted_iota(jnp.int32, (bq, 128), 1)
    stat = lse_ref[...]
    for h in range(heads):
        d_out = dot(dz, wo_ref[h * hd:(h + 1) * hd, :], NT).astype(BF16)
        do_ref[h] = d_out
        delta = jnp.sum(d_out.astype(F32) * out_ref[h], axis=-1, keepdims=True)
        stat = jnp.where(lane == heads + h, delta, stat)
    stat_ref[...] = stat.T[0:8, :]


def post(o, out, lse, x, dy, wo, gain):
    heads, tokens, hd = out.shape
    dim = x.shape[1]
    bq = 256
    rows3 = stack_spec(heads, bq, hd)
    rows2 = lambda width: rows_spec(bq, width)
    return pl.pallas_call(
        post_kernel,
        grid=(tokens // bq,),
        in_specs=[rows2(heads * hd), rows3, rows2(128), rows2(dim), rows2(dim), whole(wo.shape), whole((dim,))],
        out_specs=[rows2(dim), rows3, rows2(dim), pl.BlockSpec((8, bq), lambda i: (0, i)), whole((1, dim))],
        out_shape=[
            jax.ShapeDtypeStruct((tokens, dim), BF16),
            jax.ShapeDtypeStruct((heads, tokens, hd), BF16),
            jax.ShapeDtypeStruct((tokens, dim), BF16),
            jax.ShapeDtypeStruct((8, tokens), F32),
            jax.ShapeDtypeStruct((1, dim), F32),
        ],
        compiler_params=params(),
        cost_estimate=COST,
        name="post",
    )(o, out, lse, x, dy, wo, gain)


def grad_wo_kernel(idx_ref, o_ref, dz_ref, po_ref, pdy_low_ref, pdy_high_ref, wo_ref, gain_ref, mine_ref, theirs_ref, pdz_ref):
    _, width = o_ref.shape
    bt = pdy_low_ref.shape[0]
    hd = 256
    i = pl.program_id(0)
    rows = pl.ds(pl.multiple_of(i * bt, bt), bt)
    dy = jnp.where(idx_ref[0] >= 2, pdy_high_ref[...], pdy_low_ref[...]).astype(F32)
    pdz_ref[rows, :] = post_norm(po_ref[rows, :], wo_ref[...], 1.0 + gain_ref[...][None, :], dy)[1]

    @pl.when(i == pl.num_programs(0) - 1)
    def _():
        core = idx_ref[0] % 2
        per = width // hd // 2
        for which, ref in enumerate((mine_ref, theirs_ref)):
            for hh in range(per):
                cols = pl.ds(pl.multiple_of((((core + which) % 2) * per + hh) * hd, hd), hd)
                ref[hh * hd:(hh + 1) * hd, :] = dot(o_ref[:, cols].T, dz_ref[...]) + dot(po_ref[:, cols].T, pdz_ref[...])


def grad_wo(idx, o, dz, po, pdy_low, pdy_high, wo, gain):
    tokens, width = o.shape
    dim = dz.shape[1]
    bt = 256
    rows2 = rows_spec(bt, dim)
    return pl.pallas_call(
        grad_wo_kernel,
        grid=(tokens // bt,),
        in_specs=[
            pl.BlockSpec(memory_space=pltpu.SMEM),
            whole(o.shape),
            whole(dz.shape),
            whole(o.shape),
            rows2,
            rows2,
            whole(wo.shape),
            whole((dim,)),
        ],
        out_specs=[whole((width // 2, dim))] * 2,
        out_shape=[jax.ShapeDtypeStruct((width // 2, dim), F32)] * 2,
        scratch_shapes=[pltpu.VMEM((tokens, dim), BF16)],
        compiler_params=params(),
        cost_estimate=COST,
        name="grad_wo",
    )(idx, o, dz, po, pdy_low, pdy_high, wo, gain)


def backward_tile(q_ref, do_ref, stat_ref, dqt_ref, dkv_ref, k, v, kt, start, bq, masked):
    heads = q_ref.shape[0]
    bk = k.shape[0]
    rows = pl.ds(pl.multiple_of(start, 128), bq)
    if masked:
        keep = lax.broadcasted_iota(jnp.int32, (bk, bq), 0) <= lax.broadcasted_iota(jnp.int32, (bk, bq), 1)
    for h in range(heads):
        q = q_ref[h, rows, :]
        d_out = do_ref[h, rows, :]
        t = jnp.tanh(dot(k, q, NT) * INV_CAP)
        p = jnp.exp2(t * CAP2 - stat_ref[h:h + 1, rows])
        if masked:
            p = jnp.where(keep, p, 0.0)
        dp = dot(v, d_out, NT)
        ds = (p * (dp - stat_ref[heads + h:heads + h + 1, rows]) * (1.0 - t * t)).astype(BF16)
        dkv_ref[1] += dot(p.astype(BF16), d_out)
        dkv_ref[0] += dot(ds, q)
        dqt_ref[h, :, rows] += dot(kt, ds)


def backward_kernel(q_ref, do_ref, stat_ref, own_ref, near_ref, far_ref, mid_ref, cos_ref, sin_ref, at_ref,
                    down_ref, dq_ref, dwq_ref,
                    dqt_s, near_out, near_in, mid_out, mid_in, far_out, far_in, dwq_out, dwq_in,
                    near_send, near_recv, mid_send, mid_recv, far_send, far_recv, dwq_send, dwq_recv):
    heads, tokens, hd = q_ref.shape
    half = hd // 2
    bk = own_ref.shape[1]
    big = 2 * bk
    tiles = tokens // bk
    rank = lax.axis_index("cp")
    core = rank % 2
    i = pl.program_id(0)
    across = {"cp": (rank + 2) % 4}
    mesh_id = pl.DeviceIdType.MESH

    def near_copy(n):
        return to_sibling(rank, near_out.at[n], near_in.at[n], near_send.at[n], near_recv.at[n])

    def mid_copy(n):
        return to_sibling(rank, mid_out.at[n], mid_in.at[n], mid_send.at[n], mid_recv.at[n])

    def far_copy(n):
        return pltpu.make_async_remote_copy(
            src_ref=far_out.at[n], dst_ref=far_in.at[n], send_sem=far_send.at[n], recv_sem=far_recv.at[n],
            device_id=across, device_id_type=mesh_id,
        )

    @pl.when(i == 0)
    def _():
        dqt_s[...] = jnp.zeros_like(dqt_s)
        barrier = pltpu.get_barrier_semaphore()
        for other in (across, {"cp": rank + 1 - 2 * core}):
            pl.semaphore_signal(barrier, inc=1, device_id=other, device_id_type=mesh_id)
        pl.semaphore_wait(barrier, 2)

    def all_rows(kv_ref, dkv_ref):
        k, v = kv_ref[0], kv_ref[1]
        kt = k.T

        def step(j, _):
            backward_tile(q_ref, do_ref, stat_ref, dqt_s, dkv_ref, k, v, kt, j * big, big, False)
            return 0

        lax.fori_loop(0, tokens // big, step, 0)

    @pl.when(jnp.logical_and(rank >= 2, i < tiles))
    def _():
        mine = mid_out.at[i]
        mine[...] = jnp.zeros_like(mine)
        all_rows(mid_ref, mine)
        mid_copy(i).start()

    @pl.when(jnp.logical_and(rank >= 2, jnp.logical_and(i >= tiles, i < 2 * tiles)))
    def _():
        n = i - tiles
        mid_copy(n).wait()
        mine = far_out.at[n]
        mine[...] = mid_in[n]
        all_rows(far_ref, mine)
        far_copy(n).start()

    n = i - 2 * tiles

    @pl.when(jnp.logical_and(core == 1, n >= 0))
    def _():
        mine = near_out.at[n]
        mine[...] = jnp.zeros_like(mine)
        all_rows(near_ref, mine)
        near_copy(n).start()

    @pl.when(n >= 0)
    def _():
        down = down_ref.at[:, pl.ds(pl.multiple_of(n * bk, bk), bk), :]
        down[...] = jnp.zeros_like(down)
        k, v = own_ref[0], own_ref[1]
        kt = k.T
        backward_tile(q_ref, do_ref, stat_ref, dqt_s, down, k, v, kt, n * bk, bk, True)

        def own_step(j, _):
            backward_tile(q_ref, do_ref, stat_ref, dqt_s, down, k, v, kt, j * bk, bk, False)
            return 0

        lax.fori_loop(n + 1, tiles, own_step, 0)

    @pl.when(n == tiles - 1)
    def _():
        scale = QUERY_SCALE ** -0.5
        for h in range(heads):
            dq = dqt_s[h].T
            first, second = dq[:, :half], dq[:, half:]
            cosine, sine = cos_ref[...], sin_ref[...]
            dq_ref[:, h * hd:h * hd + half] = ((first * cosine + second * sine) * scale).astype(BF16)
            dq_ref[:, h * hd + half:(h + 1) * hd] = ((second * cosine - first * sine) * scale).astype(BF16)
        dim, width = dwq_ref.shape
        bd = dim // 3

        def product(out_ref, which):
            dq = dq_ref[:, pl.ds(pl.multiple_of((core + which) % 2 * width, width), width)]

            def rows_step(r, _):
                rows = pl.ds(pl.multiple_of(r * bd, bd), bd)
                out_ref[rows, :] = dot(at_ref[rows, :], dq)
                return 0

            lax.fori_loop(0, dim // bd, rows_step, 0)

        product(dwq_out, 1)
        copy = to_sibling(rank, dwq_out, dwq_in, dwq_send, dwq_recv)
        copy.start()
        product(dwq_ref, 0)

        def gather(copy_of, arrived):
            for t in range(tiles):
                copy_of(t).wait_recv()
                down_ref[:, t * bk:(t + 1) * bk, :] += arrived[t]

        def left(copy_of):
            for t in range(tiles):
                copy_of(t).wait_send()

        pl.when(core == 1)(lambda: left(near_copy))
        pl.when(core == 0)(lambda: gather(near_copy, near_in))
        copy.wait()
        dwq_ref[...] += dwq_in[...]
        pl.when(rank < 2)(lambda: gather(far_copy, far_in))
        pl.when(rank >= 2)(lambda: left(far_copy))


def backward(q, d_out, stat, own, near, far, mid, cosine, sine, at):
    heads, tokens, hd = q.shape
    dim = at.shape[0]
    bk = 256
    tiles = tokens // bk
    width = heads * hd // 2

    def phase(first):
        return pl.BlockSpec((2, bk, hd), lambda i: (0, jnp.clip(i - first, 0, tiles - 1), 0))

    def held(array):
        zeros = (0,) * array.ndim
        return pl.BlockSpec(array.shape, lambda i: zeros, pipeline_mode=pl.Buffered(1))

    dma = pltpu.SemaphoreType.DMA
    return pl.pallas_call(
        backward_kernel,
        grid=(3 * tiles,),
        in_specs=[
            held(q),
            held(d_out),
            held(stat),
            phase(2 * tiles),
            phase(2 * tiles),
            phase(tiles),
            phase(0),
            held(cosine),
            held(sine),
            held(at),
        ],
        out_specs=[whole((2, tokens, hd)), whole((tokens, heads * hd)), whole((dim, width))],
        out_shape=[
            jax.ShapeDtypeStruct((2, tokens, hd), F32),
            jax.ShapeDtypeStruct((tokens, heads * hd), BF16),
            jax.ShapeDtypeStruct((dim, width), F32),
        ],
        scratch_shapes=[pltpu.VMEM((heads, hd, tokens), F32)] + [pltpu.VMEM((tiles, 2, bk, hd), F32)] * 6
        + [pltpu.VMEM((dim, width), F32)] * 2 + [dma((tiles,))] * 6 + [dma] * 2,
        compiler_params=pltpu.CompilerParams(vmem_limit_bytes=VMEM_LIMIT, collective_id=0, has_side_effects=True),
        cost_estimate=COST,
        name="backward",
    )(q, d_out, stat, own, near, far, mid, cosine, sine, at)


def tail_kernel(idx_ref, down_ref, cos_ref, sin_ref, at_ref, dq_ref, wq_ref, wk_ref, wv_ref,
                x_ref, dy_ref, gain_ref, dpost_ref, dx_ref, mine_ref, theirs_ref, dgain_ref):
    _, half = cos_ref.shape
    dim = x_ref.shape[1]
    i = pl.program_id(0)
    dk = down_ref[0]
    cosine, sine = cos_ref[...], sin_ref[...]
    first, second = dk[:, :half], dk[:, half:]
    dk = jnp.concatenate([first * cosine + second * sine, second * cosine - first * sine], axis=1).astype(BF16)
    dv = down_ref[1].astype(BF16)

    @pl.when(i == 0)
    def _():
        mine_ref[...] = jnp.zeros_like(mine_ref)
        theirs_ref[...] = jnp.zeros_like(theirs_ref)
        dgain_ref[...] = jnp.zeros_like(dgain_ref)

    core = idx_ref[0] % 2
    at = at_ref[...]
    is_core0 = core == 0
    mine = jnp.where(is_core0, dk, dv)
    theirs = jnp.where(is_core0, dv, dk)
    mine_ref[0:dim, :] += dot(at, mine)
    theirs_ref[0:dim, :] += dot(at, theirs)
    da = dot(dq_ref[...], wq_ref[...], NT) + dot(dk, wk_ref[...], NT) + dot(dv, wv_ref[...], NT)
    x = x_ref[...].astype(F32)
    rstd = lax.rsqrt(jnp.mean(x * x, axis=-1, keepdims=True) + NORM_EPS)
    unit = x * rstd
    dgain_ref[...] += jnp.sum(da * unit, axis=0, keepdims=True)
    g = da * (1.0 + gain_ref[...][None, :])
    dx = rstd * (g - unit * jnp.mean(g * unit, axis=-1, keepdims=True))
    dx_ref[...] = (dy_ref[...].astype(F32) + dx).astype(BF16)

    @pl.when(i == pl.num_programs(0) - 1)
    def _():
        dpre, dpost = dgain_ref[...], dpost_ref[...]
        for ref, row in ((mine_ref, jnp.where(is_core0, dpre, dpost)), (theirs_ref, jnp.where(is_core0, dpost, dpre))):
            for c in range(dim // 128):
                ref[dim + c // 2:dim + c // 2 + 1, c % 2 * 128:(c % 2 + 1) * 128] = row[:, c * 128:(c + 1) * 128]


def tail(idx, down, cosine, sine, at, dq, wq, wk, wv, x, dy, gain, dpost):
    tokens, dim = x.shape
    hd = wk.shape[1]
    width = wq.shape[1]
    bt = 256
    kv_spec = stack_spec(2, bt, hd)
    rope_spec = rows_spec(bt, hd // 2)
    rows2 = rows_spec(bt, dim)
    return pl.pallas_call(
        tail_kernel,
        grid=(tokens // bt,),
        in_specs=[
            pl.BlockSpec(memory_space=pltpu.SMEM),
            kv_spec,
            rope_spec,
            rope_spec,
            pl.BlockSpec((dim, bt), lambda i: (0, i)),
            rows_spec(bt, width),
            whole(wq.shape),
            whole(wk.shape),
            whole(wv.shape),
            rows2,
            rows2,
            whole((dim,)),
            whole((1, dim)),
        ],
        out_specs=[rows2, whole((dim + 8, hd)), whole((dim + 8, hd))],
        out_shape=[
            jax.ShapeDtypeStruct((tokens, dim), BF16),
            jax.ShapeDtypeStruct((dim + 8, hd), F32),
            jax.ShapeDtypeStruct((dim + 8, hd), F32),
        ],
        scratch_shapes=[pltpu.VMEM((1, dim), F32)],
        compiler_params=params(),
        cost_estimate=COST,
        name="tail",
    )(idx, down, cosine, sine, at, dq, wq, wk, wv, x, dy, gain, dpost)


def join_wide_kernel(idx_ref, mine_ref, other_ref, out_ref):
    first = idx_ref[0] % 2 == 0
    rows, _ = mine_ref.shape
    mine, other = mine_ref[...], other_ref[...]
    low, high = jnp.where(first, mine, other), jnp.where(first, other, mine)
    heads = 4
    for h in range(heads):
        src = low if h < heads // 2 else high
        base = (h % (heads // 2)) * 256
        for c in range(2):
            out_ref[pl.ds(c * heads + h, rows, stride=2 * heads), :] = src[:, base + c * 128:base + (c + 1) * 128]


def join_wide(idx, mine, other, heads):
    dim, width = mine.shape
    bd = 128
    spec = rows_spec(bd, width)
    out = pl.pallas_call(
        join_wide_kernel,
        grid=(dim // bd,),
        in_specs=[pl.BlockSpec(memory_space=pltpu.SMEM), spec, spec],
        out_specs=rows_spec(bd * 8, 128),
        out_shape=jax.ShapeDtypeStruct((dim * 8, 128), F32),
        compiler_params=params(),
        cost_estimate=COST,
        name="join_wide",
    )(idx, mine, other)
    return out.reshape(dim, 2, heads, 128).transpose(0, 2, 1, 3).reshape(dim, heads, 256)


def join_pair_kernel(idx_ref, a_ref, b_ref, c_ref, d_ref, *refs, last):
    core0 = idx_ref[0] % 2 == 0

    def ordered(mine, other):
        return jnp.where(core0, mine, other), jnp.where(core0, other, mine)

    rows = a_ref.shape[0] - (8 if last else 0)
    outs = refs[2:] if last else refs
    for n, src in enumerate(ordered(a_ref[...] + b_ref[...], c_ref[...] + d_ref[...])):
        for c in range(2):
            outs[n][pl.ds(c, rows, stride=2), :] = src[0:rows, c * 128:(c + 1) * 128]
        if last:
            gain_ref = outs[n + 2]
            for c in range(gain_ref.shape[0] // 128):
                gain_ref[c * 128:(c + 1) * 128] = src[rows + c // 2, c % 2 * 128:(c % 2 + 1) * 128]


def join_pair(idx, parts, dim, begun=()):
    rows, width = parts[0].shape
    last = bool(begun)
    bd = rows - 8 if last else dim // 3
    steps = rows // bd
    first = dim // bd - 1 if last else 0
    out_spec = pl.BlockSpec((bd * 2, 128), lambda i: (i + first, 0))
    part_spec = whole(parts[0].shape) if last else rows_spec(bd, width)
    pair = [jax.ShapeDtypeStruct((dim * 2, 128), F32)] * 2
    return pl.pallas_call(
        functools.partial(join_pair_kernel, last=last),
        grid=(steps,),
        in_specs=[pl.BlockSpec(memory_space=pltpu.SMEM)] + [part_spec] * 4 + [pl.BlockSpec(memory_space=pl.ANY)] * len(begun),
        out_specs=[out_spec] * 2 + [whole((dim,))] * len(begun),
        out_shape=pair + [jax.ShapeDtypeStruct((dim,), F32)] * len(begun),
        input_output_aliases={5: 0, 6: 1} if last else {},
        compiler_params=params(),
        cost_estimate=COST,
        name="join_last" if last else "join_first",
    )(idx, *parts, *begun)


def join_rows_kernel(idx_ref, mine_ref, other_ref, out_ref):
    first = idx_ref[0] % 2 == 0
    out_ref[...] = jnp.where(first == (pl.program_id(0) == 0), mine_ref[...], other_ref[...])


def join_rows(idx, mine, other):
    rows, dim = mine.shape
    br = 256
    steps = rows // br
    spec = pl.BlockSpec((br, dim), lambda w, i: (i, 0))
    return pl.pallas_call(
        join_rows_kernel,
        grid=(2, steps),
        in_specs=[pl.BlockSpec(memory_space=pltpu.SMEM), spec, spec],
        out_specs=pl.BlockSpec((br, dim), lambda w, i: (w * steps + i, 0)),
        out_shape=jax.ShapeDtypeStruct((rows * 2, dim), F32),
        compiler_params=params(),
        cost_estimate=COST,
        name="join_rows",
    )(idx, mine, other)


def solution(mesh):
    across = [(0, 2), (2, 0), (1, 3), (3, 1)]
    beside = [(0, 1), (1, 0), (2, 3), (3, 2)]

    def permute(value, pairs):
        return lax.ppermute(value, "cp", pairs)

    def local_step(x_in, positions, dy_out, w_query, w_key, w_value, w_out, w_pre, w_post):
        batch, tokens, dim = x_in.shape
        heads, hd = w_query.shape[1], w_query.shape[2]
        half = hd // 2
        idx = lax.axis_index("cp").astype(jnp.int32).reshape(1)
        wq = w_query.reshape(dim, heads * hd)
        wk = w_key.reshape(dim, hd)
        wv = w_value.reshape(dim, hd)
        wo = w_out.reshape(heads * hd, dim)
        x = x_in.reshape(tokens, dim)
        dy = dy_out.reshape(tokens, dim)
        gain_pre = w_pre
        gain_post = w_post
        inv_freq = ROPE_BASE ** (jnp.arange(half, dtype=F32) * (-2.0 / hd))
        angles = positions.reshape(tokens, 1).astype(F32) * inv_freq
        cosine, sine = jnp.cos(angles), jnp.sin(angles)

        dy_high = permute(dy, [(2, 0), (3, 1)])
        act_t, q, own, near, far, mid, o, out, lse = forward(x, gain_pre, wk, wv, wq, cosine, sine, heads)
        dy_low = permute(dy, [(0, 2), (1, 3)])
        partner_o = permute(o, across)
        y, d_out, dz, stat, dgain_post = post(o, out, lse, x, dy, wo, gain_post)

        down, dq, dwq_part = backward(q, d_out, stat, own, near, far, mid, cosine, sine, act_t)
        dwq_mine = dwq_part + permute(dwq_part, across)
        dwq_other = permute(dwq_mine, beside)
        dwo = grad_wo(idx, o, dz, partner_o, dy_high, dy_low, wo, gain_post)
        dwo_mine = dwo[0] + permute(dwo[1], beside)
        dwo_other = permute(dwo_mine, beside)
        dx, *dwkv = tail(idx, down, cosine, sine, act_t, dq, wq, wk, wv, x, dy, gain_pre, dgain_post)
        theirs_in, mine_in = permute(dwkv[1], beside), permute(dwkv[0], beside)
        split = dim // 3 * 2
        pieces = []
        for rows in (slice(0, split), slice(split, None)):
            chip_mine = dwkv[0][rows] + theirs_in[rows]
            chip_other = dwkv[1][rows] + mine_in[rows]
            far_mine = permute(chip_mine, across)
            pieces.append((chip_mine, far_mine, chip_other, permute(far_mine, beside)))
        begun = join_pair(idx, pieces[0], dim)
        dwk_full, dwv_full, dpre_full, dpost_full = join_pair(idx, pieces[1], dim, tuple(begun))

        dwo_full = join_rows(idx, dwo_mine, dwo_other)
        dwq_full = join_wide(idx, dwq_mine, dwq_other, heads)
        return (
            y.reshape(batch, tokens, dim),
            dx.reshape(batch, tokens, dim),
            dwq_full,
            dwk_full.reshape(dim, 1, hd),
            dwv_full.reshape(dim, 1, hd),
            dwo_full.reshape(heads, hd, dim),
            dpre_full,
            dpost_full,
        )

    seq_spec = P("dp", "cp", None)
    in_specs = (seq_spec, P("dp", "cp"), seq_spec, P(), P(), P(), P(), P(), P())
    out_specs = (seq_spec, seq_spec, P("dp", None, None), P("dp", None, None), P("dp", None, None), P("dp", None, None), P("dp"), P("dp"))
    return jax.shard_map(local_step, mesh=mesh, in_specs=in_specs, out_specs=out_specs, check_vma=False)
```

```python
import functools
import math

import jax
import jax.numpy as jnp
from jax import lax
from jax.experimental import pallas as pl
from jax.experimental.pallas import tpu as pltpu
from jax.sharding import PartitionSpec as P


NORM_EPS = 1e-6
SOFT_CAP = 50.0
QUERY_SCALE = 144.0
ROPE_BASE = 10000.0
LOG2E = math.log2(math.e)
CAP2 = SOFT_CAP * LOG2E
INV_CAP = 1.0 / SOFT_CAP


F32 = jnp.float32
BF16 = jnp.bfloat16
VMEM_LIMIT = 60 * 1024 * 1024

NT = (((1,), (1,)), ((), ()))
NN = (((1,), (0,)), ((), ()))


def dot(a, b, dims=NN):
    return lax.dot_general(a, b, dims, preferred_element_type=F32)


def params():
    return pltpu.CompilerParams(vmem_limit_bytes=VMEM_LIMIT)


def whole(shape):
    zeros = (0,) * len(shape)
    return pl.BlockSpec(shape, lambda *_: zeros)


def rows_spec(rows, width):
    return pl.BlockSpec((rows, width), lambda i: (i, 0))


def stack_spec(depth, rows, width):
    return pl.BlockSpec((depth, rows, width), lambda i: (0, i, 0))


COST = pl.CostEstimate(flops=10**10, bytes_accessed=10**7, transcendentals=0)


def to_sibling(rank, src, dst, send, recv):
    return pltpu.make_async_remote_copy(
        src_ref=src, dst_ref=dst, send_sem=send, recv_sem=recv,
        device_id={"cp": rank + 1 - 2 * (rank % 2)}, device_id_type=pl.DeviceIdType.MESH,
    )


def rope(values, cosine, sine):
    half = cosine.shape[-1]
    first, second = values[:, :half], values[:, half:]
    return jnp.concatenate([first * cosine - second * sine, second * cosine + first * sine], axis=-1)


def forward_tile(q_ref, acc_ref, sum_ref, k, v, masked):
    heads, bq, _ = q_ref.shape
    bk = k.shape[0]
    if masked:
        keep = lax.broadcasted_iota(jnp.int32, (bq, bk), 1) <= lax.broadcasted_iota(jnp.int32, (bq, bk), 0)
    for h in range(heads):
        s = dot(q_ref[h], k, NT)
        p = jnp.exp2(jnp.tanh(s * INV_CAP) * CAP2)
        if masked:
            p = jnp.where(keep, p, 0.0)
        part = p[:, 0:128]
        for c in range(128, bk, 128):
            part = part + p[:, c:c + 128]
        sum_ref[h] += part
        acc_ref[h] += dot(p.astype(BF16), v)


def forward_kernel(x_ref, gain_ref, wk_ref, wv_ref, wq_ref, cos_ref, sin_ref,
                   at_ref, q_ref, own_ref, near_ref, far_ref, mid_ref, o_ref, out_ref, lse_ref,
                   a_s, own_s, near_s, far_s, mid_s, acc_s, sum_s,
                   far_send, far_recv, near_send, near_recv, mid_send, mid_recv):
    heads, tokens, hd = q_ref.shape
    bt = x_ref.shape[0]
    tiles = tokens // bt
    big = 2 * bt
    rank = lax.axis_index("cp")
    core = rank % 2
    i = pl.program_id(0)
    across = {"cp": (rank + 2) % 4}
    mesh_id = pl.DeviceIdType.MESH

    def rows_of(t, size=bt):
        return pl.ds(pl.multiple_of(t * size, size), size)

    def far_copy(t):
        rows = rows_of(t)
        return pltpu.make_async_remote_copy(
            src_ref=own_s.at[:, rows, :], dst_ref=far_s.at[:, rows, :], send_sem=far_send.at[t], recv_sem=far_recv.at[t],
            device_id=across, device_id_type=mesh_id,
        )

    def near_copy(t):
        rows = rows_of(t)
        return to_sibling(rank, own_s.at[:, rows, :], near_s.at[:, rows, :], near_send.at[t], near_recv.at[t])

    def mid_copy(c):
        rows = rows_of(c, big)
        return to_sibling(rank, far_s.at[:, rows, :], mid_s.at[:, rows, :], mid_send.at[c], mid_recv.at[c])

    @pl.when(i == 0)
    def _():
        barrier = pltpu.get_barrier_semaphore()
        for other in (across, {"cp": rank + 1 - 2 * core}):
            pl.semaphore_signal(barrier, inc=1, device_id=other, device_id_type=mesh_id)
        pl.semaphore_wait(barrier, 2)

    @pl.when(i < tiles)
    def _():
        rows = rows_of(i)
        x = x_ref[...].astype(F32)
        rstd = lax.rsqrt(jnp.mean(x * x, axis=-1, keepdims=True) + NORM_EPS)
        a = (x * rstd * (1.0 + gain_ref[...][None, :])).astype(BF16)
        a_s[rows, :] = a
        own_s[0, rows, :] = rope(dot(a, wk_ref[...]).astype(BF16).astype(F32), cos_ref[rows, :], sin_ref[rows, :]).astype(BF16)
        own_s[1, rows, :] = dot(a, wv_ref[...]).astype(BF16)
        pl.when(rank < 2)(lambda: far_copy(i).start())
        pl.when(core == 0)(lambda: near_copy(i).start())
        at_ref[...] = a.T

    def attend(t, kv_ref, start, size, masked):
        rows, keys = rows_of(t), pl.ds(pl.multiple_of(start, bt), size)
        forward_tile(q_ref.at[:, rows, :], acc_s.at[:, rows, :], sum_s.at[:, rows, :],
                     kv_ref[0, keys, :], kv_ref[1, keys, :], masked)

    @pl.when(jnp.logical_and(i >= tiles, i < 2 * tiles))
    def _():
        t = i - tiles
        rows = rows_of(t)
        a = a_s[rows, :]
        scale = QUERY_SCALE ** -0.5
        for h in range(heads):
            q = dot(a, wq_ref[:, h * hd:(h + 1) * hd]).astype(BF16).astype(F32)
            q_ref[h, rows, :] = (rope(q, cos_ref[rows, :], sin_ref[rows, :]) * scale).astype(BF16)
        acc_s[:, rows, :] = jnp.zeros((heads, bt, hd), F32)
        sum_s[:, rows, :] = jnp.zeros((heads, bt, 128), F32)
        attend(t, own_s, t * bt, bt, True)

        def own_step(j, _):
            attend(t, own_s, j * bt, bt, False)
            return 0

        lax.fori_loop(0, t, own_step, 0)

        @pl.when(core == 1)
        def _():
            pl.when(t == 0)(lambda: [near_copy(n).wait_recv() for n in range(tiles)] and None)

            def near_step(j, _):
                attend(t, near_s, j * big, big, False)
                return 0

            lax.fori_loop(0, tokens // big, near_step, 0)

    chunks = tokens // big
    c = i - 2 * tiles

    def far_chunk(kv_ref, start):
        def step(t, _):
            attend(t, kv_ref, start, big, False)
            return 0

        lax.fori_loop(0, tiles, step, 0)

    @pl.when(jnp.logical_and(rank >= 2, jnp.logical_and(c >= 0, c < chunks)))
    def _():
        far_copy(2 * c).wait_recv()
        far_copy(2 * c + 1).wait_recv()
        mid_copy(c).start()
        far_chunk(far_s, c * big)

    @pl.when(jnp.logical_and(rank >= 2, jnp.logical_and(c >= chunks, c < 2 * chunks)))
    def _():
        mid_copy(c - chunks).wait_recv()
        far_chunk(mid_s, (c - chunks) * big)

    last = i - 2 * tiles - 2 * chunks

    @pl.when(last >= 0)
    def _():
        rows = rows_of(last)
        lane = lax.broadcasted_iota(jnp.int32, (bt, 128), 1)
        lse = jnp.zeros((bt, 128), F32)
        for h in range(heads):
            total = jnp.sum(sum_s[h, rows, :], axis=-1, keepdims=True)
            lse = jnp.where(lane == h, jnp.log2(total), lse)
            out = acc_s[h, rows, :] / total
            out_ref[h] = out
            o_ref[:, h * hd:(h + 1) * hd] = out.astype(BF16)
        lse_ref[...] = lse
        for dst, src in ((own_ref, own_s), (near_ref, near_s), (far_ref, far_s), (mid_ref, mid_s)):
            dst[...] = src[:, rows, :]

    @pl.when(last == tiles - 1)
    def _():
        pl.when(rank < 2)(lambda: [far_copy(n).wait_send() for n in range(tiles)] and None)
        pl.when(core == 0)(lambda: [near_copy(n).wait_send() for n in range(tiles)] and None)
        pl.when(rank >= 2)(lambda: [mid_copy(n).wait_send() for n in range(chunks)] and None)


def forward(x, gain, wk, wv, wq, cosine, sine, heads):
    tokens, dim = x.shape
    hd = wk.shape[1]
    bt = 256
    tiles = tokens // bt
    chunks = tiles // 2
    done = 2 * tiles + 2 * chunks
    dma = pltpu.SemaphoreType.DMA
    early = lambda i: jnp.minimum(i, tiles - 1)
    late = lambda i: jnp.maximum(i - done, 0)
    kv_shape = jax.ShapeDtypeStruct((2, tokens, hd), BF16)
    kv_out = pl.BlockSpec((2, bt, hd), lambda i: (0, late(i), 0))
    return pl.pallas_call(
        forward_kernel,
        grid=(done + tiles,),
        in_specs=[
            pl.BlockSpec((bt, dim), lambda i: (early(i), 0)),
            whole(gain.shape),
            whole(wk.shape),
            whole(wv.shape),
            whole(wq.shape),
            whole(cosine.shape),
            whole(sine.shape),
        ],
        out_specs=[
            pl.BlockSpec((dim, bt), lambda i: (0, early(i))),
            whole((heads, tokens, hd)),
            kv_out,
            kv_out,
            kv_out,
            kv_out,
            pl.BlockSpec((bt, heads * hd), lambda i: (late(i), 0)),
            pl.BlockSpec((heads, bt, hd), lambda i: (0, late(i), 0)),
            pl.BlockSpec((bt, 128), lambda i: (late(i), 0)),
        ],
        out_shape=[
            jax.ShapeDtypeStruct((dim, tokens), BF16),
            jax.ShapeDtypeStruct((heads, tokens, hd), BF16),
            kv_shape,
            kv_shape,
            kv_shape,
            kv_shape,
            jax.ShapeDtypeStruct((tokens, heads * hd), BF16),
            jax.ShapeDtypeStruct((heads, tokens, hd), F32),
            jax.ShapeDtypeStruct((tokens, 128), F32),
        ],
        scratch_shapes=[pltpu.VMEM((tokens, dim), BF16)] + [pltpu.VMEM((2, tokens, hd), BF16)] * 4 + [
            pltpu.VMEM((heads, tokens, hd), F32),
            pltpu.VMEM((heads, tokens, 128), F32),
            dma((tiles,)),
            dma((tiles,)),
            dma((tiles,)),
            dma((tiles,)),
            dma((chunks,)),
            dma((chunks,)),
        ],
        compiler_params=pltpu.CompilerParams(vmem_limit_bytes=VMEM_LIMIT, collective_id=2, has_side_effects=True),
        cost_estimate=COST,
        name="forward",
    )(x, gain, wk, wv, wq, cosine, sine)


def post_norm(o, wo, gain, dy):
    z = dot(o, wo).astype(BF16).astype(F32)
    rstd = lax.rsqrt(jnp.mean(z * z, axis=-1, keepdims=True) + NORM_EPS)
    unit = z * rstd
    g = dy * gain
    dz = (rstd * (g - unit * jnp.mean(g * unit, axis=-1, keepdims=True))).astype(BF16)
    return unit, dz


def post_kernel(o_ref, out_ref, lse_ref, x_ref, dy_ref, wo_ref, gain_ref, y_ref, do_ref, dz_ref, stat_ref, dgain_ref):
    heads, bq, hd = out_ref.shape
    gain = 1.0 + gain_ref[...][None, :]
    dy = dy_ref[...].astype(F32)
    unit, dz = post_norm(o_ref[...], wo_ref[...], gain, dy)
    y_ref[...] = (x_ref[...].astype(F32) + (unit * gain).astype(BF16).astype(F32)).astype(BF16)
    dz_ref[...] = dz

    @pl.when(pl.program_id(0) == 0)
    def _():
        dgain_ref[...] = jnp.zeros_like(dgain_ref)

    dgain_ref[...] += jnp.sum(dy * unit, axis=0, keepdims=True)
    lane = lax.broadcasted_iota(jnp.int32, (bq, 128), 1)
    stat = lse_ref[...]
    for h in range(heads):
        d_out = dot(dz, wo_ref[h * hd:(h + 1) * hd, :], NT).astype(BF16)
        do_ref[h] = d_out
        delta = jnp.sum(d_out.astype(F32) * out_ref[h], axis=-1, keepdims=True)
        stat = jnp.where(lane == heads + h, delta, stat)
    stat_ref[...] = stat.T[0:8, :]


def post(o, out, lse, x, dy, wo, gain):
    heads, tokens, hd = out.shape
    dim = x.shape[1]
    bq = 256
    rows3 = stack_spec(heads, bq, hd)
    rows2 = lambda width: rows_spec(bq, width)
    return pl.pallas_call(
        post_kernel,
        grid=(tokens // bq,),
        in_specs=[rows2(heads * hd), rows3, rows2(128), rows2(dim), rows2(dim), whole(wo.shape), whole((dim,))],
        out_specs=[rows2(dim), rows3, rows2(dim), pl.BlockSpec((8, bq), lambda i: (0, i)), whole((1, dim))],
        out_shape=[
            jax.ShapeDtypeStruct((tokens, dim), BF16),
            jax.ShapeDtypeStruct((heads, tokens, hd), BF16),
            jax.ShapeDtypeStruct((tokens, dim), BF16),
            jax.ShapeDtypeStruct((8, tokens), F32),
            jax.ShapeDtypeStruct((1, dim), F32),
        ],
        compiler_params=params(),
        cost_estimate=COST,
        name="post",
    )(o, out, lse, x, dy, wo, gain)


def grad_wo_kernel(idx_ref, o_ref, dz_ref, po_ref, pdy_low_ref, pdy_high_ref, wo_ref, gain_ref, mine_ref, theirs_ref, pdz_ref):
    _, width = o_ref.shape
    bt = pdy_low_ref.shape[0]
    hd = 256
    i = pl.program_id(0)
    rows = pl.ds(pl.multiple_of(i * bt, bt), bt)
    dy = jnp.where(idx_ref[0] >= 2, pdy_high_ref[...], pdy_low_ref[...]).astype(F32)
    pdz_ref[rows, :] = post_norm(po_ref[rows, :], wo_ref[...], 1.0 + gain_ref[...][None, :], dy)[1]

    @pl.when(i == pl.num_programs(0) - 1)
    def _():
        core = idx_ref[0] % 2
        per = width // hd // 2
        for which, ref in enumerate((mine_ref, theirs_ref)):
            for hh in range(per):
                cols = pl.ds(pl.multiple_of((((core + which) % 2) * per + hh) * hd, hd), hd)
                ref[hh * hd:(hh + 1) * hd, :] = dot(o_ref[:, cols].T, dz_ref[...]) + dot(po_ref[:, cols].T, pdz_ref[...])


def grad_wo(idx, o, dz, po, pdy_low, pdy_high, wo, gain):
    tokens, width = o.shape
    dim = dz.shape[1]
    bt = 256
    rows2 = rows_spec(bt, dim)
    return pl.pallas_call(
        grad_wo_kernel,
        grid=(tokens // bt,),
        in_specs=[
            pl.BlockSpec(memory_space=pltpu.SMEM),
            whole(o.shape),
            whole(dz.shape),
            whole(o.shape),
            rows2,
            rows2,
            whole(wo.shape),
            whole((dim,)),
        ],
        out_specs=[whole((width // 2, dim))] * 2,
        out_shape=[jax.ShapeDtypeStruct((width // 2, dim), F32)] * 2,
        scratch_shapes=[pltpu.VMEM((tokens, dim), BF16)],
        compiler_params=params(),
        cost_estimate=COST,
        name="grad_wo",
    )(idx, o, dz, po, pdy_low, pdy_high, wo, gain)


def backward_tile(q_ref, do_ref, stat_ref, dqt_ref, dkv_ref, k, v, kt, start, bq, masked):
    heads = q_ref.shape[0]
    bk = k.shape[0]
    rows = pl.ds(pl.multiple_of(start, 128), bq)
    if masked:
        keep = lax.broadcasted_iota(jnp.int32, (bk, bq), 0) <= lax.broadcasted_iota(jnp.int32, (bk, bq), 1)
    for h in range(heads):
        q = q_ref[h, rows, :]
        d_out = do_ref[h, rows, :]
        t = jnp.tanh(dot(k, q, NT) * INV_CAP)
        p = jnp.exp2(t * CAP2 - stat_ref[h:h + 1, rows])
        if masked:
            p = jnp.where(keep, p, 0.0)
        dp = dot(v, d_out, NT)
        ds = (p * (dp - stat_ref[heads + h:heads + h + 1, rows]) * (1.0 - t * t)).astype(BF16)
        dkv_ref[1] += dot(p.astype(BF16), d_out)
        dkv_ref[0] += dot(ds, q)
        dqt_ref[h, :, rows] += dot(kt, ds)


def backward_kernel(q_ref, do_ref, stat_ref, own_ref, near_ref, far_ref, mid_ref, cos_ref, sin_ref, at_ref,
                    down_hbm, dq_hbm, dwq_hbm,
                    down_ref, dq_ref, dwq_ref, out_sem, dqt_s, near_out, near_in, mid_out, mid_in, far_out, far_in, dwq_out, dwq_in,
                    near_send, near_recv, mid_send, mid_recv, far_send, far_recv, dwq_send, dwq_recv):
    heads, tokens, hd = q_ref.shape
    half = hd // 2
    bk = own_ref.shape[1]
    big = 2 * bk
    tiles = tokens // bk
    rank = lax.axis_index("cp")
    core = rank % 2
    i = pl.program_id(0)
    across = {"cp": (rank + 2) % 4}
    mesh_id = pl.DeviceIdType.MESH

    def near_copy(n):
        return to_sibling(rank, near_out.at[n], near_in.at[n], near_send.at[n], near_recv.at[n])

    def mid_copy(n):
        return to_sibling(rank, mid_out.at[n], mid_in.at[n], mid_send.at[n], mid_recv.at[n])

    def far_copy(n):
        return pltpu.make_async_remote_copy(
            src_ref=far_out.at[n], dst_ref=far_in.at[n], send_sem=far_send.at[n], recv_sem=far_recv.at[n],
            device_id=across, device_id_type=mesh_id,
        )

    @pl.when(i == 0)
    def _():
        dqt_s[...] = jnp.zeros_like(dqt_s)
        barrier = pltpu.get_barrier_semaphore()
        for other in (across, {"cp": rank + 1 - 2 * core}):
            pl.semaphore_signal(barrier, inc=1, device_id=other, device_id_type=mesh_id)
        pl.semaphore_wait(barrier, 2)

    def all_rows(kv_ref, dkv_ref):
        k, v = kv_ref[0], kv_ref[1]
        kt = k.T

        def step(j, _):
            backward_tile(q_ref, do_ref, stat_ref, dqt_s, dkv_ref, k, v, kt, j * big, big, False)
            return 0

        lax.fori_loop(0, tokens // big, step, 0)

    @pl.when(jnp.logical_and(rank >= 2, i < tiles))
    def _():
        mine = mid_out.at[i]
        mine[...] = jnp.zeros_like(mine)
        all_rows(mid_ref, mine)
        mid_copy(i).start()

    @pl.when(jnp.logical_and(rank >= 2, jnp.logical_and(i >= tiles, i < 2 * tiles)))
    def _():
        n = i - tiles
        mid_copy(n).wait()
        mine = far_out.at[n]
        mine[...] = mid_in[n]
        all_rows(far_ref, mine)
        far_copy(n).start()

    n = i - 2 * tiles

    @pl.when(jnp.logical_and(core == 1, n >= 0))
    def _():
        mine = near_out.at[n]
        mine[...] = jnp.zeros_like(mine)
        all_rows(near_ref, mine)
        near_copy(n).start()

    @pl.when(n >= 0)
    def _():
        down = down_ref.at[:, pl.ds(pl.multiple_of(n * bk, bk), bk), :]
        down[...] = jnp.zeros_like(down)
        k, v = own_ref[0], own_ref[1]
        kt = k.T
        backward_tile(q_ref, do_ref, stat_ref, dqt_s, down, k, v, kt, n * bk, bk, True)

        def own_step(j, _):
            backward_tile(q_ref, do_ref, stat_ref, dqt_s, down, k, v, kt, j * bk, bk, False)
            return 0

        lax.fori_loop(n + 1, tiles, own_step, 0)

    @pl.when(n == tiles - 1)
    def _():
        scale = QUERY_SCALE ** -0.5
        for h in range(heads):
            dq = dqt_s[h].T
            first, second = dq[:, :half], dq[:, half:]
            cosine, sine = cos_ref[...], sin_ref[...]
            dq_ref[:, h * hd:h * hd + half] = ((first * cosine + second * sine) * scale).astype(BF16)
            dq_ref[:, h * hd + half:(h + 1) * hd] = ((second * cosine - first * sine) * scale).astype(BF16)
        written = [pltpu.make_async_copy(src, dst, out_sem.at[slot]) for slot, (src, dst) in
                   enumerate(((dq_ref, dq_hbm), (dwq_ref, dwq_hbm), (down_ref, down_hbm)))]
        written[0].start()
        dim, width = dwq_ref.shape
        bd = dim // 3

        def product(out_ref, which):
            dq = dq_ref[:, pl.ds(pl.multiple_of((core + which) % 2 * width, width), width)]

            def rows_step(r, _):
                rows = pl.ds(pl.multiple_of(r * bd, bd), bd)
                out_ref[rows, :] = dot(at_ref[rows, :], dq)
                return 0

            lax.fori_loop(0, dim // bd, rows_step, 0)

        product(dwq_out, 1)
        copy = to_sibling(rank, dwq_out, dwq_in, dwq_send, dwq_recv)
        copy.start()
        product(dwq_ref, 0)

        def gather(copy_of, arrived):
            for t in range(tiles):
                copy_of(t).wait_recv()
                down_ref[:, t * bk:(t + 1) * bk, :] += arrived[t]

        def left(copy_of):
            for t in range(tiles):
                copy_of(t).wait_send()

        pl.when(core == 1)(lambda: left(near_copy))
        pl.when(core == 0)(lambda: gather(near_copy, near_in))
        copy.wait()
        dwq_ref[...] += dwq_in[...]
        written[1].start()

        @pl.when(rank < 2)
        def _():
            gather(far_copy, far_in)
            written[2].start()

        @pl.when(rank >= 2)
        def _():
            written[2].start()
            left(far_copy)

        for copy_out in written:
            copy_out.wait()


def backward(q, d_out, stat, own, near, far, mid, cosine, sine, at):
    heads, tokens, hd = q.shape
    dim = at.shape[0]
    bk = 256
    tiles = tokens // bk
    width = heads * hd // 2

    def phase(first):
        return pl.BlockSpec((2, bk, hd), lambda i: (0, jnp.clip(i - first, 0, tiles - 1), 0))

    def held(array):
        zeros = (0,) * array.ndim
        return pl.BlockSpec(array.shape, lambda i: zeros, pipeline_mode=pl.Buffered(1))

    dma = pltpu.SemaphoreType.DMA
    return pl.pallas_call(
        backward_kernel,
        grid=(3 * tiles,),
        in_specs=[
            held(q),
            held(d_out),
            held(stat),
            phase(2 * tiles),
            phase(2 * tiles),
            phase(tiles),
            phase(0),
            held(cosine),
            held(sine),
            held(at),
        ],
        out_specs=[pl.BlockSpec(memory_space=pl.ANY)] * 3,
        out_shape=[
            jax.ShapeDtypeStruct((2, tokens, hd), F32),
            jax.ShapeDtypeStruct((tokens, heads * hd), BF16),
            jax.ShapeDtypeStruct((dim, width), F32),
        ],
        scratch_shapes=[
            pltpu.VMEM((2, tokens, hd), F32),
            pltpu.VMEM((tokens, heads * hd), BF16),
            pltpu.VMEM((dim, width), F32),
            dma((3,)),
            pltpu.VMEM((heads, hd, tokens), F32),
        ] + [pltpu.VMEM((tiles, 2, bk, hd), F32)] * 6
        + [pltpu.VMEM((dim, width), F32)] * 2 + [dma((tiles,))] * 6 + [dma] * 2,
        compiler_params=pltpu.CompilerParams(vmem_limit_bytes=VMEM_LIMIT, collective_id=0, has_side_effects=True),
        cost_estimate=COST,
        name="backward",
    )(q, d_out, stat, own, near, far, mid, cosine, sine, at)


def tail_kernel(idx_ref, down_ref, cos_ref, sin_ref, at_ref, dq_ref, wq_ref, wk_ref, wv_ref,
                x_ref, dy_ref, gain_ref, dpost_ref, dx_ref, mine_ref, theirs_ref, dgain_ref):
    _, half = cos_ref.shape
    dim = x_ref.shape[1]
    i = pl.program_id(0)
    dk = down_ref[0]
    cosine, sine = cos_ref[...], sin_ref[...]
    first, second = dk[:, :half], dk[:, half:]
    dk = jnp.concatenate([first * cosine + second * sine, second * cosine - first * sine], axis=1).astype(BF16)
    dv = down_ref[1].astype(BF16)

    @pl.when(i == 0)
    def _():
        mine_ref[...] = jnp.zeros_like(mine_ref)
        theirs_ref[...] = jnp.zeros_like(theirs_ref)
        dgain_ref[...] = jnp.zeros_like(dgain_ref)

    core = idx_ref[0] % 2
    at = at_ref[...]
    is_core0 = core == 0
    mine = jnp.where(is_core0, dk, dv)
    theirs = jnp.where(is_core0, dv, dk)
    mine_ref[0:dim, :] += dot(at, mine)
    theirs_ref[0:dim, :] += dot(at, theirs)
    da = dot(dq_ref[...], wq_ref[...], NT) + dot(dk, wk_ref[...], NT) + dot(dv, wv_ref[...], NT)
    x = x_ref[...].astype(F32)
    rstd = lax.rsqrt(jnp.mean(x * x, axis=-1, keepdims=True) + NORM_EPS)
    unit = x * rstd
    dgain_ref[...] += jnp.sum(da * unit, axis=0, keepdims=True)
    g = da * (1.0 + gain_ref[...][None, :])
    dx = rstd * (g - unit * jnp.mean(g * unit, axis=-1, keepdims=True))
    dx_ref[...] = (dy_ref[...].astype(F32) + dx).astype(BF16)

    @pl.when(i == pl.num_programs(0) - 1)
    def _():
        dpre, dpost = dgain_ref[...], dpost_ref[...]
        for ref, row in ((mine_ref, jnp.where(is_core0, dpre, dpost)), (theirs_ref, jnp.where(is_core0, dpost, dpre))):
            for c in range(dim // 128):
                ref[dim + c // 2:dim + c // 2 + 1, c % 2 * 128:(c % 2 + 1) * 128] = row[:, c * 128:(c + 1) * 128]


def tail(idx, down, cosine, sine, at, dq, wq, wk, wv, x, dy, gain, dpost):
    tokens, dim = x.shape
    hd = wk.shape[1]
    width = wq.shape[1]
    bt = 256
    kv_spec = stack_spec(2, bt, hd)
    rope_spec = rows_spec(bt, hd // 2)
    rows2 = rows_spec(bt, dim)
    return pl.pallas_call(
        tail_kernel,
        grid=(tokens // bt,),
        in_specs=[
            pl.BlockSpec(memory_space=pltpu.SMEM),
            kv_spec,
            rope_spec,
            rope_spec,
            pl.BlockSpec((dim, bt), lambda i: (0, i)),
            rows_spec(bt, width),
            whole(wq.shape),
            whole(wk.shape),
            whole(wv.shape),
            rows2,
            rows2,
            whole((dim,)),
            whole((1, dim)),
        ],
        out_specs=[rows2, whole((dim + 8, hd)), whole((dim + 8, hd))],
        out_shape=[
            jax.ShapeDtypeStruct((tokens, dim), BF16),
            jax.ShapeDtypeStruct((dim + 8, hd), F32),
            jax.ShapeDtypeStruct((dim + 8, hd), F32),
        ],
        scratch_shapes=[pltpu.VMEM((1, dim), F32)],
        compiler_params=params(),
        cost_estimate=COST,
        name="tail",
    )(idx, down, cosine, sine, at, dq, wq, wk, wv, x, dy, gain, dpost)


def join_wide_kernel(idx_ref, mine_ref, other_ref, out_ref):
    first = idx_ref[0] % 2 == 0
    rows, _ = mine_ref.shape
    mine, other = mine_ref[...], other_ref[...]
    low, high = jnp.where(first, mine, other), jnp.where(first, other, mine)
    heads = 4
    for h in range(heads):
        src = low if h < heads // 2 else high
        base = (h % (heads // 2)) * 256
        for c in range(2):
            out_ref[pl.ds(c * heads + h, rows, stride=2 * heads), :] = src[:, base + c * 128:base + (c + 1) * 128]


def join_wide(idx, mine, other, heads):
    dim, width = mine.shape
    bd = 128
    spec = rows_spec(bd, width)
    out = pl.pallas_call(
        join_wide_kernel,
        grid=(dim // bd,),
        in_specs=[pl.BlockSpec(memory_space=pltpu.SMEM), spec, spec],
        out_specs=rows_spec(bd * 8, 128),
        out_shape=jax.ShapeDtypeStruct((dim * 8, 128), F32),
        compiler_params=params(),
        cost_estimate=COST,
        name="join_wide",
    )(idx, mine, other)
    return out.reshape(dim, 2, heads, 128).transpose(0, 2, 1, 3).reshape(dim, heads, 256)


def join_pair_kernel(idx_ref, a_ref, b_ref, c_ref, d_ref, *refs, last):
    core0 = idx_ref[0] % 2 == 0

    def ordered(mine, other):
        return jnp.where(core0, mine, other), jnp.where(core0, other, mine)

    rows = a_ref.shape[0] - (8 if last else 0)
    outs = refs[2:] if last else refs
    for n, src in enumerate(ordered(a_ref[...] + b_ref[...], c_ref[...] + d_ref[...])):
        for c in range(2):
            outs[n][pl.ds(c, rows, stride=2), :] = src[0:rows, c * 128:(c + 1) * 128]
        if last:
            gain_ref = outs[n + 2]
            for c in range(gain_ref.shape[0] // 128):
                gain_ref[c * 128:(c + 1) * 128] = src[rows + c // 2, c % 2 * 128:(c % 2 + 1) * 128]


def join_pair(idx, parts, dim, begun=()):
    rows, width = parts[0].shape
    last = bool(begun)
    bd = rows - 8 if last else dim // 3
    steps = rows // bd
    first = dim // bd - 1 if last else 0
    out_spec = pl.BlockSpec((bd * 2, 128), lambda i: (i + first, 0))
    part_spec = whole(parts[0].shape) if last else rows_spec(bd, width)
    pair = [jax.ShapeDtypeStruct((dim * 2, 128), F32)] * 2
    return pl.pallas_call(
        functools.partial(join_pair_kernel, last=last),
        grid=(steps,),
        in_specs=[pl.BlockSpec(memory_space=pltpu.SMEM)] + [part_spec] * 4 + [pl.BlockSpec(memory_space=pl.ANY)] * len(begun),
        out_specs=[out_spec] * 2 + [whole((dim,))] * len(begun),
        out_shape=pair + [jax.ShapeDtypeStruct((dim,), F32)] * len(begun),
        input_output_aliases={5: 0, 6: 1} if last else {},
        compiler_params=params(),
        cost_estimate=COST,
        name="join_last" if last else "join_first",
    )(idx, *parts, *begun)


def join_rows_kernel(idx_ref, mine_ref, other_ref, out_ref):
    first = idx_ref[0] % 2 == 0
    out_ref[...] = jnp.where(first == (pl.program_id(0) == 0), mine_ref[...], other_ref[...])


def join_rows(idx, mine, other):
    rows, dim = mine.shape
    br = 256
    steps = rows // br
    spec = pl.BlockSpec((br, dim), lambda w, i: (i, 0))
    return pl.pallas_call(
        join_rows_kernel,
        grid=(2, steps),
        in_specs=[pl.BlockSpec(memory_space=pltpu.SMEM), spec, spec],
        out_specs=pl.BlockSpec((br, dim), lambda w, i: (w * steps + i, 0)),
        out_shape=jax.ShapeDtypeStruct((rows * 2, dim), F32),
        compiler_params=params(),
        cost_estimate=COST,
        name="join_rows",
    )(idx, mine, other)


def solution(mesh):
    across = [(0, 2), (2, 0), (1, 3), (3, 1)]
    beside = [(0, 1), (1, 0), (2, 3), (3, 2)]

    def permute(value, pairs):
        return lax.ppermute(value, "cp", pairs)

    def local_step(x_in, positions, dy_out, w_query, w_key, w_value, w_out, w_pre, w_post):
        batch, tokens, dim = x_in.shape
        heads, hd = w_query.shape[1], w_query.shape[2]
        half = hd // 2
        idx = lax.axis_index("cp").astype(jnp.int32).reshape(1)
        wq = w_query.reshape(dim, heads * hd)
        wk = w_key.reshape(dim, hd)
        wv = w_value.reshape(dim, hd)
        wo = w_out.reshape(heads * hd, dim)
        x = x_in.reshape(tokens, dim)
        dy = dy_out.reshape(tokens, dim)
        gain_pre = w_pre
        gain_post = w_post
        inv_freq = ROPE_BASE ** (jnp.arange(half, dtype=F32) * (-2.0 / hd))
        angles = positions.reshape(tokens, 1).astype(F32) * inv_freq
        cosine, sine = jnp.cos(angles), jnp.sin(angles)

        dy_high = permute(dy, [(2, 0), (3, 1)])
        act_t, q, own, near, far, mid, o, out, lse = forward(x, gain_pre, wk, wv, wq, cosine, sine, heads)
        dy_low = permute(dy, [(0, 2), (1, 3)])
        partner_o = permute(o, across)
        y, d_out, dz, stat, dgain_post = post(o, out, lse, x, dy, wo, gain_post)

        down, dq, dwq_part = backward(q, d_out, stat, own, near, far, mid, cosine, sine, act_t)
        dwq_mine = dwq_part + permute(dwq_part, across)
        dwq_other = permute(dwq_mine, beside)
        dwo = grad_wo(idx, o, dz, partner_o, dy_high, dy_low, wo, gain_post)
        dwo_in = permute(dwo[1], beside)
        dwo_mine = dwo[0] + dwo_in
        dwo_other = permute(dwo_mine, beside)
        dx, *dwkv = tail(idx, down, cosine, sine, act_t, dq, wq, wk, wv, x, dy, gain_pre, dgain_post)
        theirs_in, mine_in = permute(dwkv[1], beside), permute(dwkv[0], beside)
        split = dim // 3 * 2
        pieces = []
        for rows in (slice(0, split), slice(split, None)):
            chip_mine = dwkv[0][rows] + theirs_in[rows]
            chip_other = dwkv[1][rows] + mine_in[rows]
            far_mine = permute(chip_mine, across)
            pieces.append((chip_mine, far_mine, chip_other, permute(far_mine, beside)))
        begun = join_pair(idx, pieces[0], dim)
        dwk_full, dwv_full, dpre_full, dpost_full = join_pair(idx, pieces[1], dim, tuple(begun))

        dwo_full = join_rows(idx, dwo_mine, dwo_other)
        dwq_full = join_wide(idx, dwq_mine, dwq_other, heads)
        return (
            y.reshape(batch, tokens, dim),
            dx.reshape(batch, tokens, dim),
            dwq_full,
            dwk_full.reshape(dim, 1, hd),
            dwv_full.reshape(dim, 1, hd),
            dwo_full.reshape(heads, hd, dim),
            dpre_full,
            dpost_full,
        )

    seq_spec = P("dp", "cp", None)
    in_specs = (seq_spec, P("dp", "cp"), seq_spec, P(), P(), P(), P(), P(), P())
    out_specs = (seq_spec, seq_spec, P("dp", None, None), P("dp", None, None), P("dp", None, None), P("dp", None, None), P("dp"), P("dp"))
    return jax.shard_map(local_step, mesh=mesh, in_specs=in_specs, out_specs=out_specs, check_vma=False)
```

```python
import functools
import math

import jax
import jax.numpy as jnp
from jax import lax
from jax.experimental import pallas as pl
from jax.experimental.pallas import tpu as pltpu
from jax.sharding import PartitionSpec as P


NORM_EPS = 1e-6
SOFT_CAP = 50.0
QUERY_SCALE = 144.0
ROPE_BASE = 10000.0
LOG2E = math.log2(math.e)
CAP2 = SOFT_CAP * LOG2E
INV_CAP = 1.0 / SOFT_CAP
SHIFT2 = 20.0


F32 = jnp.float32
BF16 = jnp.bfloat16
VMEM_LIMIT = 60 * 1024 * 1024

NT = (((1,), (1,)), ((), ()))
NN = (((1,), (0,)), ((), ()))


def dot(a, b, dims=NN):
    return lax.dot_general(a, b, dims, preferred_element_type=F32)


def params():
    return pltpu.CompilerParams(vmem_limit_bytes=VMEM_LIMIT)


def whole(shape):
    zeros = (0,) * len(shape)
    return pl.BlockSpec(shape, lambda *_: zeros)


def rows_spec(rows, width):
    return pl.BlockSpec((rows, width), lambda i: (i, 0))


def stack_spec(depth, rows, width):
    return pl.BlockSpec((depth, rows, width), lambda i: (0, i, 0))


COST = pl.CostEstimate(flops=10**10, bytes_accessed=10**7, transcendentals=0)


def to_sibling(rank, src, dst, send, recv):
    return pltpu.make_async_remote_copy(
        src_ref=src, dst_ref=dst, send_sem=send, recv_sem=recv,
        device_id={"cp": rank + 1 - 2 * (rank % 2)}, device_id_type=pl.DeviceIdType.MESH,
    )


def rope(values, cosine, sine):
    half = cosine.shape[-1]
    first, second = values[:, :half], values[:, half:]
    return jnp.concatenate([first * cosine - second * sine, second * cosine + first * sine], axis=-1)


def forward_tile(q_ref, acc_ref, sum_ref, k, v, masked):
    heads, bq, _ = q_ref.shape
    bk = k.shape[0]
    if masked:
        keep = lax.broadcasted_iota(jnp.int32, (bq, bk), 1) <= lax.broadcasted_iota(jnp.int32, (bq, bk), 0)
    for h in range(heads):
        s = dot(q_ref[h], k, NT)
        p = jnp.exp2(jnp.tanh(s * INV_CAP) * CAP2 - SHIFT2)
        if masked:
            p = jnp.where(keep, p, 0.0)
        part = p[:, 0:128]
        for c in range(128, bk, 128):
            part = part + p[:, c:c + 128]
        sum_ref[h] += part
        acc_ref[h] += dot(p.astype(BF16), v)


def forward_kernel(x_ref, gain_ref, wk_ref, wv_ref, wq_ref, cos_ref, sin_ref,
                   at_ref, q_ref, own_ref, near_ref, far_ref, mid_ref, o_ref, out_ref, lse_ref,
                   a_s, own_s, near_s, far_s, mid_s, acc_s, sum_s,
                   far_send, far_recv, near_send, near_recv, mid_send, mid_recv):
    heads, tokens, hd = q_ref.shape
    bt = x_ref.shape[0]
    tiles = tokens // bt
    big = 2 * bt
    rank = lax.axis_index("cp")
    core = rank % 2
    i = pl.program_id(0)
    across = {"cp": (rank + 2) % 4}
    mesh_id = pl.DeviceIdType.MESH

    def rows_of(t, size=bt):
        return pl.ds(pl.multiple_of(t * size, size), size)

    def far_copy(t):
        rows = rows_of(t)
        return pltpu.make_async_remote_copy(
            src_ref=own_s.at[:, rows, :], dst_ref=far_s.at[:, rows, :], send_sem=far_send.at[t], recv_sem=far_recv.at[t],
            device_id=across, device_id_type=mesh_id,
        )

    def near_copy(t):
        rows = rows_of(t)
        return to_sibling(rank, own_s.at[:, rows, :], near_s.at[:, rows, :], near_send.at[t], near_recv.at[t])

    def mid_copy(c):
        rows = rows_of(c, big)
        return to_sibling(rank, far_s.at[:, rows, :], mid_s.at[:, rows, :], mid_send.at[c], mid_recv.at[c])

    @pl.when(i == 0)
    def _():
        barrier = pltpu.get_barrier_semaphore()
        for other in (across, {"cp": rank + 1 - 2 * core}):
            pl.semaphore_signal(barrier, inc=1, device_id=other, device_id_type=mesh_id)
        pl.semaphore_wait(barrier, 2)

    @pl.when(i < tiles)
    def _():
        rows = rows_of(i)
        x = x_ref[...].astype(F32)
        rstd = lax.rsqrt(jnp.mean(x * x, axis=-1, keepdims=True) + NORM_EPS)
        a = (x * rstd * (1.0 + gain_ref[...][None, :])).astype(BF16)
        a_s[rows, :] = a
        own_s[0, rows, :] = rope(dot(a, wk_ref[...]).astype(BF16).astype(F32), cos_ref[rows, :], sin_ref[rows, :]).astype(BF16)
        own_s[1, rows, :] = dot(a, wv_ref[...]).astype(BF16)
        pl.when(rank < 2)(lambda: far_copy(i).start())
        pl.when(core == 0)(lambda: near_copy(i).start())
        at_ref[...] = a.T

    def attend(t, kv_ref, start, size, masked):
        rows, keys = rows_of(t), pl.ds(pl.multiple_of(start, bt), size)
        forward_tile(q_ref.at[:, rows, :], acc_s.at[:, rows, :], sum_s.at[:, rows, :],
                     kv_ref[0, keys, :], kv_ref[1, keys, :], masked)

    @pl.when(jnp.logical_and(i >= tiles, i < 2 * tiles))
    def _():
        t = i - tiles
        rows = rows_of(t)
        a = a_s[rows, :]
        scale = QUERY_SCALE ** -0.5
        for h in range(heads):
            q = dot(a, wq_ref[:, h * hd:(h + 1) * hd]).astype(BF16).astype(F32)
            q_ref[h, rows, :] = (rope(q, cos_ref[rows, :], sin_ref[rows, :]) * scale).astype(BF16)
        acc_s[:, rows, :] = jnp.zeros((heads, bt, hd), F32)
        sum_s[:, rows, :] = jnp.zeros((heads, bt, 128), F32)
        attend(t, own_s, t * bt, bt, True)

        def own_step(j, _):
            attend(t, own_s, j * bt, bt, False)
            return 0

        lax.fori_loop(0, t, own_step, 0)

        @pl.when(core == 1)
        def _():
            pl.when(t == 0)(lambda: [near_copy(n).wait_recv() for n in range(tiles)] and None)

            def near_step(j, _):
                attend(t, near_s, j * big, big, False)
                return 0

            lax.fori_loop(0, tokens // big, near_step, 0)

    chunks = tokens // big
    c = i - 2 * tiles

    def far_chunk(kv_ref, start):
        def step(t, _):
            attend(t, kv_ref, start, big, False)
            return 0

        lax.fori_loop(0, tiles, step, 0)

    @pl.when(jnp.logical_and(rank >= 2, jnp.logical_and(c >= 0, c < chunks)))
    def _():
        far_copy(2 * c).wait_recv()
        far_copy(2 * c + 1).wait_recv()
        mid_copy(c).start()
        far_chunk(far_s, c * big)

    @pl.when(jnp.logical_and(rank >= 2, jnp.logical_and(c >= chunks, c < 2 * chunks)))
    def _():
        mid_copy(c - chunks).wait_recv()
        far_chunk(mid_s, (c - chunks) * big)

    last = i - 2 * tiles - 2 * chunks

    @pl.when(last >= 0)
    def _():
        rows = rows_of(last)
        lane = lax.broadcasted_iota(jnp.int32, (bt, 128), 1)
        lse = jnp.zeros((bt, 128), F32)
        for h in range(heads):
            total = jnp.sum(sum_s[h, rows, :], axis=-1, keepdims=True)
            lse = jnp.where(lane == h, jnp.log2(total) + SHIFT2, lse)
            out = acc_s[h, rows, :] / total
            out_ref[h] = out
            o_ref[:, h * hd:(h + 1) * hd] = out.astype(BF16)
        lse_ref[...] = lse
        for dst, src in ((own_ref, own_s), (near_ref, near_s), (far_ref, far_s), (mid_ref, mid_s)):
            dst[...] = src[:, rows, :]

    @pl.when(last == tiles - 1)
    def _():
        pl.when(rank < 2)(lambda: [far_copy(n).wait_send() for n in range(tiles)] and None)
        pl.when(core == 0)(lambda: [near_copy(n).wait_send() for n in range(tiles)] and None)
        pl.when(rank >= 2)(lambda: [mid_copy(n).wait_send() for n in range(chunks)] and None)


def forward(x, gain, wk, wv, wq, cosine, sine, heads):
    tokens, dim = x.shape
    hd = wk.shape[1]
    bt = 256
    tiles = tokens // bt
    chunks = tiles // 2
    done = 2 * tiles + 2 * chunks
    dma = pltpu.SemaphoreType.DMA
    early = lambda i: jnp.minimum(i, tiles - 1)
    late = lambda i: jnp.maximum(i - done, 0)
    kv_shape = jax.ShapeDtypeStruct((2, tokens, hd), BF16)
    kv_out = pl.BlockSpec((2, bt, hd), lambda i: (0, late(i), 0))
    return pl.pallas_call(
        forward_kernel,
        grid=(done + tiles,),
        in_specs=[
            pl.BlockSpec((bt, dim), lambda i: (early(i), 0)),
            whole(gain.shape),
            whole(wk.shape),
            whole(wv.shape),
            whole(wq.shape),
            whole(cosine.shape),
            whole(sine.shape),
        ],
        out_specs=[
            pl.BlockSpec((dim, bt), lambda i: (0, early(i))),
            whole((heads, tokens, hd)),
            kv_out,
            kv_out,
            kv_out,
            kv_out,
            pl.BlockSpec((bt, heads * hd), lambda i: (late(i), 0)),
            pl.BlockSpec((heads, bt, hd), lambda i: (0, late(i), 0)),
            pl.BlockSpec((bt, 128), lambda i: (late(i), 0)),
        ],
        out_shape=[
            jax.ShapeDtypeStruct((dim, tokens), BF16),
            jax.ShapeDtypeStruct((heads, tokens, hd), BF16),
            kv_shape,
            kv_shape,
            kv_shape,
            kv_shape,
            jax.ShapeDtypeStruct((tokens, heads * hd), BF16),
            jax.ShapeDtypeStruct((heads, tokens, hd), F32),
            jax.ShapeDtypeStruct((tokens, 128), F32),
        ],
        scratch_shapes=[pltpu.VMEM((tokens, dim), BF16)] + [pltpu.VMEM((2, tokens, hd), BF16)] * 4 + [
            pltpu.VMEM((heads, tokens, hd), F32),
            pltpu.VMEM((heads, tokens, 128), F32),
            dma((tiles,)),
            dma((tiles,)),
            dma((tiles,)),
            dma((tiles,)),
            dma((chunks,)),
            dma((chunks,)),
        ],
        compiler_params=pltpu.CompilerParams(vmem_limit_bytes=VMEM_LIMIT, collective_id=2, has_side_effects=True),
        cost_estimate=COST,
        name="forward",
    )(x, gain, wk, wv, wq, cosine, sine)


def post_norm(o, wo, gain, dy):
    z = dot(o, wo).astype(BF16).astype(F32)
    rstd = lax.rsqrt(jnp.mean(z * z, axis=-1, keepdims=True) + NORM_EPS)
    unit = z * rstd
    g = dy * gain
    dz = (rstd * (g - unit * jnp.mean(g * unit, axis=-1, keepdims=True))).astype(BF16)
    return unit, dz


def post_kernel(o_ref, out_ref, lse_ref, x_ref, dy_ref, wo_ref, gain_ref, y_ref, do_ref, dz_ref, stat_ref, dgain_ref):
    heads, bq, hd = out_ref.shape
    gain = 1.0 + gain_ref[...][None, :]
    dy = dy_ref[...].astype(F32)
    unit, dz = post_norm(o_ref[...], wo_ref[...], gain, dy)
    y_ref[...] = (x_ref[...].astype(F32) + (unit * gain).astype(BF16).astype(F32)).astype(BF16)
    dz_ref[...] = dz

    @pl.when(pl.program_id(0) == 0)
    def _():
        dgain_ref[...] = jnp.zeros_like(dgain_ref)

    dgain_ref[...] += jnp.sum(dy * unit, axis=0, keepdims=True)
    lane = lax.broadcasted_iota(jnp.int32, (bq, 128), 1)
    stat = lse_ref[...]
    for h in range(heads):
        d_out = dot(dz, wo_ref[h * hd:(h + 1) * hd, :], NT).astype(BF16)
        do_ref[h] = d_out
        delta = jnp.sum(d_out.astype(F32) * out_ref[h], axis=-1, keepdims=True)
        stat = jnp.where(lane == heads + h, delta, stat)
    stat_ref[...] = stat.T[0:8, :]


def post(o, out, lse, x, dy, wo, gain):
    heads, tokens, hd = out.shape
    dim = x.shape[1]
    bq = 256
    rows3 = stack_spec(heads, bq, hd)
    rows2 = lambda width: rows_spec(bq, width)
    return pl.pallas_call(
        post_kernel,
        grid=(tokens // bq,),
        in_specs=[rows2(heads * hd), rows3, rows2(128), rows2(dim), rows2(dim), whole(wo.shape), whole((dim,))],
        out_specs=[rows2(dim), rows3, rows2(dim), pl.BlockSpec((8, bq), lambda i: (0, i)), whole((1, dim))],
        out_shape=[
            jax.ShapeDtypeStruct((tokens, dim), BF16),
            jax.ShapeDtypeStruct((heads, tokens, hd), BF16),
            jax.ShapeDtypeStruct((tokens, dim), BF16),
            jax.ShapeDtypeStruct((8, tokens), F32),
            jax.ShapeDtypeStruct((1, dim), F32),
        ],
        compiler_params=params(),
        cost_estimate=COST,
        name="post",
    )(o, out, lse, x, dy, wo, gain)


def grad_wo_kernel(idx_ref, o_ref, dz_ref, po_ref, pdy_low_ref, pdy_high_ref, wo_ref, gain_ref, mine_ref, theirs_ref, pdz_ref):
    _, width = o_ref.shape
    bt = pdy_low_ref.shape[0]
    hd = 256
    i = pl.program_id(0)
    rows = pl.ds(pl.multiple_of(i * bt, bt), bt)
    dy = jnp.where(idx_ref[0] >= 2, pdy_high_ref[...], pdy_low_ref[...]).astype(F32)
    pdz_ref[rows, :] = post_norm(po_ref[rows, :], wo_ref[...], 1.0 + gain_ref[...][None, :], dy)[1]

    @pl.when(i == pl.num_programs(0) - 1)
    def _():
        core = idx_ref[0] % 2
        per = width // hd // 2
        for which, ref in enumerate((mine_ref, theirs_ref)):
            for hh in range(per):
                cols = pl.ds(pl.multiple_of((((core + which) % 2) * per + hh) * hd, hd), hd)
                ref[hh * hd:(hh + 1) * hd, :] = dot(o_ref[:, cols].T, dz_ref[...]) + dot(po_ref[:, cols].T, pdz_ref[...])


def grad_wo(idx, o, dz, po, pdy_low, pdy_high, wo, gain):
    tokens, width = o.shape
    dim = dz.shape[1]
    bt = 256
    rows2 = rows_spec(bt, dim)
    return pl.pallas_call(
        grad_wo_kernel,
        grid=(tokens // bt,),
        in_specs=[
            pl.BlockSpec(memory_space=pltpu.SMEM),
            whole(o.shape),
            whole(dz.shape),
            whole(o.shape),
            rows2,
            rows2,
            whole(wo.shape),
            whole((dim,)),
        ],
        out_specs=[whole((width // 2, dim))] * 2,
        out_shape=[jax.ShapeDtypeStruct((width // 2, dim), F32)] * 2,
        scratch_shapes=[pltpu.VMEM((tokens, dim), BF16)],
        compiler_params=params(),
        cost_estimate=COST,
        name="grad_wo",
    )(idx, o, dz, po, pdy_low, pdy_high, wo, gain)


def backward_tile(q_ref, do_ref, stat_ref, dqt_ref, dkv_ref, k, v, kt, start, bq, masked):
    heads = q_ref.shape[0]
    bk = k.shape[0]
    rows = pl.ds(pl.multiple_of(start, 128), bq)
    if masked:
        keep = lax.broadcasted_iota(jnp.int32, (bk, bq), 0) <= lax.broadcasted_iota(jnp.int32, (bk, bq), 1)
    for h in range(heads):
        q = q_ref[h, rows, :]
        d_out = do_ref[h, rows, :]
        t = jnp.tanh(dot(k, q, NT) * INV_CAP)
        p = jnp.exp2(t * CAP2 - stat_ref[h:h + 1, rows])
        if masked:
            p = jnp.where(keep, p, 0.0)
        dp = dot(v, d_out, NT)
        ds = (p * (dp - stat_ref[heads + h:heads + h + 1, rows]) * (1.0 - t * t)).astype(BF16)
        dkv_ref[1] += dot(p.astype(BF16), d_out)
        dkv_ref[0] += dot(ds, q)
        dqt_ref[h, :, rows] += dot(kt, ds)


def backward_kernel(q_ref, do_ref, stat_ref, own_ref, near_ref, far_ref, mid_ref, cos_ref, sin_ref, at_ref,
                    down_hbm, dq_hbm, dwq_hbm,
                    down_ref, dq_ref, dwq_ref, out_sem, dqt_s, near_out, near_in, mid_out, mid_in, far_out, far_in, dwq_out, dwq_in,
                    near_send, near_recv, mid_send, mid_recv, far_send, far_recv, dwq_send, dwq_recv):
    heads, tokens, hd = q_ref.shape
    half = hd // 2
    bk = own_ref.shape[1]
    big = 2 * bk
    tiles = tokens // bk
    rank = lax.axis_index("cp")
    core = rank % 2
    i = pl.program_id(0)
    across = {"cp": (rank + 2) % 4}
    mesh_id = pl.DeviceIdType.MESH

    def near_copy(n):
        return to_sibling(rank, near_out.at[n], near_in.at[n], near_send.at[n], near_recv.at[n])

    def mid_copy(n):
        return to_sibling(rank, mid_out.at[n], mid_in.at[n], mid_send.at[n], mid_recv.at[n])

    def far_copy(n):
        return pltpu.make_async_remote_copy(
            src_ref=far_out.at[n], dst_ref=far_in.at[n], send_sem=far_send.at[n], recv_sem=far_recv.at[n],
            device_id=across, device_id_type=mesh_id,
        )

    @pl.when(i == 0)
    def _():
        dqt_s[...] = jnp.zeros_like(dqt_s)
        barrier = pltpu.get_barrier_semaphore()
        for other in (across, {"cp": rank + 1 - 2 * core}):
            pl.semaphore_signal(barrier, inc=1, device_id=other, device_id_type=mesh_id)
        pl.semaphore_wait(barrier, 2)

    def all_rows(kv_ref, dkv_ref):
        k, v = kv_ref[0], kv_ref[1]
        kt = k.T

        def step(j, _):
            backward_tile(q_ref, do_ref, stat_ref, dqt_s, dkv_ref, k, v, kt, j * big, big, False)
            return 0

        lax.fori_loop(0, tokens // big, step, 0)

    @pl.when(jnp.logical_and(rank >= 2, i < tiles))
    def _():
        mine = mid_out.at[i]
        mine[...] = jnp.zeros_like(mine)
        all_rows(mid_ref, mine)
        mid_copy(i).start()

    @pl.when(jnp.logical_and(rank >= 2, jnp.logical_and(i >= tiles, i < 2 * tiles)))
    def _():
        n = i - tiles
        mid_copy(n).wait()
        mine = far_out.at[n]
        mine[...] = mid_in[n]
        all_rows(far_ref, mine)
        far_copy(n).start()

    n = i - 2 * tiles

    @pl.when(jnp.logical_and(core == 1, n >= 0))
    def _():
        mine = near_out.at[n]
        mine[...] = jnp.zeros_like(mine)
        all_rows(near_ref, mine)
        near_copy(n).start()

    @pl.when(n >= 0)
    def _():
        down = down_ref.at[:, pl.ds(pl.multiple_of(n * bk, bk), bk), :]
        down[...] = jnp.zeros_like(down)
        k, v = own_ref[0], own_ref[1]
        kt = k.T
        backward_tile(q_ref, do_ref, stat_ref, dqt_s, down, k, v, kt, n * bk, bk, True)

        def own_step(j, _):
            backward_tile(q_ref, do_ref, stat_ref, dqt_s, down, k, v, kt, j * bk, bk, False)
            return 0

        lax.fori_loop(n + 1, tiles, own_step, 0)

    @pl.when(n == tiles - 1)
    def _():
        scale = QUERY_SCALE ** -0.5
        for h in range(heads):
            dq = dqt_s[h].T
            first, second = dq[:, :half], dq[:, half:]
            cosine, sine = cos_ref[...], sin_ref[...]
            dq_ref[:, h * hd:h * hd + half] = ((first * cosine + second * sine) * scale).astype(BF16)
            dq_ref[:, h * hd + half:(h + 1) * hd] = ((second * cosine - first * sine) * scale).astype(BF16)
        written = [pltpu.make_async_copy(src, dst, out_sem.at[slot]) for slot, (src, dst) in
                   enumerate(((dq_ref, dq_hbm), (dwq_ref, dwq_hbm), (down_ref, down_hbm)))]
        written[0].start()
        dim, width = dwq_ref.shape
        bd = dim // 3

        def product(out_ref, which):
            dq = dq_ref[:, pl.ds(pl.multiple_of((core + which) % 2 * width, width), width)]

            def rows_step(r, _):
                rows = pl.ds(pl.multiple_of(r * bd, bd), bd)
                out_ref[rows, :] = dot(at_ref[rows, :], dq)
                return 0

            lax.fori_loop(0, dim // bd, rows_step, 0)

        product(dwq_out, 1)
        copy = to_sibling(rank, dwq_out, dwq_in, dwq_send, dwq_recv)
        copy.start()
        product(dwq_ref, 0)

        def gather(copy_of, arrived):
            for t in range(tiles):
                copy_of(t).wait_recv()
                down_ref[:, t * bk:(t + 1) * bk, :] += arrived[t]

        def left(copy_of):
            for t in range(tiles):
                copy_of(t).wait_send()

        pl.when(core == 1)(lambda: left(near_copy))
        pl.when(core == 0)(lambda: gather(near_copy, near_in))
        copy.wait()
        dwq_ref[...] += dwq_in[...]
        written[1].start()

        @pl.when(rank < 2)
        def _():
            gather(far_copy, far_in)
            written[2].start()

        @pl.when(rank >= 2)
        def _():
            written[2].start()
            left(far_copy)

        for copy_out in written:
            copy_out.wait()


def backward(q, d_out, stat, own, near, far, mid, cosine, sine, at):
    heads, tokens, hd = q.shape
    dim = at.shape[0]
    bk = 256
    tiles = tokens // bk
    width = heads * hd // 2

    def phase(first):
        return pl.BlockSpec((2, bk, hd), lambda i: (0, jnp.clip(i - first, 0, tiles - 1), 0))

    def held(array):
        zeros = (0,) * array.ndim
        return pl.BlockSpec(array.shape, lambda i: zeros, pipeline_mode=pl.Buffered(1))

    dma = pltpu.SemaphoreType.DMA
    return pl.pallas_call(
        backward_kernel,
        grid=(3 * tiles,),
        in_specs=[
            held(q),
            held(d_out),
            held(stat),
            phase(2 * tiles),
            phase(2 * tiles),
            phase(tiles),
            phase(0),
            held(cosine),
            held(sine),
            held(at),
        ],
        out_specs=[pl.BlockSpec(memory_space=pl.ANY)] * 3,
        out_shape=[
            jax.ShapeDtypeStruct((2, tokens, hd), F32),
            jax.ShapeDtypeStruct((tokens, heads * hd), BF16),
            jax.ShapeDtypeStruct((dim, width), F32),
        ],
        scratch_shapes=[
            pltpu.VMEM((2, tokens, hd), F32),
            pltpu.VMEM((tokens, heads * hd), BF16),
            pltpu.VMEM((dim, width), F32),
            dma((3,)),
            pltpu.VMEM((heads, hd, tokens), F32),
        ] + [pltpu.VMEM((tiles, 2, bk, hd), F32)] * 6
        + [pltpu.VMEM((dim, width), F32)] * 2 + [dma((tiles,))] * 6 + [dma] * 2,
        compiler_params=pltpu.CompilerParams(vmem_limit_bytes=VMEM_LIMIT, collective_id=0, has_side_effects=True),
        cost_estimate=COST,
        name="backward",
    )(q, d_out, stat, own, near, far, mid, cosine, sine, at)


def tail_kernel(idx_ref, down_ref, cos_ref, sin_ref, at_ref, dq_ref, wq_ref, wk_ref, wv_ref,
                x_ref, dy_ref, gain_ref, dpost_ref, dx_ref, mine_ref, theirs_ref, dgain_ref):
    _, half = cos_ref.shape
    dim = x_ref.shape[1]
    i = pl.program_id(0)
    dk = down_ref[0]
    cosine, sine = cos_ref[...], sin_ref[...]
    first, second = dk[:, :half], dk[:, half:]
    dk = jnp.concatenate([first * cosine + second * sine, second * cosine - first * sine], axis=1).astype(BF16)
    dv = down_ref[1].astype(BF16)

    @pl.when(i == 0)
    def _():
        mine_ref[...] = jnp.zeros_like(mine_ref)
        theirs_ref[...] = jnp.zeros_like(theirs_ref)
        dgain_ref[...] = jnp.zeros_like(dgain_ref)

    core = idx_ref[0] % 2
    at = at_ref[...]
    is_core0 = core == 0
    mine = jnp.where(is_core0, dk, dv)
    theirs = jnp.where(is_core0, dv, dk)
    mine_ref[0:dim, :] += dot(at, mine)
    theirs_ref[0:dim, :] += dot(at, theirs)
    da = dot(dq_ref[...], wq_ref[...], NT) + dot(dk, wk_ref[...], NT) + dot(dv, wv_ref[...], NT)
    x = x_ref[...].astype(F32)
    rstd = lax.rsqrt(jnp.mean(x * x, axis=-1, keepdims=True) + NORM_EPS)
    unit = x * rstd
    dgain_ref[...] += jnp.sum(da * unit, axis=0, keepdims=True)
    g = da * (1.0 + gain_ref[...][None, :])
    dx = rstd * (g - unit * jnp.mean(g * unit, axis=-1, keepdims=True))
    dx_ref[...] = (dy_ref[...].astype(F32) + dx).astype(BF16)

    @pl.when(i == pl.num_programs(0) - 1)
    def _():
        dpre, dpost = dgain_ref[...], dpost_ref[...]
        for ref, row in ((mine_ref, jnp.where(is_core0, dpre, dpost)), (theirs_ref, jnp.where(is_core0, dpost, dpre))):
            for c in range(dim // 128):
                ref[dim + c // 2:dim + c // 2 + 1, c % 2 * 128:(c % 2 + 1) * 128] = row[:, c * 128:(c + 1) * 128]


def tail(idx, down, cosine, sine, at, dq, wq, wk, wv, x, dy, gain, dpost):
    tokens, dim = x.shape
    hd = wk.shape[1]
    width = wq.shape[1]
    bt = 256
    kv_spec = stack_spec(2, bt, hd)
    rope_spec = rows_spec(bt, hd // 2)
    rows2 = rows_spec(bt, dim)
    return pl.pallas_call(
        tail_kernel,
        grid=(tokens // bt,),
        in_specs=[
            pl.BlockSpec(memory_space=pltpu.SMEM),
            kv_spec,
            rope_spec,
            rope_spec,
            pl.BlockSpec((dim, bt), lambda i: (0, i)),
            rows_spec(bt, width),
            whole(wq.shape),
            whole(wk.shape),
            whole(wv.shape),
            rows2,
            rows2,
            whole((dim,)),
            whole((1, dim)),
        ],
        out_specs=[rows2, whole((dim + 8, hd)), whole((dim + 8, hd))],
        out_shape=[
            jax.ShapeDtypeStruct((tokens, dim), BF16),
            jax.ShapeDtypeStruct((dim + 8, hd), F32),
            jax.ShapeDtypeStruct((dim + 8, hd), F32),
        ],
        scratch_shapes=[pltpu.VMEM((1, dim), F32)],
        compiler_params=params(),
        cost_estimate=COST,
        name="tail",
    )(idx, down, cosine, sine, at, dq, wq, wk, wv, x, dy, gain, dpost)


def join_wide_kernel(idx_ref, mine_ref, other_ref, out_ref):
    first = idx_ref[0] % 2 == 0
    rows, _ = mine_ref.shape
    mine, other = mine_ref[...], other_ref[...]
    low, high = jnp.where(first, mine, other), jnp.where(first, other, mine)
    heads = 4
    for h in range(heads):
        src = low if h < heads // 2 else high
        base = (h % (heads // 2)) * 256
        for c in range(2):
            out_ref[pl.ds(c * heads + h, rows, stride=2 * heads), :] = src[:, base + c * 128:base + (c + 1) * 128]


def join_wide(idx, mine, other, heads):
    dim, width = mine.shape
    bd = 128
    spec = rows_spec(bd, width)
    out = pl.pallas_call(
        join_wide_kernel,
        grid=(dim // bd,),
        in_specs=[pl.BlockSpec(memory_space=pltpu.SMEM), spec, spec],
        out_specs=rows_spec(bd * 8, 128),
        out_shape=jax.ShapeDtypeStruct((dim * 8, 128), F32),
        compiler_params=params(),
        cost_estimate=COST,
        name="join_wide",
    )(idx, mine, other)
    return out.reshape(dim, 2, heads, 128).transpose(0, 2, 1, 3).reshape(dim, heads, 256)


def join_pair_kernel(idx_ref, a_ref, b_ref, c_ref, d_ref, *refs, last, held):
    core0 = idx_ref[0] % 2 == 0

    def ordered(mine, other):
        return jnp.where(core0, mine, other), jnp.where(core0, other, mine)

    rows = a_ref.shape[0] - (8 if last else 0)
    outs = refs[held:]
    for n, src in enumerate(ordered(a_ref[...] + b_ref[...], c_ref[...] + d_ref[...])):
        for c in range(2):
            outs[n][pl.ds(c, rows, stride=2), :] = src[0:rows, c * 128:(c + 1) * 128]
        if last:
            gain_ref = outs[n + 2]
            for c in range(gain_ref.shape[0] // 128):
                gain_ref[c * 128:(c + 1) * 128] = src[rows + c // 2, c % 2 * 128:(c % 2 + 1) * 128]


def join_pair(idx, parts, dim, start, begun=()):
    rows, width = parts[0].shape
    last = start + rows > dim
    bd = rows - 8 if last else 256
    first = start // bd
    out_spec = pl.BlockSpec((bd * 2, 128), lambda i: (i + first, 0))
    part_spec = whole(parts[0].shape) if last else rows_spec(bd, width)
    gains = 2 if last else 0
    return pl.pallas_call(
        functools.partial(join_pair_kernel, last=last, held=len(begun)),
        grid=(rows // bd,),
        in_specs=[pl.BlockSpec(memory_space=pltpu.SMEM)] + [part_spec] * 4 + [pl.BlockSpec(memory_space=pl.ANY)] * len(begun),
        out_specs=[out_spec] * 2 + [whole((dim,))] * gains,
        out_shape=[jax.ShapeDtypeStruct((dim * 2, 128), F32)] * 2 + [jax.ShapeDtypeStruct((dim,), F32)] * gains,
        input_output_aliases={5: 0, 6: 1} if begun else {},
        compiler_params=params(),
        cost_estimate=COST,
    )(idx, *parts, *begun)


def join_rows_kernel(idx_ref, mine_ref, other_ref, out_ref):
    first = idx_ref[0] % 2 == 0
    out_ref[...] = jnp.where(first == (pl.program_id(0) == 0), mine_ref[...], other_ref[...])


def join_rows(idx, mine, other):
    rows, dim = mine.shape
    br = 256
    steps = rows // br
    spec = pl.BlockSpec((br, dim), lambda w, i: (i, 0))
    return pl.pallas_call(
        join_rows_kernel,
        grid=(2, steps),
        in_specs=[pl.BlockSpec(memory_space=pltpu.SMEM), spec, spec],
        out_specs=pl.BlockSpec((br, dim), lambda w, i: (w * steps + i, 0)),
        out_shape=jax.ShapeDtypeStruct((rows * 2, dim), F32),
        compiler_params=params(),
        cost_estimate=COST,
        name="join_rows",
    )(idx, mine, other)


def solution(mesh):
    across = [(0, 2), (2, 0), (1, 3), (3, 1)]
    beside = [(0, 1), (1, 0), (2, 3), (3, 2)]

    def permute(value, pairs):
        return lax.ppermute(value, "cp", pairs)

    def local_step(x_in, positions, dy_out, w_query, w_key, w_value, w_out, w_pre, w_post):
        batch, tokens, dim = x_in.shape
        heads, hd = w_query.shape[1], w_query.shape[2]
        half = hd // 2
        idx = lax.axis_index("cp").astype(jnp.int32).reshape(1)
        wq = w_query.reshape(dim, heads * hd)
        wk = w_key.reshape(dim, hd)
        wv = w_value.reshape(dim, hd)
        wo = w_out.reshape(heads * hd, dim)
        x = x_in.reshape(tokens, dim)
        dy = dy_out.reshape(tokens, dim)
        gain_pre = w_pre
        gain_post = w_post
        inv_freq = ROPE_BASE ** (jnp.arange(half, dtype=F32) * (-2.0 / hd))
        angles = positions.reshape(tokens, 1).astype(F32) * inv_freq
        cosine, sine = jnp.cos(angles), jnp.sin(angles)

        dy_high = permute(dy, [(2, 0), (3, 1)])
        act_t, q, own, near, far, mid, o, out, lse = forward(x, gain_pre, wk, wv, wq, cosine, sine, heads)
        dy_low = permute(dy, [(0, 2), (1, 3)])
        partner_o = permute(o, across)
        y, d_out, dz, stat, dgain_post = post(o, out, lse, x, dy, wo, gain_post)

        down, dq, dwq_part = backward(q, d_out, stat, own, near, far, mid, cosine, sine, act_t)
        dwq_mine = dwq_part + permute(dwq_part, across)
        dwq_other = permute(dwq_mine, beside)
        dwo = grad_wo(idx, o, dz, partner_o, dy_high, dy_low, wo, gain_post)
        dwo_in = permute(dwo[1], beside)
        dwo_mine = dwo[0] + dwo_in
        dwo_other = permute(dwo_mine, beside)
        dx, *dwkv = tail(idx, down, cosine, sine, act_t, dq, wq, wk, wv, x, dy, gain_pre, dgain_post)
        theirs_in, mine_in = permute(dwkv[1], beside), permute(dwkv[0], beside)
        bounds = (0, 512, dim - dim % 512, dim + 8)
        pieces = []
        for n in range(3):
            rows = slice(bounds[n], bounds[n + 1])
            chip_mine = dwkv[0][rows] + theirs_in[rows]
            chip_other = dwkv[1][rows] + mine_in[rows]
            far_mine = permute(chip_mine, across)
            pieces.append((chip_mine, far_mine, chip_other, permute(far_mine, beside)))
        joined = ()
        for n in range(3):
            joined = join_pair(idx, pieces[n], dim, bounds[n], tuple(joined))
        dwk_full, dwv_full, dpre_full, dpost_full = joined

        dwo_full = join_rows(idx, dwo_mine, dwo_other)
        dwq_full = join_wide(idx, dwq_mine, dwq_other, heads)
        return (
            y.reshape(batch, tokens, dim),
            dx.reshape(batch, tokens, dim),
            dwq_full,
            dwk_full.reshape(dim, 1, hd),
            dwv_full.reshape(dim, 1, hd),
            dwo_full.reshape(heads, hd, dim),
            dpre_full,
            dpost_full,
        )

    seq_spec = P("dp", "cp", None)
    in_specs = (seq_spec, P("dp", "cp"), seq_spec, P(), P(), P(), P(), P(), P())
    out_specs = (seq_spec, seq_spec, P("dp", None, None), P("dp", None, None), P("dp", None, None), P("dp", None, None), P("dp"), P("dp"))
    return jax.shard_map(local_step, mesh=mesh, in_specs=in_specs, out_specs=out_specs, check_vma=False)
```

```python
import functools
import math

import jax
import jax.numpy as jnp
from jax import lax
from jax.experimental import pallas as pl
from jax.experimental.pallas import tpu as pltpu
from jax.sharding import PartitionSpec as P


NORM_EPS = 1e-6
SOFT_CAP = 50.0
QUERY_SCALE = 144.0
ROPE_BASE = 10000.0
LOG2E = math.log2(math.e)
CAP2 = SOFT_CAP * LOG2E
INV_CAP = 1.0 / SOFT_CAP
SHIFT2 = 20.0


F32 = jnp.float32
BF16 = jnp.bfloat16
VMEM_LIMIT = 60 * 1024 * 1024

NT = (((1,), (1,)), ((), ()))
NN = (((1,), (0,)), ((), ()))


def dot(a, b, dims=NN):
    return lax.dot_general(a, b, dims, preferred_element_type=F32)


def params():
    return pltpu.CompilerParams(vmem_limit_bytes=VMEM_LIMIT)


def whole(shape):
    zeros = (0,) * len(shape)
    return pl.BlockSpec(shape, lambda *_: zeros)


def rows_spec(rows, width):
    return pl.BlockSpec((rows, width), lambda i: (i, 0))


def stack_spec(depth, rows, width):
    return pl.BlockSpec((depth, rows, width), lambda i: (0, i, 0))


COST = pl.CostEstimate(flops=10**10, bytes_accessed=10**7, transcendentals=0)


def to_sibling(rank, src, dst, send, recv):
    return pltpu.make_async_remote_copy(
        src_ref=src, dst_ref=dst, send_sem=send, recv_sem=recv,
        device_id={"cp": rank + 1 - 2 * (rank % 2)}, device_id_type=pl.DeviceIdType.MESH,
    )


def rope(values, cosine, sine):
    half = cosine.shape[-1]
    first, second = values[:, :half], values[:, half:]
    return jnp.concatenate([first * cosine - second * sine, second * cosine + first * sine], axis=-1)


def forward_tile(q_ref, acc_ref, sum_ref, k, v, masked):
    heads, bq, _ = q_ref.shape
    bk = k.shape[0]
    if masked:
        keep = lax.broadcasted_iota(jnp.int32, (bq, bk), 1) <= lax.broadcasted_iota(jnp.int32, (bq, bk), 0)
    for h in range(heads):
        s = dot(q_ref[h], k, NT)
        p = jnp.exp2(jnp.tanh(s * INV_CAP) * CAP2 - SHIFT2)
        if masked:
            p = jnp.where(keep, p, 0.0)
        part = p[:, 0:128]
        for c in range(128, bk, 128):
            part = part + p[:, c:c + 128]
        sum_ref[h] += part
        acc_ref[h] += dot(p.astype(BF16), v)


def forward_kernel(x_ref, gain_ref, wk_ref, wv_ref, wq_hbm, cos_ref, sin_ref,
                   at_ref, q_ref, own_ref, near_ref, far_ref, mid_ref, o_ref, out_ref, lse_ref,
                   wq_s, wq_sem, a_s, own_s, near_s, far_s, mid_s, acc_s, sum_s,
                   far_send, far_recv, near_send, near_recv, mid_send, mid_recv):
    heads, tokens, hd = q_ref.shape
    bt = x_ref.shape[0]
    tiles = tokens // bt
    big = 2 * bt
    rank = lax.axis_index("cp")
    core = rank % 2
    i = pl.program_id(0)
    across = {"cp": (rank + 2) % 4}
    mesh_id = pl.DeviceIdType.MESH

    def rows_of(t, size=bt):
        return pl.ds(pl.multiple_of(t * size, size), size)

    def far_copy(t):
        rows = rows_of(t)
        return pltpu.make_async_remote_copy(
            src_ref=own_s.at[:, rows, :], dst_ref=far_s.at[:, rows, :], send_sem=far_send.at[t], recv_sem=far_recv.at[t],
            device_id=across, device_id_type=mesh_id,
        )

    def near_copy(t):
        rows = rows_of(t)
        return to_sibling(rank, own_s.at[:, rows, :], near_s.at[:, rows, :], near_send.at[t], near_recv.at[t])

    def mid_copy(c):
        rows = rows_of(c, big)
        return to_sibling(rank, far_s.at[:, rows, :], mid_s.at[:, rows, :], mid_send.at[c], mid_recv.at[c])

    load_wq = pltpu.make_async_copy(wq_hbm, wq_s, wq_sem)

    @pl.when(i == 0)
    def _():
        load_wq.start()
        barrier = pltpu.get_barrier_semaphore()
        for other in (across, {"cp": rank + 1 - 2 * core}):
            pl.semaphore_signal(barrier, inc=1, device_id=other, device_id_type=mesh_id)
        pl.semaphore_wait(barrier, 2)

    @pl.when(i < tiles)
    def _():
        rows = rows_of(i)
        x = x_ref[...].astype(F32)
        rstd = lax.rsqrt(jnp.mean(x * x, axis=-1, keepdims=True) + NORM_EPS)
        a = (x * rstd * (1.0 + gain_ref[...][None, :])).astype(BF16)
        a_s[rows, :] = a
        own_s[0, rows, :] = rope(dot(a, wk_ref[...]).astype(BF16).astype(F32), cos_ref[rows, :], sin_ref[rows, :]).astype(BF16)
        own_s[1, rows, :] = dot(a, wv_ref[...]).astype(BF16)
        pl.when(rank < 2)(lambda: far_copy(i).start())
        pl.when(core == 0)(lambda: near_copy(i).start())

    def attend(t, kv_ref, start, size, masked):
        rows, keys = rows_of(t), pl.ds(pl.multiple_of(start, bt), size)
        forward_tile(q_ref.at[:, rows, :], acc_s.at[:, rows, :], sum_s.at[:, rows, :],
                     kv_ref[0, keys, :], kv_ref[1, keys, :], masked)

    @pl.when(jnp.logical_and(i >= tiles, i < 2 * tiles))
    def _():
        t = i - tiles
        rows = rows_of(t)
        a = a_s[rows, :]
        at_ref[...] = a.T
        own_ref[...] = own_s[:, rows, :]
        pl.when(t == 0)(lambda: load_wq.wait())
        scale = QUERY_SCALE ** -0.5
        for h in range(heads):
            q = dot(a, wq_s[:, h * hd:(h + 1) * hd]).astype(BF16).astype(F32)
            q_ref[h, rows, :] = (rope(q, cos_ref[rows, :], sin_ref[rows, :]) * scale).astype(BF16)
        acc_s[:, rows, :] = jnp.zeros((heads, bt, hd), F32)
        sum_s[:, rows, :] = jnp.zeros((heads, bt, 128), F32)
        attend(t, own_s, t * bt, bt, True)

        def own_step(j, _):
            attend(t, own_s, j * bt, bt, False)
            return 0

        lax.fori_loop(0, t, own_step, 0)

        @pl.when(core == 1)
        def _():
            pl.when(t == 0)(lambda: [near_copy(n).wait_recv() for n in range(tiles)] and None)

            def near_step(j, _):
                attend(t, near_s, j * big, big, False)
                return 0

            lax.fori_loop(0, tokens // big, near_step, 0)

    chunks = tokens // big
    c = i - 2 * tiles

    def far_chunk(kv_ref, start):
        def step(t, _):
            attend(t, kv_ref, start, big, False)
            return 0

        lax.fori_loop(0, tiles, step, 0)

    @pl.when(jnp.logical_and(rank >= 2, jnp.logical_and(c >= 0, c < chunks)))
    def _():
        far_copy(2 * c).wait_recv()
        far_copy(2 * c + 1).wait_recv()
        mid_copy(c).start()
        far_chunk(far_s, c * big)

    @pl.when(jnp.logical_and(rank >= 2, jnp.logical_and(c >= chunks, c < 2 * chunks)))
    def _():
        mid_copy(c - chunks).wait_recv()
        far_chunk(mid_s, (c - chunks) * big)

    last = i - 2 * tiles - 2 * chunks

    @pl.when(last >= 0)
    def _():
        rows = rows_of(last)
        lane = lax.broadcasted_iota(jnp.int32, (bt, 128), 1)
        lse = jnp.zeros((bt, 128), F32)
        for h in range(heads):
            total = jnp.sum(sum_s[h, rows, :], axis=-1, keepdims=True)
            lse = jnp.where(lane == h, jnp.log2(total) + SHIFT2, lse)
            out = acc_s[h, rows, :] / total
            out_ref[h] = out
            o_ref[:, h * hd:(h + 1) * hd] = out.astype(BF16)
        lse_ref[...] = lse
        for dst, src in ((near_ref, near_s), (far_ref, far_s), (mid_ref, mid_s)):
            dst[...] = src[:, rows, :]

    @pl.when(last == tiles - 1)
    def _():
        pl.when(rank < 2)(lambda: [far_copy(n).wait_send() for n in range(tiles)] and None)
        pl.when(core == 0)(lambda: [near_copy(n).wait_send() for n in range(tiles)] and None)
        pl.when(rank >= 2)(lambda: [mid_copy(n).wait_send() for n in range(chunks)] and None)


def forward(x, gain, wk, wv, wq, cosine, sine, heads):
    tokens, dim = x.shape
    hd = wk.shape[1]
    bt = 256
    tiles = tokens // bt
    chunks = tiles // 2
    done = 2 * tiles + 2 * chunks
    dma = pltpu.SemaphoreType.DMA
    early = lambda i: jnp.minimum(i, tiles - 1)
    second = lambda i: jnp.clip(i - tiles, 0, tiles - 1)
    late = lambda i: jnp.maximum(i - done, 0)
    kv_shape = jax.ShapeDtypeStruct((2, tokens, hd), BF16)
    kv_out = pl.BlockSpec((2, bt, hd), lambda i: (0, late(i), 0))
    return pl.pallas_call(
        forward_kernel,
        grid=(done + tiles,),
        in_specs=[
            pl.BlockSpec((bt, dim), lambda i: (early(i), 0)),
            whole(gain.shape),
            whole(wk.shape),
            whole(wv.shape),
            pl.BlockSpec(memory_space=pl.ANY),
            whole(cosine.shape),
            whole(sine.shape),
        ],
        out_specs=[
            pl.BlockSpec((dim, bt), lambda i: (0, second(i))),
            whole((heads, tokens, hd)),
            pl.BlockSpec((2, bt, hd), lambda i: (0, second(i), 0)),
            kv_out,
            kv_out,
            kv_out,
            pl.BlockSpec((bt, heads * hd), lambda i: (late(i), 0)),
            pl.BlockSpec((heads, bt, hd), lambda i: (0, late(i), 0)),
            pl.BlockSpec((bt, 128), lambda i: (late(i), 0)),
        ],
        out_shape=[
            jax.ShapeDtypeStruct((dim, tokens), BF16),
            jax.ShapeDtypeStruct((heads, tokens, hd), BF16),
            kv_shape,
            kv_shape,
            kv_shape,
            kv_shape,
            jax.ShapeDtypeStruct((tokens, heads * hd), BF16),
            jax.ShapeDtypeStruct((heads, tokens, hd), F32),
            jax.ShapeDtypeStruct((tokens, 128), F32),
        ],
        scratch_shapes=[pltpu.VMEM(wq.shape, BF16), dma, pltpu.VMEM((tokens, dim), BF16)] + [pltpu.VMEM((2, tokens, hd), BF16)] * 4 + [
            pltpu.VMEM((heads, tokens, hd), F32),
            pltpu.VMEM((heads, tokens, 128), F32),
            dma((tiles,)),
            dma((tiles,)),
            dma((tiles,)),
            dma((tiles,)),
            dma((chunks,)),
            dma((chunks,)),
        ],
        compiler_params=pltpu.CompilerParams(vmem_limit_bytes=VMEM_LIMIT, collective_id=2, has_side_effects=True),
        cost_estimate=COST,
        name="forward",
    )(x, gain, wk, wv, wq, cosine, sine)


def post_norm(o, wo, gain, dy):
    z = dot(o, wo).astype(BF16).astype(F32)
    rstd = lax.rsqrt(jnp.mean(z * z, axis=-1, keepdims=True) + NORM_EPS)
    unit = z * rstd
    g = dy * gain
    dz = (rstd * (g - unit * jnp.mean(g * unit, axis=-1, keepdims=True))).astype(BF16)
    return unit, dz


def post_kernel(o_ref, out_ref, lse_ref, x_ref, dy_ref, wo_ref, gain_ref, y_ref, do_ref, dz_ref, stat_ref, dgain_ref):
    heads, bq, hd = out_ref.shape
    gain = 1.0 + gain_ref[...][None, :]
    dy = dy_ref[...].astype(F32)
    unit, dz = post_norm(o_ref[...], wo_ref[...], gain, dy)
    y_ref[...] = (x_ref[...].astype(F32) + (unit * gain).astype(BF16).astype(F32)).astype(BF16)
    dz_ref[...] = dz

    @pl.when(pl.program_id(0) == 0)
    def _():
        dgain_ref[...] = jnp.zeros_like(dgain_ref)

    dgain_ref[...] += jnp.sum(dy * unit, axis=0, keepdims=True)
    lane = lax.broadcasted_iota(jnp.int32, (bq, 128), 1)
    stat = lse_ref[...]
    for h in range(heads):
        d_out = dot(dz, wo_ref[h * hd:(h + 1) * hd, :], NT).astype(BF16)
        do_ref[h] = d_out
        delta = jnp.sum(d_out.astype(F32) * out_ref[h], axis=-1, keepdims=True)
        stat = jnp.where(lane == heads + h, delta, stat)
    stat_ref[...] = stat.T[0:8, :]


def post(o, out, lse, x, dy, wo, gain):
    heads, tokens, hd = out.shape
    dim = x.shape[1]
    bq = 256
    rows3 = stack_spec(heads, bq, hd)
    rows2 = lambda width: rows_spec(bq, width)
    return pl.pallas_call(
        post_kernel,
        grid=(tokens // bq,),
        in_specs=[rows2(heads * hd), rows3, rows2(128), rows2(dim), rows2(dim), whole(wo.shape), whole((dim,))],
        out_specs=[rows2(dim), rows3, rows2(dim), pl.BlockSpec((8, bq), lambda i: (0, i)), whole((1, dim))],
        out_shape=[
            jax.ShapeDtypeStruct((tokens, dim), BF16),
            jax.ShapeDtypeStruct((heads, tokens, hd), BF16),
            jax.ShapeDtypeStruct((tokens, dim), BF16),
            jax.ShapeDtypeStruct((8, tokens), F32),
            jax.ShapeDtypeStruct((1, dim), F32),
        ],
        compiler_params=params(),
        cost_estimate=COST,
        name="post",
    )(o, out, lse, x, dy, wo, gain)


def grad_wo_kernel(idx_ref, o_ref, dz_ref, po_ref, pdy_low_ref, pdy_high_ref, wo_ref, gain_ref, mine_ref, theirs_ref, pdz_ref):
    _, width = o_ref.shape
    bt = pdy_low_ref.shape[0]
    hd = 256
    i = pl.program_id(0)
    rows = pl.ds(pl.multiple_of(i * bt, bt), bt)
    dy = jnp.where(idx_ref[0] >= 2, pdy_high_ref[...], pdy_low_ref[...]).astype(F32)
    pdz_ref[rows, :] = post_norm(po_ref[rows, :], wo_ref[...], 1.0 + gain_ref[...][None, :], dy)[1]

    @pl.when(i == pl.num_programs(0) - 1)
    def _():
        core = idx_ref[0] % 2
        per = width // hd // 2
        for which, ref in enumerate((mine_ref, theirs_ref)):
            for hh in range(per):
                cols = pl.ds(pl.multiple_of((((core + which) % 2) * per + hh) * hd, hd), hd)
                ref[hh * hd:(hh + 1) * hd, :] = dot(o_ref[:, cols].T, dz_ref[...]) + dot(po_ref[:, cols].T, pdz_ref[...])


def grad_wo(idx, o, dz, po, pdy_low, pdy_high, wo, gain):
    tokens, width = o.shape
    dim = dz.shape[1]
    bt = 256
    rows2 = rows_spec(bt, dim)
    return pl.pallas_call(
        grad_wo_kernel,
        grid=(tokens // bt,),
        in_specs=[
            pl.BlockSpec(memory_space=pltpu.SMEM),
            whole(o.shape),
            whole(dz.shape),
            whole(o.shape),
            rows2,
            rows2,
            whole(wo.shape),
            whole((dim,)),
        ],
        out_specs=[whole((width // 2, dim))] * 2,
        out_shape=[jax.ShapeDtypeStruct((width // 2, dim), F32)] * 2,
        scratch_shapes=[pltpu.VMEM((tokens, dim), BF16)],
        compiler_params=params(),
        cost_estimate=COST,
        name="grad_wo",
    )(idx, o, dz, po, pdy_low, pdy_high, wo, gain)


def backward_tile(q_ref, do_ref, stat_ref, dqt_ref, dkv_ref, k, v, kt, start, bq, masked):
    heads = q_ref.shape[0]
    bk = k.shape[0]
    rows = pl.ds(pl.multiple_of(start, 128), bq)
    if masked:
        keep = lax.broadcasted_iota(jnp.int32, (bk, bq), 0) <= lax.broadcasted_iota(jnp.int32, (bk, bq), 1)
    for h in range(heads):
        q = q_ref[h, rows, :]
        d_out = do_ref[h, rows, :]
        t = jnp.tanh(dot(k, q, NT) * INV_CAP)
        p = jnp.exp2(t * CAP2 - stat_ref[h:h + 1, rows])
        if masked:
            p = jnp.where(keep, p, 0.0)
        dp = dot(v, d_out, NT)
        ds = (p * (dp - stat_ref[heads + h:heads + h + 1, rows]) * (1.0 - t * t)).astype(BF16)
        dkv_ref[1] += dot(p.astype(BF16), d_out)
        dkv_ref[0] += dot(ds, q)
        dqt_ref[h, :, rows] += dot(kt, ds)


def backward_kernel(q_ref, do_ref, stat_ref, own_ref, near_ref, far_ref, mid_ref, cos_ref, sin_ref, at_ref,
                    down_hbm, dq_hbm, dwq_hbm,
                    down_ref, dq_ref, dwq_ref, out_sem, dqt_s, near_out, near_in, mid_out, mid_in, far_out, far_in, dwq_out, dwq_in,
                    near_send, near_recv, mid_send, mid_recv, far_send, far_recv, dwq_send, dwq_recv):
    heads, tokens, hd = q_ref.shape
    half = hd // 2
    bk = own_ref.shape[1]
    big = 2 * bk
    tiles = tokens // bk
    rank = lax.axis_index("cp")
    core = rank % 2
    i = pl.program_id(0)
    across = {"cp": (rank + 2) % 4}
    mesh_id = pl.DeviceIdType.MESH

    def near_copy(n):
        return to_sibling(rank, near_out.at[n], near_in.at[n], near_send.at[n], near_recv.at[n])

    def mid_copy(n):
        return to_sibling(rank, mid_out.at[n], mid_in.at[n], mid_send.at[n], mid_recv.at[n])

    def far_copy(n):
        return pltpu.make_async_remote_copy(
            src_ref=far_out.at[n], dst_ref=far_in.at[n], send_sem=far_send.at[n], recv_sem=far_recv.at[n],
            device_id=across, device_id_type=mesh_id,
        )

    @pl.when(i == 0)
    def _():
        dqt_s[...] = jnp.zeros_like(dqt_s)
        barrier = pltpu.get_barrier_semaphore()
        for other in (across, {"cp": rank + 1 - 2 * core}):
            pl.semaphore_signal(barrier, inc=1, device_id=other, device_id_type=mesh_id)
        pl.semaphore_wait(barrier, 2)

    def all_rows(kv_ref, dkv_ref):
        k, v = kv_ref[0], kv_ref[1]
        kt = k.T

        def step(j, _):
            backward_tile(q_ref, do_ref, stat_ref, dqt_s, dkv_ref, k, v, kt, j * big, big, False)
            return 0

        lax.fori_loop(0, tokens // big, step, 0)

    @pl.when(jnp.logical_and(rank >= 2, i < tiles))
    def _():
        mine = mid_out.at[i]
        mine[...] = jnp.zeros_like(mine)
        all_rows(mid_ref, mine)
        mid_copy(i).start()

    @pl.when(jnp.logical_and(rank >= 2, jnp.logical_and(i >= tiles, i < 2 * tiles)))
    def _():
        n = i - tiles
        mid_copy(n).wait()
        mine = far_out.at[n]
        mine[...] = mid_in[n]
        all_rows(far_ref, mine)
        far_copy(n).start()

    n = i - 2 * tiles

    @pl.when(jnp.logical_and(core == 1, n >= 0))
    def _():
        mine = near_out.at[n]
        mine[...] = jnp.zeros_like(mine)
        all_rows(near_ref, mine)
        near_copy(n).start()

    @pl.when(n >= 0)
    def _():
        down = down_ref.at[:, pl.ds(pl.multiple_of(n * bk, bk), bk), :]
        down[...] = jnp.zeros_like(down)
        k, v = own_ref[0], own_ref[1]
        kt = k.T
        backward_tile(q_ref, do_ref, stat_ref, dqt_s, down, k, v, kt, n * bk, bk, True)

        def own_step(j, _):
            backward_tile(q_ref, do_ref, stat_ref, dqt_s, down, k, v, kt, j * bk, bk, False)
            return 0

        lax.fori_loop(n + 1, tiles, own_step, 0)

    @pl.when(n == tiles - 1)
    def _():
        scale = QUERY_SCALE ** -0.5
        for h in range(heads):
            dq = dqt_s[h].T
            first, second = dq[:, :half], dq[:, half:]
            cosine, sine = cos_ref[...], sin_ref[...]
            dq_ref[:, h * hd:h * hd + half] = ((first * cosine + second * sine) * scale).astype(BF16)
            dq_ref[:, h * hd + half:(h + 1) * hd] = ((second * cosine - first * sine) * scale).astype(BF16)
        written = [pltpu.make_async_copy(src, dst, out_sem.at[slot]) for slot, (src, dst) in
                   enumerate(((dq_ref, dq_hbm), (dwq_ref, dwq_hbm), (down_ref, down_hbm)))]
        written[0].start()
        dim, width = dwq_ref.shape
        bd = dim // 3

        def product(out_ref, which):
            dq = dq_ref[:, pl.ds(pl.multiple_of((core + which) % 2 * width, width), width)]

            def rows_step(r, _):
                rows = pl.ds(pl.multiple_of(r * bd, bd), bd)
                out_ref[rows, :] = dot(at_ref[rows, :], dq)
                return 0

            lax.fori_loop(0, dim // bd, rows_step, 0)

        product(dwq_out, 1)
        copy = to_sibling(rank, dwq_out, dwq_in, dwq_send, dwq_recv)
        copy.start()
        product(dwq_ref, 0)

        def gather(copy_of, arrived):
            for t in range(tiles):
                copy_of(t).wait_recv()
                down_ref[:, t * bk:(t + 1) * bk, :] += arrived[t]

        def left(copy_of):
            for t in range(tiles):
                copy_of(t).wait_send()

        pl.when(core == 1)(lambda: left(near_copy))
        pl.when(core == 0)(lambda: gather(near_copy, near_in))
        copy.wait()
        dwq_ref[...] += dwq_in[...]
        written[1].start()

        @pl.when(rank < 2)
        def _():
            gather(far_copy, far_in)
            written[2].start()

        @pl.when(rank >= 2)
        def _():
            written[2].start()
            left(far_copy)

        for copy_out in written:
            copy_out.wait()


def backward(q, d_out, stat, own, near, far, mid, cosine, sine, at):
    heads, tokens, hd = q.shape
    dim = at.shape[0]
    bk = 256
    tiles = tokens // bk
    width = heads * hd // 2

    def phase(first):
        return pl.BlockSpec((2, bk, hd), lambda i: (0, jnp.clip(i - first, 0, tiles - 1), 0))

    def held(array):
        zeros = (0,) * array.ndim
        return pl.BlockSpec(array.shape, lambda i: zeros, pipeline_mode=pl.Buffered(1))

    dma = pltpu.SemaphoreType.DMA
    return pl.pallas_call(
        backward_kernel,
        grid=(3 * tiles,),
        in_specs=[
            held(q),
            held(d_out),
            held(stat),
            phase(2 * tiles),
            phase(2 * tiles),
            phase(tiles),
            phase(0),
            held(cosine),
            held(sine),
            held(at),
        ],
        out_specs=[pl.BlockSpec(memory_space=pl.ANY)] * 3,
        out_shape=[
            jax.ShapeDtypeStruct((2, tokens, hd), F32),
            jax.ShapeDtypeStruct((tokens, heads * hd), BF16),
            jax.ShapeDtypeStruct((dim, width), F32),
        ],
        scratch_shapes=[
            pltpu.VMEM((2, tokens, hd), F32),
            pltpu.VMEM((tokens, heads * hd), BF16),
            pltpu.VMEM((dim, width), F32),
            dma((3,)),
            pltpu.VMEM((heads, hd, tokens), F32),
        ] + [pltpu.VMEM((tiles, 2, bk, hd), F32)] * 6
        + [pltpu.VMEM((dim, width), F32)] * 2 + [dma((tiles,))] * 6 + [dma] * 2,
        compiler_params=pltpu.CompilerParams(vmem_limit_bytes=VMEM_LIMIT, collective_id=0, has_side_effects=True),
        cost_estimate=COST,
        name="backward",
    )(q, d_out, stat, own, near, far, mid, cosine, sine, at)


def tail_kernel(idx_ref, down_ref, cos_ref, sin_ref, at_ref, dq_ref, wq_ref, wk_ref, wv_ref,
                x_ref, dy_ref, gain_ref, dpost_ref, dx_ref, mine_ref, theirs_ref, dgain_ref):
    _, half = cos_ref.shape
    dim = x_ref.shape[1]
    i = pl.program_id(0)
    dk = down_ref[0]
    cosine, sine = cos_ref[...], sin_ref[...]
    first, second = dk[:, :half], dk[:, half:]
    dk = jnp.concatenate([first * cosine + second * sine, second * cosine - first * sine], axis=1).astype(BF16)
    dv = down_ref[1].astype(BF16)

    @pl.when(i == 0)
    def _():
        mine_ref[...] = jnp.zeros_like(mine_ref)
        theirs_ref[...] = jnp.zeros_like(theirs_ref)
        dgain_ref[...] = jnp.zeros_like(dgain_ref)

    core = idx_ref[0] % 2
    at = at_ref[...]
    is_core0 = core == 0
    mine = jnp.where(is_core0, dk, dv)
    theirs = jnp.where(is_core0, dv, dk)
    mine_ref[0:dim, :] += dot(at, mine)
    theirs_ref[0:dim, :] += dot(at, theirs)
    da = dot(dq_ref[...], wq_ref[...], NT) + dot(dk, wk_ref[...], NT) + dot(dv, wv_ref[...], NT)
    x = x_ref[...].astype(F32)
    rstd = lax.rsqrt(jnp.mean(x * x, axis=-1, keepdims=True) + NORM_EPS)
    unit = x * rstd
    dgain_ref[...] += jnp.sum(da * unit, axis=0, keepdims=True)
    g = da * (1.0 + gain_ref[...][None, :])
    dx = rstd * (g - unit * jnp.mean(g * unit, axis=-1, keepdims=True))
    dx_ref[...] = (dy_ref[...].astype(F32) + dx).astype(BF16)

    @pl.when(i == pl.num_programs(0) - 1)
    def _():
        dpre, dpost = dgain_ref[...], dpost_ref[...]
        for ref, row in ((mine_ref, jnp.where(is_core0, dpre, dpost)), (theirs_ref, jnp.where(is_core0, dpost, dpre))):
            for c in range(dim // 128):
                ref[dim + c // 2:dim + c // 2 + 1, c % 2 * 128:(c % 2 + 1) * 128] = row[:, c * 128:(c + 1) * 128]


def tail(idx, down, cosine, sine, at, dq, wq, wk, wv, x, dy, gain, dpost):
    tokens, dim = x.shape
    hd = wk.shape[1]
    width = wq.shape[1]
    bt = 256
    kv_spec = stack_spec(2, bt, hd)
    rope_spec = rows_spec(bt, hd // 2)
    rows2 = rows_spec(bt, dim)
    return pl.pallas_call(
        tail_kernel,
        grid=(tokens // bt,),
        in_specs=[
            pl.BlockSpec(memory_space=pltpu.SMEM),
            kv_spec,
            rope_spec,
            rope_spec,
            pl.BlockSpec((dim, bt), lambda i: (0, i)),
            rows_spec(bt, width),
            whole(wq.shape),
            whole(wk.shape),
            whole(wv.shape),
            rows2,
            rows2,
            whole((dim,)),
            whole((1, dim)),
        ],
        out_specs=[rows2, whole((dim + 8, hd)), whole((dim + 8, hd))],
        out_shape=[
            jax.ShapeDtypeStruct((tokens, dim), BF16),
            jax.ShapeDtypeStruct((dim + 8, hd), F32),
            jax.ShapeDtypeStruct((dim + 8, hd), F32),
        ],
        scratch_shapes=[pltpu.VMEM((1, dim), F32)],
        compiler_params=params(),
        cost_estimate=COST,
        name="tail",
    )(idx, down, cosine, sine, at, dq, wq, wk, wv, x, dy, gain, dpost)


def join_wide_kernel(idx_ref, mine_ref, other_ref, out_ref):
    first = idx_ref[0] % 2 == 0
    rows, _ = mine_ref.shape
    mine, other = mine_ref[...], other_ref[...]
    low, high = jnp.where(first, mine, other), jnp.where(first, other, mine)
    heads = 4
    for h in range(heads):
        src = low if h < heads // 2 else high
        base = (h % (heads // 2)) * 256
        for c in range(2):
            out_ref[pl.ds(c * heads + h, rows, stride=2 * heads), :] = src[:, base + c * 128:base + (c + 1) * 128]


def join_wide(idx, mine, other, heads):
    dim, width = mine.shape
    bd = 128
    spec = rows_spec(bd, width)
    out = pl.pallas_call(
        join_wide_kernel,
        grid=(dim // bd,),
        in_specs=[pl.BlockSpec(memory_space=pltpu.SMEM), spec, spec],
        out_specs=rows_spec(bd * 8, 128),
        out_shape=jax.ShapeDtypeStruct((dim * 8, 128), F32),
        compiler_params=params(),
        cost_estimate=COST,
        name="join_wide",
    )(idx, mine, other)
    return out.reshape(dim, 2, heads, 128).transpose(0, 2, 1, 3).reshape(dim, heads, 256)


def join_pair_kernel(idx_ref, a_ref, b_ref, c_ref, d_ref, *refs, last):
    core0 = idx_ref[0] % 2 == 0

    def ordered(mine, other):
        return jnp.where(core0, mine, other), jnp.where(core0, other, mine)

    rows = a_ref.shape[0] - (8 if last else 0)
    outs = refs[2:] if last else refs
    for n, src in enumerate(ordered(a_ref[...] + b_ref[...], c_ref[...] + d_ref[...])):
        for c in range(2):
            outs[n][pl.ds(c, rows, stride=2), :] = src[0:rows, c * 128:(c + 1) * 128]
        if last:
            gain_ref = outs[n + 2]
            for c in range(gain_ref.shape[0] // 128):
                gain_ref[c * 128:(c + 1) * 128] = src[rows + c // 2, c % 2 * 128:(c % 2 + 1) * 128]


def join_pair(idx, parts, dim, begun=()):
    rows, width = parts[0].shape
    last = bool(begun)
    bd = rows - 8 if last else dim // 3
    steps = rows // bd
    first = dim // bd - 1 if last else 0
    out_spec = pl.BlockSpec((bd * 2, 128), lambda i: (i + first, 0))
    part_spec = whole(parts[0].shape) if last else rows_spec(bd, width)
    pair = [jax.ShapeDtypeStruct((dim * 2, 128), F32)] * 2
    return pl.pallas_call(
        functools.partial(join_pair_kernel, last=last),
        grid=(steps,),
        in_specs=[pl.BlockSpec(memory_space=pltpu.SMEM)] + [part_spec] * 4 + [pl.BlockSpec(memory_space=pl.ANY)] * len(begun),
        out_specs=[out_spec] * 2 + [whole((dim,))] * len(begun),
        out_shape=pair + [jax.ShapeDtypeStruct((dim,), F32)] * len(begun),
        input_output_aliases={5: 0, 6: 1} if last else {},
        compiler_params=params(),
        cost_estimate=COST,
        name="join_last" if last else "join_first",
    )(idx, *parts, *begun)


def join_rows_kernel(idx_ref, mine_ref, other_ref, out_ref):
    first = idx_ref[0] % 2 == 0
    out_ref[...] = jnp.where(first == (pl.program_id(0) == 0), mine_ref[...], other_ref[...])


def join_rows(idx, mine, other):
    rows, dim = mine.shape
    br = 256
    steps = rows // br
    spec = pl.BlockSpec((br, dim), lambda w, i: (i, 0))
    return pl.pallas_call(
        join_rows_kernel,
        grid=(2, steps),
        in_specs=[pl.BlockSpec(memory_space=pltpu.SMEM), spec, spec],
        out_specs=pl.BlockSpec((br, dim), lambda w, i: (w * steps + i, 0)),
        out_shape=jax.ShapeDtypeStruct((rows * 2, dim), F32),
        compiler_params=params(),
        cost_estimate=COST,
        name="join_rows",
    )(idx, mine, other)


def solution(mesh):
    across = [(0, 2), (2, 0), (1, 3), (3, 1)]
    beside = [(0, 1), (1, 0), (2, 3), (3, 2)]

    def permute(value, pairs):
        return lax.ppermute(value, "cp", pairs)

    def local_step(x_in, positions, dy_out, w_query, w_key, w_value, w_out, w_pre, w_post):
        batch, tokens, dim = x_in.shape
        heads, hd = w_query.shape[1], w_query.shape[2]
        half = hd // 2
        idx = lax.axis_index("cp").astype(jnp.int32).reshape(1)
        wq = w_query.reshape(dim, heads * hd)
        wk = w_key.reshape(dim, hd)
        wv = w_value.reshape(dim, hd)
        wo = w_out.reshape(heads * hd, dim)
        x = x_in.reshape(tokens, dim)
        dy = dy_out.reshape(tokens, dim)
        gain_pre = w_pre
        gain_post = w_post
        inv_freq = ROPE_BASE ** (jnp.arange(half, dtype=F32) * (-2.0 / hd))
        angles = positions.reshape(tokens, 1).astype(F32) * inv_freq
        cosine, sine = jnp.cos(angles), jnp.sin(angles)

        dy_high = permute(dy, [(2, 0), (3, 1)])
        act_t, q, own, near, far, mid, o, out, lse = forward(x, gain_pre, wk, wv, wq, cosine, sine, heads)
        dy_low = permute(dy, [(0, 2), (1, 3)])
        partner_o = permute(o, across)
        y, d_out, dz, stat, dgain_post = post(o, out, lse, x, dy, wo, gain_post)

        down, dq, dwq_part = backward(q, d_out, stat, own, near, far, mid, cosine, sine, act_t)
        dwq_mine = dwq_part + permute(dwq_part, across)
        dwq_other = permute(dwq_mine, beside)
        dwo = grad_wo(idx, o, dz, partner_o, dy_high, dy_low, wo, gain_post)
        dwo_in = permute(dwo[1], beside)
        dwo_mine = dwo[0] + dwo_in
        dwo_other = permute(dwo_mine, beside)
        dx, *dwkv = tail(idx, down, cosine, sine, act_t, dq, wq, wk, wv, x, dy, gain_pre, dgain_post)
        theirs_in, mine_in = permute(dwkv[1], beside), permute(dwkv[0], beside)
        split = dim // 3 * 2
        pieces = []
        for rows in (slice(0, split), slice(split, None)):
            chip_mine = dwkv[0][rows] + theirs_in[rows]
            chip_other = dwkv[1][rows] + mine_in[rows]
            far_mine = permute(chip_mine, across)
            pieces.append((chip_mine, far_mine, chip_other, permute(far_mine, beside)))
        begun = join_pair(idx, pieces[0], dim)
        dwk_full, dwv_full, dpre_full, dpost_full = join_pair(idx, pieces[1], dim, tuple(begun))

        dwo_full = join_rows(idx, dwo_mine, dwo_other)
        dwq_full = join_wide(idx, dwq_mine, dwq_other, heads)
        return (
            y.reshape(batch, tokens, dim),
            dx.reshape(batch, tokens, dim),
            dwq_full,
            dwk_full.reshape(dim, 1, hd),
            dwv_full.reshape(dim, 1, hd),
            dwo_full.reshape(heads, hd, dim),
            dpre_full,
            dpost_full,
        )

    seq_spec = P("dp", "cp", None)
    in_specs = (seq_spec, P("dp", "cp"), seq_spec, P(), P(), P(), P(), P(), P())
    out_specs = (seq_spec, seq_spec, P("dp", None, None), P("dp", None, None), P("dp", None, None), P("dp", None, None), P("dp"), P("dp"))
    return jax.shard_map(local_step, mesh=mesh, in_specs=in_specs, out_specs=out_specs, check_vma=False)
```

```python
import functools
import math

import jax
import jax.numpy as jnp
from jax import lax
from jax.experimental import pallas as pl
from jax.experimental.pallas import tpu as pltpu
from jax.sharding import PartitionSpec as P


NORM_EPS = 1e-6
SOFT_CAP = 50.0
QUERY_SCALE = 144.0
ROPE_BASE = 10000.0
LOG2E = math.log2(math.e)
CAP2 = SOFT_CAP * LOG2E
INV_CAP = 1.0 / SOFT_CAP
SHIFT2 = 20.0


F32 = jnp.float32
BF16 = jnp.bfloat16
VMEM_LIMIT = 60 * 1024 * 1024

NT = (((1,), (1,)), ((), ()))
NN = (((1,), (0,)), ((), ()))


def dot(a, b, dims=NN):
    return lax.dot_general(a, b, dims, preferred_element_type=F32)


def params():
    return pltpu.CompilerParams(vmem_limit_bytes=VMEM_LIMIT)


def whole(shape):
    zeros = (0,) * len(shape)
    return pl.BlockSpec(shape, lambda *_: zeros)


def rows_spec(rows, width):
    return pl.BlockSpec((rows, width), lambda i: (i, 0))


def stack_spec(depth, rows, width):
    return pl.BlockSpec((depth, rows, width), lambda i: (0, i, 0))


COST = pl.CostEstimate(flops=10**10, bytes_accessed=10**7, transcendentals=0)


def to_sibling(rank, src, dst, send, recv):
    return pltpu.make_async_remote_copy(
        src_ref=src, dst_ref=dst, send_sem=send, recv_sem=recv,
        device_id={"cp": rank + 1 - 2 * (rank % 2)}, device_id_type=pl.DeviceIdType.MESH,
    )


def rope(values, cosine, sine):
    half = cosine.shape[-1]
    first, second = values[:, :half], values[:, half:]
    return jnp.concatenate([first * cosine - second * sine, second * cosine + first * sine], axis=-1)


def forward_tile(q_ref, acc_ref, sum_ref, k, v, masked):
    heads, bq, _ = q_ref.shape
    bk = k.shape[0]
    if masked:
        keep = lax.broadcasted_iota(jnp.int32, (bq, bk), 1) <= lax.broadcasted_iota(jnp.int32, (bq, bk), 0)
    for h in range(heads):
        s = dot(q_ref[h], k, NT)
        p = jnp.exp2(jnp.tanh(s * INV_CAP) * CAP2 - SHIFT2)
        if masked:
            p = jnp.where(keep, p, 0.0)
        part = p[:, 0:128]
        for c in range(128, bk, 128):
            part = part + p[:, c:c + 128]
        sum_ref[h] += part
        acc_ref[h] += dot(p.astype(BF16), v)


def forward_kernel(x_ref, gain_ref, wk_ref, wv_ref, wq_hbm, cos_ref, sin_ref, dy_hbm,
                   at_ref, q_ref, own_ref, near_ref, far_ref, mid_ref, o_ref, out_ref, lse_ref, dy_far,
                   dy_send, dy_recv, wq_s, wq_sem, a_s, own_s, near_s, far_s, mid_s, acc_s, sum_s,
                   far_send, far_recv, near_send, near_recv, mid_send, mid_recv):
    heads, tokens, hd = q_ref.shape
    bt = x_ref.shape[0]
    tiles = tokens // bt
    big = 2 * bt
    rank = lax.axis_index("cp")
    core = rank % 2
    i = pl.program_id(0)
    across = {"cp": (rank + 2) % 4}
    mesh_id = pl.DeviceIdType.MESH

    def rows_of(t, size=bt):
        return pl.ds(pl.multiple_of(t * size, size), size)

    def far_copy(t):
        rows = rows_of(t)
        return pltpu.make_async_remote_copy(
            src_ref=own_s.at[:, rows, :], dst_ref=far_s.at[:, rows, :], send_sem=far_send.at[t], recv_sem=far_recv.at[t],
            device_id=across, device_id_type=mesh_id,
        )

    def near_copy(t):
        rows = rows_of(t)
        return to_sibling(rank, own_s.at[:, rows, :], near_s.at[:, rows, :], near_send.at[t], near_recv.at[t])

    def mid_copy(c):
        rows = rows_of(c, big)
        return to_sibling(rank, far_s.at[:, rows, :], mid_s.at[:, rows, :], mid_send.at[c], mid_recv.at[c])

    load_wq = pltpu.make_async_copy(wq_hbm, wq_s, wq_sem)
    dy_copy = pltpu.make_async_remote_copy(
        src_ref=dy_hbm.at[0:bt, :], dst_ref=dy_far, send_sem=dy_send, recv_sem=dy_recv,
        device_id=across, device_id_type=mesh_id,
    )

    @pl.when(i == 0)
    def _():
        load_wq.start()
        barrier = pltpu.get_barrier_semaphore()
        for other in (across, {"cp": rank + 1 - 2 * core}):
            pl.semaphore_signal(barrier, inc=1, device_id=other, device_id_type=mesh_id)
        pl.semaphore_wait(barrier, 2)

    @pl.when(i < tiles)
    def _():
        rows = rows_of(i)
        x = x_ref[...].astype(F32)
        rstd = lax.rsqrt(jnp.mean(x * x, axis=-1, keepdims=True) + NORM_EPS)
        a = (x * rstd * (1.0 + gain_ref[...][None, :])).astype(BF16)
        a_s[rows, :] = a
        own_s[0, rows, :] = rope(dot(a, wk_ref[...]).astype(BF16).astype(F32), cos_ref[rows, :], sin_ref[rows, :]).astype(BF16)
        own_s[1, rows, :] = dot(a, wv_ref[...]).astype(BF16)
        pl.when(rank < 2)(lambda: far_copy(i).start())
        pl.when(core == 0)(lambda: near_copy(i).start())

    def attend(t, kv_ref, start, size, masked):
        rows, keys = rows_of(t), pl.ds(pl.multiple_of(start, bt), size)
        forward_tile(q_ref.at[:, rows, :], acc_s.at[:, rows, :], sum_s.at[:, rows, :],
                     kv_ref[0, keys, :], kv_ref[1, keys, :], masked)

    @pl.when(jnp.logical_and(i >= tiles, i < 2 * tiles))
    def _():
        t = i - tiles
        rows = rows_of(t)
        a = a_s[rows, :]
        at_ref[...] = a.T
        own_ref[...] = own_s[:, rows, :]
        pl.when(jnp.logical_and(t == 0, rank < 2))(lambda: dy_copy.start())
        pl.when(t == 0)(lambda: load_wq.wait())
        scale = QUERY_SCALE ** -0.5
        for h in range(heads):
            q = dot(a, wq_s[:, h * hd:(h + 1) * hd]).astype(BF16).astype(F32)
            q_ref[h, rows, :] = (rope(q, cos_ref[rows, :], sin_ref[rows, :]) * scale).astype(BF16)
        acc_s[:, rows, :] = jnp.zeros((heads, bt, hd), F32)
        sum_s[:, rows, :] = jnp.zeros((heads, bt, 128), F32)
        attend(t, own_s, t * bt, bt, True)

        def own_step(j, _):
            attend(t, own_s, j * bt, bt, False)
            return 0

        lax.fori_loop(0, t, own_step, 0)

        @pl.when(core == 1)
        def _():
            pl.when(t == 0)(lambda: [near_copy(n).wait_recv() for n in range(tiles)] and None)

            def near_step(j, _):
                attend(t, near_s, j * big, big, False)
                return 0

            lax.fori_loop(0, tokens // big, near_step, 0)

    chunks = tokens // big
    c = i - 2 * tiles

    def far_chunk(kv_ref, start):
        def step(t, _):
            attend(t, kv_ref, start, big, False)
            return 0

        lax.fori_loop(0, tiles, step, 0)

    @pl.when(jnp.logical_and(rank >= 2, jnp.logical_and(c >= 0, c < chunks)))
    def _():
        far_copy(2 * c).wait_recv()
        far_copy(2 * c + 1).wait_recv()
        mid_copy(c).start()
        far_chunk(far_s, c * big)

    @pl.when(jnp.logical_and(rank >= 2, jnp.logical_and(c >= chunks, c < 2 * chunks)))
    def _():
        mid_copy(c - chunks).wait_recv()
        far_chunk(mid_s, (c - chunks) * big)

    last = i - 2 * tiles - 2 * chunks

    @pl.when(last >= 0)
    def _():
        rows = rows_of(last)
        lane = lax.broadcasted_iota(jnp.int32, (bt, 128), 1)
        lse = jnp.zeros((bt, 128), F32)
        for h in range(heads):
            total = jnp.sum(sum_s[h, rows, :], axis=-1, keepdims=True)
            lse = jnp.where(lane == h, jnp.log2(total) + SHIFT2, lse)
            out = acc_s[h, rows, :] / total
            out_ref[h] = out
            o_ref[:, h * hd:(h + 1) * hd] = out.astype(BF16)
        lse_ref[...] = lse
        for dst, src in ((near_ref, near_s), (far_ref, far_s), (mid_ref, mid_s)):
            dst[...] = src[:, rows, :]

    @pl.when(last == tiles - 1)
    def _():
        pl.when(rank < 2)(lambda: [far_copy(n).wait_send() for n in range(tiles)] and dy_copy.wait_send())
        pl.when(rank >= 2)(lambda: dy_copy.wait_recv())
        pl.when(core == 0)(lambda: [near_copy(n).wait_send() for n in range(tiles)] and None)
        pl.when(rank >= 2)(lambda: [mid_copy(n).wait_send() for n in range(chunks)] and None)


def forward(x, gain, wk, wv, wq, cosine, sine, dy, heads):
    tokens, dim = x.shape
    hd = wk.shape[1]
    bt = 256
    tiles = tokens // bt
    chunks = tiles // 2
    done = 2 * tiles + 2 * chunks
    dma = pltpu.SemaphoreType.DMA
    early = lambda i: jnp.minimum(i, tiles - 1)
    second = lambda i: jnp.clip(i - tiles, 0, tiles - 1)
    late = lambda i: jnp.maximum(i - done, 0)
    kv_shape = jax.ShapeDtypeStruct((2, tokens, hd), BF16)
    kv_out = pl.BlockSpec((2, bt, hd), lambda i: (0, late(i), 0))
    return pl.pallas_call(
        forward_kernel,
        grid=(done + tiles,),
        in_specs=[
            pl.BlockSpec((bt, dim), lambda i: (early(i), 0)),
            whole(gain.shape),
            whole(wk.shape),
            whole(wv.shape),
            pl.BlockSpec(memory_space=pl.ANY),
            whole(cosine.shape),
            whole(sine.shape),
            pl.BlockSpec(memory_space=pl.ANY),
        ],
        out_specs=[
            pl.BlockSpec((dim, bt), lambda i: (0, second(i))),
            whole((heads, tokens, hd)),
            pl.BlockSpec((2, bt, hd), lambda i: (0, second(i), 0)),
            kv_out,
            kv_out,
            kv_out,
            pl.BlockSpec((bt, heads * hd), lambda i: (late(i), 0)),
            pl.BlockSpec((heads, bt, hd), lambda i: (0, late(i), 0)),
            pl.BlockSpec((bt, 128), lambda i: (late(i), 0)),
            pl.BlockSpec(memory_space=pl.ANY),
        ],
        out_shape=[
            jax.ShapeDtypeStruct((dim, tokens), BF16),
            jax.ShapeDtypeStruct((heads, tokens, hd), BF16),
            kv_shape,
            kv_shape,
            kv_shape,
            kv_shape,
            jax.ShapeDtypeStruct((tokens, heads * hd), BF16),
            jax.ShapeDtypeStruct((heads, tokens, hd), F32),
            jax.ShapeDtypeStruct((tokens, 128), F32),
            jax.ShapeDtypeStruct((bt, dim), BF16),
        ],
        scratch_shapes=[dma, dma, pltpu.VMEM(wq.shape, BF16), dma, pltpu.VMEM((tokens, dim), BF16)] + [pltpu.VMEM((2, tokens, hd), BF16)] * 4 + [
            pltpu.VMEM((heads, tokens, hd), F32),
            pltpu.VMEM((heads, tokens, 128), F32),
            dma((tiles,)),
            dma((tiles,)),
            dma((tiles,)),
            dma((tiles,)),
            dma((chunks,)),
            dma((chunks,)),
        ],
        compiler_params=pltpu.CompilerParams(vmem_limit_bytes=VMEM_LIMIT, collective_id=2, has_side_effects=True),
        cost_estimate=COST,
        name="forward",
    )(x, gain, wk, wv, wq, cosine, sine, dy)


def post_norm(o, wo, gain, dy):
    z = dot(o, wo).astype(BF16).astype(F32)
    rstd = lax.rsqrt(jnp.mean(z * z, axis=-1, keepdims=True) + NORM_EPS)
    unit = z * rstd
    g = dy * gain
    dz = (rstd * (g - unit * jnp.mean(g * unit, axis=-1, keepdims=True))).astype(BF16)
    return unit, dz


def post_kernel(o_ref, out_ref, lse_ref, x_ref, dy_ref, wo_ref, gain_ref, y_ref, do_ref, dz_ref, stat_ref, dgain_ref):
    heads, bq, hd = out_ref.shape
    gain = 1.0 + gain_ref[...][None, :]
    dy = dy_ref[...].astype(F32)
    unit, dz = post_norm(o_ref[...], wo_ref[...], gain, dy)
    y_ref[...] = (x_ref[...].astype(F32) + (unit * gain).astype(BF16).astype(F32)).astype(BF16)
    dz_ref[...] = dz

    @pl.when(pl.program_id(0) == 0)
    def _():
        dgain_ref[...] = jnp.zeros_like(dgain_ref)

    dgain_ref[...] += jnp.sum(dy * unit, axis=0, keepdims=True)
    lane = lax.broadcasted_iota(jnp.int32, (bq, 128), 1)
    stat = lse_ref[...]
    for h in range(heads):
        d_out = dot(dz, wo_ref[h * hd:(h + 1) * hd, :], NT).astype(BF16)
        do_ref[h] = d_out
        delta = jnp.sum(d_out.astype(F32) * out_ref[h], axis=-1, keepdims=True)
        stat = jnp.where(lane == heads + h, delta, stat)
    stat_ref[...] = stat.T[0:8, :]


def post(o, out, lse, x, dy, wo, gain):
    heads, tokens, hd = out.shape
    dim = x.shape[1]
    bq = 256
    rows3 = stack_spec(heads, bq, hd)
    rows2 = lambda width: rows_spec(bq, width)
    return pl.pallas_call(
        post_kernel,
        grid=(tokens // bq,),
        in_specs=[rows2(heads * hd), rows3, rows2(128), rows2(dim), rows2(dim), whole(wo.shape), whole((dim,))],
        out_specs=[rows2(dim), rows3, rows2(dim), pl.BlockSpec((8, bq), lambda i: (0, i)), whole((1, dim))],
        out_shape=[
            jax.ShapeDtypeStruct((tokens, dim), BF16),
            jax.ShapeDtypeStruct((heads, tokens, hd), BF16),
            jax.ShapeDtypeStruct((tokens, dim), BF16),
            jax.ShapeDtypeStruct((8, tokens), F32),
            jax.ShapeDtypeStruct((1, dim), F32),
        ],
        compiler_params=params(),
        cost_estimate=COST,
        name="post",
    )(o, out, lse, x, dy, wo, gain)


def grad_wo_kernel(idx_ref, o_ref, dz_ref, po_ref, pdy_low_ref, pdy_head_ref, pdy_high_ref, wo_ref, gain_ref, mine_ref, theirs_ref, pdz_ref):
    _, width = o_ref.shape
    bt = pdy_low_ref.shape[0]
    hd = 256
    i = pl.program_id(0)
    rows = pl.ds(pl.multiple_of(i * bt, bt), bt)
    high = jnp.where(i == 0, pdy_head_ref[...], pdy_high_ref[...])
    dy = jnp.where(idx_ref[0] >= 2, high, pdy_low_ref[...]).astype(F32)
    pdz_ref[rows, :] = post_norm(po_ref[rows, :], wo_ref[...], 1.0 + gain_ref[...][None, :], dy)[1]

    @pl.when(i == pl.num_programs(0) - 1)
    def _():
        core = idx_ref[0] % 2
        per = width // hd // 2
        for which, ref in enumerate((mine_ref, theirs_ref)):
            for hh in range(per):
                cols = pl.ds(pl.multiple_of((((core + which) % 2) * per + hh) * hd, hd), hd)
                ref[hh * hd:(hh + 1) * hd, :] = dot(o_ref[:, cols].T, dz_ref[...]) + dot(po_ref[:, cols].T, pdz_ref[...])


def grad_wo(idx, o, dz, po, pdy_low, pdy_head, pdy_high, wo, gain):
    tokens, width = o.shape
    dim = dz.shape[1]
    bt = 256
    rows2 = rows_spec(bt, dim)
    return pl.pallas_call(
        grad_wo_kernel,
        grid=(tokens // bt,),
        in_specs=[
            pl.BlockSpec(memory_space=pltpu.SMEM),
            whole(o.shape),
            whole(dz.shape),
            whole(o.shape),
            rows2,
            whole(pdy_head.shape),
            pl.BlockSpec((bt, dim), lambda i: (jnp.maximum(i - 1, 0), 0)),
            whole(wo.shape),
            whole((dim,)),
        ],
        out_specs=[whole((width // 2, dim))] * 2,
        out_shape=[jax.ShapeDtypeStruct((width // 2, dim), F32)] * 2,
        scratch_shapes=[pltpu.VMEM((tokens, dim), BF16)],
        compiler_params=params(),
        cost_estimate=COST,
        name="grad_wo",
    )(idx, o, dz, po, pdy_low, pdy_head, pdy_high, wo, gain)


def backward_tile(q_ref, do_ref, stat_ref, dqt_ref, dkv_ref, k, v, kt, start, bq, masked):
    heads = q_ref.shape[0]
    bk = k.shape[0]
    rows = pl.ds(pl.multiple_of(start, 128), bq)
    if masked:
        keep = lax.broadcasted_iota(jnp.int32, (bk, bq), 0) <= lax.broadcasted_iota(jnp.int32, (bk, bq), 1)
    for h in range(heads):
        q = q_ref[h, rows, :]
        d_out = do_ref[h, rows, :]
        t = jnp.tanh(dot(k, q, NT) * INV_CAP)
        p = jnp.exp2(t * CAP2 - stat_ref[h:h + 1, rows])
        if masked:
            p = jnp.where(keep, p, 0.0)
        dp = dot(v, d_out, NT)
        ds = (p * (dp - stat_ref[heads + h:heads + h + 1, rows]) * (1.0 - t * t)).astype(BF16)
        dkv_ref[1] += dot(p.astype(BF16), d_out)
        dkv_ref[0] += dot(ds, q)
        dqt_ref[h, :, rows] += dot(kt, ds)


def backward_kernel(q_ref, do_ref, stat_ref, own_ref, near_ref, far_ref, mid_ref, cos_ref, sin_ref, at_ref,
                    down_hbm, dq_hbm, dwq_hbm,
                    down_ref, dq_ref, dwq_ref, out_sem, dqt_s, near_out, near_in, mid_out, mid_in, far_out, far_in, dwq_out, dwq_in,
                    near_send, near_recv, mid_send, mid_recv, far_send, far_recv, dwq_send, dwq_recv):
    heads, tokens, hd = q_ref.shape
    half = hd // 2
    bk = own_ref.shape[1]
    big = 2 * bk
    tiles = tokens // bk
    rank = lax.axis_index("cp")
    core = rank % 2
    i = pl.program_id(0)
    across = {"cp": (rank + 2) % 4}
    mesh_id = pl.DeviceIdType.MESH

    def near_copy(n):
        return to_sibling(rank, near_out.at[n], near_in.at[n], near_send.at[n], near_recv.at[n])

    def mid_copy(n):
        return to_sibling(rank, mid_out.at[n], mid_in.at[n], mid_send.at[n], mid_recv.at[n])

    def far_copy(n):
        return pltpu.make_async_remote_copy(
            src_ref=far_out.at[n], dst_ref=far_in.at[n], send_sem=far_send.at[n], recv_sem=far_recv.at[n],
            device_id=across, device_id_type=mesh_id,
        )

    @pl.when(i == 0)
    def _():
        dqt_s[...] = jnp.zeros_like(dqt_s)
        barrier = pltpu.get_barrier_semaphore()
        for other in (across, {"cp": rank + 1 - 2 * core}):
            pl.semaphore_signal(barrier, inc=1, device_id=other, device_id_type=mesh_id)
        pl.semaphore_wait(barrier, 2)

    def all_rows(kv_ref, dkv_ref):
        k, v = kv_ref[0], kv_ref[1]
        kt = k.T

        def step(j, _):
            backward_tile(q_ref, do_ref, stat_ref, dqt_s, dkv_ref, k, v, kt, j * big, big, False)
            return 0

        lax.fori_loop(0, tokens // big, step, 0)

    @pl.when(jnp.logical_and(rank >= 2, i < tiles))
    def _():
        mine = mid_out.at[i]
        mine[...] = jnp.zeros_like(mine)
        all_rows(mid_ref, mine)
        mid_copy(i).start()

    @pl.when(jnp.logical_and(rank >= 2, jnp.logical_and(i >= tiles, i < 2 * tiles)))
    def _():
        n = i - tiles
        mid_copy(n).wait()
        mine = far_out.at[n]
        mine[...] = mid_in[n]
        all_rows(far_ref, mine)
        far_copy(n).start()

    n = i - 2 * tiles

    @pl.when(jnp.logical_and(core == 1, n >= 0))
    def _():
        mine = near_out.at[n]
        mine[...] = jnp.zeros_like(mine)
        all_rows(near_ref, mine)
        near_copy(n).start()

    @pl.when(n >= 0)
    def _():
        down = down_ref.at[:, pl.ds(pl.multiple_of(n * bk, bk), bk), :]
        down[...] = jnp.zeros_like(down)
        k, v = own_ref[0], own_ref[1]
        kt = k.T
        backward_tile(q_ref, do_ref, stat_ref, dqt_s, down, k, v, kt, n * bk, bk, True)

        def own_step(j, _):
            backward_tile(q_ref, do_ref, stat_ref, dqt_s, down, k, v, kt, j * bk, bk, False)
            return 0

        lax.fori_loop(n + 1, tiles, own_step, 0)

    @pl.when(n == tiles - 1)
    def _():
        scale = QUERY_SCALE ** -0.5
        for h in range(heads):
            dq = dqt_s[h].T
            first, second = dq[:, :half], dq[:, half:]
            cosine, sine = cos_ref[...], sin_ref[...]
            dq_ref[:, h * hd:h * hd + half] = ((first * cosine + second * sine) * scale).astype(BF16)
            dq_ref[:, h * hd + half:(h + 1) * hd] = ((second * cosine - first * sine) * scale).astype(BF16)
        written = [pltpu.make_async_copy(src, dst, out_sem.at[slot]) for slot, (src, dst) in
                   enumerate(((dq_ref, dq_hbm), (dwq_ref, dwq_hbm), (down_ref, down_hbm)))]
        written[0].start()
        dim, width = dwq_ref.shape
        bd = dim // 3

        def product(out_ref, which):
            dq = dq_ref[:, pl.ds(pl.multiple_of((core + which) % 2 * width, width), width)]

            def rows_step(r, _):
                rows = pl.ds(pl.multiple_of(r * bd, bd), bd)
                out_ref[rows, :] = dot(at_ref[rows, :], dq)
                return 0

            lax.fori_loop(0, dim // bd, rows_step, 0)

        product(dwq_out, 1)
        copy = to_sibling(rank, dwq_out, dwq_in, dwq_send, dwq_recv)
        copy.start()
        product(dwq_ref, 0)

        def gather(copy_of, arrived):
            for t in range(tiles):
                copy_of(t).wait_recv()
                down_ref[:, t * bk:(t + 1) * bk, :] += arrived[t]

        def left(copy_of):
            for t in range(tiles):
                copy_of(t).wait_send()

        pl.when(core == 1)(lambda: left(near_copy))
        pl.when(core == 0)(lambda: gather(near_copy, near_in))
        copy.wait()
        dwq_ref[...] += dwq_in[...]
        written[1].start()

        @pl.when(rank < 2)
        def _():
            gather(far_copy, far_in)
            written[2].start()

        @pl.when(rank >= 2)
        def _():
            written[2].start()
            left(far_copy)

        for copy_out in written:
            copy_out.wait()


def backward(q, d_out, stat, own, near, far, mid, cosine, sine, at):
    heads, tokens, hd = q.shape
    dim = at.shape[0]
    bk = 256
    tiles = tokens // bk
    width = heads * hd // 2

    def phase(first):
        return pl.BlockSpec((2, bk, hd), lambda i: (0, jnp.clip(i - first, 0, tiles - 1), 0))

    def held(array):
        zeros = (0,) * array.ndim
        return pl.BlockSpec(array.shape, lambda i: zeros, pipeline_mode=pl.Buffered(1))

    dma = pltpu.SemaphoreType.DMA
    return pl.pallas_call(
        backward_kernel,
        grid=(3 * tiles,),
        in_specs=[
            held(q),
            held(d_out),
            held(stat),
            phase(2 * tiles),
            phase(2 * tiles),
            phase(tiles),
            phase(0),
            held(cosine),
            held(sine),
            held(at),
        ],
        out_specs=[pl.BlockSpec(memory_space=pl.ANY)] * 3,
        out_shape=[
            jax.ShapeDtypeStruct((2, tokens, hd), F32),
            jax.ShapeDtypeStruct((tokens, heads * hd), BF16),
            jax.ShapeDtypeStruct((dim, width), F32),
        ],
        scratch_shapes=[
            pltpu.VMEM((2, tokens, hd), F32),
            pltpu.VMEM((tokens, heads * hd), BF16),
            pltpu.VMEM((dim, width), F32),
            dma((3,)),
            pltpu.VMEM((heads, hd, tokens), F32),
        ] + [pltpu.VMEM((tiles, 2, bk, hd), F32)] * 6
        + [pltpu.VMEM((dim, width), F32)] * 2 + [dma((tiles,))] * 6 + [dma] * 2,
        compiler_params=pltpu.CompilerParams(vmem_limit_bytes=VMEM_LIMIT, collective_id=0, has_side_effects=True),
        cost_estimate=COST,
        name="backward",
    )(q, d_out, stat, own, near, far, mid, cosine, sine, at)


def tail_kernel(idx_ref, down_ref, cos_ref, sin_ref, at_ref, dq_ref, wq_ref, wk_ref, wv_ref,
                x_ref, dy_ref, gain_ref, dpost_ref, dx_ref, mine_ref, theirs_ref, dgain_ref):
    _, half = cos_ref.shape
    dim = x_ref.shape[1]
    i = pl.program_id(0)
    dk = down_ref[0]
    cosine, sine = cos_ref[...], sin_ref[...]
    first, second = dk[:, :half], dk[:, half:]
    dk = jnp.concatenate([first * cosine + second * sine, second * cosine - first * sine], axis=1).astype(BF16)
    dv = down_ref[1].astype(BF16)

    @pl.when(i == 0)
    def _():
        mine_ref[...] = jnp.zeros_like(mine_ref)
        theirs_ref[...] = jnp.zeros_like(theirs_ref)
        dgain_ref[...] = jnp.zeros_like(dgain_ref)

    core = idx_ref[0] % 2
    at = at_ref[...]
    is_core0 = core == 0
    mine = jnp.where(is_core0, dk, dv)
    theirs = jnp.where(is_core0, dv, dk)
    mine_ref[0:dim, :] += dot(at, mine)
    theirs_ref[0:dim, :] += dot(at, theirs)
    da = dot(dq_ref[...], wq_ref[...], NT) + dot(dk, wk_ref[...], NT) + dot(dv, wv_ref[...], NT)
    x = x_ref[...].astype(F32)
    rstd = lax.rsqrt(jnp.mean(x * x, axis=-1, keepdims=True) + NORM_EPS)
    unit = x * rstd
    dgain_ref[...] += jnp.sum(da * unit, axis=0, keepdims=True)
    g = da * (1.0 + gain_ref[...][None, :])
    dx = rstd * (g - unit * jnp.mean(g * unit, axis=-1, keepdims=True))
    dx_ref[...] = (dy_ref[...].astype(F32) + dx).astype(BF16)

    @pl.when(i == pl.num_programs(0) - 1)
    def _():
        dpre, dpost = dgain_ref[...], dpost_ref[...]
        for ref, row in ((mine_ref, jnp.where(is_core0, dpre, dpost)), (theirs_ref, jnp.where(is_core0, dpost, dpre))):
            for c in range(dim // 128):
                ref[dim + c // 2:dim + c // 2 + 1, c % 2 * 128:(c % 2 + 1) * 128] = row[:, c * 128:(c + 1) * 128]


def tail(idx, down, cosine, sine, at, dq, wq, wk, wv, x, dy, gain, dpost):
    tokens, dim = x.shape
    hd = wk.shape[1]
    width = wq.shape[1]
    bt = 256
    kv_spec = stack_spec(2, bt, hd)
    rope_spec = rows_spec(bt, hd // 2)
    rows2 = rows_spec(bt, dim)
    return pl.pallas_call(
        tail_kernel,
        grid=(tokens // bt,),
        in_specs=[
            pl.BlockSpec(memory_space=pltpu.SMEM),
            kv_spec,
            rope_spec,
            rope_spec,
            pl.BlockSpec((dim, bt), lambda i: (0, i)),
            rows_spec(bt, width),
            whole(wq.shape),
            whole(wk.shape),
            whole(wv.shape),
            rows2,
            rows2,
            whole((dim,)),
            whole((1, dim)),
        ],
        out_specs=[rows2, whole((dim + 8, hd)), whole((dim + 8, hd))],
        out_shape=[
            jax.ShapeDtypeStruct((tokens, dim), BF16),
            jax.ShapeDtypeStruct((dim + 8, hd), F32),
            jax.ShapeDtypeStruct((dim + 8, hd), F32),
        ],
        scratch_shapes=[pltpu.VMEM((1, dim), F32)],
        compiler_params=params(),
        cost_estimate=COST,
        name="tail",
    )(idx, down, cosine, sine, at, dq, wq, wk, wv, x, dy, gain, dpost)


def join_wide_kernel(idx_ref, mine_ref, other_ref, out_ref):
    first = idx_ref[0] % 2 == 0
    rows, _ = mine_ref.shape
    mine, other = mine_ref[...], other_ref[...]
    low, high = jnp.where(first, mine, other), jnp.where(first, other, mine)
    heads = 4
    for h in range(heads):
        src = low if h < heads // 2 else high
        base = (h % (heads // 2)) * 256
        for c in range(2):
            out_ref[pl.ds(c * heads + h, rows, stride=2 * heads), :] = src[:, base + c * 128:base + (c + 1) * 128]


def join_wide(idx, mine, other, heads):
    dim, width = mine.shape
    bd = dim // 3
    spec = rows_spec(bd, width)
    out = pl.pallas_call(
        join_wide_kernel,
        grid=(dim // bd,),
        in_specs=[pl.BlockSpec(memory_space=pltpu.SMEM), spec, spec],
        out_specs=rows_spec(bd * 8, 128),
        out_shape=jax.ShapeDtypeStruct((dim * 8, 128), F32),
        compiler_params=params(),
        cost_estimate=COST,
        name="join_wide",
    )(idx, mine, other)
    return out.reshape(dim, 2, heads, 128).transpose(0, 2, 1, 3).reshape(dim, heads, 256)


def join_pair_kernel(idx_ref, a_ref, b_ref, c_ref, d_ref, *refs, last):
    core0 = idx_ref[0] % 2 == 0

    def ordered(mine, other):
        return jnp.where(core0, mine, other), jnp.where(core0, other, mine)

    rows = a_ref.shape[0] - (8 if last else 0)
    outs = refs[2:] if last else refs
    for n, src in enumerate(ordered(a_ref[...] + b_ref[...], c_ref[...] + d_ref[...])):
        for c in range(2):
            outs[n][pl.ds(c, rows, stride=2), :] = src[0:rows, c * 128:(c + 1) * 128]
        if last:
            gain_ref = outs[n + 2]
            for c in range(gain_ref.shape[0] // 128):
                gain_ref[c * 128:(c + 1) * 128] = src[rows + c // 2, c % 2 * 128:(c % 2 + 1) * 128]


def join_pair(idx, parts, dim, begun=()):
    rows, width = parts[0].shape
    last = bool(begun)
    bd = rows - 8 if last else dim // 3
    steps = rows // bd
    first = dim // bd - 1 if last else 0
    out_spec = pl.BlockSpec((bd * 2, 128), lambda i: (i + first, 0))
    part_spec = whole(parts[0].shape) if last else rows_spec(bd, width)
    pair = [jax.ShapeDtypeStruct((dim * 2, 128), F32)] * 2
    return pl.pallas_call(
        functools.partial(join_pair_kernel, last=last),
        grid=(steps,),
        in_specs=[pl.BlockSpec(memory_space=pltpu.SMEM)] + [part_spec] * 4 + [pl.BlockSpec(memory_space=pl.ANY)] * len(begun),
        out_specs=[out_spec] * 2 + [whole((dim,))] * len(begun),
        out_shape=pair + [jax.ShapeDtypeStruct((dim,), F32)] * len(begun),
        input_output_aliases={5: 0, 6: 1} if last else {},
        compiler_params=params(),
        cost_estimate=COST,
        name="join_last" if last else "join_first",
    )(idx, *parts, *begun)


def join_rows_kernel(idx_ref, mine_ref, other_ref, out_ref):
    first = idx_ref[0] % 2 == 0
    out_ref[...] = jnp.where(first == (pl.program_id(0) == 0), mine_ref[...], other_ref[...])


def join_rows(idx, mine, other):
    rows, dim = mine.shape
    br = 256
    steps = rows // br
    spec = pl.BlockSpec((br, dim), lambda w, i: (i, 0))
    return pl.pallas_call(
        join_rows_kernel,
        grid=(2, steps),
        in_specs=[pl.BlockSpec(memory_space=pltpu.SMEM), spec, spec],
        out_specs=pl.BlockSpec((br, dim), lambda w, i: (w * steps + i, 0)),
        out_shape=jax.ShapeDtypeStruct((rows * 2, dim), F32),
        compiler_params=params(),
        cost_estimate=COST,
        name="join_rows",
    )(idx, mine, other)


def solution(mesh):
    across = [(0, 2), (2, 0), (1, 3), (3, 1)]
    beside = [(0, 1), (1, 0), (2, 3), (3, 2)]

    def permute(value, pairs):
        return lax.ppermute(value, "cp", pairs)

    def local_step(x_in, positions, dy_out, w_query, w_key, w_value, w_out, w_pre, w_post):
        batch, tokens, dim = x_in.shape
        heads, hd = w_query.shape[1], w_query.shape[2]
        half = hd // 2
        idx = lax.axis_index("cp").astype(jnp.int32).reshape(1)
        wq = w_query.reshape(dim, heads * hd)
        wk = w_key.reshape(dim, hd)
        wv = w_value.reshape(dim, hd)
        wo = w_out.reshape(heads * hd, dim)
        x = x_in.reshape(tokens, dim)
        dy = dy_out.reshape(tokens, dim)
        gain_pre = w_pre
        gain_post = w_post
        inv_freq = ROPE_BASE ** (jnp.arange(half, dtype=F32) * (-2.0 / hd))
        angles = positions.reshape(tokens, 1).astype(F32) * inv_freq
        cosine, sine = jnp.cos(angles), jnp.sin(angles)

        dy_high = permute(dy, [(2, 0), (3, 1)])
        act_t, q, own, near, far, mid, o, out, lse, dy_head = forward(x, gain_pre, wk, wv, wq, cosine, sine, dy, heads)
        dy_low = permute(dy[dy_head.shape[0]:], [(0, 2), (1, 3)])
        partner_o = permute(o, across)
        y, d_out, dz, stat, dgain_post = post(o, out, lse, x, dy, wo, gain_post)

        down, dq, dwq_part = backward(q, d_out, stat, own, near, far, mid, cosine, sine, act_t)
        dwq_mine = dwq_part + permute(dwq_part, across)
        dwq_other = permute(dwq_mine, beside)
        dwo = grad_wo(idx, o, dz, partner_o, dy_high, dy_head, dy_low, wo, gain_post)
        dwo_in = permute(dwo[1], beside)
        dwo_mine = dwo[0] + dwo_in
        dwo_other = permute(dwo_mine, beside)
        dx, *dwkv = tail(idx, down, cosine, sine, act_t, dq, wq, wk, wv, x, dy, gain_pre, dgain_post)
        theirs_in, mine_in = permute(dwkv[1], beside), permute(dwkv[0], beside)
        split = dim // 3 * 2
        pieces = []
        for rows in (slice(0, split), slice(split, None)):
            chip_mine = dwkv[0][rows] + theirs_in[rows]
            chip_other = dwkv[1][rows] + mine_in[rows]
            far_mine = permute(chip_mine, across)
            pieces.append((chip_mine, far_mine, chip_other, permute(far_mine, beside)))
        begun = join_pair(idx, pieces[0], dim)
        dwk_full, dwv_full, dpre_full, dpost_full = join_pair(idx, pieces[1], dim, tuple(begun))

        dwo_full = join_rows(idx, dwo_mine, dwo_other)
        dwq_full = join_wide(idx, dwq_mine, dwq_other, heads)
        return (
            y.reshape(batch, tokens, dim),
            dx.reshape(batch, tokens, dim),
            dwq_full,
            dwk_full.reshape(dim, 1, hd),
            dwv_full.reshape(dim, 1, hd),
            dwo_full.reshape(heads, hd, dim),
            dpre_full,
            dpost_full,
        )

    seq_spec = P("dp", "cp", None)
    in_specs = (seq_spec, P("dp", "cp"), seq_spec, P(), P(), P(), P(), P(), P())
    out_specs = (seq_spec, seq_spec, P("dp", None, None), P("dp", None, None), P("dp", None, None), P("dp", None, None), P("dp"), P("dp"))
    return jax.shard_map(local_step, mesh=mesh, in_specs=in_specs, out_specs=out_specs, check_vma=False)
```

```python
import functools
import math

import jax
import jax.numpy as jnp
from jax import lax
from jax.experimental import pallas as pl
from jax.experimental.pallas import tpu as pltpu
from jax.sharding import PartitionSpec as P


NORM_EPS = 1e-6
SOFT_CAP = 50.0
QUERY_SCALE = 144.0
ROPE_BASE = 10000.0
LOG2E = math.log2(math.e)
CAP2 = SOFT_CAP * LOG2E
INV_CAP = 1.0 / SOFT_CAP
SHIFT2 = 20.0


F32 = jnp.float32
BF16 = jnp.bfloat16
VMEM_LIMIT = 60 * 1024 * 1024

NT = (((1,), (1,)), ((), ()))
NN = (((1,), (0,)), ((), ()))


def dot(a, b, dims=NN):
    return lax.dot_general(a, b, dims, preferred_element_type=F32)


def params():
    return pltpu.CompilerParams(vmem_limit_bytes=VMEM_LIMIT)


def whole(shape):
    zeros = (0,) * len(shape)
    return pl.BlockSpec(shape, lambda *_: zeros)


def rows_spec(rows, width):
    return pl.BlockSpec((rows, width), lambda i: (i, 0))


def stack_spec(depth, rows, width):
    return pl.BlockSpec((depth, rows, width), lambda i: (0, i, 0))


COST = pl.CostEstimate(flops=10**10, bytes_accessed=10**7, transcendentals=0)


def to_sibling(rank, src, dst, send, recv):
    return pltpu.make_async_remote_copy(
        src_ref=src, dst_ref=dst, send_sem=send, recv_sem=recv,
        device_id={"cp": rank + 1 - 2 * (rank % 2)}, device_id_type=pl.DeviceIdType.MESH,
    )


def rope(values, cosine, sine):
    half = cosine.shape[-1]
    first, second = values[:, :half], values[:, half:]
    return jnp.concatenate([first * cosine - second * sine, second * cosine + first * sine], axis=-1)


def forward_tile(q_ref, acc_ref, sum_ref, k, v, masked):
    heads, bq, _ = q_ref.shape
    bk = k.shape[0]
    if masked:
        keep = lax.broadcasted_iota(jnp.int32, (bq, bk), 1) <= lax.broadcasted_iota(jnp.int32, (bq, bk), 0)
    for h in range(heads):
        s = dot(q_ref[h], k, NT)
        p = jnp.exp2(jnp.tanh(s * INV_CAP) * CAP2 - SHIFT2)
        if masked:
            p = jnp.where(keep, p, 0.0)
        part = p[:, 0:128]
        for c in range(128, bk, 128):
            part = part + p[:, c:c + 128]
        sum_ref[h] += part
        acc_ref[h] += dot(p.astype(BF16), v)


def forward_kernel(x_ref, gain_ref, wk_ref, wv_ref, wq_hbm, cos_ref, sin_ref, dy_hbm,
                   at_ref, q_ref, own_ref, near_ref, far_ref, mid_ref, o_ref, out_ref, lse_ref, dy_far,
                   dy_send, dy_recv, wq_s, wq_sem, a_s, own_s, near_s, far_s, mid_s, acc_s, sum_s,
                   far_send, far_recv, near_send, near_recv, mid_send, mid_recv):
    heads, tokens, hd = q_ref.shape
    bt = x_ref.shape[0]
    tiles = tokens // bt
    big = 2 * bt
    rank = lax.axis_index("cp")
    core = rank % 2
    i = pl.program_id(0)
    across = {"cp": (rank + 2) % 4}
    mesh_id = pl.DeviceIdType.MESH

    def rows_of(t, size=bt):
        return pl.ds(pl.multiple_of(t * size, size), size)

    def far_copy(t):
        rows = rows_of(t)
        return pltpu.make_async_remote_copy(
            src_ref=own_s.at[:, rows, :], dst_ref=far_s.at[:, rows, :], send_sem=far_send.at[t], recv_sem=far_recv.at[t],
            device_id=across, device_id_type=mesh_id,
        )

    def near_copy(t):
        rows = rows_of(t)
        return to_sibling(rank, own_s.at[:, rows, :], near_s.at[:, rows, :], near_send.at[t], near_recv.at[t])

    def mid_copy(c):
        rows = rows_of(c, big)
        return to_sibling(rank, far_s.at[:, rows, :], mid_s.at[:, rows, :], mid_send.at[c], mid_recv.at[c])

    load_wq = pltpu.make_async_copy(wq_hbm, wq_s, wq_sem)
    dy_copy = pltpu.make_async_remote_copy(
        src_ref=dy_hbm.at[0:bt, :], dst_ref=dy_far, send_sem=dy_send, recv_sem=dy_recv,
        device_id=across, device_id_type=mesh_id,
    )

    @pl.when(i == 0)
    def _():
        load_wq.start()
        barrier = pltpu.get_barrier_semaphore()
        for other in (across, {"cp": rank + 1 - 2 * core}):
            pl.semaphore_signal(barrier, inc=1, device_id=other, device_id_type=mesh_id)
        pl.semaphore_wait(barrier, 2)

    @pl.when(i < tiles)
    def _():
        rows = rows_of(i)
        x = x_ref[...].astype(F32)
        rstd = lax.rsqrt(jnp.mean(x * x, axis=-1, keepdims=True) + NORM_EPS)
        a = (x * rstd * (1.0 + gain_ref[...][None, :])).astype(BF16)
        a_s[rows, :] = a
        own_s[0, rows, :] = rope(dot(a, wk_ref[...]).astype(BF16).astype(F32), cos_ref[rows, :], sin_ref[rows, :]).astype(BF16)
        own_s[1, rows, :] = dot(a, wv_ref[...]).astype(BF16)
        pl.when(rank < 2)(lambda: far_copy(i).start())
        pl.when(core == 0)(lambda: near_copy(i).start())

    def attend(t, kv_ref, start, size, masked):
        rows, keys = rows_of(t), pl.ds(pl.multiple_of(start, bt), size)
        forward_tile(q_ref.at[:, rows, :], acc_s.at[:, rows, :], sum_s.at[:, rows, :],
                     kv_ref[0, keys, :], kv_ref[1, keys, :], masked)

    @pl.when(jnp.logical_and(i >= tiles, i < 2 * tiles))
    def _():
        t = i - tiles
        rows = rows_of(t)
        a = a_s[rows, :]
        at_ref[...] = a.T
        own_ref[...] = own_s[:, rows, :]
        pl.when(jnp.logical_and(t == 0, rank < 2))(lambda: dy_copy.start())
        pl.when(t == 0)(lambda: load_wq.wait())
        scale = QUERY_SCALE ** -0.5
        for h in range(heads):
            q = dot(a, wq_s[:, h * hd:(h + 1) * hd]).astype(BF16).astype(F32)
            q_ref[h, rows, :] = (rope(q, cos_ref[rows, :], sin_ref[rows, :]) * scale).astype(BF16)
        acc_s[:, rows, :] = jnp.zeros((heads, bt, hd), F32)
        sum_s[:, rows, :] = jnp.zeros((heads, bt, 128), F32)
        attend(t, own_s, t * bt, bt, True)

        def own_step(j, _):
            attend(t, own_s, j * bt, bt, False)
            return 0

        lax.fori_loop(0, t, own_step, 0)

        @pl.when(core == 1)
        def _():
            pl.when(t == 0)(lambda: [near_copy(n).wait_recv() for n in range(tiles)] and None)

            def near_step(j, _):
                attend(t, near_s, j * big, big, False)
                return 0

            lax.fori_loop(0, tokens // big, near_step, 0)

    chunks = tokens // big
    c = i - 2 * tiles

    def far_chunk(kv_ref, start):
        def step(t, _):
            attend(t, kv_ref, start, big, False)
            return 0

        lax.fori_loop(0, tiles, step, 0)

    @pl.when(jnp.logical_and(rank >= 2, jnp.logical_and(c >= 0, c < chunks)))
    def _():
        far_copy(2 * c).wait_recv()
        far_copy(2 * c + 1).wait_recv()
        mid_copy(c).start()
        far_chunk(far_s, c * big)

    @pl.when(jnp.logical_and(rank >= 2, jnp.logical_and(c >= chunks, c < 2 * chunks)))
    def _():
        mid_copy(c - chunks).wait_recv()
        far_chunk(mid_s, (c - chunks) * big)

    last = i - 2 * tiles - 2 * chunks

    @pl.when(last >= 0)
    def _():
        rows = rows_of(last)
        lane = lax.broadcasted_iota(jnp.int32, (bt, 128), 1)
        lse = jnp.zeros((bt, 128), F32)
        for h in range(heads):
            total = jnp.sum(sum_s[h, rows, :], axis=-1, keepdims=True)
            lse = jnp.where(lane == h, jnp.log2(total) + SHIFT2, lse)
            out = acc_s[h, rows, :] / total
            out_ref[h] = out
            o_ref[:, h * hd:(h + 1) * hd] = out.astype(BF16)
        lse_ref[...] = lse
        for dst, src in ((near_ref, near_s), (far_ref, far_s), (mid_ref, mid_s)):
            dst[...] = src[:, rows, :]

    @pl.when(last == tiles - 1)
    def _():
        pl.when(rank < 2)(lambda: [far_copy(n).wait_send() for n in range(tiles)] and dy_copy.wait_send())
        pl.when(rank >= 2)(lambda: dy_copy.wait_recv())
        pl.when(core == 0)(lambda: [near_copy(n).wait_send() for n in range(tiles)] and None)
        pl.when(rank >= 2)(lambda: [mid_copy(n).wait_send() for n in range(chunks)] and None)


def forward(x, gain, wk, wv, wq, cosine, sine, dy, heads):
    tokens, dim = x.shape
    hd = wk.shape[1]
    bt = 256
    tiles = tokens // bt
    chunks = tiles // 2
    done = 2 * tiles + 2 * chunks
    dma = pltpu.SemaphoreType.DMA
    early = lambda i: jnp.minimum(i, tiles - 1)
    second = lambda i: jnp.clip(i - tiles, 0, tiles - 1)
    late = lambda i: jnp.maximum(i - done, 0)
    kv_shape = jax.ShapeDtypeStruct((2, tokens, hd), BF16)
    kv_out = pl.BlockSpec((2, bt, hd), lambda i: (0, late(i), 0))
    return pl.pallas_call(
        forward_kernel,
        grid=(done + tiles,),
        in_specs=[
            pl.BlockSpec((bt, dim), lambda i: (early(i), 0)),
            whole(gain.shape),
            whole(wk.shape),
            whole(wv.shape),
            pl.BlockSpec(memory_space=pl.ANY),
            whole(cosine.shape),
            whole(sine.shape),
            pl.BlockSpec(memory_space=pl.ANY),
        ],
        out_specs=[
            pl.BlockSpec((dim, bt), lambda i: (0, second(i))),
            whole((heads, tokens, hd)),
            pl.BlockSpec((2, bt, hd), lambda i: (0, second(i), 0)),
            kv_out,
            kv_out,
            kv_out,
            pl.BlockSpec((bt, heads * hd), lambda i: (late(i), 0)),
            pl.BlockSpec((heads, bt, hd), lambda i: (0, late(i), 0)),
            pl.BlockSpec((bt, 128), lambda i: (late(i), 0)),
            pl.BlockSpec(memory_space=pl.ANY),
        ],
        out_shape=[
            jax.ShapeDtypeStruct((dim, tokens), BF16),
            jax.ShapeDtypeStruct((heads, tokens, hd), BF16),
            kv_shape,
            kv_shape,
            kv_shape,
            kv_shape,
            jax.ShapeDtypeStruct((tokens, heads * hd), BF16),
            jax.ShapeDtypeStruct((heads, tokens, hd), F32),
            jax.ShapeDtypeStruct((tokens, 128), F32),
            jax.ShapeDtypeStruct((bt, dim), BF16),
        ],
        scratch_shapes=[dma, dma, pltpu.VMEM(wq.shape, BF16), dma, pltpu.VMEM((tokens, dim), BF16)] + [pltpu.VMEM((2, tokens, hd), BF16)] * 4 + [
            pltpu.VMEM((heads, tokens, hd), F32),
            pltpu.VMEM((heads, tokens, 128), F32),
            dma((tiles,)),
            dma((tiles,)),
            dma((tiles,)),
            dma((tiles,)),
            dma((chunks,)),
            dma((chunks,)),
        ],
        compiler_params=pltpu.CompilerParams(vmem_limit_bytes=VMEM_LIMIT, collective_id=2, has_side_effects=True),
        cost_estimate=COST,
        name="forward",
    )(x, gain, wk, wv, wq, cosine, sine, dy)


def post_norm(o, wo, gain, dy):
    z = dot(o, wo).astype(BF16).astype(F32)
    rstd = lax.rsqrt(jnp.mean(z * z, axis=-1, keepdims=True) + NORM_EPS)
    unit = z * rstd
    g = dy * gain
    dz = (rstd * (g - unit * jnp.mean(g * unit, axis=-1, keepdims=True))).astype(BF16)
    return unit, dz


def post_kernel(o_ref, out_ref, lse_ref, x_ref, dy_ref, wo_ref, gain_ref, y_ref, do_ref, dz_ref, stat_ref, dgain_ref):
    heads, bq, hd = out_ref.shape
    gain = 1.0 + gain_ref[...][None, :]
    dy = dy_ref[...].astype(F32)
    unit, dz = post_norm(o_ref[...], wo_ref[...], gain, dy)
    y_ref[...] = (x_ref[...].astype(F32) + (unit * gain).astype(BF16).astype(F32)).astype(BF16)
    dz_ref[...] = dz

    @pl.when(pl.program_id(0) == 0)
    def _():
        dgain_ref[...] = jnp.zeros_like(dgain_ref)

    dgain_ref[...] += jnp.sum(dy * unit, axis=0, keepdims=True)
    lane = lax.broadcasted_iota(jnp.int32, (bq, 128), 1)
    stat = lse_ref[...]
    for h in range(heads):
        d_out = dot(dz, wo_ref[h * hd:(h + 1) * hd, :], NT).astype(BF16)
        do_ref[h] = d_out
        delta = jnp.sum(d_out.astype(F32) * out_ref[h], axis=-1, keepdims=True)
        stat = jnp.where(lane == heads + h, delta, stat)
    stat_ref[...] = stat.T[0:8, :]


def post(o, out, lse, x, dy, wo, gain):
    heads, tokens, hd = out.shape
    dim = x.shape[1]
    bq = 256
    rows3 = stack_spec(heads, bq, hd)
    rows2 = lambda width: rows_spec(bq, width)
    return pl.pallas_call(
        post_kernel,
        grid=(tokens // bq,),
        in_specs=[rows2(heads * hd), rows3, rows2(128), rows2(dim), rows2(dim), whole(wo.shape), whole((dim,))],
        out_specs=[rows2(dim), rows3, rows2(dim), pl.BlockSpec((8, bq), lambda i: (0, i)), whole((1, dim))],
        out_shape=[
            jax.ShapeDtypeStruct((tokens, dim), BF16),
            jax.ShapeDtypeStruct((heads, tokens, hd), BF16),
            jax.ShapeDtypeStruct((tokens, dim), BF16),
            jax.ShapeDtypeStruct((8, tokens), F32),
            jax.ShapeDtypeStruct((1, dim), F32),
        ],
        compiler_params=params(),
        cost_estimate=COST,
        name="post",
    )(o, out, lse, x, dy, wo, gain)


def grad_wo_kernel(idx_ref, o_ref, dz_ref, po_ref, pdy_low_ref, pdy_head_ref, pdy_high_ref, wo_ref, gain_ref, mine_ref, theirs_ref, pdz_ref):
    _, width = o_ref.shape
    bt = pdy_low_ref.shape[0]
    hd = 256
    i = pl.program_id(0)
    rows = pl.ds(pl.multiple_of(i * bt, bt), bt)
    high = jnp.where(i == 0, pdy_head_ref[...], pdy_high_ref[...])
    dy = jnp.where(idx_ref[0] >= 2, high, pdy_low_ref[...]).astype(F32)
    pdz_ref[rows, :] = post_norm(po_ref[rows, :], wo_ref[...], 1.0 + gain_ref[...][None, :], dy)[1]

    @pl.when(i == pl.num_programs(0) - 1)
    def _():
        core = idx_ref[0] % 2
        per = width // hd // 2
        for which, ref in enumerate((mine_ref, theirs_ref)):
            for hh in range(per):
                cols = pl.ds(pl.multiple_of((((core + which) % 2) * per + hh) * hd, hd), hd)
                ref[hh * hd:(hh + 1) * hd, :] = dot(o_ref[:, cols].T, dz_ref[...]) + dot(po_ref[:, cols].T, pdz_ref[...])


def grad_wo(idx, o, dz, po, pdy_low, pdy_head, pdy_high, wo, gain):
    tokens, width = o.shape
    dim = dz.shape[1]
    bt = 256
    rows2 = rows_spec(bt, dim)
    return pl.pallas_call(
        grad_wo_kernel,
        grid=(tokens // bt,),
        in_specs=[
            pl.BlockSpec(memory_space=pltpu.SMEM),
            whole(o.shape),
            whole(dz.shape),
            whole(o.shape),
            rows2,
            whole(pdy_head.shape),
            pl.BlockSpec((bt, dim), lambda i: (jnp.maximum(i - 1, 0), 0)),
            whole(wo.shape),
            whole((dim,)),
        ],
        out_specs=[whole((width // 2, dim))] * 2,
        out_shape=[jax.ShapeDtypeStruct((width // 2, dim), F32)] * 2,
        scratch_shapes=[pltpu.VMEM((tokens, dim), BF16)],
        compiler_params=params(),
        cost_estimate=COST,
        name="grad_wo",
    )(idx, o, dz, po, pdy_low, pdy_head, pdy_high, wo, gain)


def backward_tile(q_ref, do_ref, stat_ref, dqt_ref, dkv_ref, k, v, kt, start, bq, masked):
    heads = q_ref.shape[0]
    bk = k.shape[0]
    rows = pl.ds(pl.multiple_of(start, 128), bq)
    if masked:
        keep = lax.broadcasted_iota(jnp.int32, (bk, bq), 0) <= lax.broadcasted_iota(jnp.int32, (bk, bq), 1)
    for h in range(heads):
        q = q_ref[h, rows, :]
        d_out = do_ref[h, rows, :]
        t = jnp.tanh(dot(k, q, NT) * INV_CAP)
        p = jnp.exp2(t * CAP2 - stat_ref[h:h + 1, rows])
        if masked:
            p = jnp.where(keep, p, 0.0)
        dp = dot(v, d_out, NT)
        ds = (p * (dp - stat_ref[heads + h:heads + h + 1, rows]) * (1.0 - t * t)).astype(BF16)
        dkv_ref[1] += dot(p.astype(BF16), d_out)
        dkv_ref[0] += dot(ds, q)
        dqt_ref[h, :, rows] += dot(kt, ds)


def backward_kernel(q_ref, do_ref, stat_ref, own_ref, near_ref, far_ref, mid_ref, cos_ref, sin_ref, at_ref,
                    down_hbm, dq_hbm, dwq_hbm,
                    down_ref, dq_ref, dwq_ref, out_sem, dqt_s, near_out, near_in, mid_out, mid_in, far_out, far_in, dwq_out, dwq_in,
                    near_send, near_recv, mid_send, mid_recv, far_send, far_recv, dwq_send, dwq_recv):
    heads, tokens, hd = q_ref.shape
    half = hd // 2
    bk = own_ref.shape[1]
    big = 2 * bk
    tiles = tokens // bk
    rank = lax.axis_index("cp")
    core = rank % 2
    i = pl.program_id(0)
    across = {"cp": (rank + 2) % 4}
    mesh_id = pl.DeviceIdType.MESH

    def near_copy(n):
        return to_sibling(rank, near_out.at[n], near_in.at[n], near_send.at[n], near_recv.at[n])

    def mid_copy(n):
        return to_sibling(rank, mid_out.at[n], mid_in.at[n], mid_send.at[n], mid_recv.at[n])

    def far_copy(n):
        return pltpu.make_async_remote_copy(
            src_ref=far_out.at[n], dst_ref=far_in.at[n], send_sem=far_send.at[n], recv_sem=far_recv.at[n],
            device_id=across, device_id_type=mesh_id,
        )

    @pl.when(i == 0)
    def _():
        dqt_s[...] = jnp.zeros_like(dqt_s)
        barrier = pltpu.get_barrier_semaphore()
        for other in (across, {"cp": rank + 1 - 2 * core}):
            pl.semaphore_signal(barrier, inc=1, device_id=other, device_id_type=mesh_id)
        pl.semaphore_wait(barrier, 2)

    def all_rows(kv_ref, dkv_ref):
        k, v = kv_ref[0], kv_ref[1]
        kt = k.T

        def step(j, _):
            backward_tile(q_ref, do_ref, stat_ref, dqt_s, dkv_ref, k, v, kt, j * big, big, False)
            return 0

        lax.fori_loop(0, tokens // big, step, 0)

    @pl.when(jnp.logical_and(rank >= 2, i < tiles))
    def _():
        mine = mid_out.at[i]
        mine[...] = jnp.zeros_like(mine)
        all_rows(mid_ref, mine)
        mid_copy(i).start()

    @pl.when(jnp.logical_and(rank >= 2, jnp.logical_and(i >= tiles, i < 2 * tiles)))
    def _():
        n = i - tiles
        mid_copy(n).wait()
        mine = far_out.at[n]
        mine[...] = mid_in[n]
        all_rows(far_ref, mine)
        far_copy(n).start()

    n = i - 2 * tiles

    @pl.when(jnp.logical_and(core == 1, n >= 0))
    def _():
        mine = near_out.at[n]
        mine[...] = jnp.zeros_like(mine)
        all_rows(near_ref, mine)
        near_copy(n).start()

    @pl.when(n >= 0)
    def _():
        down = down_ref.at[:, pl.ds(pl.multiple_of(n * bk, bk), bk), :]
        down[...] = jnp.zeros_like(down)
        k, v = own_ref[0], own_ref[1]
        kt = k.T
        backward_tile(q_ref, do_ref, stat_ref, dqt_s, down, k, v, kt, n * bk, bk, True)

        def own_step(j, _):
            backward_tile(q_ref, do_ref, stat_ref, dqt_s, down, k, v, kt, j * bk, bk, False)
            return 0

        lax.fori_loop(n + 1, tiles, own_step, 0)

    @pl.when(n == tiles - 1)
    def _():
        scale = QUERY_SCALE ** -0.5
        for h in range(heads):
            dq = dqt_s[h].T
            first, second = dq[:, :half], dq[:, half:]
            cosine, sine = cos_ref[...], sin_ref[...]
            dq_ref[:, h * hd:h * hd + half] = ((first * cosine + second * sine) * scale).astype(BF16)
            dq_ref[:, h * hd + half:(h + 1) * hd] = ((second * cosine - first * sine) * scale).astype(BF16)
        written = [pltpu.make_async_copy(src, dst, out_sem.at[slot]) for slot, (src, dst) in
                   enumerate(((dq_ref, dq_hbm), (dwq_ref, dwq_hbm), (down_ref, down_hbm)))]
        written[0].start()
        dim, width = dwq_ref.shape
        bd = dim // 3

        def product(out_ref, which):
            dq = dq_ref[:, pl.ds(pl.multiple_of((core + which) % 2 * width, width), width)]

            def rows_step(r, _):
                rows = pl.ds(pl.multiple_of(r * bd, bd), bd)
                out_ref[rows, :] = dot(at_ref[rows, :], dq)
                return 0

            lax.fori_loop(0, dim // bd, rows_step, 0)

        product(dwq_out, 1)
        copy = to_sibling(rank, dwq_out, dwq_in, dwq_send, dwq_recv)
        copy.start()
        product(dwq_ref, 0)

        def gather(copy_of, arrived):
            for t in range(tiles):
                copy_of(t).wait_recv()
                down_ref[:, t * bk:(t + 1) * bk, :] += arrived[t]

        def left(copy_of):
            for t in range(tiles):
                copy_of(t).wait_send()

        pl.when(core == 1)(lambda: left(near_copy))
        pl.when(core == 0)(lambda: gather(near_copy, near_in))
        copy.wait()
        dwq_ref[...] += dwq_in[...]
        written[1].start()

        @pl.when(rank < 2)
        def _():
            gather(far_copy, far_in)
            written[2].start()

        @pl.when(rank >= 2)
        def _():
            written[2].start()
            left(far_copy)

        for copy_out in written:
            copy_out.wait()


def backward(q, d_out, stat, own, near, far, mid, cosine, sine, at):
    heads, tokens, hd = q.shape
    dim = at.shape[0]
    bk = 256
    tiles = tokens // bk
    width = heads * hd // 2

    def phase(first):
        return pl.BlockSpec((2, bk, hd), lambda i: (0, jnp.clip(i - first, 0, tiles - 1), 0))

    def held(array):
        zeros = (0,) * array.ndim
        return pl.BlockSpec(array.shape, lambda i: zeros, pipeline_mode=pl.Buffered(1))

    dma = pltpu.SemaphoreType.DMA
    return pl.pallas_call(
        backward_kernel,
        grid=(3 * tiles,),
        in_specs=[
            held(q),
            held(d_out),
            held(stat),
            phase(2 * tiles),
            phase(2 * tiles),
            phase(tiles),
            phase(0),
            held(cosine),
            held(sine),
            held(at),
        ],
        out_specs=[pl.BlockSpec(memory_space=pl.ANY)] * 3,
        out_shape=[
            jax.ShapeDtypeStruct((2, tokens, hd), F32),
            jax.ShapeDtypeStruct((tokens, heads * hd), BF16),
            jax.ShapeDtypeStruct((dim, width), F32),
        ],
        scratch_shapes=[
            pltpu.VMEM((2, tokens, hd), F32),
            pltpu.VMEM((tokens, heads * hd), BF16),
            pltpu.VMEM((dim, width), F32),
            dma((3,)),
            pltpu.VMEM((heads, hd, tokens), F32),
        ] + [pltpu.VMEM((tiles, 2, bk, hd), F32)] * 6
        + [pltpu.VMEM((dim, width), F32)] * 2 + [dma((tiles,))] * 6 + [dma] * 2,
        compiler_params=pltpu.CompilerParams(vmem_limit_bytes=VMEM_LIMIT, collective_id=0, has_side_effects=True),
        cost_estimate=COST,
        name="backward",
    )(q, d_out, stat, own, near, far, mid, cosine, sine, at)


def tail_kernel(idx_ref, down_ref, cos_ref, sin_ref, at_ref, dq_ref, wq_ref, wk_ref, wv_ref,
                x_ref, dy_ref, gain_ref, dpost_ref, dx_ref, mine_ref, theirs_ref, dgain_ref):
    _, half = cos_ref.shape
    dim = x_ref.shape[1]
    i = pl.program_id(0)
    dk = down_ref[0]
    cosine, sine = cos_ref[...], sin_ref[...]
    first, second = dk[:, :half], dk[:, half:]
    dk = jnp.concatenate([first * cosine + second * sine, second * cosine - first * sine], axis=1).astype(BF16)
    dv = down_ref[1].astype(BF16)

    @pl.when(i == 0)
    def _():
        mine_ref[...] = jnp.zeros_like(mine_ref)
        theirs_ref[...] = jnp.zeros_like(theirs_ref)
        dgain_ref[...] = jnp.zeros_like(dgain_ref)

    core = idx_ref[0] % 2
    at = at_ref[...]
    is_core0 = core == 0
    mine = jnp.where(is_core0, dk, dv)
    theirs = jnp.where(is_core0, dv, dk)
    mine_ref[0:dim, :] += dot(at, mine)
    theirs_ref[0:dim, :] += dot(at, theirs)
    da = dot(dq_ref[...], wq_ref[...], NT) + dot(dk, wk_ref[...], NT) + dot(dv, wv_ref[...], NT)
    x = x_ref[...].astype(F32)
    rstd = lax.rsqrt(jnp.mean(x * x, axis=-1, keepdims=True) + NORM_EPS)
    unit = x * rstd
    dgain_ref[...] += jnp.sum(da * unit, axis=0, keepdims=True)
    g = da * (1.0 + gain_ref[...][None, :])
    dx = rstd * (g - unit * jnp.mean(g * unit, axis=-1, keepdims=True))
    dx_ref[...] = (dy_ref[...].astype(F32) + dx).astype(BF16)

    @pl.when(i == pl.num_programs(0) - 1)
    def _():
        dpre, dpost = dgain_ref[...], dpost_ref[...]
        for ref, row in ((mine_ref, jnp.where(is_core0, dpre, dpost)), (theirs_ref, jnp.where(is_core0, dpost, dpre))):
            for c in range(dim // 128):
                ref[dim + c // 2:dim + c // 2 + 1, c % 2 * 128:(c % 2 + 1) * 128] = row[:, c * 128:(c + 1) * 128]


def tail(idx, down, cosine, sine, at, dq, wq, wk, wv, x, dy, gain, dpost):
    tokens, dim = x.shape
    hd = wk.shape[1]
    width = wq.shape[1]
    bt = 256
    kv_spec = stack_spec(2, bt, hd)
    rope_spec = rows_spec(bt, hd // 2)
    rows2 = rows_spec(bt, dim)
    return pl.pallas_call(
        tail_kernel,
        grid=(tokens // bt,),
        in_specs=[
            pl.BlockSpec(memory_space=pltpu.SMEM),
            kv_spec,
            rope_spec,
            rope_spec,
            pl.BlockSpec((dim, bt), lambda i: (0, i)),
            rows_spec(bt, width),
            whole(wq.shape),
            whole(wk.shape),
            whole(wv.shape),
            rows2,
            rows2,
            whole((dim,)),
            whole((1, dim)),
        ],
        out_specs=[rows2, whole((dim + 8, hd)), whole((dim + 8, hd))],
        out_shape=[
            jax.ShapeDtypeStruct((tokens, dim), BF16),
            jax.ShapeDtypeStruct((dim + 8, hd), F32),
            jax.ShapeDtypeStruct((dim + 8, hd), F32),
        ],
        scratch_shapes=[pltpu.VMEM((1, dim), F32)],
        compiler_params=params(),
        cost_estimate=COST,
        name="tail",
    )(idx, down, cosine, sine, at, dq, wq, wk, wv, x, dy, gain, dpost)


def join_wide_kernel(idx_ref, mine_ref, other_ref, out_ref):
    first = idx_ref[0] % 2 == 0
    rows, _ = mine_ref.shape
    mine, other = mine_ref[...], other_ref[...]
    low, high = jnp.where(first, mine, other), jnp.where(first, other, mine)
    heads = 4
    for h in range(heads):
        src = low if h < heads // 2 else high
        base = (h % (heads // 2)) * 256
        for c in range(2):
            out_ref[pl.ds(c * heads + h, rows, stride=2 * heads), :] = src[:, base + c * 128:base + (c + 1) * 128]


def join_wide(idx, mine, other, heads):
    dim, width = mine.shape
    bd = dim // 3
    spec = rows_spec(bd, width)
    out = pl.pallas_call(
        join_wide_kernel,
        grid=(dim // bd,),
        in_specs=[pl.BlockSpec(memory_space=pltpu.SMEM), spec, spec],
        out_specs=rows_spec(bd * 8, 128),
        out_shape=jax.ShapeDtypeStruct((dim * 8, 128), F32),
        compiler_params=params(),
        cost_estimate=COST,
        name="join_wide",
    )(idx, mine, other)
    return out.reshape(dim, 2, heads, 128).transpose(0, 2, 1, 3).reshape(dim, heads, 256)


def join_pair_kernel(idx_ref, a_ref, b_ref, c_ref, d_ref, *refs, last):
    core0 = idx_ref[0] % 2 == 0

    def ordered(mine, other):
        return jnp.where(core0, mine, other), jnp.where(core0, other, mine)

    rows = a_ref.shape[0] - (8 if last else 0)
    outs = refs[2:] if last else refs
    for n, src in enumerate(ordered(a_ref[...] + b_ref[...], c_ref[...] + d_ref[...])):
        for c in range(2):
            outs[n][pl.ds(c, rows, stride=2), :] = src[0:rows, c * 128:(c + 1) * 128]
        if last:
            gain_ref = outs[n + 2]
            for c in range(gain_ref.shape[0] // 128):
                gain_ref[c * 128:(c + 1) * 128] = src[rows + c // 2, c % 2 * 128:(c % 2 + 1) * 128]


def join_pair(idx, parts, dim, begun=()):
    rows, width = parts[0].shape
    last = bool(begun)
    bd = rows - 8 if last else dim // 3
    steps = rows // bd
    first = dim // bd - 1 if last else 0
    out_spec = pl.BlockSpec((bd * 2, 128), lambda i: (i + first, 0))
    part_spec = pl.BlockSpec(memory_space=pltpu.VMEM) if last else rows_spec(bd, width)
    pair = [jax.ShapeDtypeStruct((dim * 2, 128), F32)] * 2
    held = [pltpu.with_memory_space_constraint(p, pltpu.VMEM) if last and n % 2 else p for n, p in enumerate(parts)]
    return pl.pallas_call(
        functools.partial(join_pair_kernel, last=last),
        grid=(steps,),
        in_specs=[pl.BlockSpec(memory_space=pltpu.SMEM)] + [part_spec] * 4 + [pl.BlockSpec(memory_space=pl.ANY)] * len(begun),
        out_specs=[out_spec] * 2 + [whole((dim,))] * len(begun),
        out_shape=pair + [jax.ShapeDtypeStruct((dim,), F32)] * len(begun),
        input_output_aliases={5: 0, 6: 1} if last else {},
        compiler_params=params(),
        cost_estimate=COST,
        name="join_last" if last else "join_first",
    )(idx, *held, *begun)


def join_rows_kernel(idx_ref, mine_ref, other_ref, out_ref):
    first = idx_ref[0] % 2 == 0
    out_ref[...] = jnp.where(first == (pl.program_id(0) == 0), mine_ref[...], other_ref[...])


def join_rows(idx, mine, other):
    rows, dim = mine.shape
    br = 256
    steps = rows // br
    spec = pl.BlockSpec((br, dim), lambda w, i: (i, 0))
    return pl.pallas_call(
        join_rows_kernel,
        grid=(2, steps),
        in_specs=[pl.BlockSpec(memory_space=pltpu.SMEM), spec, spec],
        out_specs=pl.BlockSpec((br, dim), lambda w, i: (w * steps + i, 0)),
        out_shape=jax.ShapeDtypeStruct((rows * 2, dim), F32),
        compiler_params=params(),
        cost_estimate=COST,
        name="join_rows",
    )(idx, mine, other)


def solution(mesh):
    across = [(0, 2), (2, 0), (1, 3), (3, 1)]
    beside = [(0, 1), (1, 0), (2, 3), (3, 2)]

    def permute(value, pairs):
        return lax.ppermute(value, "cp", pairs)

    def local_step(x_in, positions, dy_out, w_query, w_key, w_value, w_out, w_pre, w_post):
        batch, tokens, dim = x_in.shape
        heads, hd = w_query.shape[1], w_query.shape[2]
        half = hd // 2
        idx = lax.axis_index("cp").astype(jnp.int32).reshape(1)
        wq = w_query.reshape(dim, heads * hd)
        wk = w_key.reshape(dim, hd)
        wv = w_value.reshape(dim, hd)
        wo = w_out.reshape(heads * hd, dim)
        x = x_in.reshape(tokens, dim)
        dy = dy_out.reshape(tokens, dim)
        gain_pre = w_pre
        gain_post = w_post
        inv_freq = ROPE_BASE ** (jnp.arange(half, dtype=F32) * (-2.0 / hd))
        angles = positions.reshape(tokens, 1).astype(F32) * inv_freq
        cosine, sine = jnp.cos(angles), jnp.sin(angles)

        dy_high = permute(dy, [(2, 0), (3, 1)])
        act_t, q, own, near, far, mid, o, out, lse, dy_head = forward(x, gain_pre, wk, wv, wq, cosine, sine, dy, heads)
        dy_low = permute(dy[dy_head.shape[0]:], [(0, 2), (1, 3)])
        partner_o = permute(o, across)
        y, d_out, dz, stat, dgain_post = post(o, out, lse, x, dy, wo, gain_post)

        down, dq, dwq_part = backward(q, d_out, stat, own, near, far, mid, cosine, sine, act_t)
        dwq_mine = dwq_part + permute(dwq_part, across)
        dwq_other = permute(dwq_mine, beside)
        dwo = grad_wo(idx, o, dz, partner_o, dy_high, dy_head, dy_low, wo, gain_post)
        dwo_in = permute(dwo[1], beside)
        dwo_mine = dwo[0] + dwo_in
        dwo_other = permute(dwo_mine, beside)
        dx, *dwkv = tail(idx, down, cosine, sine, act_t, dq, wq, wk, wv, x, dy, gain_pre, dgain_post)
        theirs_in, mine_in = permute(dwkv[1], beside), permute(dwkv[0], beside)
        split = dim // 3 * 2
        pieces = []
        for rows in (slice(0, split), slice(split, None)):
            chip_mine = dwkv[0][rows] + theirs_in[rows]
            chip_other = dwkv[1][rows] + mine_in[rows]
            far_mine = permute(chip_mine, across)
            pieces.append((chip_mine, far_mine, chip_other, permute(far_mine, beside)))
        begun = join_pair(idx, pieces[0], dim)
        dwk_full, dwv_full, dpre_full, dpost_full = join_pair(idx, pieces[1], dim, tuple(begun))

        dwo_full = join_rows(idx, dwo_mine, dwo_other)
        dwq_full = join_wide(idx, dwq_mine, dwq_other, heads)
        return (
            y.reshape(batch, tokens, dim),
            dx.reshape(batch, tokens, dim),
            dwq_full,
            dwk_full.reshape(dim, 1, hd),
            dwv_full.reshape(dim, 1, hd),
            dwo_full.reshape(heads, hd, dim),
            dpre_full,
            dpost_full,
        )

    seq_spec = P("dp", "cp", None)
    in_specs = (seq_spec, P("dp", "cp"), seq_spec, P(), P(), P(), P(), P(), P())
    out_specs = (seq_spec, seq_spec, P("dp", None, None), P("dp", None, None), P("dp", None, None), P("dp", None, None), P("dp"), P("dp"))
    return jax.shard_map(local_step, mesh=mesh, in_specs=in_specs, out_specs=out_specs, check_vma=False)
```
